32 devices in a mesh: dp: 16 (over z, y, core), tensor: 2 (over x).
Axes of the slice: x: 2, y: 2, z: 4, core: 2. Of those that a mesh axis runs over, the one named last changes fastest.
Arguments:
- tokens: bfloat16 [3, 8192, 512], P(None, ('dp', 'tensor')), may hold values from -6 to 6
- w_qkv: bfloat16 [512, 8, 192], P('dp', 'tensor'), may hold values from -0.25 to 0.25
- w_proj: bfloat16 [8, 64, 512], P('tensor', 'dp'), may hold values from -1 to 1
- w_in: bfloat16 [16, 512, 2048], P('dp', None, 'tensor'), may hold values from -0.25 to 0.25
- w_out: bfloat16 [16, 2048, 512], P('dp', 'tensor'), may hold values from -4 to 4
- w_router: bfloat16 [512, 16], P(('dp', 'tensor')), may hold values from -0.25 to 0.25
- gain_attn: bfloat16 [512], P(('dp', 'tensor')), may hold values from 0.5 to 1.5
- shift_attn: bfloat16 [512], P(('dp', 'tensor')), may hold values from -0.59765625 to 0.59765625
- gain_moe: bfloat16 [512], P(('dp', 'tensor')), may hold values from 0.5 to 1.5
- shift_moe: bfloat16 [512], P(('dp', 'tensor')), may hold values from -0.59765625 to 0.59765625
- live_rows: int32 [3, 8192], P(None, 'dp'), may hold values from 0 to 1, as said below
- chosen: int32 [3, 8192, 2], P(None, 'dp'), may hold values from 0 to 15, all different within a row
- priority: int32 [3, 16, 512], P(None, 'dp'), may hold values from 0 to 511, each once within a row
- cotangent: bfloat16 [3, 8192, 512], P(None, ('dp', 'tensor')), may hold values from -6 to 6
Outputs:
- output: bfloat16 [3, 8192, 512], P(None, ('dp', 'tensor'))
- grad_tokens: float32 [3, 8192, 512], P(None, ('dp', 'tensor'))
- grad_qkv: float32 [512, 8, 192], P('dp', 'tensor')
- grad_proj: float32 [8, 64, 512], P('tensor', 'dp')
- grad_in: float32 [16, 512, 2048], P('dp', None, 'tensor')
- grad_out: float32 [16, 2048, 512], P('dp', 'tensor')
- grad_router: float32 [512, 16], P(('dp', 'tensor'))
- grad_gain_attn: float32 [512], P(('dp', 'tensor'))
- grad_shift_attn: float32 [512], P(('dp', 'tensor'))
- grad_gain_moe: float32 [512], P(('dp', 'tensor'))
- grad_shift_moe: float32 [512], P(('dp', 'tensor'))
The draws below stay inside these ranges and needn't reach their ends.
Inputs may be any that keep to these rules, and one draw needn't show every extreme that they name: live_rows is constant on each image of 197 rows of a dp group (image i is rows i * 197 to i * 197 + 196 of the group) and 0 on the group's rows from 394 on.
All inputs are finite; a program needn't handle non-finite values.
Results may differ from the reference program's by a relative error of at most 0.025.
Values may be sent and summed in bfloat16 or wider, within the bound.
A program may use at most 256 MiB of HBM per device.

```python
import jax
import jax.numpy as jnp
from jax import lax

D = 512
HEADS = 8
HEAD_DIM = 64
FF = 2048
SEQ = 197
MB = 3
EXPERTS = 16
ROWS = 512
IMAGES = 2
CAP = 64
TOKENS = 8192
N_DP = 16


def draw_live_rows(key, part):
    present = (jax.random.randint(key, (MB, N_DP, IMAGES), 0, 5) > 0).astype(jnp.int32)
    positions = jnp.arange(ROWS, dtype=jnp.int32)
    image_of = jnp.minimum(positions // SEQ, IMAGES - 1)
    inside = (positions < IMAGES * SEQ).astype(jnp.int32)
    rows_live = present[:, :, image_of] * inside[None, None, :]
    return rows_live.reshape(MB, N_DP * ROWS)


def block_scale(stream_key, dims, cuts, low, high):
    level = 1.0
    for dim, blocks in cuts:
        draws = jax.random.uniform(jax.random.fold_in(jax.random.fold_in(stream_key, 6), dim), (blocks,), jnp.float32, low / len(cuts), high / len(cuts))
        level = level * jnp.repeat(jnp.exp(draws), dims[dim] // blocks).reshape((-1,) + (1,) * (len(dims) - 1 - dim))
    return level


def choose_distinct(own_key, rows, count, top, lift):
    order = jax.random.permutation(jax.random.fold_in(own_key, 1), count)
    boost = order
    for power in range(3):
        boost = boost * boost // count
    boost = boost * lift // count
    tickets = jax.random.randint(jax.random.fold_in(own_key, 2), (rows, count), 0, 4096) + boost
    sure = jax.random.permutation(jax.random.fold_in(own_key, 3), rows)[jnp.arange(count) % rows]
    tickets = jnp.where(jnp.arange(rows)[:, None] == sure[None, :], 1 << 14, tickets)
    score = tickets * count + jnp.arange(count)
    return lax.top_k(score.astype(jnp.int32), top)[1].astype(jnp.int32)


def centred(key, dims, scale, bound, split=(), kind=jnp.bfloat16):
    drawn = jax.random.normal(key, dims, jnp.float32) * scale
    if len(split) > 0:
        drawn = block_scale(key, dims, split, -0.22, 0.18) * drawn
    return jnp.clip(drawn, min=-bound, max=bound).astype(kind)


def setup_inputs(seed: int = 0) -> dict:
    arg_keys = jax.random.split(jax.random.key(seed), 15)
    tokens = centred(arg_keys[0], (MB, TOKENS, D), 1.0, 6.0, ((1, 32),))
    w_qkv = centred(arg_keys[1], (D, HEADS, 3 * HEAD_DIM), D ** -0.5, 0.25, ((0, 16), (1, 2)))
    w_proj = centred(arg_keys[2], (HEADS, HEAD_DIM, D), (D // 16) ** -0.5, 1.0, ((0, 2), (1, 16)))
    w_in = centred(arg_keys[3], (EXPERTS, D, FF), D ** -0.5, 0.25, ((0, 16), (2, 2)))
    w_out = centred(arg_keys[4], (EXPERTS, FF, D), (max(1, FF // 1024)) ** -0.5, 4.0, ((0, 16), (1, 2)))
    w_router = centred(arg_keys[5], (D, EXPERTS), D ** -0.5, 0.25, ((0, 32),))
    gain_attn = jnp.clip(1.0 + 0.1 * jax.random.normal(arg_keys[6], (D,), jnp.float32), 0.5, 1.5).astype(jnp.bfloat16)
    shift_attn = centred(arg_keys[7], (D,), 0.1, 0.59765625, ((0, 32),))
    gain_moe = jnp.clip(1.0 + 0.1 * jax.random.normal(arg_keys[8], (D,), jnp.float32), 0.5, 1.5).astype(jnp.bfloat16)
    shift_moe = centred(arg_keys[9], (D,), 0.1, 0.59765625, ((0, 32),))
    live_rows = draw_live_rows(jax.random.fold_in(arg_keys[14], 71), 0)
    chosen = choose_distinct(arg_keys[11], MB * TOKENS, EXPERTS, 2, 1024).reshape((MB, TOKENS, 2))
    priority = jax.vmap(lambda own: jax.random.permutation(own, ROWS))(jax.random.split(arg_keys[12], MB * N_DP)).reshape((MB, N_DP, ROWS)).astype(jnp.int32)
    cotangent = centred(arg_keys[13], (MB, TOKENS, D), 1.0, 6.0, ((1, 32),))
    return dict(tokens=tokens, w_qkv=w_qkv, w_proj=w_proj, w_in=w_in, w_out=w_out, w_router=w_router, gain_attn=gain_attn, shift_attn=shift_attn, gain_moe=gain_moe, shift_moe=shift_moe, live_rows=live_rows, chosen=chosen, priority=priority, cotangent=cotangent)


@jax.custom_vjp
def low(v):
    return lax.optimization_barrier(v.astype(jnp.bfloat16)).astype(jnp.float32)

@jax.custom_vjp
def low_back(v):
    return v

def low_keep(v):
    return (low(v), None)

def low_pass(kept, grad):
    return (grad,)

def back_keep(v):
    return (v, None)

def back_low(kept, grad):
    return (low(grad),)
low.defvjp(low_keep, low_pass)
low_back.defvjp(back_keep, back_low)
norm_eps = 1e-06

def layer_norm(values, gain_vec, shift_vec):
    centre = lax.optimization_barrier(jnp.mean(values, axis=-1, keepdims=True))
    centered = values - centre
    spread = lax.optimization_barrier(jnp.mean(centered * centered, axis=-1, keepdims=True))
    return centered * lax.rsqrt(spread + norm_eps) * gain_vec + shift_vec

def route_slots(picks, ranking, living, expert_count, capacity):
    row_count = picks.shape[0]
    row_ids = jnp.arange(row_count, dtype=jnp.int32)
    ordering = jnp.zeros((row_count,), jnp.int32).at[ranking].set(row_ids)
    sorted_picks = picks[ordering]
    sorted_live = living[ordering].astype(jnp.int32)
    labels = jnp.arange(expert_count, dtype=jnp.int32)
    first_hit = (sorted_picks[:, 0:1] == labels[None, :]).astype(jnp.int32) * sorted_live[:, None]
    second_hit = (sorted_picks[:, 1:2] == labels[None, :]).astype(jnp.int32) * sorted_live[:, None]
    first_before = jnp.cumsum(first_hit, axis=0, dtype=jnp.int32) - first_hit
    first_total = lax.optimization_barrier(jnp.sum(first_hit, axis=0, dtype=jnp.int32))
    second_before = jnp.cumsum(second_hit, axis=0, dtype=jnp.int32) - second_hit + first_total[None, :]
    place_first = lax.optimization_barrier(jnp.sum(first_before * first_hit, axis=1, dtype=jnp.int32))
    place_second = lax.optimization_barrier(jnp.sum(second_before * second_hit, axis=1, dtype=jnp.int32))
    placed = jnp.stack([place_first, place_second], axis=1)
    sorted_keep = (placed < capacity) & (sorted_live[:, None] > 0)
    sorted_slot = jnp.where(sorted_keep, placed, capacity).astype(jnp.int32)
    slots = sorted_slot[ranking]
    keep_flag = slots < capacity
    flat_index = jnp.where(keep_flag, picks * capacity + slots, expert_count * capacity).astype(jnp.int32)
    owners = jnp.broadcast_to(row_ids[:, None], (row_count, 2)).reshape(-1)
    table = jnp.full((expert_count * capacity + 1,), row_count, jnp.int32).at[flat_index.reshape(-1)].set(owners)
    return (keep_flag, flat_index, table[:expert_count * capacity])

def block(inputs, weights, living, picks, keep_flag, flat_index, table):
    w_qkv, w_proj, w_in, w_out, w_router, gain_one, shift_one, gain_two, shift_two = weights
    row_count, feature_dim = inputs.shape
    heads = w_qkv.shape[1]
    head_width = w_qkv.shape[2] // 3
    image_count = row_count // SEQ
    span_rows = image_count * SEQ
    highest = lax.Precision.HIGHEST
    factor = head_width ** (-0.5)
    sent_one = low(layer_norm(inputs, gain_one, shift_one))
    mixed = jnp.einsum('rd,dhc->rhc', sent_one[:span_rows], w_qkv, precision=highest)
    query = low(low_back(mixed[:, :, :head_width] * factor)).reshape(image_count, SEQ, heads, head_width)
    keys_img = low(low_back(mixed[:, :, head_width:2 * head_width])).reshape(image_count, SEQ, heads, head_width)
    values_img = low(low_back(mixed[:, :, 2 * head_width:])).reshape(image_count, SEQ, heads, head_width)
    scores = low_back(jnp.einsum('iqhc,ikhc->ihqk', query, keys_img, precision=highest))
    attn_weights = low(jax.nn.softmax(scores, axis=-1))
    context = jnp.einsum('ihqk,ikhc->iqhc', attn_weights, values_img, precision=highest)
    context = low(low_back(context.reshape(span_rows, heads * head_width)))
    attn = low_back(jnp.dot(context, w_proj.reshape(heads * head_width, feature_dim), precision=highest))
    attn = jnp.concatenate([attn, jnp.zeros((row_count - span_rows, feature_dim), jnp.float32)], axis=0)
    hidden = inputs + living[:, None] * attn
    sent_two = low(layer_norm(hidden, gain_two, shift_two))
    logits = jnp.dot(sent_two, w_router, precision=highest)
    gate_probs = jax.nn.softmax(logits, axis=-1)
    labels = jnp.arange(w_router.shape[1], dtype=jnp.int32)
    hits = (picks[:, :, None] == labels[None, None, :]).astype(jnp.float32)
    gates = lax.optimization_barrier(jnp.sum(hits * gate_probs[:, None, :], axis=-1)) * keep_flag.astype(jnp.float32)
    padded_two = jnp.concatenate([sent_two, jnp.zeros((1, feature_dim), jnp.float32)], axis=0)
    expert_in = padded_two[table].reshape(w_in.shape[0], -1, feature_dim)
    pre = low_back(jnp.einsum('ecd,edf->ecf', expert_in, w_in, precision=highest))
    active = low(jax.nn.gelu(pre, approximate=True))
    produced = low_back(jnp.einsum('ecf,efd->ecd', active, w_out, precision=highest)).reshape(-1, feature_dim)
    padded_out = jnp.concatenate([produced, jnp.zeros((1, feature_dim), jnp.float32)], axis=0)
    mixture = gates[:, 0:1] * padded_out[flat_index[:, 0]] + gates[:, 1:2] * padded_out[flat_index[:, 1]]
    return hidden + low_back(mixture)

def reference(tokens, w_qkv, w_proj, w_in, w_out, w_router, gain_attn, shift_attn, gain_moe, shift_moe, live_rows, chosen, priority, cotangent):
    groups = MB * N_DP
    token_groups = tokens.reshape(groups, ROWS, D)
    live_groups = live_rows.reshape(groups, ROWS)
    pick_groups = chosen.reshape(groups, ROWS, 2)
    rank_groups = priority.reshape(groups, ROWS)
    cot_groups = cotangent.reshape(groups, ROWS, D)
    params = tuple((array_in.astype(jnp.float32) for array_in in (w_qkv, w_proj, w_in, w_out, w_router, gain_attn, shift_attn, gain_moe, shift_moe)))

    def one_group(carry, item):
        x_group, live_group, pick_group, rank_group, cot_group = item
        keep_flag, flat_index, table = route_slots(pick_group, rank_group, live_group, EXPERTS, CAP)

        def forward(x_in, weights):
            return block(x_in, weights, live_group.astype(jnp.float32), pick_group, keep_flag, flat_index, table)
        result, back = jax.vjp(forward, x_group.astype(jnp.float32), params)
        grad_x, grad_weights = back(cot_group.astype(jnp.float32))
        return (jax.tree.map(jnp.add, carry, grad_weights), (result.astype(jnp.bfloat16), grad_x))
    start = jax.tree.map(jnp.zeros_like, params)
    sums, outs_pair = lax.scan(one_group, start, (token_groups, live_groups, pick_groups, rank_groups, cot_groups))
    output = outs_pair[0].reshape(MB, TOKENS, D)
    grad_tokens = outs_pair[1].reshape(MB, TOKENS, D)
    return (output, grad_tokens, sums[0], sums[1], sums[2], sums[3], sums[4], sums[5], sums[6], sums[7], sums[8])
```

```python
import functools

import jax
import jax.numpy as jnp
from jax import lax
from jax.experimental import pallas as pl
from jax.experimental.pallas import tpu as pltpu
from jax.sharding import PartitionSpec as P

SEQ = 197
EPS = 1e-06
F32 = jnp.float32
BF16 = jnp.bfloat16
GELU_A = 0.7978845608028654
GELU_B = 0.044715


def dot(a, b, dims):
    return lax.dot_general(a, b, (dims, ((), ())), preferred_element_type=F32)


def layer_norm(values, gain_vec, shift_vec):
    centre = jnp.mean(values, axis=-1, keepdims=True)
    centered = values - centre
    spread = jnp.mean(centered * centered, axis=-1, keepdims=True)
    return centered * lax.rsqrt(spread + EPS) * gain_vec + shift_vec


def expert_kernel(x_ref, dp_ref, win_ref, wout_ref, y_ref, dx_ref, gin_ref, gout_ref, y_acc, dx_acc):
    step = pl.program_id(0)
    last = pl.num_programs(0) - 1
    x = x_ref[...]
    dprod = dp_ref[...]
    win = win_ref[...]
    wout = wout_ref[...]
    pre = dot(x, win, ((1,), (0,)))
    square = pre * pre
    th = jnp.tanh(GELU_A * pre * (1.0 + GELU_B * square))
    active = (0.5 * pre * (1.0 + th)).astype(BF16)
    slope = 0.5 * (1.0 + th) + 0.5 * pre * (1.0 - th * th) * (GELU_A * (1.0 + 3.0 * GELU_B * square))
    dact = dot(dprod, wout, ((1,), (1,)))
    dpre = (dact * slope).astype(BF16)
    gin_ref[...] = dot(x, dpre, ((0,), (0,))).astype(BF16)
    gout_ref[...] = dot(active, dprod, ((0,), (0,))).astype(BF16)
    part_y = dot(active, wout, ((1,), (0,)))
    part_dx = dot(dpre, win, ((1,), (1,)))

    @pl.when(step == 0)
    def _():
        y_acc[...] = part_y
        dx_acc[...] = part_dx

    @pl.when(step > 0)
    def _():
        y_acc[...] += part_y
        dx_acc[...] += part_dx

    @pl.when(step == last)
    def _():
        y_ref[...] = y_acc[...].astype(BF16)
        dx_ref[...] = dx_acc[...].astype(BF16)


def expert(x, dprod, win, wout, tile=256):
    n, d = x.shape
    ff = win.shape[1]
    return pl.pallas_call(
        expert_kernel,
        grid=(ff // tile,),
        in_specs=[
            pl.BlockSpec((n, d), lambda i: (0, 0)),
            pl.BlockSpec((n, d), lambda i: (0, 0)),
            pl.BlockSpec((d, tile), lambda i: (0, i)),
            pl.BlockSpec((tile, d), lambda i: (i, 0)),
        ],
        out_specs=[
            pl.BlockSpec((n, d), lambda i: (0, 0)),
            pl.BlockSpec((n, d), lambda i: (0, 0)),
            pl.BlockSpec((d, tile), lambda i: (0, i)),
            pl.BlockSpec((tile, d), lambda i: (i, 0)),
        ],
        out_shape=[
            jax.ShapeDtypeStruct((n, d), BF16),
            jax.ShapeDtypeStruct((n, d), BF16),
            jax.ShapeDtypeStruct((d, ff), BF16),
            jax.ShapeDtypeStruct((ff, d), BF16),
        ],
        scratch_shapes=[pltpu.VMEM((n, d), F32), pltpu.VMEM((n, d), F32)],
        compiler_params=pltpu.CompilerParams(vmem_limit_bytes=60 * 1024 * 1024),
        cost_estimate=pl.CostEstimate(
            flops=12 * n * d * ff, transcendentals=n * ff, bytes_accessed=8 * n * d + 8 * d * ff
        ),
    )(x, dprod, win, wout)


def local(
    tokens,
    w_qkv,
    w_proj,
    w_in,
    w_out,
    w_router,
    gain_attn,
    shift_attn,
    gain_moe,
    shift_moe,
    live_rows,
    chosen,
    priority,
    cotangent,
):
    batches, own_rows, d = tokens.shape
    rows = live_rows.shape[1]
    n_dp = lax.axis_size("dp")
    n_t = lax.axis_size("tensor")
    t = lax.axis_index("tensor")
    heads_here = w_qkv.shape[1]
    heads = heads_here * n_t
    width = w_qkv.shape[2] // 3
    experts = w_in.shape[0] * n_dp
    cap = 2 * rows // experts
    share = cap // n_t
    images = rows // SEQ
    span = images * SEQ
    per = -(-images // n_t)
    work = per * SEQ
    total = n_t * work
    factor = width ** (-0.5)
    highest = lax.Precision.HIGHEST

    small = jnp.concatenate(
        [w_router] + [v[:, None] for v in (gain_attn, shift_attn, gain_moe, shift_moe)], axis=1
    )
    small = lax.all_gather(small, ("dp", "tensor"), axis=0, tiled=True)
    router = small[:, :experts]
    gain_one, shift_one, gain_two, shift_two = (small[:, experts + i].astype(F32) for i in range(4))
    qkv = lax.all_gather(w_qkv.reshape(-1, 128), ("dp", "tensor"), axis=0, tiled=False)
    qkv = qkv.reshape(n_dp, n_t, w_qkv.shape[0], heads_here, 3, width)
    qkv = qkv.transpose(0, 2, 4, 1, 3, 5).reshape(d, 3 * heads * width)
    proj = lax.all_gather(w_proj.reshape(-1, 128), ("dp", "tensor"), axis=0, tiled=False)
    proj = proj.reshape(n_dp, n_t, heads_here, w_proj.shape[1], d)
    proj = proj.transpose(1, 2, 0, 3, 4).reshape(heads * width, d)
    win = lax.all_gather(w_in[0], "tensor", axis=1, tiled=True)
    wout = lax.all_gather(w_out[0], "tensor", axis=0, tiled=True)
    cot_all = lax.all_gather(cotangent, "tensor", axis=1, tiled=True)

    def pad_rows(v, n):
        return jnp.pad(v, ((0, 0), (0, n - v.shape[1])) + ((0, 0),) * (v.ndim - 2))

    def own(v):
        return lax.dynamic_slice_in_dim(v, t * work, work, 1)

    edge = own_rows - work
    direct = n_t == 2 and per == 1 and edge >= 0
    if direct:
        moved = lax.ppermute(tokens[:, work:], "tensor", [(0, 1)])
        x = jnp.where(
            t == 0, tokens[:, :work], jnp.concatenate([moved, tokens[:, : work - edge]], axis=1)
        )
    else:
        x = own(pad_rows(lax.all_gather(tokens, "tensor", axis=1, tiled=True)[:, :span], total))
    x = x.astype(F32)
    live = live_rows[:, :span]
    live_all = pad_rows(live, total)
    live_own = own(live_all).astype(F32)[:, :, None]
    cot_all = pad_rows(cot_all[:, :span], total)
    dy = own(cot_all).astype(F32)

    rank = priority[:, 0, :span]
    first, second = chosen[:, :span, 0], chosen[:, :span, 1]
    labels = jnp.arange(experts, dtype=jnp.int32)
    earlier = (rank[:, None, :] < rank[:, :, None]).astype(BF16)
    hit_one = (first[:, :, None] == labels).astype(F32)
    hit_two = (second[:, :, None] == labels).astype(F32)
    live_one = hit_one * live[:, :, None].astype(F32)
    live_two = hit_two * live[:, :, None].astype(F32)
    counts = jnp.einsum(
        "mrs,mse->mre",
        earlier,
        jnp.concatenate([live_one, live_two], axis=-1).astype(BF16),
        preferred_element_type=F32,
    )
    first_total = jnp.sum(live_one, axis=1, keepdims=True)
    slot_one = jnp.sum(counts[:, :, :experts] * hit_one, axis=-1).astype(jnp.int32)
    slot_two = jnp.sum((counts[:, :, experts:] + first_total) * hit_two, axis=-1).astype(jnp.int32)
    keep_one = (live > 0) & (slot_one < cap)
    keep_two = (live > 0) & (slot_two < cap)
    flat_one = jnp.where(keep_one, first * cap + slot_one, -1)
    flat_two = jnp.where(keep_two, second * cap + slot_two, -1)

    def spread(v, fill):
        return jnp.pad(v, ((0, 0), (0, total - span)), constant_values=fill)

    flat_one, flat_two = spread(flat_one, -1), spread(flat_two, -1)
    keep_one, keep_two = spread(keep_one, False), spread(keep_two, False)
    first, second = spread(first, 0), spread(second, 0)
    codes = (jnp.arange(experts)[:, None] * cap + t * share + jnp.arange(share)[None, :]).reshape(-1)
    pick_one = flat_one[:, None, :] == codes[None, :, None]
    pick_two = flat_two[:, None, :] == codes[None, :, None]

    normed_one = layer_norm(x, gain_one, shift_one).astype(BF16)
    mixed = dot(normed_one, qkv, ((2,), (0,)))
    split = heads * width
    shape = (batches * per, SEQ, heads, width)
    query = (mixed[..., :split] * factor).astype(BF16).reshape(shape)
    keys = mixed[..., split : 2 * split].astype(BF16).reshape(shape)
    values = mixed[..., 2 * split :].astype(BF16).reshape(shape)
    scores = jnp.einsum("iqhc,ikhc->ihqk", query, keys, preferred_element_type=F32)
    probs = jax.nn.softmax(scores, axis=-1)
    weights = probs.astype(BF16)
    context = jnp.einsum("ihqk,ikhc->iqhc", weights, values, preferred_element_type=F32)
    context = context.astype(BF16).reshape(batches, work, split)
    attn = dot(context, proj, ((2,), (0,)))
    hidden = x + live_own * attn
    normed_two = layer_norm(hidden, gain_two, shift_two).astype(BF16)

    c_all = lax.all_gather(normed_two, "tensor", axis=1, tiled=True)
    gate_probs = jax.nn.softmax(dot(c_all, router, ((2,), (0,))), axis=-1)
    hits_one = (first[:, :, None] == labels).astype(F32)
    hits_two = (second[:, :, None] == labels).astype(F32)
    gate_one = jnp.sum(gate_probs * hits_one, axis=-1) * keep_one
    gate_two = jnp.sum(gate_probs * hits_two, axis=-1) * keep_two
    picked = (pick_one | pick_two).astype(BF16)
    sent = jnp.einsum(
        "mqr,mrd->mqd",
        picked,
        jnp.concatenate([c_all, cot_all], axis=-1),
        preferred_element_type=F32,
    )
    gate_slot = jnp.sum(
        jnp.where(pick_one, gate_one[:, None, :], 0.0) + jnp.where(pick_two, gate_two[:, None, :], 0.0),
        axis=-1,
        keepdims=True,
    )
    sent = jnp.concatenate(
        [sent[..., :d].astype(BF16), (sent[..., d:] * gate_slot).astype(BF16)], axis=-1
    )
    sent = sent.reshape(batches, experts, share, 2 * d)
    got = lax.all_to_all(sent, "dp", 1, 1, tiled=True).reshape(-1, 2 * d)
    produced, d_in, grad_in, grad_out = expert(got[:, :d], got[:, d:], win, wout)
    back = jnp.concatenate([produced, d_in], axis=-1).reshape(batches, n_dp, share, 2 * d)
    back = lax.all_to_all(back, "dp", 1, 1, tiled=True).reshape(batches, experts * share, 2 * d)
    grad_in = lax.psum_scatter(grad_in, "tensor", scatter_dimension=1, tiled=True).astype(F32)
    grad_out = lax.psum_scatter(grad_out, "tensor", scatter_dimension=0, tiled=True).astype(F32)

    part_one = jnp.einsum("mqr,mqd->mrd", pick_one.astype(BF16), back[..., :d], preferred_element_type=F32)
    part_two = jnp.einsum("mqr,mqd->mrd", pick_two.astype(BF16), back[..., :d], preferred_element_type=F32)
    d_rows = jnp.einsum("mqr,mqd->mrd", picked, back[..., d:], preferred_element_type=F32)
    mixture = gate_one[:, :, None] * part_one + gate_two[:, :, None] * part_two
    cot_wide = cot_all.astype(F32)
    dgate_one = jnp.sum(part_one * cot_wide, axis=-1, keepdims=True)
    dgate_two = jnp.sum(part_two * cot_wide, axis=-1, keepdims=True)
    dgates = jnp.concatenate([dgate_one, dgate_two], axis=-1)
    payload = jnp.concatenate(
        [mixture, d_rows, jnp.pad(dgates, ((0, 0), (0, 0), (0, 126)))], axis=-1
    ).astype(BF16)
    payload = lax.psum_scatter(payload, "tensor", scatter_dimension=1, tiled=True).astype(F32)
    output = (hidden + payload[..., :d]).astype(BF16)
    dgates = payload[..., 2 * d : 2 * d + 2]

    own_probs = own(gate_probs)
    dprobs = own(hits_one) * dgates[..., 0:1] * own(keep_one)[:, :, None]
    dprobs = dprobs + own(hits_two) * dgates[..., 1:2] * own(keep_two)[:, :, None]
    dlogits = own_probs * (dprobs - jnp.sum(dprobs * own_probs, axis=-1, keepdims=True))
    grad_router = lax.dot_general(
        normed_two.astype(F32), dlogits, (((0, 1), (0, 1)), ((), ())), precision=highest
    )
    dc = payload[..., d : 2 * d] + lax.dot_general(
        dlogits, router.astype(F32), (((2,), (1,)), ((), ())), precision=highest
    )
    _, back_two = jax.vjp(layer_norm, hidden, gain_two, shift_two)
    dnorm, grad_gain_two, grad_shift_two = back_two(dc)
    dhidden = dy + dnorm
    dattn = (live_own * dhidden).astype(BF16)

    grad_proj = dot(context, dattn, ((0, 1), (0, 1)))
    dcontext = dot(dattn, proj, ((2,), (1,))).astype(BF16).reshape(shape)
    dvalues = jnp.einsum("ihqk,iqhc->ikhc", weights, dcontext, preferred_element_type=F32).astype(BF16)
    dweights = jnp.einsum("iqhc,ikhc->ihqk", dcontext, values, preferred_element_type=F32)
    dscores = (probs * (dweights - jnp.sum(dweights * probs, axis=-1, keepdims=True))).astype(BF16)
    dquery = jnp.einsum("ihqk,ikhc->iqhc", dscores, keys, preferred_element_type=F32).astype(BF16)
    dkeys = jnp.einsum("ihqk,iqhc->ikhc", dscores, query, preferred_element_type=F32).astype(BF16)
    dmixed = jnp.concatenate(
        [v.reshape(batches, work, split) for v in (dquery * BF16(factor), dkeys, dvalues)], axis=-1
    )
    grad_qkv = dot(normed_one, dmixed, ((0, 1), (0, 1)))
    da = dot(dmixed, qkv, ((2,), (1,)))
    _, back_one = jax.vjp(layer_norm, x, gain_one, shift_one)
    dnorm, grad_gain_one, grad_shift_one = back_one(da)
    grad_x = dhidden + dnorm

    if direct:
        out_edge = lax.ppermute(output[:, :edge], "tensor", [(1, 0)])
        grad_edge = lax.ppermute(grad_x[:, :edge], "tensor", [(1, 0)])
        result = jnp.where(
            t == 0,
            jnp.concatenate([output, out_edge], axis=1),
            jnp.concatenate([output[:, edge:], tokens[:, work - edge :]], axis=1),
        )
        grad_tokens = jnp.where(
            t == 0,
            jnp.concatenate([grad_x, grad_edge], axis=1),
            jnp.concatenate([grad_x[:, edge:], cotangent[:, work - edge :].astype(F32)], axis=1),
        )
    else:
        here = (t * own_rows + jnp.arange(own_rows) < span)[None, :, None]

        def home(v, rest):
            full = pad_rows(lax.all_gather(v, "tensor", axis=1, tiled=True)[:, :span], rows)
            return jnp.where(here, lax.dynamic_slice_in_dim(full, t * own_rows, own_rows, 1), rest)

        result = home(output, tokens)
        grad_tokens = home(grad_x, cotangent.astype(F32))

    grad_qkv = grad_qkv.astype(BF16).reshape(n_dp, -1, 3, n_t, heads_here, width)
    grad_qkv = grad_qkv.transpose(0, 3, 1, 4, 2, 5).reshape(n_dp * n_t * w_qkv.shape[0], heads_here * 3 * width)
    grad_qkv = lax.psum_scatter(grad_qkv, ("dp", "tensor"), scatter_dimension=0, tiled=True)
    grad_proj = grad_proj.astype(BF16).reshape(n_t, heads_here, n_dp, -1, d)
    grad_proj = grad_proj.transpose(2, 0, 1, 3, 4).reshape(-1, d)
    grad_proj = lax.psum_scatter(grad_proj, ("dp", "tensor"), scatter_dimension=0, tiled=True)
    smalls = jnp.concatenate(
        [grad_router] + [v[:, None] for v in (grad_gain_one, grad_shift_one, grad_gain_two, grad_shift_two)],
        axis=1,
    )
    smalls = lax.psum_scatter(smalls, ("dp", "tensor"), scatter_dimension=0, tiled=True)
    return (
        result,
        grad_tokens,
        grad_qkv.astype(F32).reshape(w_qkv.shape),
        grad_proj.astype(F32).reshape(w_proj.shape),
        grad_in[None],
        grad_out[None],
        smalls[:, :experts],
        smalls[:, experts],
        smalls[:, experts + 1],
        smalls[:, experts + 2],
        smalls[:, experts + 3],
    )


def solution(mesh):
    both = ("dp", "tensor")
    return jax.shard_map(
        local,
        mesh=mesh,
        in_specs=(
            P(None, both, None),
            P("dp", "tensor", None),
            P("tensor", "dp", None),
            P("dp", None, "tensor"),
            P("dp", "tensor", None),
            P(both, None),
            P(both),
            P(both),
            P(both),
            P(both),
            P(None, "dp"),
            P(None, "dp", None),
            P(None, "dp", None),
            P(None, both, None),
        ),
        out_specs=(
            P(None, both, None),
            P(None, both, None),
            P("dp", "tensor", None),
            P("tensor", "dp", None),
            P("dp", None, "tensor"),
            P("dp", "tensor", None),
            P(both, None),
            P(both),
            P(both),
            P(both),
            P(both),
        ),
        check_vma=False,
    )
```

```python
import functools

import jax
import jax.numpy as jnp
from jax import lax
from jax.experimental import pallas as pl
from jax.experimental.pallas import tpu as pltpu
from jax.sharding import PartitionSpec as P

SEQ = 197
EPS = 1e-06
F32 = jnp.float32
BF16 = jnp.bfloat16
GELU_A = 0.7978845608028654
GELU_B = 0.044715


def dot(a, b, dims):
    return lax.dot_general(a, b, (dims, ((), ())), preferred_element_type=F32)


def layer_norm(values, gain_vec, shift_vec):
    centre = jnp.mean(values, axis=-1, keepdims=True)
    centered = values - centre
    spread = jnp.mean(centered * centered, axis=-1, keepdims=True)
    return centered * lax.rsqrt(spread + EPS) * gain_vec + shift_vec


def expert_kernel(x_ref, dp_ref, win_ref, wout_ref, y_ref, dx_ref, gin_ref, gout_ref, y_acc, dx_acc):
    step = pl.program_id(0)
    last = pl.num_programs(0) - 1
    x = x_ref[...]
    dprod = dp_ref[...]
    win = win_ref[...]
    wout = wout_ref[...]
    pre = dot(x, win, ((1,), (0,)))
    square = pre * pre
    th = jnp.tanh(GELU_A * pre * (1.0 + GELU_B * square))
    active = (0.5 * pre * (1.0 + th)).astype(BF16)
    slope = 0.5 * (1.0 + th) + 0.5 * pre * (1.0 - th * th) * (GELU_A * (1.0 + 3.0 * GELU_B * square))
    dact = dot(dprod, wout, ((1,), (1,)))
    dpre = (dact * slope).astype(BF16)
    gin_ref[...] = dot(x, dpre, ((0,), (0,))).astype(BF16)
    gout_ref[...] = dot(active, dprod, ((0,), (0,))).astype(BF16)
    part_y = dot(active, wout, ((1,), (0,)))
    part_dx = dot(dpre, win, ((1,), (1,)))

    @pl.when(step == 0)
    def _():
        y_acc[...] = part_y
        dx_acc[...] = part_dx

    @pl.when(step > 0)
    def _():
        y_acc[...] += part_y
        dx_acc[...] += part_dx

    @pl.when(step == last)
    def _():
        y_ref[...] = y_acc[...].astype(BF16)
        dx_ref[...] = dx_acc[...].astype(BF16)


def expert(x, dprod, win, wout, tile=256):
    n, d = x.shape
    ff = win.shape[1]
    return pl.pallas_call(
        expert_kernel,
        grid=(ff // tile,),
        in_specs=[
            pl.BlockSpec((n, d), lambda i: (0, 0)),
            pl.BlockSpec((n, d), lambda i: (0, 0)),
            pl.BlockSpec((d, tile), lambda i: (0, i)),
            pl.BlockSpec((tile, d), lambda i: (i, 0)),
        ],
        out_specs=[
            pl.BlockSpec((n, d), lambda i: (0, 0)),
            pl.BlockSpec((n, d), lambda i: (0, 0)),
            pl.BlockSpec((d, tile), lambda i: (0, i)),
            pl.BlockSpec((tile, d), lambda i: (i, 0)),
        ],
        out_shape=[
            jax.ShapeDtypeStruct((n, d), BF16),
            jax.ShapeDtypeStruct((n, d), BF16),
            jax.ShapeDtypeStruct((d, ff), BF16),
            jax.ShapeDtypeStruct((ff, d), BF16),
        ],
        scratch_shapes=[pltpu.VMEM((n, d), F32), pltpu.VMEM((n, d), F32)],
        compiler_params=pltpu.CompilerParams(vmem_limit_bytes=60 * 1024 * 1024),
        cost_estimate=pl.CostEstimate(
            flops=12 * n * d * ff, transcendentals=n * ff, bytes_accessed=8 * n * d + 8 * d * ff
        ),
    )(x, dprod, win, wout)


MESH = pl.DeviceIdType.MESH
ANYWHERE = pl.BlockSpec(memory_space=pltpu.VMEM)


def grid_sizes(n_dp):
    ny = 1
    while 2 * ny * 2 * ny <= n_dp // 2:
        ny *= 2
    return n_dp // (2 * ny), ny


def position(ny):
    dp = lax.axis_index("dp")
    return dp, lax.axis_index("tensor"), dp % 2, (dp // 2) % ny, dp // (2 * ny)


def neighbours(ny, nz, n_t):
    dp, t, c, y, z = position(ny)

    def along_core(k):
        return (dp - c + (c + k) % 2, t)

    def along_tensor(k):
        return (dp, (t + k) % n_t)

    def along_y(k):
        return (dp + ((y + k) % ny - y) * 2, t)

    def along_z(k):
        return (dp + ((z + k) % nz - z) * 2 * ny, t)

    return {"core": (2, along_core), "tensor": (n_t, along_tensor), "y": (ny, along_y), "z": (nz, along_z)}


def greet(stages):
    barrier = pltpu.get_barrier_semaphore()
    count = 0
    for size, device in stages.values():
        for k in range(1, size):
            pl.semaphore_signal(barrier, inc=1, device_id=device(k), device_id_type=MESH)
            count += 1
    pl.semaphore_wait(barrier, count)


def gather_kernel(ny, nz, n_t, qkv, proj, small, qkv_out, proj_out, small_out, send, recv, copied):
    _, t, c, y, z = position(ny)
    stages = neighbours(ny, nz, n_t)
    greet(stages)
    cols = qkv.shape[1]

    def views(zs, ys, cs, ts):
        lanes = pl.ds(pl.multiple_of(ts * cols, 128), cols)
        return (
            qkv_out.at[zs, ys, cs, :, lanes],
            proj_out.at[zs, ys, cs, ts],
            small_out.at[zs, ys, cs, ts],
        )

    whole = slice(None)
    mine = views(z, y, c, t)
    local = [
        pltpu.make_async_copy(src, dst, copied.at[i])
        for i, (src, dst) in enumerate(zip((qkv, proj, small), mine))
    ]
    for copy in local:
        copy.start()
    slot = 0
    for name in ("z", "y", "tensor", "core"):
        size, device = stages[name]
        if name == "z":
            sources, targets = (qkv, proj, small), mine
        elif name == "y":
            sources = targets = views(whole, y, c, t)
        elif name == "tensor":
            sources = targets = views(whole, whole, c, t)
        else:
            sources = targets = (
                qkv_out.at[:, :, c],
                proj_out.at[:, :, c],
                small_out.at[:, :, c],
            )
        copies = []
        for k in range(1, size):
            for src, dst in zip(sources, targets):
                copies.append(
                    pltpu.make_async_remote_copy(
                        src_ref=src,
                        dst_ref=dst,
                        send_sem=send.at[slot],
                        recv_sem=recv.at[slot],
                        device_id=device(k),
                        device_id_type=MESH,
                    )
                )
                slot += 1
        for copy in copies:
            copy.start()
        if name == "z":
            for copy in local:
                copy.wait()
        for copy in copies:
            copy.wait()


def gather_weights(qkv, proj, small, n_dp, n_t):
    nz, ny = grid_sizes(n_dp)
    slots = 3 * (1 + (n_t - 1) + (ny - 1) + (nz - 1))
    outs = pl.pallas_call(
        functools.partial(gather_kernel, ny, nz, n_t),
        out_shape=[
            jax.ShapeDtypeStruct((nz, ny, 2, qkv.shape[0], n_t * qkv.shape[1]), BF16),
            jax.ShapeDtypeStruct((nz, ny, 2, n_t) + proj.shape, BF16),
            jax.ShapeDtypeStruct((nz, ny, 2, n_t) + small.shape, BF16),
        ],
        in_specs=[ANYWHERE] * 3,
        out_specs=[ANYWHERE] * 3,
        scratch_shapes=[
            pltpu.SemaphoreType.DMA((slots,)),
            pltpu.SemaphoreType.DMA((slots,)),
            pltpu.SemaphoreType.DMA((3,)),
        ],
        compiler_params=pltpu.CompilerParams(collective_id=0, has_side_effects=True),
    )(qkv, proj, small)
    qkv_all = outs[0].reshape(n_dp * qkv.shape[0], n_t * qkv.shape[1])
    return qkv_all, outs[1].reshape((n_dp, n_t) + proj.shape), outs[2].reshape(-1, small.shape[1])


def scatter_kernel(ny, nz, n_t, *refs):
    ins, refs = refs[:3], refs[3:]
    outs, refs = refs[:3], refs[3:]
    got = [refs[3 * i : 3 * i + 3] for i in range(4)]
    held = [refs[12 + 3 * i : 15 + 3 * i] for i in range(3)]
    send, recv = refs[21], refs[22]
    _, t, c, y, z = position(ny)
    stages = neighbours(ny, nz, n_t)
    greet(stages)
    cols = outs[0].shape[1]
    slot = 0

    def lanes(ts):
        return pl.ds(pl.multiple_of(ts * cols, 128), cols)

    def exchange(name, me, piece):
        nonlocal slot
        size, device = stages[name]
        level = ("core", "tensor", "y", "z").index(name)
        copies = []
        for k in range(1, size):
            for i, src in enumerate(piece((me + k) % size)):
                copies.append(
                    pltpu.make_async_remote_copy(
                        src_ref=src,
                        dst_ref=got[level][i].at[k - 1],
                        send_sem=send.at[slot],
                        recv_sem=recv.at[slot],
                        device_id=device(k),
                        device_id_type=MESH,
                    )
                )
                slot += 1
        for copy in copies:
            copy.start()
        for copy in copies:
            copy.wait()

    def total(own, level, index, i):
        value = own.astype(F32)
        for k in range(got[level][i].shape[0]):
            value = value + got[level][i][(k,) + index].astype(F32)
        return value

    def over_zy(body):
        def step(n, carry):
            body(n // ny, n % ny)
            return carry

        lax.fori_loop(0, nz * ny, step, 0)

    exchange("core", c, lambda j: [ref.at[:, :, j] for ref in ins])

    def add_core(zi, yi):
        for i in range(3):
            held[0][i][zi, yi] = total(ins[i][zi, yi, c], 0, (zi, yi), i).astype(held[0][i].dtype)

    over_zy(add_core)
    exchange(
        "tensor",
        t,
        lambda j: [held[0][0].at[:, :, :, lanes(j)], held[0][1].at[:, :, j], held[0][2].at[:, :, j]],
    )

    def add_tensor(zi, yi):
        owns = (held[0][0][zi, yi, :, lanes(t)], held[0][1][zi, yi, t], held[0][2][zi, yi, t])
        for i in range(3):
            held[1][i][zi, yi] = total(owns[i], 1, (zi, yi), i).astype(held[1][i].dtype)

    over_zy(add_tensor)
    exchange("y", y, lambda j: [ref.at[:, j] for ref in held[1]])

    def add_y(zi, carry):
        for i in range(3):
            held[2][i][zi] = total(held[1][i][zi, y], 2, (zi,), i).astype(held[2][i].dtype)
        return carry

    lax.fori_loop(0, nz, add_y, 0)
    exchange("z", z, lambda j: [ref.at[j] for ref in held[2]])
    for i in range(3):
        outs[i][...] = total(held[2][i][z], 3, (), i)


def scatter_grads(qkv, proj, small, n_dp, n_t):
    nz, ny = qkv.shape[:2]
    rows, cols = qkv.shape[3], qkv.shape[4] // n_t
    tails = [(rows, cols), proj.shape[4:], small.shape[4:]]
    kinds = [BF16, BF16, F32]
    wide = [(rows, n_t * cols), (n_t,) + proj.shape[4:], (n_t,) + small.shape[4:]]
    scratch = [pltpu.VMEM((1, nz, ny) + wide[i], kinds[i]) for i in range(3)]
    scratch += [pltpu.VMEM((n_t - 1, nz, ny) + tails[i], kinds[i]) for i in range(3)]
    scratch += [pltpu.VMEM((ny - 1, nz) + tails[i], kinds[i]) for i in range(3)]
    scratch += [pltpu.VMEM((nz - 1,) + tails[i], kinds[i]) for i in range(3)]
    scratch += [pltpu.VMEM((nz, ny) + wide[i], kinds[i]) for i in range(3)]
    scratch += [pltpu.VMEM((nz, ny) + tails[i], kinds[i]) for i in range(3)]
    scratch += [pltpu.VMEM((nz,) + tails[i], kinds[i]) for i in range(3)]
    slots = 3 * (1 + (n_t - 1) + (ny - 1) + (nz - 1))
    scratch += [pltpu.SemaphoreType.DMA((slots,)), pltpu.SemaphoreType.DMA((slots,))]
    return pl.pallas_call(
        functools.partial(scatter_kernel, ny, nz, n_t),
        out_shape=[jax.ShapeDtypeStruct(tail, F32) for tail in tails],
        in_specs=[ANYWHERE] * 3,
        out_specs=[ANYWHERE] * 3,
        scratch_shapes=scratch,
        compiler_params=pltpu.CompilerParams(collective_id=1, has_side_effects=True),
    )(qkv, proj, small)


def local(
    tokens,
    w_qkv,
    w_proj,
    w_in,
    w_out,
    w_router,
    gain_attn,
    shift_attn,
    gain_moe,
    shift_moe,
    live_rows,
    chosen,
    priority,
    cotangent,
):
    batches, own_rows, d = tokens.shape
    rows = live_rows.shape[1]
    n_dp = lax.axis_size("dp")
    n_t = lax.axis_size("tensor")
    t = lax.axis_index("tensor")
    heads_here = w_qkv.shape[1]
    heads = heads_here * n_t
    width = w_qkv.shape[2] // 3
    experts = w_in.shape[0] * n_dp
    cap = 2 * rows // experts
    share = cap // n_t
    images = rows // SEQ
    span = images * SEQ
    per = -(-images // n_t)
    work = per * SEQ
    total = n_t * work
    factor = width ** (-0.5)
    highest = lax.Precision.HIGHEST

    small = jnp.concatenate(
        [w_router] + [v[:, None] for v in (gain_attn, shift_attn, gain_moe, shift_moe)], axis=1
    )
    small = jnp.pad(small, ((0, 0), (0, 128 - small.shape[1])))
    block = heads_here * width
    qkv_block = w_qkv.reshape(-1, heads_here, 3, width).transpose(0, 2, 1, 3).reshape(-1, 3 * block)
    fill = -3 * block % 128
    qkv_block = jnp.pad(qkv_block, ((0, 0), (0, fill)))
    qkv, proj, small = gather_weights(qkv_block, w_proj.reshape(-1, d), small, n_dp, n_t)
    qkv = qkv.reshape(d, n_t, 3 * block + fill)[:, :, : 3 * block].reshape(d, -1)
    router = small[:, :experts]
    gain_one, shift_one, gain_two, shift_two = (small[:, experts + i].astype(F32) for i in range(4))
    proj = proj.reshape(n_dp, n_t, heads_here, w_proj.shape[1], d)
    proj = proj.transpose(1, 2, 0, 3, 4).reshape(heads * width, d)
    win = lax.all_gather(w_in[0], "tensor", axis=1, tiled=True)
    wout = lax.all_gather(w_out[0], "tensor", axis=0, tiled=True)
    cot_all = lax.all_gather(cotangent, "tensor", axis=1, tiled=True)

    def pad_rows(v, n):
        return jnp.pad(v, ((0, 0), (0, n - v.shape[1])) + ((0, 0),) * (v.ndim - 2))

    def own(v):
        return lax.dynamic_slice_in_dim(v, t * work, work, 1)

    edge = own_rows - work
    direct = n_t == 2 and per == 1 and edge >= 0
    if direct:
        moved = lax.ppermute(tokens[:, work:], "tensor", [(0, 1)])
        x = jnp.where(
            t == 0, tokens[:, :work], jnp.concatenate([moved, tokens[:, : work - edge]], axis=1)
        )
    else:
        x = own(pad_rows(lax.all_gather(tokens, "tensor", axis=1, tiled=True)[:, :span], total))
    x = x.astype(F32)
    live = live_rows[:, :span]
    live_all = pad_rows(live, total)
    live_own = own(live_all).astype(F32)[:, :, None]
    cot_all = pad_rows(cot_all[:, :span], total)
    dy = own(cot_all).astype(F32)

    rank = priority[:, 0, :span]
    first, second = chosen[:, :span, 0], chosen[:, :span, 1]
    labels = jnp.arange(experts, dtype=jnp.int32)
    earlier = (rank[:, None, :] < rank[:, :, None]).astype(BF16)
    hit_one = (first[:, :, None] == labels).astype(F32)
    hit_two = (second[:, :, None] == labels).astype(F32)
    live_one = hit_one * live[:, :, None].astype(F32)
    live_two = hit_two * live[:, :, None].astype(F32)
    counts = jnp.einsum(
        "mrs,mse->mre",
        earlier,
        jnp.concatenate([live_one, live_two], axis=-1).astype(BF16),
        preferred_element_type=F32,
    )
    first_total = jnp.sum(live_one, axis=1, keepdims=True)
    slot_one = jnp.sum(counts[:, :, :experts] * hit_one, axis=-1).astype(jnp.int32)
    slot_two = jnp.sum((counts[:, :, experts:] + first_total) * hit_two, axis=-1).astype(jnp.int32)
    keep_one = (live > 0) & (slot_one < cap)
    keep_two = (live > 0) & (slot_two < cap)
    flat_one = jnp.where(keep_one, first * cap + slot_one, -1)
    flat_two = jnp.where(keep_two, second * cap + slot_two, -1)

    def spread(v, fill):
        return jnp.pad(v, ((0, 0), (0, total - span)), constant_values=fill)

    flat_one, flat_two = spread(flat_one, -1), spread(flat_two, -1)
    keep_one, keep_two = spread(keep_one, False), spread(keep_two, False)
    first, second = spread(first, 0), spread(second, 0)
    codes = (jnp.arange(experts)[:, None] * cap + t * share + jnp.arange(share)[None, :]).reshape(-1)
    pick_one = flat_one[:, None, :] == codes[None, :, None]
    pick_two = flat_two[:, None, :] == codes[None, :, None]

    normed_one = layer_norm(x, gain_one, shift_one).astype(BF16)
    mixed = dot(normed_one, qkv, ((2,), (0,)))
    split = heads * width
    shape = (batches * per, SEQ, heads, width)
    mixed = mixed.reshape(batches, work, n_t, 3, block)
    query = (mixed[:, :, :, 0] * factor).astype(BF16).reshape(shape)
    keys = mixed[:, :, :, 1].astype(BF16).reshape(shape)
    values = mixed[:, :, :, 2].astype(BF16).reshape(shape)
    scores = jnp.einsum("iqhc,ikhc->ihqk", query, keys, preferred_element_type=F32)
    probs = jax.nn.softmax(scores, axis=-1)
    weights = probs.astype(BF16)
    context = jnp.einsum("ihqk,ikhc->iqhc", weights, values, preferred_element_type=F32)
    context = context.astype(BF16).reshape(batches, work, split)
    attn = dot(context, proj, ((2,), (0,)))
    hidden = x + live_own * attn
    normed_two = layer_norm(hidden, gain_two, shift_two).astype(BF16)

    c_all = lax.all_gather(normed_two, "tensor", axis=1, tiled=True)
    gate_probs = jax.nn.softmax(dot(c_all, router, ((2,), (0,))), axis=-1)
    hits_one = (first[:, :, None] == labels).astype(F32)
    hits_two = (second[:, :, None] == labels).astype(F32)
    gate_one = jnp.sum(gate_probs * hits_one, axis=-1) * keep_one
    gate_two = jnp.sum(gate_probs * hits_two, axis=-1) * keep_two
    picked = (pick_one | pick_two).astype(BF16)
    sent = jnp.einsum(
        "mqr,mrd->mqd",
        picked,
        jnp.concatenate([c_all, cot_all], axis=-1),
        preferred_element_type=F32,
    )
    gate_slot = jnp.sum(
        jnp.where(pick_one, gate_one[:, None, :], 0.0) + jnp.where(pick_two, gate_two[:, None, :], 0.0),
        axis=-1,
        keepdims=True,
    )
    sent = jnp.concatenate(
        [sent[..., :d].astype(BF16), (sent[..., d:] * gate_slot).astype(BF16)], axis=-1
    )
    sent = sent.reshape(batches, experts, share, 2 * d)
    got = lax.all_to_all(sent, "dp", 1, 1, tiled=True).reshape(-1, 2 * d)
    produced, d_in, grad_in, grad_out = expert(got[:, :d], got[:, d:], win, wout)
    back = jnp.concatenate([produced, d_in], axis=-1).reshape(batches, n_dp, share, 2 * d)
    back = lax.all_to_all(back, "dp", 1, 1, tiled=True).reshape(batches, experts * share, 2 * d)
    grad_in = lax.psum_scatter(grad_in, "tensor", scatter_dimension=1, tiled=True).astype(F32)
    grad_out = lax.psum_scatter(grad_out, "tensor", scatter_dimension=0, tiled=True).astype(F32)

    part_one = jnp.einsum("mqr,mqd->mrd", pick_one.astype(BF16), back[..., :d], preferred_element_type=F32)
    part_two = jnp.einsum("mqr,mqd->mrd", pick_two.astype(BF16), back[..., :d], preferred_element_type=F32)
    d_rows = jnp.einsum("mqr,mqd->mrd", picked, back[..., d:], preferred_element_type=F32)
    mixture = gate_one[:, :, None] * part_one + gate_two[:, :, None] * part_two
    cot_wide = cot_all.astype(F32)
    dgate_one = jnp.sum(part_one * cot_wide, axis=-1, keepdims=True)
    dgate_two = jnp.sum(part_two * cot_wide, axis=-1, keepdims=True)
    dgates = jnp.concatenate([dgate_one, dgate_two], axis=-1)
    payload = jnp.concatenate(
        [mixture, d_rows, jnp.pad(dgates, ((0, 0), (0, 0), (0, 126)))], axis=-1
    ).astype(BF16)
    pieces = payload.reshape(batches, n_t, work, payload.shape[-1])

    def piece(k):
        return lax.dynamic_index_in_dim(pieces, (t + k) % n_t, 1, keepdims=False)

    payload = piece(0).astype(F32)
    for k in range(1, n_t):
        payload = payload + lax.ppermute(
            piece(k), "tensor", [(j, (j + k) % n_t) for j in range(n_t)]
        ).astype(F32)
    output = (hidden + payload[..., :d]).astype(BF16)
    dgates = payload[..., 2 * d : 2 * d + 2]

    own_probs = own(gate_probs)
    dprobs = own(hits_one) * dgates[..., 0:1] * own(keep_one)[:, :, None]
    dprobs = dprobs + own(hits_two) * dgates[..., 1:2] * own(keep_two)[:, :, None]
    dlogits = own_probs * (dprobs - jnp.sum(dprobs * own_probs, axis=-1, keepdims=True))
    grad_router = lax.dot_general(
        normed_two.astype(F32), dlogits, (((0, 1), (0, 1)), ((), ())), precision=highest
    )
    dc = payload[..., d : 2 * d] + lax.dot_general(
        dlogits, router.astype(F32), (((2,), (1,)), ((), ())), precision=highest
    )
    _, back_two = jax.vjp(layer_norm, hidden, gain_two, shift_two)
    dnorm, grad_gain_two, grad_shift_two = back_two(dc)
    dhidden = dy + dnorm
    dattn = (live_own * dhidden).astype(BF16)

    grad_proj = dot(context, dattn, ((0, 1), (0, 1)))
    dcontext = dot(dattn, proj, ((2,), (1,))).astype(BF16).reshape(shape)
    dvalues = jnp.einsum("ihqk,iqhc->ikhc", weights, dcontext, preferred_element_type=F32).astype(BF16)
    dweights = jnp.einsum("iqhc,ikhc->ihqk", dcontext, values, preferred_element_type=F32)
    dscores = (probs * (dweights - jnp.sum(dweights * probs, axis=-1, keepdims=True))).astype(BF16)
    dquery = jnp.einsum("ihqk,ikhc->iqhc", dscores, keys, preferred_element_type=F32).astype(BF16)
    dkeys = jnp.einsum("ihqk,iqhc->ikhc", dscores, query, preferred_element_type=F32).astype(BF16)
    dmixed = jnp.stack(
        [v.reshape(batches, work, n_t, block) for v in (dquery * BF16(factor), dkeys, dvalues)], axis=3
    ).reshape(batches, work, 3 * split)
    grad_qkv = dot(normed_one, dmixed, ((0, 1), (0, 1)))
    da = dot(dmixed, qkv, ((2,), (1,)))
    _, back_one = jax.vjp(layer_norm, x, gain_one, shift_one)
    dnorm, grad_gain_one, grad_shift_one = back_one(da)
    grad_x = dhidden + dnorm

    if direct:
        out_edge = lax.ppermute(output[:, :edge], "tensor", [(1, 0)])
        grad_edge = lax.ppermute(grad_x[:, :edge], "tensor", [(1, 0)])
        result = jnp.where(
            t == 0,
            jnp.concatenate([output, out_edge], axis=1),
            jnp.concatenate([output[:, edge:], tokens[:, work - edge :]], axis=1),
        )
        grad_tokens = jnp.where(
            t == 0,
            jnp.concatenate([grad_x, grad_edge], axis=1),
            jnp.concatenate([grad_x[:, edge:], cotangent[:, work - edge :].astype(F32)], axis=1),
        )
    else:
        here = (t * own_rows + jnp.arange(own_rows) < span)[None, :, None]

        def home(v, rest):
            full = pad_rows(lax.all_gather(v, "tensor", axis=1, tiled=True)[:, :span], rows)
            return jnp.where(here, lax.dynamic_slice_in_dim(full, t * own_rows, own_rows, 1), rest)

        result = home(output, tokens)
        grad_tokens = home(grad_x, cotangent.astype(F32))

    nz, ny = grid_sizes(n_dp)
    grad_qkv = jnp.pad(grad_qkv.astype(BF16).reshape(d, n_t, 3 * block), ((0, 0), (0, 0), (0, fill)))
    grad_qkv = grad_qkv.reshape(nz, ny, 2, d // n_dp, -1)
    grad_proj = grad_proj.astype(BF16).reshape(n_t, heads_here, n_dp, -1, d)
    grad_proj = grad_proj.transpose(2, 0, 1, 3, 4).reshape(nz, ny, 2, n_t, -1, d)
    smalls = jnp.concatenate(
        [grad_router] + [v[:, None] for v in (grad_gain_one, grad_shift_one, grad_gain_two, grad_shift_two)],
        axis=1,
    )
    smalls = jnp.pad(smalls, ((0, 0), (0, 128 - smalls.shape[1]))).reshape(nz, ny, 2, n_t, -1, 128)
    grad_qkv, grad_proj, smalls = scatter_grads(grad_qkv, grad_proj, smalls, n_dp, n_t)
    grad_qkv = grad_qkv[:, : 3 * block].reshape(-1, 3, heads_here, width).transpose(0, 2, 1, 3)
    return (
        result,
        grad_tokens,
        grad_qkv.reshape(w_qkv.shape),
        grad_proj.reshape(w_proj.shape),
        grad_in[None],
        grad_out[None],
        smalls[:, :experts],
        smalls[:, experts],
        smalls[:, experts + 1],
        smalls[:, experts + 2],
        smalls[:, experts + 3],
    )


def solution(mesh):
    both = ("dp", "tensor")
    return jax.shard_map(
        local,
        mesh=mesh,
        in_specs=(
            P(None, both, None),
            P("dp", "tensor", None),
            P("tensor", "dp", None),
            P("dp", None, "tensor"),
            P("dp", "tensor", None),
            P(both, None),
            P(both),
            P(both),
            P(both),
            P(both),
            P(None, "dp"),
            P(None, "dp", None),
            P(None, "dp", None),
            P(None, both, None),
        ),
        out_specs=(
            P(None, both, None),
            P(None, both, None),
            P("dp", "tensor", None),
            P("tensor", "dp", None),
            P("dp", None, "tensor"),
            P("dp", "tensor", None),
            P(both, None),
            P(both),
            P(both),
            P(both),
            P(both),
        ),
        check_vma=False,
    )
```

```python
import functools

import jax
import jax.numpy as jnp
from jax import lax
from jax.experimental import pallas as pl
from jax.experimental.pallas import tpu as pltpu
from jax.sharding import PartitionSpec as P

SEQ = 197
EPS = 1e-06
F32 = jnp.float32
BF16 = jnp.bfloat16
GELU_A = 0.7978845608028654
GELU_B = 0.044715


def dot(a, b, dims):
    return lax.dot_general(a, b, (dims, ((), ())), preferred_element_type=F32)


def layer_norm(values, gain_vec, shift_vec):
    centre = jnp.mean(values, axis=-1, keepdims=True)
    centered = values - centre
    spread = jnp.mean(centered * centered, axis=-1, keepdims=True)
    return centered * lax.rsqrt(spread + EPS) * gain_vec + shift_vec


def expert_kernel(x_ref, dp_ref, win_ref, wout_ref, y_ref, dx_ref, gin_ref, gout_ref, y_acc, dx_acc):
    step = pl.program_id(0)
    last = pl.num_programs(0) - 1
    x = x_ref[...]
    dprod = dp_ref[...]
    win = win_ref[...]
    wout = wout_ref[...]
    pre = dot(x, win, ((1,), (0,)))
    square = pre * pre
    th = jnp.tanh(GELU_A * pre * (1.0 + GELU_B * square))
    active = (0.5 * pre * (1.0 + th)).astype(BF16)
    slope = 0.5 * (1.0 + th) + 0.5 * pre * (1.0 - th * th) * (GELU_A * (1.0 + 3.0 * GELU_B * square))
    dact = dot(dprod, wout, ((1,), (1,)))
    dpre = (dact * slope).astype(BF16)
    gin_ref[...] = dot(x, dpre, ((0,), (0,))).astype(BF16)
    gout_ref[...] = dot(active, dprod, ((0,), (0,))).astype(BF16)
    part_y = dot(active, wout, ((1,), (0,)))
    part_dx = dot(dpre, win, ((1,), (1,)))

    @pl.when(step == 0)
    def _():
        y_acc[...] = part_y
        dx_acc[...] = part_dx

    @pl.when(step > 0)
    def _():
        y_acc[...] += part_y
        dx_acc[...] += part_dx

    @pl.when(step == last)
    def _():
        y_ref[...] = y_acc[...].astype(BF16)
        dx_ref[...] = dx_acc[...].astype(BF16)


def expert(x, dprod, win, wout, tile=256):
    n, d = x.shape
    ff = win.shape[1]
    return pl.pallas_call(
        expert_kernel,
        grid=(ff // tile,),
        in_specs=[
            pl.BlockSpec((n, d), lambda i: (0, 0)),
            pl.BlockSpec((n, d), lambda i: (0, 0)),
            pl.BlockSpec((d, tile), lambda i: (0, i)),
            pl.BlockSpec((tile, d), lambda i: (i, 0)),
        ],
        out_specs=[
            pl.BlockSpec((n, d), lambda i: (0, 0)),
            pl.BlockSpec((n, d), lambda i: (0, 0)),
            pl.BlockSpec((d, tile), lambda i: (0, i)),
            pl.BlockSpec((tile, d), lambda i: (i, 0)),
        ],
        out_shape=[
            jax.ShapeDtypeStruct((n, d), BF16),
            jax.ShapeDtypeStruct((n, d), BF16),
            jax.ShapeDtypeStruct((d, ff), BF16),
            jax.ShapeDtypeStruct((ff, d), BF16),
        ],
        scratch_shapes=[pltpu.VMEM((n, d), F32), pltpu.VMEM((n, d), F32)],
        compiler_params=pltpu.CompilerParams(vmem_limit_bytes=60 * 1024 * 1024),
        cost_estimate=pl.CostEstimate(
            flops=12 * n * d * ff, transcendentals=n * ff, bytes_accessed=8 * n * d + 8 * d * ff
        ),
    )(x, dprod, win, wout)


MESH = pl.DeviceIdType.MESH
ANYWHERE = pl.BlockSpec(memory_space=pltpu.VMEM)


def grid_sizes(n_dp):
    ny = 1
    while 2 * ny * 2 * ny <= n_dp // 2:
        ny *= 2
    return n_dp // (2 * ny), ny


def position(ny):
    dp = lax.axis_index("dp")
    return dp, lax.axis_index("tensor"), dp % 2, (dp // 2) % ny, dp // (2 * ny)


def neighbours(ny, nz, n_t):
    dp, t, c, y, z = position(ny)

    def along_core(k):
        return (dp - c + (c + k) % 2, t)

    def along_tensor(k):
        return (dp, (t + k) % n_t)

    def along_y(k):
        return (dp + ((y + k) % ny - y) * 2, t)

    def along_z(k):
        return (dp + ((z + k) % nz - z) * 2 * ny, t)

    return {"core": (2, along_core), "tensor": (n_t, along_tensor), "y": (ny, along_y), "z": (nz, along_z)}


def greet(stages):
    barrier = pltpu.get_barrier_semaphore()
    count = 0
    for size, device in stages.values():
        for k in range(1, size):
            pl.semaphore_signal(barrier, inc=1, device_id=device(k), device_id_type=MESH)
            count += 1
    pl.semaphore_wait(barrier, count)


def gather_kernel(ny, nz, n_t, qkv, proj, small, qkv_out, proj_out, small_out, send, recv, copied):
    _, t, c, y, z = position(ny)
    stages = neighbours(ny, nz, n_t)
    greet(stages)
    cols = qkv.shape[1]

    def views(zs, ys, cs, ts):
        lanes = pl.ds(pl.multiple_of(ts * cols, 128), cols)
        return (
            qkv_out.at[zs, ys, cs, :, lanes],
            proj_out.at[zs, ys, cs, ts],
            small_out.at[zs, ys, cs, ts],
        )

    whole = slice(None)
    mine = views(z, y, c, t)
    local = [
        pltpu.make_async_copy(src, dst, copied.at[i])
        for i, (src, dst) in enumerate(zip((qkv, proj, small), mine))
    ]
    for copy in local:
        copy.start()
    slot = 0
    for name in ("z", "y", "tensor", "core"):
        size, device = stages[name]
        if name == "z":
            sources, targets = (qkv, proj, small), mine
        elif name == "y":
            sources = targets = views(whole, y, c, t)
        elif name == "tensor":
            sources = targets = views(whole, whole, c, t)
        else:
            sources = targets = (
                qkv_out.at[:, :, c],
                proj_out.at[:, :, c],
                small_out.at[:, :, c],
            )
        copies = []
        for k in range(1, size):
            for src, dst in zip(sources, targets):
                copies.append(
                    pltpu.make_async_remote_copy(
                        src_ref=src,
                        dst_ref=dst,
                        send_sem=send.at[slot],
                        recv_sem=recv.at[slot],
                        device_id=device(k),
                        device_id_type=MESH,
                    )
                )
                slot += 1
        for copy in copies:
            copy.start()
        if name == "z":
            for copy in local:
                copy.wait()
        for copy in copies:
            copy.wait()


def gather_weights(qkv, proj, small, n_dp, n_t):
    nz, ny = grid_sizes(n_dp)
    slots = 3 * (1 + (n_t - 1) + (ny - 1) + (nz - 1))
    outs = pl.pallas_call(
        functools.partial(gather_kernel, ny, nz, n_t),
        out_shape=[
            jax.ShapeDtypeStruct((nz, ny, 2, qkv.shape[0], n_t * qkv.shape[1]), BF16),
            jax.ShapeDtypeStruct((nz, ny, 2, n_t) + proj.shape, BF16),
            jax.ShapeDtypeStruct((nz, ny, 2, n_t) + small.shape, BF16),
        ],
        in_specs=[ANYWHERE] * 3,
        out_specs=[ANYWHERE] * 3,
        scratch_shapes=[
            pltpu.SemaphoreType.DMA((slots,)),
            pltpu.SemaphoreType.DMA((slots,)),
            pltpu.SemaphoreType.DMA((3,)),
        ],
        compiler_params=pltpu.CompilerParams(collective_id=0, has_side_effects=True),
    )(qkv, proj, small)
    qkv_all = outs[0].reshape(n_dp * qkv.shape[0], n_t * qkv.shape[1])
    return qkv_all, outs[1].reshape((n_dp, n_t) + proj.shape), outs[2].reshape(-1, small.shape[1])


def scatter_kernel(ny, nz, n_t, *refs):
    ins, refs = refs[:3], refs[3:]
    outs, refs = refs[:3], refs[3:]
    got = [refs[3 * i : 3 * i + 3] for i in range(4)]
    held = [refs[12 + 3 * i : 15 + 3 * i] for i in range(3)]
    send, recv = refs[21], refs[22]
    _, t, c, y, z = position(ny)
    stages = neighbours(ny, nz, n_t)
    greet(stages)
    cols = outs[0].shape[1]
    slot = 0

    def lanes(ts):
        return pl.ds(pl.multiple_of(ts * cols, 128), cols)

    def exchange(name, me, piece):
        nonlocal slot
        size, device = stages[name]
        level = ("core", "tensor", "y", "z").index(name)
        copies = []
        for k in range(1, size):
            for i, src in enumerate(piece((me + k) % size)):
                copies.append(
                    pltpu.make_async_remote_copy(
                        src_ref=src,
                        dst_ref=got[level][i].at[k - 1],
                        send_sem=send.at[slot],
                        recv_sem=recv.at[slot],
                        device_id=device(k),
                        device_id_type=MESH,
                    )
                )
                slot += 1
        for copy in copies:
            copy.start()
        for copy in copies:
            copy.wait()

    def total(own, level, index, i):
        value = own.astype(F32)
        for k in range(got[level][i].shape[0]):
            value = value + got[level][i][(k,) + index].astype(F32)
        return value

    def over_zy(body):
        def step(n, carry):
            body(n // ny, n % ny)
            return carry

        lax.fori_loop(0, nz * ny, step, 0)

    exchange("core", c, lambda j: [ref.at[:, :, j] for ref in ins])

    def add_core(zi, yi):
        for i in range(3):
            held[0][i][zi, yi] = total(ins[i][zi, yi, c], 0, (zi, yi), i).astype(held[0][i].dtype)

    over_zy(add_core)
    exchange(
        "tensor",
        t,
        lambda j: [held[0][0].at[:, :, :, lanes(j)], held[0][1].at[:, :, j], held[0][2].at[:, :, j]],
    )

    def add_tensor(zi, yi):
        owns = (held[0][0][zi, yi, :, lanes(t)], held[0][1][zi, yi, t], held[0][2][zi, yi, t])
        for i in range(3):
            held[1][i][zi, yi] = total(owns[i], 1, (zi, yi), i).astype(held[1][i].dtype)

    over_zy(add_tensor)
    exchange("y", y, lambda j: [ref.at[:, j] for ref in held[1]])

    def add_y(zi, carry):
        for i in range(3):
            held[2][i][zi] = total(held[1][i][zi, y], 2, (zi,), i).astype(held[2][i].dtype)
        return carry

    lax.fori_loop(0, nz, add_y, 0)
    exchange("z", z, lambda j: [ref.at[j] for ref in held[2]])
    for i in range(3):
        outs[i][...] = total(held[2][i][z], 3, (), i)


def scatter_grads(qkv, proj, small, n_dp, n_t):
    nz, ny = qkv.shape[:2]
    rows, cols = qkv.shape[3], qkv.shape[4] // n_t
    tails = [(rows, cols), proj.shape[4:], small.shape[4:]]
    kinds = [BF16, BF16, F32]
    wide = [(rows, n_t * cols), (n_t,) + proj.shape[4:], (n_t,) + small.shape[4:]]
    scratch = [pltpu.VMEM((1, nz, ny) + wide[i], kinds[i]) for i in range(3)]
    scratch += [pltpu.VMEM((n_t - 1, nz, ny) + tails[i], kinds[i]) for i in range(3)]
    scratch += [pltpu.VMEM((ny - 1, nz) + tails[i], kinds[i]) for i in range(3)]
    scratch += [pltpu.VMEM((nz - 1,) + tails[i], kinds[i]) for i in range(3)]
    scratch += [pltpu.VMEM((nz, ny) + wide[i], kinds[i]) for i in range(3)]
    scratch += [pltpu.VMEM((nz, ny) + tails[i], kinds[i]) for i in range(3)]
    scratch += [pltpu.VMEM((nz,) + tails[i], kinds[i]) for i in range(3)]
    slots = 3 * (1 + (n_t - 1) + (ny - 1) + (nz - 1))
    scratch += [pltpu.SemaphoreType.DMA((slots,)), pltpu.SemaphoreType.DMA((slots,))]
    return pl.pallas_call(
        functools.partial(scatter_kernel, ny, nz, n_t),
        out_shape=[jax.ShapeDtypeStruct(tail, F32) for tail in tails],
        in_specs=[ANYWHERE] * 3,
        out_specs=[ANYWHERE] * 3,
        scratch_shapes=scratch,
        compiler_params=pltpu.CompilerParams(collective_id=1, has_side_effects=True),
    )(qkv, proj, small)


def moe_kernel(
    experts,
    c_own,
    cot_all,
    router,
    flat_row,
    flat_col,
    expert_col,
    code_row,
    code_col,
    win,
    wout,
    mix,
    dx,
    dgate,
    gin_out,
    gout_out,
    c_all,
    gates,
    sent,
    got,
    back,
    ret,
    pay,
    paid,
    y_acc,
    dx_acc,
    gin,
    gout,
    gin_half,
    gout_half,
    gin_got,
    gout_got,
    c_sems,
    go_send,
    go_recv,
    back_send,
    back_recv,
    pay_sems,
    grad_sems,
):
    batches, rows, d = c_own.shape
    n_dp = lax.axis_size("dp")
    dp, t = lax.axis_index("dp"), lax.axis_index("tensor")
    share = sent.shape[1] // n_dp
    hidden = win.shape[1]
    half = hidden // 2
    other = 1 - t
    partner = (dp, other)

    barrier = pltpu.get_barrier_semaphore()
    pl.semaphore_signal(barrier, inc=1, device_id=partner, device_id_type=MESH)

    def hello(k, carry):
        pl.semaphore_signal(barrier, inc=1, device_id=((dp + k) % n_dp, t), device_id_type=MESH)
        return carry

    lax.fori_loop(1, n_dp, hello, 0)
    pl.semaphore_wait(barrier, n_dp)

    def image(i):
        return pl.ds(pl.multiple_of(i * rows, 16), rows)

    def part(i):
        return pl.ds(pl.multiple_of(i * share, 16), share)

    def remote(src, dst, sems, i, j, device):
        return pltpu.make_async_remote_copy(
            src_ref=src,
            dst_ref=dst,
            send_sem=sems[0].at[i, j],
            recv_sem=sems[1].at[i, j],
            device_id=device,
            device_id_type=MESH,
        )

    def c_copy(m):
        return pltpu.make_async_remote_copy(
            src_ref=c_own.at[m],
            dst_ref=c_all.at[m, image(t)],
            send_sem=c_sems.at[0, m],
            recv_sem=c_sems.at[1, m],
            device_id=partner,
            device_id_type=MESH,
        )

    def go_copy(m, k):
        to = (dp + k) % n_dp
        return remote(sent.at[m, part(to)], got.at[m, part(dp)], (go_send, go_recv), m, k - 1, (to, t))

    def back_copy(m, k):
        to = (dp + k) % n_dp
        return remote(back.at[m, part(to)], ret.at[m, part(dp)], (back_send, back_recv), m, k - 1, (to, t))

    def pay_copy(m):
        return pltpu.make_async_remote_copy(
            src_ref=pay.at[m],
            dst_ref=paid.at[m],
            send_sem=pay_sems.at[0, m],
            recv_sem=pay_sems.at[1, m],
            device_id=partner,
            device_id_type=MESH,
        )

    def grad_copy(i):
        return pltpu.make_async_remote_copy(
            src_ref=(gin_half, gout_half)[i],
            dst_ref=(gin_got, gout_got)[i],
            send_sem=grad_sems.at[0, i],
            recv_sem=grad_sems.at[1, i],
            device_id=partner,
            device_id_type=MESH,
        )

    def every(body):
        def step(k, carry):
            body(k)
            return carry

        lax.fori_loop(1, n_dp, step, 0)

    for m in range(batches):
        c_copy(m).start()
        c_all[m, image(t)] = c_own[m]

    lane = lax.broadcasted_iota(jnp.int32, (2 * rows, router.shape[1]), 1)

    def dispatch(m, carry):
        c_copy(m).wait_recv()
        c = c_all[m]
        logits = jnp.where(lane < experts, dot(c, router[...], ((1,), (0,))), -1e30)
        raised = jnp.exp(logits - jnp.max(logits, axis=-1, keepdims=True))
        probs = raised / jnp.sum(raised, axis=-1, keepdims=True)
        cot = cot_all[m].astype(F32)
        scaled = []
        for k in range(2):
            gate = jnp.sum(jnp.where(lane == expert_col[m, :, k : k + 1], probs, 0.0), axis=-1, keepdims=True)
            gates[m, :, k : k + 1] = gate
            scaled.append((gate * cot).astype(BF16))
        codes = code_col[...]
        picks = [(flat_row[m, k : k + 1, :] == codes).astype(F32).astype(BF16) for k in range(2)]
        sent[m, :, :d] = dot(picks[0] + picks[1], c, ((1,), (0,))).astype(BF16)
        moved = dot(picks[0], scaled[0], ((1,), (0,))) + dot(picks[1], scaled[1], ((1,), (0,)))
        sent[m, :, d:] = moved.astype(BF16)
        every(lambda k: go_copy(m, k).start())
        got[m, part(dp)] = sent[m, part(dp)]
        return carry

    lax.fori_loop(0, batches, dispatch, 0)

    tile = 256

    def clear(i, carry):
        cols = pl.ds(pl.multiple_of(i * tile, tile), tile)
        gin[:, cols] = jnp.zeros((d, tile), F32)
        gout[cols, :] = jnp.zeros((tile, d), F32)
        return carry

    lax.fori_loop(0, hidden // tile, clear, 0)

    def expert_step(m, carry):
        every(lambda k: go_copy(m, k).wait_recv())
        y_acc[...] = jnp.zeros_like(y_acc)
        dx_acc[...] = jnp.zeros_like(dx_acc)

        def chunk(i, inner):
            cols = pl.ds(pl.multiple_of(i * tile, tile), tile)
            x = got[m, :, :d]
            dprod = got[m, :, d:]
            w1 = win[:, cols]
            w2 = wout[cols, :]
            pre = dot(x, w1, ((1,), (0,)))
            square = pre * pre
            th = jnp.tanh(GELU_A * pre * (1.0 + GELU_B * square))
            active = (0.5 * pre * (1.0 + th)).astype(BF16)
            slope = 0.5 * (1.0 + th) + 0.5 * pre * (1.0 - th * th) * (GELU_A * (1.0 + 3.0 * GELU_B * square))
            dpre = (dot(dprod, w2, ((1,), (1,))) * slope).astype(BF16)
            gin[:, cols] += dot(x, dpre, ((0,), (0,)))
            gout[cols, :] += dot(active, dprod, ((0,), (0,)))
            y_acc[...] += dot(active, w2, ((1,), (0,)))
            dx_acc[...] += dot(dpre, w1, ((1,), (1,)))
            return inner

        lax.fori_loop(0, hidden // tile, chunk, 0)
        back[m, :, :d] = y_acc[...].astype(BF16)
        back[m, :, d:] = dx_acc[...].astype(BF16)
        every(lambda k: back_copy(m, k).start())
        ret[m, part(dp)] = back[m, part(dp)]
        return carry

    lax.fori_loop(0, batches, expert_step, 0)

    gin_half[...] = gin[:, pl.ds(pl.multiple_of(other * half, 128), half)].astype(BF16)
    gout_half[...] = gout[pl.ds(pl.multiple_of(other * half, 128), half), :].astype(BF16)
    grad_copy(0).start()
    grad_copy(1).start()

    def combine(m, carry):
        every(lambda k: back_copy(m, k).wait_recv())
        codes = code_row[...]
        for i in (other, t):
            picks = [(flat_col[m, image(i), k : k + 1] == codes).astype(F32).astype(BF16) for k in range(2)]
            one = dot(picks[0], ret[m, :, :d], ((1,), (0,)))
            two = dot(picks[1], ret[m, :, :d], ((1,), (0,)))
            d_rows = dot(picks[0] + picks[1], ret[m, :, d:], ((1,), (0,)))
            cot = cot_all[m, image(i)].astype(F32)
            gate = gates[m, image(i)]
            mixture = gate[:, 0:1] * one + gate[:, 1:2] * two
            col = lax.broadcasted_iota(jnp.int32, (rows, 128), 1)
            dg = jnp.where(col == 0, jnp.sum(one * cot, axis=-1, keepdims=True), 0.0)
            dg = dg + jnp.where(col == 1, jnp.sum(two * cot, axis=-1, keepdims=True), 0.0)
            if i is other:
                pay[m, :, :d] = mixture.astype(BF16)
                pay[m, :, d : 2 * d] = d_rows.astype(BF16)
                pay[m, :, 2 * d :] = dg.astype(BF16)
                pay_copy(m).start()
            else:
                mix[m] = mixture
                dx[m] = d_rows
                dgate[m] = dg
        return carry

    lax.fori_loop(0, batches, combine, 0)

    def settle(m, carry):
        pay_copy(m).wait_recv()
        mix[m] += paid[m, :, :d].astype(F32)
        dx[m] += paid[m, :, d : 2 * d].astype(F32)
        dgate[m] += paid[m, :, 2 * d :].astype(F32)
        return carry

    lax.fori_loop(0, batches, settle, 0)
    grad_copy(0).wait()
    grad_copy(1).wait()
    gin_out[...] = gin[:, pl.ds(pl.multiple_of(t * half, 128), half)] + gin_got[...].astype(F32)
    gout_out[...] = gout[pl.ds(pl.multiple_of(t * half, 128), half), :] + gout_got[...].astype(F32)

    def drain(m, carry):
        c_copy(m).wait_send()
        pay_copy(m).wait_send()
        every(lambda k: go_copy(m, k).wait_send())
        every(lambda k: back_copy(m, k).wait_send())
        return carry

    lax.fori_loop(0, batches, drain, 0)


def moe(c_own, cot_all, router, flat, expert_of, codes, win, wout, experts, n_dp):
    batches, rows, d = c_own.shape
    slots = codes.shape[0]
    hidden = win.shape[1]
    half = hidden // 2
    dma = pltpu.SemaphoreType.DMA
    return pl.pallas_call(
        functools.partial(moe_kernel, experts),
        out_shape=[
            jax.ShapeDtypeStruct((batches, rows, d), F32),
            jax.ShapeDtypeStruct((batches, rows, d), F32),
            jax.ShapeDtypeStruct((batches, rows, 128), F32),
            jax.ShapeDtypeStruct((d, half), F32),
            jax.ShapeDtypeStruct((half, d), F32),
        ],
        in_specs=[ANYWHERE] * 10,
        out_specs=[ANYWHERE] * 5,
        scratch_shapes=[
            pltpu.VMEM((batches, 2 * rows, d), BF16),
            pltpu.VMEM((batches, 2 * rows, 128), F32),
            pltpu.VMEM((batches, slots, 2 * d), BF16),
            pltpu.VMEM((batches, slots, 2 * d), BF16),
            pltpu.VMEM((batches, slots, 2 * d), BF16),
            pltpu.VMEM((batches, slots, 2 * d), BF16),
            pltpu.VMEM((batches, rows, 2 * d + 128), BF16),
            pltpu.VMEM((batches, rows, 2 * d + 128), BF16),
            pltpu.VMEM((slots, d), F32),
            pltpu.VMEM((slots, d), F32),
            pltpu.VMEM((d, hidden), F32),
            pltpu.VMEM((hidden, d), F32),
            pltpu.VMEM((d, half), BF16),
            pltpu.VMEM((half, d), BF16),
            pltpu.VMEM((d, half), BF16),
            pltpu.VMEM((half, d), BF16),
            dma((2, batches)),
            dma((batches, n_dp - 1)),
            dma((batches, n_dp - 1)),
            dma((batches, n_dp - 1)),
            dma((batches, n_dp - 1)),
            dma((2, batches)),
            dma((2, 2)),
        ],
        compiler_params=pltpu.CompilerParams(
            collective_id=2, has_side_effects=True, vmem_limit_bytes=62 * 1024 * 1024
        ),
    )(
        c_own,
        cot_all,
        router,
        flat,
        flat.transpose(0, 2, 1),
        expert_of.transpose(0, 2, 1),
        codes[None, :],
        codes[:, None],
        win,
        wout,
    )


def local(
    tokens,
    w_qkv,
    w_proj,
    w_in,
    w_out,
    w_router,
    gain_attn,
    shift_attn,
    gain_moe,
    shift_moe,
    live_rows,
    chosen,
    priority,
    cotangent,
):
    batches, own_rows, d = tokens.shape
    rows = live_rows.shape[1]
    n_dp = lax.axis_size("dp")
    n_t = lax.axis_size("tensor")
    t = lax.axis_index("tensor")
    heads_here = w_qkv.shape[1]
    heads = heads_here * n_t
    width = w_qkv.shape[2] // 3
    experts = w_in.shape[0] * n_dp
    cap = 2 * rows // experts
    share = cap // n_t
    images = rows // SEQ
    span = images * SEQ
    per = -(-images // n_t)
    work = per * SEQ
    total = n_t * work
    factor = width ** (-0.5)
    highest = lax.Precision.HIGHEST

    small = jnp.concatenate(
        [w_router] + [v[:, None] for v in (gain_attn, shift_attn, gain_moe, shift_moe)], axis=1
    )
    small = jnp.pad(small, ((0, 0), (0, 128 - small.shape[1])))
    block = heads_here * width
    qkv_block = w_qkv.reshape(-1, heads_here, 3, width).transpose(0, 2, 1, 3).reshape(-1, 3 * block)
    fill = -3 * block % 128
    qkv_block = jnp.pad(qkv_block, ((0, 0), (0, fill)))
    qkv, proj, small = gather_weights(qkv_block, w_proj.reshape(-1, d), small, n_dp, n_t)
    qkv = qkv.reshape(d, n_t, 3 * block + fill)[:, :, : 3 * block].reshape(d, -1)
    router = small[:, :experts]
    gain_one, shift_one, gain_two, shift_two = (small[:, experts + i].astype(F32) for i in range(4))
    proj = proj.reshape(n_dp, n_t, heads_here, w_proj.shape[1], d)
    proj = proj.transpose(1, 2, 0, 3, 4).reshape(heads * width, d)
    win = lax.all_gather(w_in[0], "tensor", axis=1, tiled=True)
    wout = lax.all_gather(w_out[0], "tensor", axis=0, tiled=True)
    cot_all = lax.all_gather(cotangent, "tensor", axis=1, tiled=True)

    def pad_rows(v, n):
        return jnp.pad(v, ((0, 0), (0, n - v.shape[1])) + ((0, 0),) * (v.ndim - 2))

    def own(v):
        return lax.dynamic_slice_in_dim(v, t * work, work, 1)

    edge = own_rows - work
    direct = n_t == 2 and per == 1 and edge >= 0
    if direct:
        moved = lax.ppermute(tokens[:, work:], "tensor", [(0, 1)])
        x = jnp.where(
            t == 0, tokens[:, :work], jnp.concatenate([moved, tokens[:, : work - edge]], axis=1)
        )
    else:
        x = own(pad_rows(lax.all_gather(tokens, "tensor", axis=1, tiled=True)[:, :span], total))
    x = x.astype(F32)
    live = live_rows[:, :span]
    live_all = pad_rows(live, total)
    live_own = own(live_all).astype(F32)[:, :, None]
    cot_all = pad_rows(cot_all[:, :span], total)
    dy = own(cot_all).astype(F32)

    rank = priority[:, 0, :span]
    first, second = chosen[:, :span, 0], chosen[:, :span, 1]
    labels = jnp.arange(experts, dtype=jnp.int32)
    earlier = (rank[:, None, :] < rank[:, :, None]).astype(BF16)
    hit_one = (first[:, :, None] == labels).astype(F32)
    hit_two = (second[:, :, None] == labels).astype(F32)
    live_one = hit_one * live[:, :, None].astype(F32)
    live_two = hit_two * live[:, :, None].astype(F32)
    counts = jnp.einsum(
        "mrs,mse->mre",
        earlier,
        jnp.concatenate([live_one, live_two], axis=-1).astype(BF16),
        preferred_element_type=F32,
    )
    first_total = jnp.sum(live_one, axis=1, keepdims=True)
    slot_one = jnp.sum(counts[:, :, :experts] * hit_one, axis=-1).astype(jnp.int32)
    slot_two = jnp.sum((counts[:, :, experts:] + first_total) * hit_two, axis=-1).astype(jnp.int32)
    keep_one = (live > 0) & (slot_one < cap)
    keep_two = (live > 0) & (slot_two < cap)
    flat_one = jnp.where(keep_one, first * cap + slot_one, -1)
    flat_two = jnp.where(keep_two, second * cap + slot_two, -1)

    def spread(v, fill):
        return jnp.pad(v, ((0, 0), (0, total - span)), constant_values=fill)

    flat_one, flat_two = spread(flat_one, -1), spread(flat_two, -1)
    keep_one, keep_two = spread(keep_one, False), spread(keep_two, False)
    first, second = spread(first, 0), spread(second, 0)
    codes = (jnp.arange(experts)[:, None] * cap + t * share + jnp.arange(share)[None, :]).reshape(-1)
    pick_one = flat_one[:, None, :] == codes[None, :, None]
    pick_two = flat_two[:, None, :] == codes[None, :, None]

    normed_one = layer_norm(x, gain_one, shift_one).astype(BF16)
    mixed = dot(normed_one, qkv, ((2,), (0,)))
    split = heads * width
    shape = (batches * per, SEQ, heads, width)
    mixed = mixed.reshape(batches, work, n_t, 3, block)
    query = (mixed[:, :, :, 0] * factor).astype(BF16).reshape(shape)
    keys = mixed[:, :, :, 1].astype(BF16).reshape(shape)
    values = mixed[:, :, :, 2].astype(BF16).reshape(shape)
    scores = jnp.einsum("iqhc,ikhc->ihqk", query, keys, preferred_element_type=F32)
    probs = jax.nn.softmax(scores, axis=-1)
    weights = probs.astype(BF16)
    context = jnp.einsum("ihqk,ikhc->iqhc", weights, values, preferred_element_type=F32)
    context = context.astype(BF16).reshape(batches, work, split)
    attn = dot(context, proj, ((2,), (0,)))
    hidden = x + live_own * attn
    normed_two = layer_norm(hidden, gain_two, shift_two).astype(BF16)

    padded = -(-SEQ // 16) * 16
    if direct:
        def lay(v, fill=0):
            v = v.reshape((batches, n_t, work) + v.shape[2:])
            v = jnp.pad(v, ((0, 0), (0, 0), (0, padded - work)) + ((0, 0),) * (v.ndim - 3), constant_values=fill)
            return v.reshape((batches, n_t * padded) + v.shape[3:])

        flat = jnp.stack([lay(flat_one, -1), lay(flat_two, -1)], axis=1)
        expert_of = jnp.stack(
            [lay(jnp.where(keep_one, first, -1), -1), lay(jnp.where(keep_two, second, -1), -1)], axis=1
        )
        mixture, d_rows, dgates, grad_in, grad_out = moe(
            jnp.pad(normed_two, ((0, 0), (0, padded - work), (0, 0))),
            lay(cot_all),
            jnp.pad(router, ((0, 0), (0, 128 - experts))),
            flat,
            expert_of,
            codes,
            win,
            wout,
            experts,
            n_dp,
        )
        output = (hidden + mixture[:, :work]).astype(BF16)
        d_rows = d_rows[:, :work]
        dgates = dgates[:, :work, :2]
        own_probs = jax.nn.softmax(dot(normed_two, router, ((2,), (0,))), axis=-1)
        hits_one = (first[:, :, None] == labels).astype(F32)
        hits_two = (second[:, :, None] == labels).astype(F32)
    else:
        c_all = lax.all_gather(normed_two, "tensor", axis=1, tiled=True)
        gate_probs = jax.nn.softmax(dot(c_all, router, ((2,), (0,))), axis=-1)
        hits_one = (first[:, :, None] == labels).astype(F32)
        hits_two = (second[:, :, None] == labels).astype(F32)
        gate_one = jnp.sum(gate_probs * hits_one, axis=-1) * keep_one
        gate_two = jnp.sum(gate_probs * hits_two, axis=-1) * keep_two
        picked = (pick_one | pick_two).astype(BF16)
        sent = jnp.einsum(
            "mqr,mrd->mqd",
            picked,
            jnp.concatenate([c_all, cot_all], axis=-1),
            preferred_element_type=F32,
        )
        gate_slot = jnp.sum(
            jnp.where(pick_one, gate_one[:, None, :], 0.0) + jnp.where(pick_two, gate_two[:, None, :], 0.0),
            axis=-1,
            keepdims=True,
        )
        sent = jnp.concatenate(
            [sent[..., :d].astype(BF16), (sent[..., d:] * gate_slot).astype(BF16)], axis=-1
        )
        sent = sent.reshape(batches, experts, share, 2 * d)
        got = lax.all_to_all(sent, "dp", 1, 1, tiled=True).reshape(-1, 2 * d)
        produced, d_in, grad_in, grad_out = expert(got[:, :d], got[:, d:], win, wout)
        back = jnp.concatenate([produced, d_in], axis=-1).reshape(batches, n_dp, share, 2 * d)
        back = lax.all_to_all(back, "dp", 1, 1, tiled=True).reshape(batches, experts * share, 2 * d)
        grad_in = lax.psum_scatter(grad_in, "tensor", scatter_dimension=1, tiled=True).astype(F32)
        grad_out = lax.psum_scatter(grad_out, "tensor", scatter_dimension=0, tiled=True).astype(F32)

        part_one = jnp.einsum("mqr,mqd->mrd", pick_one.astype(BF16), back[..., :d], preferred_element_type=F32)
        part_two = jnp.einsum("mqr,mqd->mrd", pick_two.astype(BF16), back[..., :d], preferred_element_type=F32)
        d_rows = jnp.einsum("mqr,mqd->mrd", picked, back[..., d:], preferred_element_type=F32)
        mixture = gate_one[:, :, None] * part_one + gate_two[:, :, None] * part_two
        cot_wide = cot_all.astype(F32)
        dgate_one = jnp.sum(part_one * cot_wide, axis=-1, keepdims=True)
        dgate_two = jnp.sum(part_two * cot_wide, axis=-1, keepdims=True)
        dgates = jnp.concatenate([dgate_one, dgate_two], axis=-1)
        payload = jnp.concatenate(
            [mixture, d_rows, jnp.pad(dgates, ((0, 0), (0, 0), (0, 126)))], axis=-1
        ).astype(BF16)
        pieces = payload.reshape(batches, n_t, work, payload.shape[-1])

        def piece(k):
            return lax.dynamic_index_in_dim(pieces, (t + k) % n_t, 1, keepdims=False)

        payload = piece(0).astype(F32)
        for k in range(1, n_t):
            payload = payload + lax.ppermute(
                piece(k), "tensor", [(j, (j + k) % n_t) for j in range(n_t)]
            ).astype(F32)
        output = (hidden + payload[..., :d]).astype(BF16)
        dgates = payload[..., 2 * d : 2 * d + 2]
        d_rows = payload[..., d : 2 * d]
        own_probs = own(gate_probs)

    dprobs = own(hits_one) * dgates[..., 0:1] * own(keep_one)[:, :, None]
    dprobs = dprobs + own(hits_two) * dgates[..., 1:2] * own(keep_two)[:, :, None]
    dlogits = own_probs * (dprobs - jnp.sum(dprobs * own_probs, axis=-1, keepdims=True))
    grad_router = lax.dot_general(
        normed_two.astype(F32), dlogits, (((0, 1), (0, 1)), ((), ())), precision=highest
    )
    dc = d_rows + lax.dot_general(
        dlogits, router.astype(F32), (((2,), (1,)), ((), ())), precision=highest
    )
    _, back_two = jax.vjp(layer_norm, hidden, gain_two, shift_two)
    dnorm, grad_gain_two, grad_shift_two = back_two(dc)
    dhidden = dy + dnorm
    dattn = (live_own * dhidden).astype(BF16)

    grad_proj = dot(context, dattn, ((0, 1), (0, 1)))
    dcontext = dot(dattn, proj, ((2,), (1,))).astype(BF16).reshape(shape)
    dvalues = jnp.einsum("ihqk,iqhc->ikhc", weights, dcontext, preferred_element_type=F32).astype(BF16)
    dweights = jnp.einsum("iqhc,ikhc->ihqk", dcontext, values, preferred_element_type=F32)
    dscores = (probs * (dweights - jnp.sum(dweights * probs, axis=-1, keepdims=True))).astype(BF16)
    dquery = jnp.einsum("ihqk,ikhc->iqhc", dscores, keys, preferred_element_type=F32).astype(BF16)
    dkeys = jnp.einsum("ihqk,iqhc->ikhc", dscores, query, preferred_element_type=F32).astype(BF16)
    dmixed = jnp.stack(
        [v.reshape(batches, work, n_t, block) for v in (dquery * BF16(factor), dkeys, dvalues)], axis=3
    ).reshape(batches, work, 3 * split)
    grad_qkv = dot(normed_one, dmixed, ((0, 1), (0, 1)))
    da = dot(dmixed, qkv, ((2,), (1,)))
    _, back_one = jax.vjp(layer_norm, x, gain_one, shift_one)
    dnorm, grad_gain_one, grad_shift_one = back_one(da)
    grad_x = dhidden + dnorm

    if direct:
        out_edge = lax.ppermute(output[:, :edge], "tensor", [(1, 0)])
        grad_edge = lax.ppermute(grad_x[:, :edge], "tensor", [(1, 0)])
        result = jnp.where(
            t == 0,
            jnp.concatenate([output, out_edge], axis=1),
            jnp.concatenate([output[:, edge:], tokens[:, work - edge :]], axis=1),
        )
        grad_tokens = jnp.where(
            t == 0,
            jnp.concatenate([grad_x, grad_edge], axis=1),
            jnp.concatenate([grad_x[:, edge:], cotangent[:, work - edge :].astype(F32)], axis=1),
        )
    else:
        here = (t * own_rows + jnp.arange(own_rows) < span)[None, :, None]

        def home(v, rest):
            full = pad_rows(lax.all_gather(v, "tensor", axis=1, tiled=True)[:, :span], rows)
            return jnp.where(here, lax.dynamic_slice_in_dim(full, t * own_rows, own_rows, 1), rest)

        result = home(output, tokens)
        grad_tokens = home(grad_x, cotangent.astype(F32))

    nz, ny = grid_sizes(n_dp)
    grad_qkv = jnp.pad(grad_qkv.astype(BF16).reshape(d, n_t, 3 * block), ((0, 0), (0, 0), (0, fill)))
    grad_qkv = grad_qkv.reshape(nz, ny, 2, d // n_dp, -1)
    grad_proj = grad_proj.astype(BF16).reshape(n_t, heads_here, n_dp, -1, d)
    grad_proj = grad_proj.transpose(2, 0, 1, 3, 4).reshape(nz, ny, 2, n_t, -1, d)
    smalls = jnp.concatenate(
        [grad_router] + [v[:, None] for v in (grad_gain_one, grad_shift_one, grad_gain_two, grad_shift_two)],
        axis=1,
    )
    smalls = jnp.pad(smalls, ((0, 0), (0, 128 - smalls.shape[1]))).reshape(nz, ny, 2, n_t, -1, 128)
    grad_qkv, grad_proj, smalls = scatter_grads(grad_qkv, grad_proj, smalls, n_dp, n_t)
    grad_qkv = grad_qkv[:, : 3 * block].reshape(-1, 3, heads_here, width).transpose(0, 2, 1, 3)
    return (
        result,
        grad_tokens,
        grad_qkv.reshape(w_qkv.shape),
        grad_proj.reshape(w_proj.shape),
        grad_in[None],
        grad_out[None],
        smalls[:, :experts],
        smalls[:, experts],
        smalls[:, experts + 1],
        smalls[:, experts + 2],
        smalls[:, experts + 3],
    )


def solution(mesh):
    both = ("dp", "tensor")
    return jax.shard_map(
        local,
        mesh=mesh,
        in_specs=(
            P(None, both, None),
            P("dp", "tensor", None),
            P("tensor", "dp", None),
            P("dp", None, "tensor"),
            P("dp", "tensor", None),
            P(both, None),
            P(both),
            P(both),
            P(both),
            P(both),
            P(None, "dp"),
            P(None, "dp", None),
            P(None, "dp", None),
            P(None, both, None),
        ),
        out_specs=(
            P(None, both, None),
            P(None, both, None),
            P("dp", "tensor", None),
            P("tensor", "dp", None),
            P("dp", None, "tensor"),
            P("dp", "tensor", None),
            P(both, None),
            P(both),
            P(both),
            P(both),
            P(both),
        ),
        check_vma=False,
    )
```

```python
import functools

import jax
import jax.numpy as jnp
from jax import lax
from jax.experimental import pallas as pl
from jax.experimental.pallas import tpu as pltpu
from jax.sharding import PartitionSpec as P

SEQ = 197
EPS = 1e-06
F32 = jnp.float32
BF16 = jnp.bfloat16
GELU_A = 0.7978845608028654
GELU_B = 0.044715


def dot(a, b, dims):
    return lax.dot_general(a, b, (dims, ((), ())), preferred_element_type=F32)


def layer_norm(values, gain_vec, shift_vec):
    centre = jnp.mean(values, axis=-1, keepdims=True)
    centered = values - centre
    spread = jnp.mean(centered * centered, axis=-1, keepdims=True)
    return centered * lax.rsqrt(spread + EPS) * gain_vec + shift_vec


def expert_kernel(x_ref, dp_ref, win_ref, wout_ref, y_ref, dx_ref, gin_ref, gout_ref, y_acc, dx_acc):
    step = pl.program_id(0)
    last = pl.num_programs(0) - 1
    x = x_ref[...]
    dprod = dp_ref[...]
    win = win_ref[...]
    wout = wout_ref[...]
    pre = dot(x, win, ((1,), (0,)))
    square = pre * pre
    th = jnp.tanh(GELU_A * pre * (1.0 + GELU_B * square))
    active = (0.5 * pre * (1.0 + th)).astype(BF16)
    slope = 0.5 * (1.0 + th) + 0.5 * pre * (1.0 - th * th) * (GELU_A * (1.0 + 3.0 * GELU_B * square))
    dact = dot(dprod, wout, ((1,), (1,)))
    dpre = (dact * slope).astype(BF16)
    gin_ref[...] = dot(x, dpre, ((0,), (0,))).astype(BF16)
    gout_ref[...] = dot(active, dprod, ((0,), (0,))).astype(BF16)
    part_y = dot(active, wout, ((1,), (0,)))
    part_dx = dot(dpre, win, ((1,), (1,)))

    @pl.when(step == 0)
    def _():
        y_acc[...] = part_y
        dx_acc[...] = part_dx

    @pl.when(step > 0)
    def _():
        y_acc[...] += part_y
        dx_acc[...] += part_dx

    @pl.when(step == last)
    def _():
        y_ref[...] = y_acc[...].astype(BF16)
        dx_ref[...] = dx_acc[...].astype(BF16)


def expert(x, dprod, win, wout, tile=256):
    n, d = x.shape
    ff = win.shape[1]
    return pl.pallas_call(
        expert_kernel,
        grid=(ff // tile,),
        in_specs=[
            pl.BlockSpec((n, d), lambda i: (0, 0)),
            pl.BlockSpec((n, d), lambda i: (0, 0)),
            pl.BlockSpec((d, tile), lambda i: (0, i)),
            pl.BlockSpec((tile, d), lambda i: (i, 0)),
        ],
        out_specs=[
            pl.BlockSpec((n, d), lambda i: (0, 0)),
            pl.BlockSpec((n, d), lambda i: (0, 0)),
            pl.BlockSpec((d, tile), lambda i: (0, i)),
            pl.BlockSpec((tile, d), lambda i: (i, 0)),
        ],
        out_shape=[
            jax.ShapeDtypeStruct((n, d), BF16),
            jax.ShapeDtypeStruct((n, d), BF16),
            jax.ShapeDtypeStruct((d, ff), BF16),
            jax.ShapeDtypeStruct((ff, d), BF16),
        ],
        scratch_shapes=[pltpu.VMEM((n, d), F32), pltpu.VMEM((n, d), F32)],
        compiler_params=pltpu.CompilerParams(vmem_limit_bytes=60 * 1024 * 1024),
        cost_estimate=pl.CostEstimate(
            flops=12 * n * d * ff, transcendentals=n * ff, bytes_accessed=8 * n * d + 8 * d * ff
        ),
    )(x, dprod, win, wout)


MESH = pl.DeviceIdType.MESH
ANYWHERE = pl.BlockSpec(memory_space=pltpu.VMEM)


def grid_sizes(n_dp):
    ny = 1
    while 2 * ny * 2 * ny <= n_dp // 2:
        ny *= 2
    return n_dp // (2 * ny), ny


def position(ny):
    dp = lax.axis_index("dp")
    return dp, lax.axis_index("tensor"), dp % 2, (dp // 2) % ny, dp // (2 * ny)


def neighbours(ny, nz, n_t):
    dp, t, c, y, z = position(ny)

    def along_core(k):
        return (dp - c + (c + k) % 2, t)

    def along_tensor(k):
        return (dp, (t + k) % n_t)

    def along_y(k):
        return (dp + ((y + k) % ny - y) * 2, t)

    def along_z(k):
        return (dp + ((z + k) % nz - z) * 2 * ny, t)

    return {"core": (2, along_core), "tensor": (n_t, along_tensor), "y": (ny, along_y), "z": (nz, along_z)}


def greet(stages):
    barrier = pltpu.get_barrier_semaphore()
    count = 0
    for size, device in stages.values():
        for k in range(1, size):
            pl.semaphore_signal(barrier, inc=1, device_id=device(k), device_id_type=MESH)
            count += 1
    pl.semaphore_wait(barrier, count)


def gather_kernel(ny, nz, n_t, extras, *refs):
    (qkv, proj, small), refs = refs[:3], refs[3:]
    side, refs = refs[:extras], refs[extras:]
    (qkv_out, proj_out, small_out), refs = refs[:3], refs[3:]
    side_out, (send, recv, copied) = refs[:extras], refs[extras:]
    dp, t, c, y, z = position(ny)
    stages = neighbours(ny, nz, n_t)
    greet(stages)
    aside = []
    for i in range(extras):
        aside.append(
            pltpu.make_async_remote_copy(
                src_ref=side[i],
                dst_ref=side_out[i].at[t] if i == 0 else side_out[i],
                send_sem=send.at[send.shape[0] - 1 - i],
                recv_sem=recv.at[recv.shape[0] - 1 - i],
                device_id=(dp, 1 - t),
                device_id_type=MESH,
            )
        )
    for copy in aside:
        copy.start()
    cols = qkv.shape[1]

    def views(zs, ys, cs, ts):
        lanes = pl.ds(pl.multiple_of(ts * cols, 128), cols)
        return (
            qkv_out.at[zs, ys, cs, :, lanes],
            proj_out.at[zs, ys, cs, ts],
            small_out.at[zs, ys, cs, ts],
        )

    whole = slice(None)
    mine = views(z, y, c, t)
    local = [
        pltpu.make_async_copy(src, dst, copied.at[i])
        for i, (src, dst) in enumerate(zip((qkv, proj, small), mine))
    ]
    if extras:
        local.append(pltpu.make_async_copy(side[0], side_out[0].at[t], copied.at[3]))
    for copy in local:
        copy.start()
    slot = 0
    for name in ("z", "y", "tensor", "core"):
        size, device = stages[name]
        if name == "z":
            sources, targets = (qkv, proj, small), mine
        elif name == "y":
            sources = targets = views(whole, y, c, t)
        elif name == "tensor":
            sources = targets = views(whole, whole, c, t)
        else:
            sources = targets = (
                qkv_out.at[:, :, c],
                proj_out.at[:, :, c],
                small_out.at[:, :, c],
            )
        copies = []
        for k in range(1, size):
            for src, dst in zip(sources, targets):
                copies.append(
                    pltpu.make_async_remote_copy(
                        src_ref=src,
                        dst_ref=dst,
                        send_sem=send.at[slot],
                        recv_sem=recv.at[slot],
                        device_id=device(k),
                        device_id_type=MESH,
                    )
                )
                slot += 1
        for copy in copies:
            copy.start()
        if name == "z":
            for copy in local:
                copy.wait()
        for copy in copies:
            copy.wait()
    for copy in aside:
        copy.wait()


def gather_weights(qkv, proj, small, n_dp, n_t, side=()):
    nz, ny = grid_sizes(n_dp)
    slots = 3 * (1 + (n_t - 1) + (ny - 1) + (nz - 1)) + len(side)
    side_shapes = [
        jax.ShapeDtypeStruct(((n_t,) if i == 0 else ()) + v.shape, v.dtype) for i, v in enumerate(side)
    ]
    outs = pl.pallas_call(
        functools.partial(gather_kernel, ny, nz, n_t, len(side)),
        out_shape=[
            jax.ShapeDtypeStruct((nz, ny, 2, qkv.shape[0], n_t * qkv.shape[1]), BF16),
            jax.ShapeDtypeStruct((nz, ny, 2, n_t) + proj.shape, BF16),
            jax.ShapeDtypeStruct((nz, ny, 2, n_t) + small.shape, BF16),
        ]
        + side_shapes,
        in_specs=[ANYWHERE] * (3 + len(side)),
        out_specs=[ANYWHERE] * (3 + len(side)),
        scratch_shapes=[
            pltpu.SemaphoreType.DMA((slots,)),
            pltpu.SemaphoreType.DMA((slots,)),
            pltpu.SemaphoreType.DMA((4,)),
        ],
        compiler_params=pltpu.CompilerParams(collective_id=0, has_side_effects=True),
    )(qkv, proj, small, *side)
    qkv_all = outs[0].reshape(n_dp * qkv.shape[0], n_t * qkv.shape[1])
    return (qkv_all, outs[1].reshape((n_dp, n_t) + proj.shape), outs[2].reshape(-1, small.shape[1])) + tuple(outs[3:])


def scatter_kernel(ny, nz, n_t, *refs):
    ins, refs = refs[:3], refs[3:]
    outs, refs = refs[:3], refs[3:]
    got = [refs[3 * i : 3 * i + 3] for i in range(4)]
    held = [refs[12 + 3 * i : 15 + 3 * i] for i in range(3)]
    send, recv = refs[21], refs[22]
    _, t, c, y, z = position(ny)
    stages = neighbours(ny, nz, n_t)
    greet(stages)
    cols = outs[0].shape[1]
    slot = 0

    def lanes(ts):
        return pl.ds(pl.multiple_of(ts * cols, 128), cols)

    def exchange(name, me, piece):
        nonlocal slot
        size, device = stages[name]
        level = ("core", "tensor", "y", "z").index(name)
        copies = []
        for k in range(1, size):
            for i, src in enumerate(piece((me + k) % size)):
                copies.append(
                    pltpu.make_async_remote_copy(
                        src_ref=src,
                        dst_ref=got[level][i].at[k - 1],
                        send_sem=send.at[slot],
                        recv_sem=recv.at[slot],
                        device_id=device(k),
                        device_id_type=MESH,
                    )
                )
                slot += 1
        for copy in copies:
            copy.start()
        for copy in copies:
            copy.wait()

    def total(own, level, index, i):
        value = own.astype(F32)
        for k in range(got[level][i].shape[0]):
            value = value + got[level][i][(k,) + index].astype(F32)
        return value

    def over_zy(body):
        def step(n, carry):
            body(n // ny, n % ny)
            return carry

        lax.fori_loop(0, nz * ny, step, 0)

    exchange("core", c, lambda j: [ref.at[:, :, j] for ref in ins])

    def add_core(zi, yi):
        for i in range(3):
            held[0][i][zi, yi] = total(ins[i][zi, yi, c], 0, (zi, yi), i).astype(held[0][i].dtype)

    over_zy(add_core)
    exchange(
        "tensor",
        t,
        lambda j: [held[0][0].at[:, :, :, lanes(j)], held[0][1].at[:, :, j], held[0][2].at[:, :, j]],
    )

    def add_tensor(zi, yi):
        owns = (held[0][0][zi, yi, :, lanes(t)], held[0][1][zi, yi, t], held[0][2][zi, yi, t])
        for i in range(3):
            held[1][i][zi, yi] = total(owns[i], 1, (zi, yi), i).astype(held[1][i].dtype)

    over_zy(add_tensor)
    exchange("y", y, lambda j: [ref.at[:, j] for ref in held[1]])

    def add_y(zi, carry):
        for i in range(3):
            held[2][i][zi] = total(held[1][i][zi, y], 2, (zi,), i).astype(held[2][i].dtype)
        return carry

    lax.fori_loop(0, nz, add_y, 0)
    exchange("z", z, lambda j: [ref.at[j] for ref in held[2]])
    for i in range(3):
        outs[i][...] = total(held[2][i][z], 3, (), i)


def scatter_grads(qkv, proj, small, n_dp, n_t):
    nz, ny = qkv.shape[:2]
    rows, cols = qkv.shape[3], qkv.shape[4] // n_t
    tails = [(rows, cols), proj.shape[4:], small.shape[4:]]
    kinds = [BF16, BF16, F32]
    wide = [(rows, n_t * cols), (n_t,) + proj.shape[4:], (n_t,) + small.shape[4:]]
    scratch = [pltpu.VMEM((1, nz, ny) + wide[i], kinds[i]) for i in range(3)]
    scratch += [pltpu.VMEM((n_t - 1, nz, ny) + tails[i], kinds[i]) for i in range(3)]
    scratch += [pltpu.VMEM((ny - 1, nz) + tails[i], kinds[i]) for i in range(3)]
    scratch += [pltpu.VMEM((nz - 1,) + tails[i], kinds[i]) for i in range(3)]
    scratch += [pltpu.VMEM((nz, ny) + wide[i], kinds[i]) for i in range(3)]
    scratch += [pltpu.VMEM((nz, ny) + tails[i], kinds[i]) for i in range(3)]
    scratch += [pltpu.VMEM((nz,) + tails[i], kinds[i]) for i in range(3)]
    slots = 3 * (1 + (n_t - 1) + (ny - 1) + (nz - 1))
    scratch += [pltpu.SemaphoreType.DMA((slots,)), pltpu.SemaphoreType.DMA((slots,))]
    return pl.pallas_call(
        functools.partial(scatter_kernel, ny, nz, n_t),
        out_shape=[jax.ShapeDtypeStruct(tail, F32) for tail in tails],
        in_specs=[ANYWHERE] * 3,
        out_specs=[ANYWHERE] * 3,
        scratch_shapes=scratch,
        compiler_params=pltpu.CompilerParams(collective_id=1, has_side_effects=True),
    )(qkv, proj, small)


def moe_kernel(
    experts,
    c_own,
    cot_all,
    router,
    flat_row,
    flat_col,
    expert_col,
    code_row,
    code_col,
    win,
    wout,
    mix,
    dx,
    dgate,
    gin_out,
    gout_out,
    c_all,
    gates,
    sent,
    got,
    back,
    ret,
    pay,
    paid,
    y_acc,
    dx_acc,
    win_got,
    wout_got,
    gin_mine,
    gout_mine,
    gin,
    gout,
    gin_half,
    gout_half,
    gin_got,
    gout_got,
    w_sems,
    c_sems,
    go_send,
    go_recv,
    back_send,
    back_recv,
    pay_sems,
    grad_sems,
):
    batches, rows, d = c_own.shape
    n_dp = lax.axis_size("dp")
    dp, t = lax.axis_index("dp"), lax.axis_index("tensor")
    share = sent.shape[1] // n_dp
    hidden = win.shape[1]
    other = 1 - t
    partner = (dp, other)

    barrier = pltpu.get_barrier_semaphore()
    pl.semaphore_signal(barrier, inc=1, device_id=partner, device_id_type=MESH)

    def hello(k, carry):
        pl.semaphore_signal(barrier, inc=1, device_id=((dp + k) % n_dp, t), device_id_type=MESH)
        return carry

    lax.fori_loop(1, n_dp, hello, 0)
    pl.semaphore_wait(barrier, n_dp)

    def image(i):
        return pl.ds(pl.multiple_of(i * rows, 16), rows)

    def part(i):
        return pl.ds(pl.multiple_of(i * share, 16), share)

    def remote(src, dst, sems, i, j, device):
        return pltpu.make_async_remote_copy(
            src_ref=src,
            dst_ref=dst,
            send_sem=sems[0].at[i, j],
            recv_sem=sems[1].at[i, j],
            device_id=device,
            device_id_type=MESH,
        )

    def c_copy(m):
        return pltpu.make_async_remote_copy(
            src_ref=c_own.at[m],
            dst_ref=c_all.at[m, image(t)],
            send_sem=c_sems.at[0, m],
            recv_sem=c_sems.at[1, m],
            device_id=partner,
            device_id_type=MESH,
        )

    def go_copy(m, k):
        to = (dp + k) % n_dp
        return remote(sent.at[m, part(to)], got.at[m, part(dp)], (go_send, go_recv), m, k - 1, (to, t))

    def back_copy(m, k):
        to = (dp + k) % n_dp
        return remote(back.at[m, part(to)], ret.at[m, part(dp)], (back_send, back_recv), m, k - 1, (to, t))

    def pay_copy(m):
        return pltpu.make_async_remote_copy(
            src_ref=pay.at[m],
            dst_ref=paid.at[m],
            send_sem=pay_sems.at[0, m],
            recv_sem=pay_sems.at[1, m],
            device_id=partner,
            device_id_type=MESH,
        )

    def grad_copy(i):
        src, dst = ((gin_half, gin_got), (gout_half, gout_got))[i // 2]
        size = src.shape[0] // 2
        band = pl.ds(i % 2 * size, size)
        return pltpu.make_async_remote_copy(
            src_ref=src.at[band],
            dst_ref=dst.at[band],
            send_sem=grad_sems.at[0, i],
            recv_sem=grad_sems.at[1, i],
            device_id=partner,
            device_id_type=MESH,
        )

    def w_copy(i):
        return pltpu.make_async_remote_copy(
            src_ref=(win, wout)[i],
            dst_ref=(win_got, wout_got)[i],
            send_sem=w_sems.at[0, i],
            recv_sem=w_sems.at[1, i],
            device_id=partner,
            device_id_type=MESH,
        )

    def every(body):
        def step(k, carry):
            body(k)
            return carry

        lax.fori_loop(1, n_dp, step, 0)

    for m in range(batches):
        c_copy(m).start()
        c_all[m, image(t)] = c_own[m]
    w_copy(0).start()
    w_copy(1).start()

    lane = lax.broadcasted_iota(jnp.int32, (2 * rows, router.shape[1]), 1)

    def dispatch(m, carry):
        c_copy(m).wait_recv()
        c = c_all[m]
        logits = jnp.where(lane < experts, dot(c, router[...], ((1,), (0,))), -1e30)
        raised = jnp.exp(logits - jnp.max(logits, axis=-1, keepdims=True))
        probs = raised / jnp.sum(raised, axis=-1, keepdims=True)
        cot = cot_all[m].astype(F32)
        scaled = []
        for k in range(2):
            gate = jnp.sum(jnp.where(lane == expert_col[m, :, k : k + 1], probs, 0.0), axis=-1, keepdims=True)
            gates[m, :, k : k + 1] = gate
            scaled.append((gate * cot).astype(BF16))
        codes = code_col[...]
        picks = [(flat_row[m, k : k + 1, :] == codes).astype(F32).astype(BF16) for k in range(2)]
        sent[m, :, :d] = dot(picks[0] + picks[1], c, ((1,), (0,))).astype(BF16)
        moved = dot(picks[0], scaled[0], ((1,), (0,))) + dot(picks[1], scaled[1], ((1,), (0,)))
        sent[m, :, d:] = moved.astype(BF16)
        every(lambda k: go_copy(m, k).start())
        got[m, part(dp)] = sent[m, part(dp)]
        return carry

    lax.fori_loop(0, batches, dispatch, 0)

    tile = 256

    def clear(i, carry):
        cols = pl.ds(pl.multiple_of(i * tile, tile), tile)
        for into in (gin, gin_mine):
            into[:, cols] = jnp.zeros((d, tile), F32)
        for into in (gout, gout_mine):
            into[cols, :] = jnp.zeros((tile, d), F32)
        return carry

    lax.fori_loop(0, hidden // tile, clear, 0)

    def expert_step(m, carry):
        every(lambda k: go_copy(m, k).wait_recv())
        y_acc[...] = jnp.zeros_like(y_acc)
        dx_acc[...] = jnp.zeros_like(dx_acc)

        def chunk(win, wout, gin, gout, i, inner):
            cols = pl.ds(pl.multiple_of(i * tile, tile), tile)
            x = got[m, :, :d]
            dprod = got[m, :, d:]
            w1 = win[:, cols]
            w2 = wout[cols, :]
            pre = dot(x, w1, ((1,), (0,)))
            square = pre * pre
            th = jnp.tanh(GELU_A * pre * (1.0 + GELU_B * square))
            active = (0.5 * pre * (1.0 + th)).astype(BF16)
            slope = 0.5 * (1.0 + th) + 0.5 * pre * (1.0 - th * th) * (GELU_A * (1.0 + 3.0 * GELU_B * square))
            dpre = (dot(dprod, w2, ((1,), (1,))) * slope).astype(BF16)
            gin[:, cols] += dot(x, dpre, ((0,), (0,)))
            gout[cols, :] += dot(active, dprod, ((0,), (0,)))
            y_acc[...] += dot(active, w2, ((1,), (0,)))
            dx_acc[...] += dot(dpre, w1, ((1,), (1,)))
            return inner

        lax.fori_loop(
            0, hidden // tile, functools.partial(chunk, win, wout, gin_mine, gout_mine), 0
        )

        @pl.when(m == 0)
        def _():
            w_copy(0).wait_recv()
            w_copy(1).wait_recv()

        lax.fori_loop(
            0, hidden // tile, functools.partial(chunk, win_got, wout_got, gin, gout), 0
        )
        back[m, :, :d] = y_acc[...].astype(BF16)
        back[m, :, d:] = dx_acc[...].astype(BF16)
        every(lambda k: back_copy(m, k).start())
        ret[m, part(dp)] = back[m, part(dp)]
        return carry

    lax.fori_loop(0, batches, expert_step, 0)

    gin_half[...] = gin[...].astype(BF16)
    gout_half[...] = gout[...].astype(BF16)

    def combine(m, carry):
        every(lambda k: back_copy(m, k).wait_recv())
        codes = code_row[...]
        for i in (other, t):
            picks = [(flat_col[m, image(i), k : k + 1] == codes).astype(F32).astype(BF16) for k in range(2)]
            one = dot(picks[0], ret[m, :, :d], ((1,), (0,)))
            two = dot(picks[1], ret[m, :, :d], ((1,), (0,)))
            d_rows = dot(picks[0] + picks[1], ret[m, :, d:], ((1,), (0,)))
            cot = cot_all[m, image(i)].astype(F32)
            gate = gates[m, image(i)]
            mixture = gate[:, 0:1] * one + gate[:, 1:2] * two
            col = lax.broadcasted_iota(jnp.int32, (rows, 128), 1)
            dg = jnp.where(col == 0, jnp.sum(one * cot, axis=-1, keepdims=True), 0.0)
            dg = dg + jnp.where(col == 1, jnp.sum(two * cot, axis=-1, keepdims=True), 0.0)
            if i is other:
                pay[m, :, :d] = mixture.astype(BF16)
                pay[m, :, d : 2 * d] = d_rows.astype(BF16)
                pay[m, :, 2 * d :] = dg.astype(BF16)
                pay_copy(m).start()
            else:
                mix[m] = mixture
                dx[m] = d_rows
                dgate[m] = dg
        return carry

    pieces = 4
    for m in range(batches):
        if m < pieces:
            grad_copy(m).start()
        combine(m, 0)
    for i in range(batches, pieces):
        grad_copy(i).start()

    def settle(m, carry):
        pay_copy(m).wait_recv()
        mix[m] += paid[m, :, :d].astype(F32)
        dx[m] += paid[m, :, d : 2 * d].astype(F32)
        dgate[m] += paid[m, :, 2 * d :].astype(F32)
        return carry

    lax.fori_loop(0, batches, settle, 0)
    for i in range(pieces):
        grad_copy(i).wait()
    gin_out[...] = gin_mine[...] + gin_got[...].astype(F32)
    gout_out[...] = gout_mine[...] + gout_got[...].astype(F32)
    w_copy(0).wait_send()
    w_copy(1).wait_send()

    def drain(m, carry):
        c_copy(m).wait_send()
        pay_copy(m).wait_send()
        every(lambda k: go_copy(m, k).wait_send())
        every(lambda k: back_copy(m, k).wait_send())
        return carry

    lax.fori_loop(0, batches, drain, 0)


def moe(c_own, cot_all, router, flat, expert_of, codes, win, wout, experts, n_dp):
    batches, rows, d = c_own.shape
    slots = codes.shape[0]
    half = win.shape[1]
    dma = pltpu.SemaphoreType.DMA
    return pl.pallas_call(
        functools.partial(moe_kernel, experts),
        out_shape=[
            jax.ShapeDtypeStruct((batches, rows, d), F32),
            jax.ShapeDtypeStruct((batches, rows, d), F32),
            jax.ShapeDtypeStruct((batches, rows, 128), F32),
            jax.ShapeDtypeStruct((d, half), F32),
            jax.ShapeDtypeStruct((half, d), F32),
        ],
        in_specs=[ANYWHERE] * 10,
        out_specs=[ANYWHERE] * 5,
        scratch_shapes=[
            pltpu.VMEM((batches, 2 * rows, d), BF16),
            pltpu.VMEM((batches, 2 * rows, 128), F32),
            pltpu.VMEM((batches, slots, 2 * d), BF16),
            pltpu.VMEM((batches, slots, 2 * d), BF16),
            pltpu.VMEM((batches, slots, 2 * d), BF16),
            pltpu.VMEM((batches, slots, 2 * d), BF16),
            pltpu.VMEM((batches, rows, 2 * d + 128), BF16),
            pltpu.VMEM((batches, rows, 2 * d + 128), BF16),
            pltpu.VMEM((slots, d), F32),
            pltpu.VMEM((slots, d), F32),
            pltpu.VMEM((d, half), BF16),
            pltpu.VMEM((half, d), BF16),
            pltpu.VMEM((d, half), F32),
            pltpu.VMEM((half, d), F32),
            pltpu.VMEM((d, half), F32),
            pltpu.VMEM((half, d), F32),
            pltpu.VMEM((d, half), BF16),
            pltpu.VMEM((half, d), BF16),
            pltpu.VMEM((d, half), BF16),
            pltpu.VMEM((half, d), BF16),
            dma((2, 2)),
            dma((2, batches)),
            dma((batches, n_dp - 1)),
            dma((batches, n_dp - 1)),
            dma((batches, n_dp - 1)),
            dma((batches, n_dp - 1)),
            dma((2, batches)),
            dma((2, 4)),
        ],
        compiler_params=pltpu.CompilerParams(
            collective_id=2, has_side_effects=True, vmem_limit_bytes=62 * 1024 * 1024
        ),
    )(
        c_own,
        cot_all,
        router,
        flat,
        flat.transpose(0, 2, 1),
        expert_of.transpose(0, 2, 1),
        codes[None, :],
        codes[:, None],
        win,
        wout,
    )


def general(
    tokens,
    w_qkv,
    w_proj,
    w_in,
    w_out,
    w_router,
    gain_attn,
    shift_attn,
    gain_moe,
    shift_moe,
    live_rows,
    chosen,
    priority,
    cotangent,
):
    batches, own_rows, d = tokens.shape
    rows = live_rows.shape[1]
    n_dp = lax.axis_size("dp")
    n_t = lax.axis_size("tensor")
    t = lax.axis_index("tensor")
    heads_here = w_qkv.shape[1]
    heads = heads_here * n_t
    width = w_qkv.shape[2] // 3
    experts = w_in.shape[0] * n_dp
    cap = 2 * rows // experts
    share = cap // n_t
    images = rows // SEQ
    span = images * SEQ
    per = -(-images // n_t)
    work = per * SEQ
    total = n_t * work
    factor = width ** (-0.5)
    highest = lax.Precision.HIGHEST

    small = jnp.concatenate(
        [w_router] + [v[:, None] for v in (gain_attn, shift_attn, gain_moe, shift_moe)], axis=1
    )
    small = jnp.pad(small, ((0, 0), (0, 128 - small.shape[1])))
    block = heads_here * width
    qkv_block = w_qkv.reshape(-1, heads_here, 3, width).transpose(0, 2, 1, 3).reshape(-1, 3 * block)
    fill = -3 * block % 128
    qkv_block = jnp.pad(qkv_block, ((0, 0), (0, fill)))
    qkv, proj, small = gather_weights(qkv_block, w_proj.reshape(-1, d), small, n_dp, n_t)
    qkv = qkv.reshape(d, n_t, 3 * block + fill)[:, :, : 3 * block].reshape(d, -1)
    router = small[:, :experts]
    gain_one, shift_one, gain_two, shift_two = (small[:, experts + i].astype(F32) for i in range(4))
    proj = proj.reshape(n_dp, n_t, heads_here, w_proj.shape[1], d)
    proj = proj.transpose(1, 2, 0, 3, 4).reshape(heads * width, d)
    win = lax.all_gather(w_in[0], "tensor", axis=1, tiled=True)
    wout = lax.all_gather(w_out[0], "tensor", axis=0, tiled=True)
    cot_all = lax.all_gather(cotangent, "tensor", axis=1, tiled=True)

    def pad_rows(v, n):
        return jnp.pad(v, ((0, 0), (0, n - v.shape[1])) + ((0, 0),) * (v.ndim - 2))

    def own(v):
        return lax.dynamic_slice_in_dim(v, t * work, work, 1)

    edge = own_rows - work
    direct = n_t == 2 and per == 1 and edge >= 0
    if direct:
        moved = lax.ppermute(tokens[:, work:], "tensor", [(0, 1)])
        x = jnp.where(
            t == 0, tokens[:, :work], jnp.concatenate([moved, tokens[:, : work - edge]], axis=1)
        )
    else:
        x = own(pad_rows(lax.all_gather(tokens, "tensor", axis=1, tiled=True)[:, :span], total))
    x = x.astype(F32)
    live = live_rows[:, :span]
    live_all = pad_rows(live, total)
    live_own = own(live_all).astype(F32)[:, :, None]
    cot_all = pad_rows(cot_all[:, :span], total)
    dy = own(cot_all).astype(F32)

    rank = priority[:, 0, :span]
    first, second = chosen[:, :span, 0], chosen[:, :span, 1]
    labels = jnp.arange(experts, dtype=jnp.int32)
    earlier = (rank[:, None, :] < rank[:, :, None]).astype(BF16)
    hit_one = (first[:, :, None] == labels).astype(F32)
    hit_two = (second[:, :, None] == labels).astype(F32)
    live_one = hit_one * live[:, :, None].astype(F32)
    live_two = hit_two * live[:, :, None].astype(F32)
    counts = jnp.einsum(
        "mrs,mse->mre",
        earlier,
        jnp.concatenate([live_one, live_two], axis=-1).astype(BF16),
        preferred_element_type=F32,
    )
    first_total = jnp.sum(live_one, axis=1, keepdims=True)
    slot_one = jnp.sum(counts[:, :, :experts] * hit_one, axis=-1).astype(jnp.int32)
    slot_two = jnp.sum((counts[:, :, experts:] + first_total) * hit_two, axis=-1).astype(jnp.int32)
    keep_one = (live > 0) & (slot_one < cap)
    keep_two = (live > 0) & (slot_two < cap)
    flat_one = jnp.where(keep_one, first * cap + slot_one, -1)
    flat_two = jnp.where(keep_two, second * cap + slot_two, -1)

    def spread(v, fill):
        return jnp.pad(v, ((0, 0), (0, total - span)), constant_values=fill)

    flat_one, flat_two = spread(flat_one, -1), spread(flat_two, -1)
    keep_one, keep_two = spread(keep_one, False), spread(keep_two, False)
    first, second = spread(first, 0), spread(second, 0)
    codes = (jnp.arange(experts)[:, None] * cap + t * share + jnp.arange(share)[None, :]).reshape(-1)
    pick_one = flat_one[:, None, :] == codes[None, :, None]
    pick_two = flat_two[:, None, :] == codes[None, :, None]

    normed_one = layer_norm(x, gain_one, shift_one).astype(BF16)
    mixed = dot(normed_one, qkv, ((2,), (0,)))
    split = heads * width
    shape = (batches * per, SEQ, heads, width)
    mixed = mixed.reshape(batches, work, n_t, 3, block)
    query = (mixed[:, :, :, 0] * factor).astype(BF16).reshape(shape)
    keys = mixed[:, :, :, 1].astype(BF16).reshape(shape)
    values = mixed[:, :, :, 2].astype(BF16).reshape(shape)
    scores = jnp.einsum("iqhc,ikhc->ihqk", query, keys, preferred_element_type=F32)
    probs = jax.nn.softmax(scores, axis=-1)
    weights = probs.astype(BF16)
    context = jnp.einsum("ihqk,ikhc->iqhc", weights, values, preferred_element_type=F32)
    context = context.astype(BF16).reshape(batches, work, split)
    attn = dot(context, proj, ((2,), (0,)))
    hidden = x + live_own * attn
    normed_two = layer_norm(hidden, gain_two, shift_two).astype(BF16)

    c_all = lax.all_gather(normed_two, "tensor", axis=1, tiled=True)
    gate_probs = jax.nn.softmax(dot(c_all, router, ((2,), (0,))), axis=-1)
    hits_one = (first[:, :, None] == labels).astype(F32)
    hits_two = (second[:, :, None] == labels).astype(F32)
    gate_one = jnp.sum(gate_probs * hits_one, axis=-1) * keep_one
    gate_two = jnp.sum(gate_probs * hits_two, axis=-1) * keep_two
    picked = (pick_one | pick_two).astype(BF16)
    sent = jnp.einsum(
        "mqr,mrd->mqd",
        picked,
        jnp.concatenate([c_all, cot_all], axis=-1),
        preferred_element_type=F32,
    )
    gate_slot = jnp.sum(
        jnp.where(pick_one, gate_one[:, None, :], 0.0) + jnp.where(pick_two, gate_two[:, None, :], 0.0),
        axis=-1,
        keepdims=True,
    )
    sent = jnp.concatenate(
        [sent[..., :d].astype(BF16), (sent[..., d:] * gate_slot).astype(BF16)], axis=-1
    )
    sent = sent.reshape(batches, experts, share, 2 * d)
    got = lax.all_to_all(sent, "dp", 1, 1, tiled=True).reshape(-1, 2 * d)
    produced, d_in, grad_in, grad_out = expert(got[:, :d], got[:, d:], win, wout)
    back = jnp.concatenate([produced, d_in], axis=-1).reshape(batches, n_dp, share, 2 * d)
    back = lax.all_to_all(back, "dp", 1, 1, tiled=True).reshape(batches, experts * share, 2 * d)
    grad_in = lax.psum_scatter(grad_in, "tensor", scatter_dimension=1, tiled=True).astype(F32)
    grad_out = lax.psum_scatter(grad_out, "tensor", scatter_dimension=0, tiled=True).astype(F32)

    part_one = jnp.einsum("mqr,mqd->mrd", pick_one.astype(BF16), back[..., :d], preferred_element_type=F32)
    part_two = jnp.einsum("mqr,mqd->mrd", pick_two.astype(BF16), back[..., :d], preferred_element_type=F32)
    d_rows = jnp.einsum("mqr,mqd->mrd", picked, back[..., d:], preferred_element_type=F32)
    mixture = gate_one[:, :, None] * part_one + gate_two[:, :, None] * part_two
    cot_wide = cot_all.astype(F32)
    dgate_one = jnp.sum(part_one * cot_wide, axis=-1, keepdims=True)
    dgate_two = jnp.sum(part_two * cot_wide, axis=-1, keepdims=True)
    dgates = jnp.concatenate([dgate_one, dgate_two], axis=-1)
    payload = jnp.concatenate(
        [mixture, d_rows, jnp.pad(dgates, ((0, 0), (0, 0), (0, 126)))], axis=-1
    ).astype(BF16)
    pieces = payload.reshape(batches, n_t, work, payload.shape[-1])

    def piece(k):
        return lax.dynamic_index_in_dim(pieces, (t + k) % n_t, 1, keepdims=False)

    payload = piece(0).astype(F32)
    for k in range(1, n_t):
        payload = payload + lax.ppermute(
            piece(k), "tensor", [(j, (j + k) % n_t) for j in range(n_t)]
        ).astype(F32)
    output = (hidden + payload[..., :d]).astype(BF16)
    dgates = payload[..., 2 * d : 2 * d + 2]

    own_probs = own(gate_probs)
    dprobs = own(hits_one) * dgates[..., 0:1] * own(keep_one)[:, :, None]
    dprobs = dprobs + own(hits_two) * dgates[..., 1:2] * own(keep_two)[:, :, None]
    dlogits = own_probs * (dprobs - jnp.sum(dprobs * own_probs, axis=-1, keepdims=True))
    grad_router = lax.dot_general(
        normed_two.astype(F32), dlogits, (((0, 1), (0, 1)), ((), ())), precision=highest
    )
    dc = payload[..., d : 2 * d] + lax.dot_general(
        dlogits, router.astype(F32), (((2,), (1,)), ((), ())), precision=highest
    )
    _, back_two = jax.vjp(layer_norm, hidden, gain_two, shift_two)
    dnorm, grad_gain_two, grad_shift_two = back_two(dc)
    dhidden = dy + dnorm
    dattn = (live_own * dhidden).astype(BF16)

    grad_proj = dot(context, dattn, ((0, 1), (0, 1)))
    dcontext = dot(dattn, proj, ((2,), (1,))).astype(BF16).reshape(shape)
    dvalues = jnp.einsum("ihqk,iqhc->ikhc", weights, dcontext, preferred_element_type=F32).astype(BF16)
    dweights = jnp.einsum("iqhc,ikhc->ihqk", dcontext, values, preferred_element_type=F32)
    dscores = (probs * (dweights - jnp.sum(dweights * probs, axis=-1, keepdims=True))).astype(BF16)
    dquery = jnp.einsum("ihqk,ikhc->iqhc", dscores, keys, preferred_element_type=F32).astype(BF16)
    dkeys = jnp.einsum("ihqk,iqhc->ikhc", dscores, query, preferred_element_type=F32).astype(BF16)
    dmixed = jnp.stack(
        [v.reshape(batches, work, n_t, block) for v in (dquery * BF16(factor), dkeys, dvalues)], axis=3
    ).reshape(batches, work, 3 * split)
    grad_qkv = dot(normed_one, dmixed, ((0, 1), (0, 1)))
    da = dot(dmixed, qkv, ((2,), (1,)))
    _, back_one = jax.vjp(layer_norm, x, gain_one, shift_one)
    dnorm, grad_gain_one, grad_shift_one = back_one(da)
    grad_x = dhidden + dnorm

    if direct:
        out_edge = lax.ppermute(output[:, :edge], "tensor", [(1, 0)])
        grad_edge = lax.ppermute(grad_x[:, :edge], "tensor", [(1, 0)])
        result = jnp.where(
            t == 0,
            jnp.concatenate([output, out_edge], axis=1),
            jnp.concatenate([output[:, edge:], tokens[:, work - edge :]], axis=1),
        )
        grad_tokens = jnp.where(
            t == 0,
            jnp.concatenate([grad_x, grad_edge], axis=1),
            jnp.concatenate([grad_x[:, edge:], cotangent[:, work - edge :].astype(F32)], axis=1),
        )
    else:
        here = (t * own_rows + jnp.arange(own_rows) < span)[None, :, None]

        def home(v, rest):
            full = pad_rows(lax.all_gather(v, "tensor", axis=1, tiled=True)[:, :span], rows)
            return jnp.where(here, lax.dynamic_slice_in_dim(full, t * own_rows, own_rows, 1), rest)

        result = home(output, tokens)
        grad_tokens = home(grad_x, cotangent.astype(F32))

    nz, ny = grid_sizes(n_dp)
    grad_qkv = jnp.pad(grad_qkv.astype(BF16).reshape(d, n_t, 3 * block), ((0, 0), (0, 0), (0, fill)))
    grad_qkv = grad_qkv.reshape(nz, ny, 2, d // n_dp, -1)
    grad_proj = grad_proj.astype(BF16).reshape(n_t, heads_here, n_dp, -1, d)
    grad_proj = grad_proj.transpose(2, 0, 1, 3, 4).reshape(nz, ny, 2, n_t, -1, d)
    smalls = jnp.concatenate(
        [grad_router] + [v[:, None] for v in (grad_gain_one, grad_shift_one, grad_gain_two, grad_shift_two)],
        axis=1,
    )
    smalls = jnp.pad(smalls, ((0, 0), (0, 128 - smalls.shape[1]))).reshape(nz, ny, 2, n_t, -1, 128)
    grad_qkv, grad_proj, smalls = scatter_grads(grad_qkv, grad_proj, smalls, n_dp, n_t)
    grad_qkv = grad_qkv[:, : 3 * block].reshape(-1, 3, heads_here, width).transpose(0, 2, 1, 3)
    return (
        result,
        grad_tokens,
        grad_qkv.reshape(w_qkv.shape),
        grad_proj.reshape(w_proj.shape),
        grad_in[None],
        grad_out[None],
        smalls[:, :experts],
        smalls[:, experts],
        smalls[:, experts + 1],
        smalls[:, experts + 2],
        smalls[:, experts + 3],
    )


def standardise(v):
    centre = jnp.mean(v, axis=-1, keepdims=True)
    centered = v - centre
    inverse = lax.rsqrt(jnp.mean(centered * centered, axis=-1, keepdims=True) + EPS)
    return centered * inverse, inverse


def norm_back(grad, unit, inverse):
    return inverse * (
        grad
        - jnp.mean(grad, axis=-1, keepdims=True)
        - unit * jnp.mean(grad * unit, axis=-1, keepdims=True)
    )


def two_parts(v):
    high = v.astype(BF16)
    return high, (v - high.astype(F32)).astype(BF16)


def gate_softmax(c, router, experts):
    lane = lax.broadcasted_iota(jnp.int32, (c.shape[0], router.shape[1]), 1)
    logits = jnp.where(lane < experts, dot(c, router, ((1,), (0,))), -1e30)
    raised = jnp.exp(logits - jnp.max(logits, axis=-1, keepdims=True))
    return raised / jnp.sum(raised, axis=-1, keepdims=True), lane


def key_softmax(query, keys, count):
    scores = dot(query, keys, ((1,), (1,)))
    col = lax.broadcasted_iota(jnp.int32, scores.shape, 1)
    scores = jnp.where(col < count, scores, -1e30)
    raised = jnp.exp(scores - jnp.max(scores, axis=-1, keepdims=True))
    return raised * (1.0 / jnp.sum(raised, axis=-1, keepdims=True))


def pairs(n_t, block):
    return [
        (3 * block * s + 128 * i, block * s + 128 * i) for s in range(n_t) for i in range(block // 128)
    ]


def attend_kernel(n_t, block, count, factor, x, live, norms, qkv, proj, c_out, hidden_out, mixed_out, context_out):
    xf = x[0].astype(F32)
    unit, _ = standardise(xf)
    a = (unit * norms[0:1] + norms[1:2]).astype(BF16)
    for s in range(n_t):
        for i in range(3):
            cols = slice((3 * s + i) * block, (3 * s + i + 1) * block)
            part = dot(a, qkv[:, cols], ((1,), (0,)))
            mixed_out[0, :, cols] = (part * factor if i == 0 else part).astype(BF16)
    low = lax.broadcasted_iota(jnp.int32, (x.shape[1], 128), 1) < 64
    for col, dest in pairs(n_t, block):
        query = mixed_out[0, :, col : col + 128]
        keys = mixed_out[0, :, col + block : col + block + 128]
        values = mixed_out[0, :, col + 2 * block : col + 2 * block + 128]
        zero = jnp.zeros_like(query)
        parts = []
        for own in (low, ~low):
            probs = key_softmax(jnp.where(own, query, zero), keys, count)
            parts.append(dot(probs.astype(BF16), values, ((1,), (0,))))
        context_out[0, :, dest : dest + 128] = jnp.where(low, parts[0], parts[1]).astype(BF16)
    hidden = xf + live[0] * dot(context_out[0], proj[...], ((1,), (0,)))
    hidden_out[0] = hidden
    unit, _ = standardise(hidden)
    c_out[0] = (unit * norms[2:3] + norms[3:4]).astype(BF16)


def attend(x, live, norms, qkv, proj, n_t, block, count, factor):
    batches, rows, d = x.shape
    wide = qkv.shape[1]

    def each(n):
        return pl.BlockSpec((1, rows, n), lambda m: (m, 0, 0))

    def fixed(shape):
        return pl.BlockSpec(shape, lambda m: (0, 0))

    return pl.pallas_call(
        functools.partial(attend_kernel, n_t, block, count, factor),
        grid=(batches,),
        in_specs=[each(d), each(1), fixed(norms.shape), fixed(qkv.shape), fixed(proj.shape)],
        out_specs=[each(d), each(d), each(wide), each(d)],
        out_shape=[
            jax.ShapeDtypeStruct((batches, rows, d), BF16),
            jax.ShapeDtypeStruct((batches, rows, d), F32),
            jax.ShapeDtypeStruct((batches, rows, wide), BF16),
            jax.ShapeDtypeStruct((batches, rows, d), BF16),
        ],
        compiler_params=pltpu.CompilerParams(vmem_limit_bytes=32 * 1024 * 1024),
        cost_estimate=pl.CostEstimate(
            flops=2 * batches * rows * d * (wide + d), transcendentals=0, bytes_accessed=8 * batches * rows * d
        ),
    )(x, live, norms, qkv, proj)


def retreat_kernel(
    n_t,
    block,
    count,
    factor,
    experts,
    x,
    hidden_in,
    mixed,
    context,
    mix,
    d_rows,
    dgate,
    dy,
    live,
    expert_own,
    norms,
    qkv,
    proj,
    router,
    out,
    grad_x,
    gqkv_out,
    gproj_out,
    grouter,
    gnorms,
    dmixed,
    gqkv,
    gproj,
):
    step = pl.program_id(0)

    @pl.when(step == 0)
    def _():
        gqkv[...] = jnp.zeros_like(gqkv)
        gproj[...] = jnp.zeros_like(gproj)
        grouter[...] = jnp.zeros_like(grouter)
        gnorms[...] = jnp.zeros_like(gnorms)

    hidden = hidden_in[0]
    out[0] = (hidden + mix[0]).astype(BF16)
    unit, inverse = standardise(hidden)
    c = (unit * norms[2:3] + norms[3:4]).astype(BF16)
    probs, lane = gate_softmax(c, router[...], experts)
    dprobs = jnp.where(lane == expert_own[0, :, 0:1], dgate[0, :, 0:1], 0.0)
    dprobs = dprobs + jnp.where(lane == expert_own[0, :, 1:2], dgate[0, :, 1:2], 0.0)
    dlogits = probs * (dprobs - jnp.sum(dprobs * probs, axis=-1, keepdims=True))
    dc = d_rows[0]
    for piece in two_parts(dlogits):
        grouter[...] += dot(c, piece, ((0,), (0,)))
        dc = dc + dot(piece, router[...], ((1,), (1,)))
    gnorms[2:3] += jnp.sum(dc * unit, axis=0, keepdims=True)
    gnorms[3:4] += jnp.sum(dc, axis=0, keepdims=True)
    dhidden = dy[0].astype(F32) + norm_back(dc * norms[2:3], unit, inverse)
    dattn = (live[0] * dhidden).astype(BF16)
    gproj[...] += dot(context[0], dattn, ((0,), (0,)))
    dcontext = dot(dattn, proj[...], ((1,), (1,))).astype(BF16)
    low = lax.broadcasted_iota(jnp.int32, (x.shape[1], 128), 1) < 64
    for col, dest in pairs(n_t, block):
        query = mixed[0, :, col : col + 128]
        keys = mixed[0, :, col + block : col + block + 128]
        values = mixed[0, :, col + 2 * block : col + 2 * block + 128]
        grads = dcontext[:, dest : dest + 128]
        zero = jnp.zeros_like(query)
        parts = []
        for own in (low, ~low):
            probs = key_softmax(jnp.where(own, query, zero), keys, count)
            dvalues = dot(probs.astype(BF16), grads, ((0,), (0,)))
            dweights = dot(jnp.where(own, grads, zero), values, ((1,), (1,)))
            dscores = probs * (dweights - jnp.sum(dweights * probs, axis=-1, keepdims=True))
            dscores = dscores.astype(BF16)
            parts.append(
                (dot(dscores, keys, ((1,), (0,))), dot(dscores, query, ((0,), (0,))), dvalues)
            )
        for i in range(3):
            both = jnp.where(low, parts[0][i], parts[1][i]).astype(BF16)
            if i == 0:
                both = both * BF16(factor)
            dmixed[:, col + i * block : col + i * block + 128] = both
    xf = x[0].astype(F32)
    unit, inverse = standardise(xf)
    a = (unit * norms[0:1] + norms[1:2]).astype(BF16)
    gqkv[...] += dot(a, dmixed[...], ((0,), (0,)))
    da = dot(dmixed[...], qkv[...], ((1,), (1,)))
    gnorms[0:1] += jnp.sum(da * unit, axis=0, keepdims=True)
    gnorms[1:2] += jnp.sum(da, axis=0, keepdims=True)
    grad_x[0] = dhidden + norm_back(da * norms[0:1], unit, inverse)

    @pl.when(step == pl.num_programs(0) - 1)
    def _():
        gqkv_out[...] = gqkv[...].astype(BF16)
        gproj_out[...] = gproj[...].astype(BF16)


def retreat(x, saved, arrived, dy, live, expert_own, norms, qkv, proj, router, n_t, block, count, factor, experts):
    batches, rows, d = x.shape
    wide = qkv.shape[1]

    def each(n):
        return pl.BlockSpec((1, rows, n), lambda m: (m, 0, 0))

    def fixed(v):
        return pl.BlockSpec(v.shape, lambda m: (0, 0))

    whole = [
        jax.ShapeDtypeStruct((d, wide), BF16),
        jax.ShapeDtypeStruct((d, d), BF16),
        jax.ShapeDtypeStruct((d, router.shape[1]), F32),
        jax.ShapeDtypeStruct((8, d), F32),
    ]
    return pl.pallas_call(
        functools.partial(retreat_kernel, n_t, block, count, factor, experts),
        grid=(batches,),
        in_specs=[each(d), each(d), each(wide), each(d), each(d), each(d), each(128), each(d), each(1), each(2)]
        + [fixed(v) for v in (norms, qkv, proj, router)],
        out_specs=[each(d), each(d)] + [fixed(v) for v in whole],
        out_shape=[
            jax.ShapeDtypeStruct((batches, rows, d), BF16),
            jax.ShapeDtypeStruct((batches, rows, d), F32),
        ]
        + whole,
        scratch_shapes=[
            pltpu.VMEM((rows, wide), BF16),
            pltpu.VMEM((d, wide), F32),
            pltpu.VMEM((d, d), F32),
        ],
        compiler_params=pltpu.CompilerParams(vmem_limit_bytes=48 * 1024 * 1024),
        cost_estimate=pl.CostEstimate(
            flops=6 * batches * rows * d * (wide + d), transcendentals=0, bytes_accessed=16 * batches * rows * d
        ),
    )(x, *saved, *arrived, dy, live, expert_own, norms, qkv, proj, router)


def fast(
    tokens,
    w_qkv,
    w_proj,
    w_in,
    w_out,
    w_router,
    gain_attn,
    shift_attn,
    gain_moe,
    shift_moe,
    live_rows,
    chosen,
    priority,
    cotangent,
):
    batches, own_rows, d = tokens.shape
    rows = live_rows.shape[1]
    n_dp = lax.axis_size("dp")
    n_t = lax.axis_size("tensor")
    t = lax.axis_index("tensor")
    heads_here = w_qkv.shape[1]
    width = w_qkv.shape[2] // 3
    block = heads_here * width
    experts = n_dp
    cap = 2 * rows // experts
    share = cap // n_t
    span = n_t * SEQ
    padded = -(-SEQ // 16) * 16
    edge = own_rows - SEQ
    factor = width ** (-0.5)

    small = jnp.concatenate(
        [w_router] + [v[:, None] for v in (gain_attn, shift_attn, gain_moe, shift_moe)], axis=1
    )
    small = jnp.pad(small, ((0, 0), (0, 128 - small.shape[1])))
    qkv_block = w_qkv.reshape(-1, heads_here, 3, width).transpose(0, 2, 1, 3).reshape(-1, 3 * block)
    qkv, proj, small, cot_all, moved = gather_weights(
        qkv_block, w_proj.reshape(-1, d), small, n_dp, n_t, (cotangent, tokens[:, SEQ:])
    )
    cot_all = cot_all.transpose(1, 0, 2, 3).reshape(batches, rows, d)
    router = jnp.where(jnp.arange(128) < experts, small, 0)
    norms = jnp.pad(small[:, experts : experts + 4].astype(F32).T, ((0, 4), (0, 0)))
    proj = proj.reshape(n_dp, n_t, heads_here, w_proj.shape[1], d)
    proj = proj.transpose(1, 2, 0, 3, 4).reshape(n_t * block, d)

    def pad_rows(v, axis, fill=0):
        spec = [(0, 0)] * v.ndim
        spec[axis] = (0, padded - SEQ)
        return jnp.pad(v, spec, constant_values=fill)

    def lay(v, axis, fill=0):
        shape = v.shape
        v = v.reshape(shape[:axis] + (n_t, SEQ) + shape[axis + 1 :])
        v = pad_rows(v, axis + 1, fill)
        return v.reshape(shape[:axis] + (n_t * padded,) + shape[axis + 1 :])

    def own(v, axis):
        return lax.dynamic_slice_in_dim(v, t * padded, padded, axis)

    x = jnp.where(t == 0, tokens[:, :SEQ], jnp.concatenate([moved, tokens[:, : SEQ - edge]], axis=1))
    x = pad_rows(x, 1)
    cot_all = lay(cot_all[:, :span], 1)

    live = live_rows[:, :span]
    rank = priority[:, 0, :span]
    picks = chosen[:, :span].transpose(0, 2, 1)
    labels = jnp.arange(experts, dtype=jnp.int32)
    earlier = (rank[:, None, :] < rank[:, :, None]).astype(BF16)
    hits = (picks[..., None] == labels).astype(F32)
    live_hits = hits * live[:, None, :, None].astype(F32)
    ahead = jnp.einsum("mrs,mkse->mkre", earlier, live_hits.astype(BF16), preferred_element_type=F32)
    firsts = jnp.sum(live_hits[:, :1], axis=2, keepdims=True)
    ahead = ahead + jnp.concatenate([jnp.zeros_like(firsts), firsts], axis=1)
    slot = jnp.sum(ahead * hits, axis=-1).astype(jnp.int32)
    keep = (live[:, None, :] > 0) & (slot < cap)
    flat = lay(jnp.where(keep, picks * cap + slot, -1), 2, -1)
    expert_of = lay(jnp.where(keep, picks, -1), 2, -1)
    codes = (jnp.arange(experts)[:, None] * cap + t * share + jnp.arange(share)[None, :]).reshape(-1)
    live_own = own(lay(live.astype(F32)[:, :, None], 1), 1)

    c, hidden, mixed, context = attend(x, live_own, norms, qkv, proj, n_t, block, SEQ, factor)
    mixture, d_rows, dgates, grad_in, grad_out = moe(
        c, cot_all, router, flat, expert_of, codes, w_in[0], w_out[0], experts, n_dp
    )
    output, grad_x, grad_qkv, grad_proj, grad_router, grad_norms = retreat(
        x,
        (hidden, mixed, context),
        (mixture, d_rows, dgates),
        own(cot_all, 1),
        live_own,
        own(expert_of, 2).transpose(0, 2, 1),
        norms,
        qkv,
        proj,
        router,
        n_t,
        block,
        SEQ,
        factor,
        experts,
    )

    out_edge = lax.ppermute(output[:, :edge], "tensor", [(1, 0)])
    grad_edge = lax.ppermute(grad_x[:, :edge], "tensor", [(1, 0)])
    rest = SEQ - edge

    def home(v, moved_rows, other):
        return jnp.where(
            t == 0,
            jnp.concatenate([v[:, :SEQ], moved_rows], axis=1),
            jnp.concatenate([v[:, edge:SEQ], other[:, rest:].astype(v.dtype)], axis=1),
        )

    nz, ny = grid_sizes(n_dp)
    grad_proj = grad_proj.reshape(n_t, heads_here, n_dp, -1, d)
    grad_proj = grad_proj.transpose(2, 0, 1, 3, 4).reshape(nz, ny, 2, n_t, -1, d)
    lane = jnp.arange(128)
    smalls = jnp.where(lane < experts, grad_router, 0.0)
    smalls = smalls + jnp.pad(grad_norms[:4].T, ((0, 0), (experts, 124 - experts)))
    grad_qkv, grad_proj, smalls = scatter_grads(
        grad_qkv.reshape(nz, ny, 2, d // n_dp, -1), grad_proj, smalls.reshape(nz, ny, 2, n_t, -1, 128), n_dp, n_t
    )
    grad_qkv = grad_qkv.reshape(-1, 3, heads_here, width).transpose(0, 2, 1, 3)
    return (
        home(output, out_edge, tokens),
        home(grad_x, grad_edge, cotangent),
        grad_qkv.reshape(w_qkv.shape),
        grad_proj.reshape(w_proj.shape),
        grad_in[None],
        grad_out[None],
        smalls[:, :experts],
        smalls[:, experts],
        smalls[:, experts + 1],
        smalls[:, experts + 2],
        smalls[:, experts + 3],
    )


def local(*args):
    tokens, w_qkv, live_rows = args[0], args[1], args[10]
    n_t = lax.axis_size("tensor")
    images = live_rows.shape[1] // SEQ
    block = w_qkv.shape[1] * (w_qkv.shape[2] // 3)
    if n_t == 2 and images == 2 and tokens.shape[1] >= SEQ and block % 128 == 0 and w_qkv.shape[2] == 192:
        return fast(*args)
    return general(*args)


def solution(mesh):
    both = ("dp", "tensor")
    return jax.shard_map(
        local,
        mesh=mesh,
        in_specs=(
            P(None, both, None),
            P("dp", "tensor", None),
            P("tensor", "dp", None),
            P("dp", None, "tensor"),
            P("dp", "tensor", None),
            P(both, None),
            P(both),
            P(both),
            P(both),
            P(both),
            P(None, "dp"),
            P(None, "dp", None),
            P(None, "dp", None),
            P(None, both, None),
        ),
        out_specs=(
            P(None, both, None),
            P(None, both, None),
            P("dp", "tensor", None),
            P("tensor", "dp", None),
            P("dp", None, "tensor"),
            P("dp", "tensor", None),
            P(both, None),
            P(both),
            P(both),
            P(both),
            P(both),
        ),
        check_vma=False,
    )
```

```python
import functools

import jax
import jax.numpy as jnp
from jax import lax
from jax.experimental import pallas as pl
from jax.experimental.pallas import tpu as pltpu
from jax.sharding import PartitionSpec as P

SEQ = 197
EPS = 1e-06
F32 = jnp.float32
BF16 = jnp.bfloat16
GELU_A = 0.7978845608028654
GELU_B = 0.044715


def dot(a, b, dims):
    return lax.dot_general(a, b, (dims, ((), ())), preferred_element_type=F32)


def layer_norm(values, gain_vec, shift_vec):
    centre = jnp.mean(values, axis=-1, keepdims=True)
    centered = values - centre
    spread = jnp.mean(centered * centered, axis=-1, keepdims=True)
    return centered * lax.rsqrt(spread + EPS) * gain_vec + shift_vec


def expert_kernel(x_ref, dp_ref, win_ref, wout_ref, y_ref, dx_ref, gin_ref, gout_ref, y_acc, dx_acc):
    step = pl.program_id(0)
    last = pl.num_programs(0) - 1
    x = x_ref[...]
    dprod = dp_ref[...]
    win = win_ref[...]
    wout = wout_ref[...]
    pre = dot(x, win, ((1,), (0,)))
    square = pre * pre
    th = jnp.tanh(GELU_A * pre * (1.0 + GELU_B * square))
    active = (0.5 * pre * (1.0 + th)).astype(BF16)
    slope = 0.5 * (1.0 + th) + 0.5 * pre * (1.0 - th * th) * (GELU_A * (1.0 + 3.0 * GELU_B * square))
    dact = dot(dprod, wout, ((1,), (1,)))
    dpre = (dact * slope).astype(BF16)
    gin_ref[...] = dot(x, dpre, ((0,), (0,))).astype(BF16)
    gout_ref[...] = dot(active, dprod, ((0,), (0,))).astype(BF16)
    part_y = dot(active, wout, ((1,), (0,)))
    part_dx = dot(dpre, win, ((1,), (1,)))

    @pl.when(step == 0)
    def _():
        y_acc[...] = part_y
        dx_acc[...] = part_dx

    @pl.when(step > 0)
    def _():
        y_acc[...] += part_y
        dx_acc[...] += part_dx

    @pl.when(step == last)
    def _():
        y_ref[...] = y_acc[...].astype(BF16)
        dx_ref[...] = dx_acc[...].astype(BF16)


def expert(x, dprod, win, wout, tile=256):
    n, d = x.shape
    ff = win.shape[1]
    return pl.pallas_call(
        expert_kernel,
        grid=(ff // tile,),
        in_specs=[
            pl.BlockSpec((n, d), lambda i: (0, 0)),
            pl.BlockSpec((n, d), lambda i: (0, 0)),
            pl.BlockSpec((d, tile), lambda i: (0, i)),
            pl.BlockSpec((tile, d), lambda i: (i, 0)),
        ],
        out_specs=[
            pl.BlockSpec((n, d), lambda i: (0, 0)),
            pl.BlockSpec((n, d), lambda i: (0, 0)),
            pl.BlockSpec((d, tile), lambda i: (0, i)),
            pl.BlockSpec((tile, d), lambda i: (i, 0)),
        ],
        out_shape=[
            jax.ShapeDtypeStruct((n, d), BF16),
            jax.ShapeDtypeStruct((n, d), BF16),
            jax.ShapeDtypeStruct((d, ff), BF16),
            jax.ShapeDtypeStruct((ff, d), BF16),
        ],
        scratch_shapes=[pltpu.VMEM((n, d), F32), pltpu.VMEM((n, d), F32)],
        compiler_params=pltpu.CompilerParams(vmem_limit_bytes=60 * 1024 * 1024),
        cost_estimate=pl.CostEstimate(
            flops=12 * n * d * ff, transcendentals=n * ff, bytes_accessed=8 * n * d + 8 * d * ff
        ),
    )(x, dprod, win, wout)


MESH = pl.DeviceIdType.MESH
ANYWHERE = pl.BlockSpec(memory_space=pltpu.VMEM)


def grid_sizes(n_dp):
    ny = 1
    while 2 * ny * 2 * ny <= n_dp // 2:
        ny *= 2
    return n_dp // (2 * ny), ny


def position(ny):
    dp = lax.axis_index("dp")
    return dp, lax.axis_index("tensor"), dp % 2, (dp // 2) % ny, dp // (2 * ny)


def neighbours(ny, nz, n_t):
    dp, t, c, y, z = position(ny)

    def along_core(k):
        return (dp - c + (c + k) % 2, t)

    def along_tensor(k):
        return (dp, (t + k) % n_t)

    def along_y(k):
        return (dp + ((y + k) % ny - y) * 2, t)

    def along_z(k):
        return (dp + ((z + k) % nz - z) * 2 * ny, t)

    return {"core": (2, along_core), "tensor": (n_t, along_tensor), "y": (ny, along_y), "z": (nz, along_z)}


def greet(stages):
    barrier = pltpu.get_barrier_semaphore()
    count = 0
    for size, device in stages.values():
        for k in range(1, size):
            pl.semaphore_signal(barrier, inc=1, device_id=device(k), device_id_type=MESH)
            count += 1
    pl.semaphore_wait(barrier, count)


def gather_kernel(ny, nz, n_t, extras, *refs):
    (qkv, proj, small), refs = refs[:3], refs[3:]
    side, refs = refs[:extras], refs[extras:]
    (qkv_out, proj_out, small_out), refs = refs[:3], refs[3:]
    side_out, (send, recv, copied) = refs[:extras], refs[extras:]
    dp, t, c, y, z = position(ny)
    stages = neighbours(ny, nz, n_t)
    greet(stages)
    aside = []
    for i in range(extras):
        aside.append(
            pltpu.make_async_remote_copy(
                src_ref=side[i],
                dst_ref=side_out[i].at[t] if i == 0 else side_out[i],
                send_sem=send.at[send.shape[0] - 1 - i],
                recv_sem=recv.at[recv.shape[0] - 1 - i],
                device_id=(dp, 1 - t),
                device_id_type=MESH,
            )
        )
    for copy in aside:
        copy.start()
    cols = qkv.shape[1]

    def views(zs, ys, cs, ts):
        lanes = pl.ds(pl.multiple_of(ts * cols, 128), cols)
        return (
            qkv_out.at[zs, ys, cs, :, lanes],
            proj_out.at[zs, ys, cs, ts],
            small_out.at[zs, ys, cs, ts],
        )

    whole = slice(None)
    mine = views(z, y, c, t)
    local = [
        pltpu.make_async_copy(src, dst, copied.at[i])
        for i, (src, dst) in enumerate(zip((qkv, proj, small), mine))
    ]
    if extras:
        local.append(pltpu.make_async_copy(side[0], side_out[0].at[t], copied.at[3]))
    for copy in local:
        copy.start()
    slot = 0
    for name in ("z", "y", "tensor", "core"):
        size, device = stages[name]
        if name == "z":
            sources, targets = (qkv, proj, small), mine
        elif name == "y":
            sources = targets = views(whole, y, c, t)
        elif name == "tensor":
            sources = targets = views(whole, whole, c, t)
        else:
            sources = targets = (
                qkv_out.at[:, :, c],
                proj_out.at[:, :, c],
                small_out.at[:, :, c],
            )
        copies = []
        for k in range(1, size):
            for src, dst in zip(sources, targets):
                copies.append(
                    pltpu.make_async_remote_copy(
                        src_ref=src,
                        dst_ref=dst,
                        send_sem=send.at[slot],
                        recv_sem=recv.at[slot],
                        device_id=device(k),
                        device_id_type=MESH,
                    )
                )
                slot += 1
        for copy in copies:
            copy.start()
        if name == "z":
            for copy in local:
                copy.wait()
        for copy in copies:
            copy.wait()
    for copy in aside:
        copy.wait()


def gather_weights(qkv, proj, small, n_dp, n_t, side=()):
    nz, ny = grid_sizes(n_dp)
    slots = 3 * (1 + (n_t - 1) + (ny - 1) + (nz - 1)) + len(side)
    side_shapes = [
        jax.ShapeDtypeStruct(((n_t,) if i == 0 else ()) + v.shape, v.dtype) for i, v in enumerate(side)
    ]
    outs = pl.pallas_call(
        functools.partial(gather_kernel, ny, nz, n_t, len(side)),
        out_shape=[
            jax.ShapeDtypeStruct((nz, ny, 2, qkv.shape[0], n_t * qkv.shape[1]), BF16),
            jax.ShapeDtypeStruct((nz, ny, 2, n_t) + proj.shape, BF16),
            jax.ShapeDtypeStruct((nz, ny, 2, n_t) + small.shape, BF16),
        ]
        + side_shapes,
        in_specs=[ANYWHERE] * (3 + len(side)),
        out_specs=[ANYWHERE] * (3 + len(side)),
        scratch_shapes=[
            pltpu.SemaphoreType.DMA((slots,)),
            pltpu.SemaphoreType.DMA((slots,)),
            pltpu.SemaphoreType.DMA((4,)),
        ],
        compiler_params=pltpu.CompilerParams(collective_id=0, has_side_effects=True),
    )(qkv, proj, small, *side)
    qkv_all = outs[0].reshape(n_dp * qkv.shape[0], n_t * qkv.shape[1])
    return (qkv_all, outs[1].reshape((n_dp, n_t) + proj.shape), outs[2].reshape(-1, small.shape[1])) + tuple(outs[3:])


def scatter_kernel(ny, nz, n_t, *refs):
    ins, refs = refs[:3], refs[3:]
    outs, refs = refs[:3], refs[3:]
    got = [refs[3 * i : 3 * i + 3] for i in range(4)]
    held = [refs[12 + 3 * i : 15 + 3 * i] for i in range(3)]
    send, recv = refs[21], refs[22]
    _, t, c, y, z = position(ny)
    stages = neighbours(ny, nz, n_t)
    greet(stages)
    cols = outs[0].shape[1]
    slot = 0

    def lanes(ts):
        return pl.ds(pl.multiple_of(ts * cols, 128), cols)

    def exchange(name, me, piece):
        nonlocal slot
        size, device = stages[name]
        level = ("core", "tensor", "y", "z").index(name)
        copies = []
        for k in range(1, size):
            for i, src in enumerate(piece((me + k) % size)):
                copies.append(
                    pltpu.make_async_remote_copy(
                        src_ref=src,
                        dst_ref=got[level][i].at[k - 1],
                        send_sem=send.at[slot],
                        recv_sem=recv.at[slot],
                        device_id=device(k),
                        device_id_type=MESH,
                    )
                )
                slot += 1
        for copy in copies:
            copy.start()
        for copy in copies:
            copy.wait()

    def total(own, level, index, i):
        value = own.astype(F32)
        for k in range(got[level][i].shape[0]):
            value = value + got[level][i][(k,) + index].astype(F32)
        return value

    def over_zy(body):
        def step(n, carry):
            body(n // ny, n % ny)
            return carry

        lax.fori_loop(0, nz * ny, step, 0)

    exchange("core", c, lambda j: [ref.at[:, :, j] for ref in ins])

    def add_core(zi, yi):
        for i in range(3):
            held[0][i][zi, yi] = total(ins[i][zi, yi, c], 0, (zi, yi), i).astype(held[0][i].dtype)

    over_zy(add_core)
    exchange(
        "tensor",
        t,
        lambda j: [held[0][0].at[:, :, :, lanes(j)], held[0][1].at[:, :, j], held[0][2].at[:, :, j]],
    )

    def add_tensor(zi, yi):
        owns = (held[0][0][zi, yi, :, lanes(t)], held[0][1][zi, yi, t], held[0][2][zi, yi, t])
        for i in range(3):
            held[1][i][zi, yi] = total(owns[i], 1, (zi, yi), i).astype(held[1][i].dtype)

    over_zy(add_tensor)
    exchange("y", y, lambda j: [ref.at[:, j] for ref in held[1]])

    def add_y(zi, carry):
        for i in range(3):
            held[2][i][zi] = total(held[1][i][zi, y], 2, (zi,), i).astype(held[2][i].dtype)
        return carry

    lax.fori_loop(0, nz, add_y, 0)
    exchange("z", z, lambda j: [ref.at[j] for ref in held[2]])
    for i in range(3):
        outs[i][...] = total(held[2][i][z], 3, (), i)


def scatter_grads(qkv, proj, small, n_dp, n_t):
    nz, ny = qkv.shape[:2]
    rows, cols = qkv.shape[3], qkv.shape[4] // n_t
    tails = [(rows, cols), proj.shape[4:], small.shape[4:]]
    kinds = [BF16, BF16, F32]
    wide = [(rows, n_t * cols), (n_t,) + proj.shape[4:], (n_t,) + small.shape[4:]]
    scratch = [pltpu.VMEM((1, nz, ny) + wide[i], kinds[i]) for i in range(3)]
    scratch += [pltpu.VMEM((n_t - 1, nz, ny) + tails[i], kinds[i]) for i in range(3)]
    scratch += [pltpu.VMEM((ny - 1, nz) + tails[i], kinds[i]) for i in range(3)]
    scratch += [pltpu.VMEM((nz - 1,) + tails[i], kinds[i]) for i in range(3)]
    scratch += [pltpu.VMEM((nz, ny) + wide[i], kinds[i]) for i in range(3)]
    scratch += [pltpu.VMEM((nz, ny) + tails[i], kinds[i]) for i in range(3)]
    scratch += [pltpu.VMEM((nz,) + tails[i], kinds[i]) for i in range(3)]
    slots = 3 * (1 + (n_t - 1) + (ny - 1) + (nz - 1))
    scratch += [pltpu.SemaphoreType.DMA((slots,)), pltpu.SemaphoreType.DMA((slots,))]
    return pl.pallas_call(
        functools.partial(scatter_kernel, ny, nz, n_t),
        out_shape=[jax.ShapeDtypeStruct(tail, F32) for tail in tails],
        in_specs=[ANYWHERE] * 3,
        out_specs=[ANYWHERE] * 3,
        scratch_shapes=scratch,
        compiler_params=pltpu.CompilerParams(collective_id=1, has_side_effects=True),
    )(qkv, proj, small)


def standardise(v):
    centre = jnp.mean(v, axis=-1, keepdims=True)
    centered = v - centre
    inverse = lax.rsqrt(jnp.mean(centered * centered, axis=-1, keepdims=True) + EPS)
    return centered * inverse, inverse


def norm_back(grad, unit, inverse):
    return inverse * (
        grad
        - jnp.mean(grad, axis=-1, keepdims=True)
        - unit * jnp.mean(grad * unit, axis=-1, keepdims=True)
    )


def two_parts(v):
    high = v.astype(BF16)
    return high, (v - high.astype(F32)).astype(BF16)


def gate_softmax(c, router, experts):
    lane = lax.broadcasted_iota(jnp.int32, (c.shape[0], router.shape[1]), 1)
    logits = jnp.where(lane < experts, dot(c, router, ((1,), (0,))), -1e30)
    raised = jnp.exp(logits - jnp.max(logits, axis=-1, keepdims=True))
    return raised / jnp.sum(raised, axis=-1, keepdims=True), lane


def key_softmax(query, keys, count):
    scores = dot(query, keys, ((1,), (1,)))
    col = lax.broadcasted_iota(jnp.int32, scores.shape, 1)
    scores = jnp.where(col < count, scores, -1e30)
    raised = jnp.exp(scores - jnp.max(scores, axis=-1, keepdims=True))
    return raised * (1.0 / jnp.sum(raised, axis=-1, keepdims=True))


def pairs(n_t, block):
    return [
        (3 * block * s + 128 * i, block * s + 128 * i) for s in range(n_t) for i in range(block // 128)
    ]


def moe_kernel(
    experts,
    n_t,
    block,
    count,
    factor,
    c_own,
    cot_all,
    router,
    flat_row,
    flat_col,
    expert_col,
    code_row,
    code_col,
    win,
    wout,
    x_in,
    hidden_in,
    mixed,
    context,
    live,
    norms,
    qkv,
    proj,
    out,
    grad_x,
    gqkv_out,
    gproj_out,
    grouter,
    gnorms,
    gin_mine,
    gout_mine,
    c_all,
    gates,
    sent,
    got,
    ret,
    pay,
    paid,
    mix,
    dx,
    dgate,
    dmixed,
    gqkv,
    gproj,
    y_acc,
    dx_acc,
    win_got,
    wout_got,
    gin,
    gout,
    gin_half,
    gout_half,
    gin_got,
    gout_got,
    w_sems,
    c_sems,
    go_send,
    go_recv,
    back_send,
    back_recv,
    pay_sems,
    grad_sems,
):
    batches, rows, d = c_own.shape
    n_dp = lax.axis_size("dp")
    dp, t = lax.axis_index("dp"), lax.axis_index("tensor")
    share = sent.shape[1] // n_dp
    hidden = win.shape[1]
    other = 1 - t
    partner = (dp, other)

    barrier = pltpu.get_barrier_semaphore()
    pl.semaphore_signal(barrier, inc=1, device_id=partner, device_id_type=MESH)

    def hello(k, carry):
        pl.semaphore_signal(barrier, inc=1, device_id=((dp + k) % n_dp, t), device_id_type=MESH)
        return carry

    lax.fori_loop(1, n_dp, hello, 0)
    pl.semaphore_wait(barrier, n_dp)

    def image(i):
        return pl.ds(pl.multiple_of(i * rows, 16), rows)

    def part(i):
        return pl.ds(pl.multiple_of(i * share, 16), share)

    def remote(src, dst, sems, i, j, device):
        return pltpu.make_async_remote_copy(
            src_ref=src,
            dst_ref=dst,
            send_sem=sems[0].at[i, j],
            recv_sem=sems[1].at[i, j],
            device_id=device,
            device_id_type=MESH,
        )

    def c_copy(m):
        return pltpu.make_async_remote_copy(
            src_ref=c_own.at[m],
            dst_ref=c_all.at[m, image(t)],
            send_sem=c_sems.at[0, m],
            recv_sem=c_sems.at[1, m],
            device_id=partner,
            device_id_type=MESH,
        )

    def go_copy(m, k):
        to = (dp + k) % n_dp
        return remote(sent.at[m, part(to)], got.at[m, part(dp)], (go_send, go_recv), m, k - 1, (to, t))

    def back_copy(m, k):
        to = (dp + k) % n_dp
        return remote(got.at[m, part(to)], ret.at[m, part(dp)], (back_send, back_recv), m, k - 1, (to, t))

    def pay_copy(m):
        return pltpu.make_async_remote_copy(
            src_ref=pay.at[m],
            dst_ref=paid.at[m],
            send_sem=pay_sems.at[0, m],
            recv_sem=pay_sems.at[1, m],
            device_id=partner,
            device_id_type=MESH,
        )

    def grad_copy(i):
        src, dst = ((gin_half, gin_got), (gout_half, gout_got))[i // 2]
        size = src.shape[0] // 2
        band = pl.ds(i % 2 * size, size)
        return pltpu.make_async_remote_copy(
            src_ref=src.at[band],
            dst_ref=dst.at[band],
            send_sem=grad_sems.at[0, i],
            recv_sem=grad_sems.at[1, i],
            device_id=partner,
            device_id_type=MESH,
        )

    def w_copy(i):
        return pltpu.make_async_remote_copy(
            src_ref=(win, wout)[i],
            dst_ref=(win_got, wout_got)[i],
            send_sem=w_sems.at[0, i],
            recv_sem=w_sems.at[1, i],
            device_id=partner,
            device_id_type=MESH,
        )

    def every(body):
        def step(k, carry):
            body(k)
            return carry

        lax.fori_loop(1, n_dp, step, 0)

    for m in range(batches):
        c_copy(m).start()
        c_all[m, image(t)] = c_own[m]
    w_copy(0).start()
    w_copy(1).start()

    lane = lax.broadcasted_iota(jnp.int32, (2 * rows, router.shape[1]), 1)

    def dispatch(m, carry):
        c_copy(m).wait_recv()
        c = c_all[m]
        logits = jnp.where(lane < experts, dot(c, router[...], ((1,), (0,))), -1e30)
        raised = jnp.exp(logits - jnp.max(logits, axis=-1, keepdims=True))
        probs = raised / jnp.sum(raised, axis=-1, keepdims=True)
        cot = cot_all[m].astype(F32)
        scaled = []
        for k in range(2):
            gate = jnp.sum(jnp.where(lane == expert_col[m, :, k : k + 1], probs, 0.0), axis=-1, keepdims=True)
            gates[m, :, k : k + 1] = gate
            scaled.append((gate * cot).astype(BF16))
        codes = code_col[...]
        picks = [(flat_row[m, k : k + 1, :] == codes).astype(F32).astype(BF16) for k in range(2)]
        sent[m, :, :d] = dot(picks[0] + picks[1], c, ((1,), (0,))).astype(BF16)
        moved = dot(picks[0], scaled[0], ((1,), (0,))) + dot(picks[1], scaled[1], ((1,), (0,)))
        sent[m, :, d:] = moved.astype(BF16)
        every(lambda k: go_copy(m, k).start())
        got[m, part(dp)] = sent[m, part(dp)]
        return carry

    lax.fori_loop(0, batches, dispatch, 0)

    tile = 256

    def clear(i, carry):
        cols = pl.ds(pl.multiple_of(i * tile, tile), tile)
        for into in (gin, gin_mine):
            into[:, cols] = jnp.zeros((d, tile), F32)
        for into in (gout, gout_mine):
            into[cols, :] = jnp.zeros((tile, d), F32)
        return carry

    lax.fori_loop(0, hidden // tile, clear, 0)

    def expert_step(m, carry):
        every(lambda k: go_copy(m, k).wait_recv())
        y_acc[...] = jnp.zeros_like(y_acc)
        dx_acc[...] = jnp.zeros_like(dx_acc)

        def chunk(win, wout, gin, gout, i, inner):
            cols = pl.ds(pl.multiple_of(i * tile, tile), tile)
            x = got[m, :, :d]
            dprod = got[m, :, d:]
            w1 = win[:, cols]
            w2 = wout[cols, :]
            pre = dot(x, w1, ((1,), (0,)))
            square = pre * pre
            th = jnp.tanh(GELU_A * pre * (1.0 + GELU_B * square))
            active = (0.5 * pre * (1.0 + th)).astype(BF16)
            slope = 0.5 * (1.0 + th) + 0.5 * pre * (1.0 - th * th) * (GELU_A * (1.0 + 3.0 * GELU_B * square))
            dpre = (dot(dprod, w2, ((1,), (1,))) * slope).astype(BF16)
            gin[:, cols] += dot(x, dpre, ((0,), (0,)))
            gout[cols, :] += dot(active, dprod, ((0,), (0,)))
            y_acc[...] += dot(active, w2, ((1,), (0,)))
            dx_acc[...] += dot(dpre, w1, ((1,), (1,)))
            return inner

        lax.fori_loop(
            0, hidden // tile, functools.partial(chunk, win, wout, gin_mine, gout_mine), 0
        )

        @pl.when(m == 0)
        def _():
            w_copy(0).wait_recv()
            w_copy(1).wait_recv()

        lax.fori_loop(
            0, hidden // tile, functools.partial(chunk, win_got, wout_got, gin, gout), 0
        )
        got[m, :, :d] = y_acc[...].astype(BF16)
        got[m, :, d:] = dx_acc[...].astype(BF16)
        every(lambda k: back_copy(m, k).start())
        ret[m, part(dp)] = got[m, part(dp)]
        return carry

    lax.fori_loop(0, batches, expert_step, 0)

    gin_half[...] = gin[...].astype(BF16)
    gout_half[...] = gout[...].astype(BF16)

    def combine(m, carry):
        every(lambda k: back_copy(m, k).wait_recv())
        codes = code_row[...]
        for i in (other, t):
            picks = [(flat_col[m, image(i), k : k + 1] == codes).astype(F32).astype(BF16) for k in range(2)]
            one = dot(picks[0], ret[m, :, :d], ((1,), (0,)))
            two = dot(picks[1], ret[m, :, :d], ((1,), (0,)))
            d_rows = dot(picks[0] + picks[1], ret[m, :, d:], ((1,), (0,)))
            cot = cot_all[m, image(i)].astype(F32)
            gate = gates[m, image(i)]
            mixture = gate[:, 0:1] * one + gate[:, 1:2] * two
            col = lax.broadcasted_iota(jnp.int32, (rows, 128), 1)
            dg = jnp.where(col == 0, jnp.sum(one * cot, axis=-1, keepdims=True), 0.0)
            dg = dg + jnp.where(col == 1, jnp.sum(two * cot, axis=-1, keepdims=True), 0.0)
            if i is other:
                pay[m, :, :d] = mixture.astype(BF16)
                pay[m, :, d : 2 * d] = d_rows.astype(BF16)
                pay[m, :, 2 * d :] = dg.astype(BF16)
                pay_copy(m).start()
            else:
                mix[m] = mixture
                dx[m] = d_rows
                dgate[m] = dg
        return carry

    gqkv[...] = jnp.zeros_like(gqkv)
    gproj[...] = jnp.zeros_like(gproj)
    grouter[...] = jnp.zeros_like(grouter)
    gnorms[...] = jnp.zeros_like(gnorms)
    low = lax.broadcasted_iota(jnp.int32, (rows, 128), 1) < 64

    def retreat(m):
        pay_copy(m).wait_recv()
        hidden = hidden_in[m]
        out[m] = (hidden + mix[m] + paid[m, :, :d].astype(F32)).astype(BF16)
        unit, inverse = standardise(hidden)
        c = (unit * norms[2:3] + norms[3:4]).astype(BF16)
        probs, lane = gate_softmax(c, router[...], experts)
        dg = dgate[m] + paid[m, :, 2 * d :].astype(F32)
        dprobs = jnp.zeros_like(probs)
        for k in range(2):
            dprobs = dprobs + jnp.where(lane == expert_col[m, image(t), k : k + 1], dg[:, k : k + 1], 0.0)
        dlogits = probs * (dprobs - jnp.sum(dprobs * probs, axis=-1, keepdims=True))
        dc = dx[m] + paid[m, :, d : 2 * d].astype(F32)
        for piece in two_parts(dlogits):
            grouter[...] += dot(c, piece, ((0,), (0,)))
            dc = dc + dot(piece, router[...], ((1,), (1,)))
        gnorms[2:3] += jnp.sum(dc * unit, axis=0, keepdims=True)
        gnorms[3:4] += jnp.sum(dc, axis=0, keepdims=True)
        dhidden = cot_all[m, image(t)].astype(F32) + norm_back(dc * norms[2:3], unit, inverse)
        grad_x[m] = dhidden
        dattn = (live[m] * dhidden).astype(BF16)
        gproj[...] += dot(context[m], dattn, ((0,), (0,)))
        dcontext = dot(dattn, proj[...], ((1,), (1,))).astype(BF16)
        for col, dest in pairs(n_t, block):
            query = mixed[m, :, col : col + 128]
            keys = mixed[m, :, col + block : col + block + 128]
            values = mixed[m, :, col + 2 * block : col + 2 * block + 128]
            grads = dcontext[:, dest : dest + 128]
            zero = jnp.zeros_like(query)
            parts = []
            for own in (low, ~low):
                probs = key_softmax(jnp.where(own, query, zero), keys, count)
                dvalues = dot(probs.astype(BF16), grads, ((0,), (0,)))
                dweights = dot(jnp.where(own, grads, zero), values, ((1,), (1,)))
                dscores = probs * (dweights - jnp.sum(dweights * probs, axis=-1, keepdims=True))
                dscores = dscores.astype(BF16)
                parts.append(
                    (dot(dscores, keys, ((1,), (0,))), dot(dscores, query, ((0,), (0,))), dvalues)
                )
            for i in range(3):
                both = jnp.where(low, parts[0][i], parts[1][i]).astype(BF16)
                if i == 0:
                    both = both * BF16(factor)
                dmixed[:, col + i * block : col + i * block + 128] = both
        unit, inverse = standardise(x_in[m].astype(F32))
        a = (unit * norms[0:1] + norms[1:2]).astype(BF16)
        gqkv[...] += dot(a, dmixed[...], ((0,), (0,)))
        da = dot(dmixed[...], qkv[...], ((1,), (1,)))
        gnorms[0:1] += jnp.sum(da * unit, axis=0, keepdims=True)
        gnorms[1:2] += jnp.sum(da, axis=0, keepdims=True)
        grad_x[m] += norm_back(da * norms[0:1], unit, inverse)

    pieces = 4

    def finish(m, carry):
        for i in range(pieces):

            @pl.when(m == i)
            def _(i=i):
                grad_copy(i).start()

        @pl.when(m < batches)
        def _():
            combine(m, 0)

        @pl.when(m > 0)
        def _():
            retreat(m - 1)

        return carry

    lax.fori_loop(0, batches + 1, finish, 0)
    for i in range(batches + 1, pieces):
        grad_copy(i).start()
    gqkv_out[...] = gqkv[...].astype(BF16)
    gproj_out[...] = gproj[...].astype(BF16)
    for i in range(pieces):
        grad_copy(i).wait()
    gin_mine[...] += gin_got[...].astype(F32)
    gout_mine[...] += gout_got[...].astype(F32)
    w_copy(0).wait_send()
    w_copy(1).wait_send()

    def drain(m, carry):
        c_copy(m).wait_send()
        pay_copy(m).wait_send()
        every(lambda k: go_copy(m, k).wait_send())
        every(lambda k: back_copy(m, k).wait_send())
        return carry

    lax.fori_loop(0, batches, drain, 0)


def moe(c_own, cot_all, router, flat, expert_of, codes, win, wout, saved, experts, n_dp, n_t, block, count, factor):
    batches, rows, d = c_own.shape
    slots = codes.shape[0]
    half = win.shape[1]
    wide = saved[2].shape[2]
    dma = pltpu.SemaphoreType.DMA
    return pl.pallas_call(
        functools.partial(moe_kernel, experts, n_t, block, count, factor),
        out_shape=[
            jax.ShapeDtypeStruct((batches, rows, d), BF16),
            jax.ShapeDtypeStruct((batches, rows, d), F32),
            jax.ShapeDtypeStruct((d, wide), BF16),
            jax.ShapeDtypeStruct((d, d), BF16),
            jax.ShapeDtypeStruct((d, router.shape[1]), F32),
            jax.ShapeDtypeStruct((8, d), F32),
            jax.ShapeDtypeStruct((d, half), F32),
            jax.ShapeDtypeStruct((half, d), F32),
        ],
        in_specs=[ANYWHERE] * 18,
        out_specs=[ANYWHERE] * 8,
        scratch_shapes=[
            pltpu.VMEM((batches, 2 * rows, d), BF16),
            pltpu.VMEM((batches, 2 * rows, 128), F32),
            pltpu.VMEM((batches, slots, 2 * d), BF16),
            pltpu.VMEM((batches, slots, 2 * d), BF16),
            pltpu.VMEM((batches, slots, 2 * d), BF16),
            pltpu.VMEM((batches, rows, 2 * d + 128), BF16),
            pltpu.VMEM((batches, rows, 2 * d + 128), BF16),
            pltpu.VMEM((batches, rows, d), F32),
            pltpu.VMEM((batches, rows, d), F32),
            pltpu.VMEM((batches, rows, 128), F32),
            pltpu.VMEM((rows, wide), BF16),
            pltpu.VMEM((d, wide), F32),
            pltpu.VMEM((d, d), F32),
            pltpu.VMEM((slots, d), F32),
            pltpu.VMEM((slots, d), F32),
            pltpu.VMEM((d, half), BF16),
            pltpu.VMEM((half, d), BF16),
            pltpu.VMEM((d, half), F32),
            pltpu.VMEM((half, d), F32),
            pltpu.VMEM((d, half), BF16),
            pltpu.VMEM((half, d), BF16),
            pltpu.VMEM((d, half), BF16),
            pltpu.VMEM((half, d), BF16),
            dma((2, 2)),
            dma((2, batches)),
            dma((batches, n_dp - 1)),
            dma((batches, n_dp - 1)),
            dma((batches, n_dp - 1)),
            dma((batches, n_dp - 1)),
            dma((2, batches)),
            dma((2, 4)),
        ],
        compiler_params=pltpu.CompilerParams(
            collective_id=2, has_side_effects=True, vmem_limit_bytes=67043328
        ),
    )(
        c_own,
        cot_all,
        router,
        flat,
        flat.transpose(0, 2, 1),
        expert_of.transpose(0, 2, 1),
        codes[None, :],
        codes[:, None],
        win,
        wout,
        *saved,
    )


def general(
    tokens,
    w_qkv,
    w_proj,
    w_in,
    w_out,
    w_router,
    gain_attn,
    shift_attn,
    gain_moe,
    shift_moe,
    live_rows,
    chosen,
    priority,
    cotangent,
):
    batches, own_rows, d = tokens.shape
    rows = live_rows.shape[1]
    n_dp = lax.axis_size("dp")
    n_t = lax.axis_size("tensor")
    t = lax.axis_index("tensor")
    heads_here = w_qkv.shape[1]
    heads = heads_here * n_t
    width = w_qkv.shape[2] // 3
    experts = w_in.shape[0] * n_dp
    cap = 2 * rows // experts
    share = cap // n_t
    images = rows // SEQ
    span = images * SEQ
    per = -(-images // n_t)
    work = per * SEQ
    total = n_t * work
    factor = width ** (-0.5)
    highest = lax.Precision.HIGHEST

    small = jnp.concatenate(
        [w_router] + [v[:, None] for v in (gain_attn, shift_attn, gain_moe, shift_moe)], axis=1
    )
    small = jnp.pad(small, ((0, 0), (0, 128 - small.shape[1])))
    block = heads_here * width
    qkv_block = w_qkv.reshape(-1, heads_here, 3, width).transpose(0, 2, 1, 3).reshape(-1, 3 * block)
    fill = -3 * block % 128
    qkv_block = jnp.pad(qkv_block, ((0, 0), (0, fill)))
    qkv, proj, small = gather_weights(qkv_block, w_proj.reshape(-1, d), small, n_dp, n_t)
    qkv = qkv.reshape(d, n_t, 3 * block + fill)[:, :, : 3 * block].reshape(d, -1)
    router = small[:, :experts]
    gain_one, shift_one, gain_two, shift_two = (small[:, experts + i].astype(F32) for i in range(4))
    proj = proj.reshape(n_dp, n_t, heads_here, w_proj.shape[1], d)
    proj = proj.transpose(1, 2, 0, 3, 4).reshape(heads * width, d)
    win = lax.all_gather(w_in[0], "tensor", axis=1, tiled=True)
    wout = lax.all_gather(w_out[0], "tensor", axis=0, tiled=True)
    cot_all = lax.all_gather(cotangent, "tensor", axis=1, tiled=True)

    def pad_rows(v, n):
        return jnp.pad(v, ((0, 0), (0, n - v.shape[1])) + ((0, 0),) * (v.ndim - 2))

    def own(v):
        return lax.dynamic_slice_in_dim(v, t * work, work, 1)

    edge = own_rows - work
    direct = n_t == 2 and per == 1 and edge >= 0
    if direct:
        moved = lax.ppermute(tokens[:, work:], "tensor", [(0, 1)])
        x = jnp.where(
            t == 0, tokens[:, :work], jnp.concatenate([moved, tokens[:, : work - edge]], axis=1)
        )
    else:
        x = own(pad_rows(lax.all_gather(tokens, "tensor", axis=1, tiled=True)[:, :span], total))
    x = x.astype(F32)
    live = live_rows[:, :span]
    live_all = pad_rows(live, total)
    live_own = own(live_all).astype(F32)[:, :, None]
    cot_all = pad_rows(cot_all[:, :span], total)
    dy = own(cot_all).astype(F32)

    rank = priority[:, 0, :span]
    first, second = chosen[:, :span, 0], chosen[:, :span, 1]
    labels = jnp.arange(experts, dtype=jnp.int32)
    earlier = (rank[:, None, :] < rank[:, :, None]).astype(BF16)
    hit_one = (first[:, :, None] == labels).astype(F32)
    hit_two = (second[:, :, None] == labels).astype(F32)
    live_one = hit_one * live[:, :, None].astype(F32)
    live_two = hit_two * live[:, :, None].astype(F32)
    counts = jnp.einsum(
        "mrs,mse->mre",
        earlier,
        jnp.concatenate([live_one, live_two], axis=-1).astype(BF16),
        preferred_element_type=F32,
    )
    first_total = jnp.sum(live_one, axis=1, keepdims=True)
    slot_one = jnp.sum(counts[:, :, :experts] * hit_one, axis=-1).astype(jnp.int32)
    slot_two = jnp.sum((counts[:, :, experts:] + first_total) * hit_two, axis=-1).astype(jnp.int32)
    keep_one = (live > 0) & (slot_one < cap)
    keep_two = (live > 0) & (slot_two < cap)
    flat_one = jnp.where(keep_one, first * cap + slot_one, -1)
    flat_two = jnp.where(keep_two, second * cap + slot_two, -1)

    def spread(v, fill):
        return jnp.pad(v, ((0, 0), (0, total - span)), constant_values=fill)

    flat_one, flat_two = spread(flat_one, -1), spread(flat_two, -1)
    keep_one, keep_two = spread(keep_one, False), spread(keep_two, False)
    first, second = spread(first, 0), spread(second, 0)
    codes = (jnp.arange(experts)[:, None] * cap + t * share + jnp.arange(share)[None, :]).reshape(-1)
    pick_one = flat_one[:, None, :] == codes[None, :, None]
    pick_two = flat_two[:, None, :] == codes[None, :, None]

    normed_one = layer_norm(x, gain_one, shift_one).astype(BF16)
    mixed = dot(normed_one, qkv, ((2,), (0,)))
    split = heads * width
    shape = (batches * per, SEQ, heads, width)
    mixed = mixed.reshape(batches, work, n_t, 3, block)
    query = (mixed[:, :, :, 0] * factor).astype(BF16).reshape(shape)
    keys = mixed[:, :, :, 1].astype(BF16).reshape(shape)
    values = mixed[:, :, :, 2].astype(BF16).reshape(shape)
    scores = jnp.einsum("iqhc,ikhc->ihqk", query, keys, preferred_element_type=F32)
    probs = jax.nn.softmax(scores, axis=-1)
    weights = probs.astype(BF16)
    context = jnp.einsum("ihqk,ikhc->iqhc", weights, values, preferred_element_type=F32)
    context = context.astype(BF16).reshape(batches, work, split)
    attn = dot(context, proj, ((2,), (0,)))
    hidden = x + live_own * attn
    normed_two = layer_norm(hidden, gain_two, shift_two).astype(BF16)

    c_all = lax.all_gather(normed_two, "tensor", axis=1, tiled=True)
    gate_probs = jax.nn.softmax(dot(c_all, router, ((2,), (0,))), axis=-1)
    hits_one = (first[:, :, None] == labels).astype(F32)
    hits_two = (second[:, :, None] == labels).astype(F32)
    gate_one = jnp.sum(gate_probs * hits_one, axis=-1) * keep_one
    gate_two = jnp.sum(gate_probs * hits_two, axis=-1) * keep_two
    picked = (pick_one | pick_two).astype(BF16)
    sent = jnp.einsum(
        "mqr,mrd->mqd",
        picked,
        jnp.concatenate([c_all, cot_all], axis=-1),
        preferred_element_type=F32,
    )
    gate_slot = jnp.sum(
        jnp.where(pick_one, gate_one[:, None, :], 0.0) + jnp.where(pick_two, gate_two[:, None, :], 0.0),
        axis=-1,
        keepdims=True,
    )
    sent = jnp.concatenate(
        [sent[..., :d].astype(BF16), (sent[..., d:] * gate_slot).astype(BF16)], axis=-1
    )
    sent = sent.reshape(batches, experts, share, 2 * d)
    got = lax.all_to_all(sent, "dp", 1, 1, tiled=True).reshape(-1, 2 * d)
    produced, d_in, grad_in, grad_out = expert(got[:, :d], got[:, d:], win, wout)
    back = jnp.concatenate([produced, d_in], axis=-1).reshape(batches, n_dp, share, 2 * d)
    back = lax.all_to_all(back, "dp", 1, 1, tiled=True).reshape(batches, experts * share, 2 * d)
    grad_in = lax.psum_scatter(grad_in, "tensor", scatter_dimension=1, tiled=True).astype(F32)
    grad_out = lax.psum_scatter(grad_out, "tensor", scatter_dimension=0, tiled=True).astype(F32)

    part_one = jnp.einsum("mqr,mqd->mrd", pick_one.astype(BF16), back[..., :d], preferred_element_type=F32)
    part_two = jnp.einsum("mqr,mqd->mrd", pick_two.astype(BF16), back[..., :d], preferred_element_type=F32)
    d_rows = jnp.einsum("mqr,mqd->mrd", picked, back[..., d:], preferred_element_type=F32)
    mixture = gate_one[:, :, None] * part_one + gate_two[:, :, None] * part_two
    cot_wide = cot_all.astype(F32)
    dgate_one = jnp.sum(part_one * cot_wide, axis=-1, keepdims=True)
    dgate_two = jnp.sum(part_two * cot_wide, axis=-1, keepdims=True)
    dgates = jnp.concatenate([dgate_one, dgate_two], axis=-1)
    payload = jnp.concatenate(
        [mixture, d_rows, jnp.pad(dgates, ((0, 0), (0, 0), (0, 126)))], axis=-1
    ).astype(BF16)
    pieces = payload.reshape(batches, n_t, work, payload.shape[-1])

    def piece(k):
        return lax.dynamic_index_in_dim(pieces, (t + k) % n_t, 1, keepdims=False)

    payload = piece(0).astype(F32)
    for k in range(1, n_t):
        payload = payload + lax.ppermute(
            piece(k), "tensor", [(j, (j + k) % n_t) for j in range(n_t)]
        ).astype(F32)
    output = (hidden + payload[..., :d]).astype(BF16)
    dgates = payload[..., 2 * d : 2 * d + 2]

    own_probs = own(gate_probs)
    dprobs = own(hits_one) * dgates[..., 0:1] * own(keep_one)[:, :, None]
    dprobs = dprobs + own(hits_two) * dgates[..., 1:2] * own(keep_two)[:, :, None]
    dlogits = own_probs * (dprobs - jnp.sum(dprobs * own_probs, axis=-1, keepdims=True))
    grad_router = lax.dot_general(
        normed_two.astype(F32), dlogits, (((0, 1), (0, 1)), ((), ())), precision=highest
    )
    dc = payload[..., d : 2 * d] + lax.dot_general(
        dlogits, router.astype(F32), (((2,), (1,)), ((), ())), precision=highest
    )
    _, back_two = jax.vjp(layer_norm, hidden, gain_two, shift_two)
    dnorm, grad_gain_two, grad_shift_two = back_two(dc)
    dhidden = dy + dnorm
    dattn = (live_own * dhidden).astype(BF16)

    grad_proj = dot(context, dattn, ((0, 1), (0, 1)))
    dcontext = dot(dattn, proj, ((2,), (1,))).astype(BF16).reshape(shape)
    dvalues = jnp.einsum("ihqk,iqhc->ikhc", weights, dcontext, preferred_element_type=F32).astype(BF16)
    dweights = jnp.einsum("iqhc,ikhc->ihqk", dcontext, values, preferred_element_type=F32)
    dscores = (probs * (dweights - jnp.sum(dweights * probs, axis=-1, keepdims=True))).astype(BF16)
    dquery = jnp.einsum("ihqk,ikhc->iqhc", dscores, keys, preferred_element_type=F32).astype(BF16)
    dkeys = jnp.einsum("ihqk,iqhc->ikhc", dscores, query, preferred_element_type=F32).astype(BF16)
    dmixed = jnp.stack(
        [v.reshape(batches, work, n_t, block) for v in (dquery * BF16(factor), dkeys, dvalues)], axis=3
    ).reshape(batches, work, 3 * split)
    grad_qkv = dot(normed_one, dmixed, ((0, 1), (0, 1)))
    da = dot(dmixed, qkv, ((2,), (1,)))
    _, back_one = jax.vjp(layer_norm, x, gain_one, shift_one)
    dnorm, grad_gain_one, grad_shift_one = back_one(da)
    grad_x = dhidden + dnorm

    if direct:
        out_edge = lax.ppermute(output[:, :edge], "tensor", [(1, 0)])
        grad_edge = lax.ppermute(grad_x[:, :edge], "tensor", [(1, 0)])
        result = jnp.where(
            t == 0,
            jnp.concatenate([output, out_edge], axis=1),
            jnp.concatenate([output[:, edge:], tokens[:, work - edge :]], axis=1),
        )
        grad_tokens = jnp.where(
            t == 0,
            jnp.concatenate([grad_x, grad_edge], axis=1),
            jnp.concatenate([grad_x[:, edge:], cotangent[:, work - edge :].astype(F32)], axis=1),
        )
    else:
        here = (t * own_rows + jnp.arange(own_rows) < span)[None, :, None]

        def home(v, rest):
            full = pad_rows(lax.all_gather(v, "tensor", axis=1, tiled=True)[:, :span], rows)
            return jnp.where(here, lax.dynamic_slice_in_dim(full, t * own_rows, own_rows, 1), rest)

        result = home(output, tokens)
        grad_tokens = home(grad_x, cotangent.astype(F32))

    nz, ny = grid_sizes(n_dp)
    grad_qkv = jnp.pad(grad_qkv.astype(BF16).reshape(d, n_t, 3 * block), ((0, 0), (0, 0), (0, fill)))
    grad_qkv = grad_qkv.reshape(nz, ny, 2, d // n_dp, -1)
    grad_proj = grad_proj.astype(BF16).reshape(n_t, heads_here, n_dp, -1, d)
    grad_proj = grad_proj.transpose(2, 0, 1, 3, 4).reshape(nz, ny, 2, n_t, -1, d)
    smalls = jnp.concatenate(
        [grad_router] + [v[:, None] for v in (grad_gain_one, grad_shift_one, grad_gain_two, grad_shift_two)],
        axis=1,
    )
    smalls = jnp.pad(smalls, ((0, 0), (0, 128 - smalls.shape[1]))).reshape(nz, ny, 2, n_t, -1, 128)
    grad_qkv, grad_proj, smalls = scatter_grads(grad_qkv, grad_proj, smalls, n_dp, n_t)
    grad_qkv = grad_qkv[:, : 3 * block].reshape(-1, 3, heads_here, width).transpose(0, 2, 1, 3)
    return (
        result,
        grad_tokens,
        grad_qkv.reshape(w_qkv.shape),
        grad_proj.reshape(w_proj.shape),
        grad_in[None],
        grad_out[None],
        smalls[:, :experts],
        smalls[:, experts],
        smalls[:, experts + 1],
        smalls[:, experts + 2],
        smalls[:, experts + 3],
    )


def attend_kernel(n_t, block, count, factor, x, live, norms, qkv, proj, c_out, hidden_out, mixed_out, context_out):
    xf = x[0].astype(F32)
    unit, _ = standardise(xf)
    a = (unit * norms[0:1] + norms[1:2]).astype(BF16)
    for s in range(n_t):
        for i in range(3):
            cols = slice((3 * s + i) * block, (3 * s + i + 1) * block)
            part = dot(a, qkv[:, cols], ((1,), (0,)))
            mixed_out[0, :, cols] = (part * factor if i == 0 else part).astype(BF16)
    low = lax.broadcasted_iota(jnp.int32, (x.shape[1], 128), 1) < 64
    for col, dest in pairs(n_t, block):
        query = mixed_out[0, :, col : col + 128]
        keys = mixed_out[0, :, col + block : col + block + 128]
        values = mixed_out[0, :, col + 2 * block : col + 2 * block + 128]
        zero = jnp.zeros_like(query)
        parts = []
        for own in (low, ~low):
            probs = key_softmax(jnp.where(own, query, zero), keys, count)
            parts.append(dot(probs.astype(BF16), values, ((1,), (0,))))
        context_out[0, :, dest : dest + 128] = jnp.where(low, parts[0], parts[1]).astype(BF16)
    hidden = xf + live[0] * dot(context_out[0], proj[...], ((1,), (0,)))
    hidden_out[0] = hidden
    unit, _ = standardise(hidden)
    c_out[0] = (unit * norms[2:3] + norms[3:4]).astype(BF16)


def attend(x, live, norms, qkv, proj, n_t, block, count, factor):
    batches, rows, d = x.shape
    wide = qkv.shape[1]

    def each(n):
        return pl.BlockSpec((1, rows, n), lambda m: (m, 0, 0))

    def fixed(shape):
        return pl.BlockSpec(shape, lambda m: (0, 0))

    return pl.pallas_call(
        functools.partial(attend_kernel, n_t, block, count, factor),
        grid=(batches,),
        in_specs=[each(d), each(1), fixed(norms.shape), fixed(qkv.shape), fixed(proj.shape)],
        out_specs=[each(d), each(d), each(wide), each(d)],
        out_shape=[
            jax.ShapeDtypeStruct((batches, rows, d), BF16),
            jax.ShapeDtypeStruct((batches, rows, d), F32),
            jax.ShapeDtypeStruct((batches, rows, wide), BF16),
            jax.ShapeDtypeStruct((batches, rows, d), BF16),
        ],
        compiler_params=pltpu.CompilerParams(vmem_limit_bytes=32 * 1024 * 1024),
        cost_estimate=pl.CostEstimate(
            flops=2 * batches * rows * d * (wide + d), transcendentals=0, bytes_accessed=8 * batches * rows * d
        ),
    )(x, live, norms, qkv, proj)


def fast(
    tokens,
    w_qkv,
    w_proj,
    w_in,
    w_out,
    w_router,
    gain_attn,
    shift_attn,
    gain_moe,
    shift_moe,
    live_rows,
    chosen,
    priority,
    cotangent,
):
    batches, own_rows, d = tokens.shape
    rows = live_rows.shape[1]
    n_dp = lax.axis_size("dp")
    n_t = lax.axis_size("tensor")
    t = lax.axis_index("tensor")
    heads_here = w_qkv.shape[1]
    width = w_qkv.shape[2] // 3
    block = heads_here * width
    experts = n_dp
    cap = 2 * rows // experts
    share = cap // n_t
    span = n_t * SEQ
    padded = -(-SEQ // 16) * 16
    edge = own_rows - SEQ
    factor = width ** (-0.5)

    small = jnp.concatenate(
        [w_router] + [v[:, None] for v in (gain_attn, shift_attn, gain_moe, shift_moe)], axis=1
    )
    small = jnp.pad(small, ((0, 0), (0, 128 - small.shape[1])))
    qkv_block = w_qkv.reshape(-1, heads_here, 3, width).transpose(0, 2, 1, 3).reshape(-1, 3 * block)
    qkv, proj, small, cot_all, moved = gather_weights(
        qkv_block, w_proj.reshape(-1, d), small, n_dp, n_t, (cotangent, tokens[:, SEQ:])
    )
    cot_all = cot_all.transpose(1, 0, 2, 3).reshape(batches, rows, d)
    router = jnp.where(jnp.arange(128) < experts, small, 0)
    norms = jnp.pad(small[:, experts : experts + 4].astype(F32).T, ((0, 4), (0, 0)))
    proj = proj.reshape(n_dp, n_t, heads_here, w_proj.shape[1], d)
    proj = proj.transpose(1, 2, 0, 3, 4).reshape(n_t * block, d)

    def pad_rows(v, axis, fill=0):
        spec = [(0, 0)] * v.ndim
        spec[axis] = (0, padded - SEQ)
        return jnp.pad(v, spec, constant_values=fill)

    def lay(v, axis, fill=0):
        shape = v.shape
        v = v.reshape(shape[:axis] + (n_t, SEQ) + shape[axis + 1 :])
        v = pad_rows(v, axis + 1, fill)
        return v.reshape(shape[:axis] + (n_t * padded,) + shape[axis + 1 :])

    def own(v, axis):
        return lax.dynamic_slice_in_dim(v, t * padded, padded, axis)

    x = jnp.where(t == 0, tokens[:, :SEQ], jnp.concatenate([moved, tokens[:, : SEQ - edge]], axis=1))
    x = pad_rows(x, 1)
    cot_all = lay(cot_all[:, :span], 1)

    live = live_rows[:, :span]
    rank = priority[:, 0, :span]
    picks = chosen[:, :span].transpose(0, 2, 1)
    labels = jnp.arange(experts, dtype=jnp.int32)
    earlier = (rank[:, None, :] < rank[:, :, None]).astype(BF16)
    hits = (picks[..., None] == labels).astype(F32)
    live_hits = hits * live[:, None, :, None].astype(F32)
    ahead = jnp.einsum("mrs,mkse->mkre", earlier, live_hits.astype(BF16), preferred_element_type=F32)
    firsts = jnp.sum(live_hits[:, :1], axis=2, keepdims=True)
    ahead = ahead + jnp.concatenate([jnp.zeros_like(firsts), firsts], axis=1)
    slot = jnp.sum(ahead * hits, axis=-1).astype(jnp.int32)
    keep = (live[:, None, :] > 0) & (slot < cap)
    flat = lay(jnp.where(keep, picks * cap + slot, -1), 2, -1)
    expert_of = lay(jnp.where(keep, picks, -1), 2, -1)
    codes = (jnp.arange(experts)[:, None] * cap + t * share + jnp.arange(share)[None, :]).reshape(-1)
    live_own = own(lay(live.astype(F32)[:, :, None], 1), 1)

    c, hidden, mixed, context = attend(x, live_own, norms, qkv, proj, n_t, block, SEQ, factor)
    output, grad_x, grad_qkv, grad_proj, grad_router, grad_norms, grad_in, grad_out = moe(
        c,
        cot_all,
        router,
        flat,
        expert_of,
        codes,
        w_in[0],
        w_out[0],
        (x, hidden, mixed, context, live_own, norms, qkv, proj),
        experts,
        n_dp,
        n_t,
        block,
        SEQ,
        factor,
    )

    out_edge = lax.ppermute(output[:, :edge], "tensor", [(1, 0)])
    grad_edge = lax.ppermute(grad_x[:, :edge], "tensor", [(1, 0)])
    rest = SEQ - edge

    def home(v, moved_rows, other):
        return jnp.where(
            t == 0,
            jnp.concatenate([v[:, :SEQ], moved_rows], axis=1),
            jnp.concatenate([v[:, edge:SEQ], other[:, rest:].astype(v.dtype)], axis=1),
        )

    nz, ny = grid_sizes(n_dp)
    grad_proj = grad_proj.reshape(n_t, heads_here, n_dp, -1, d)
    grad_proj = grad_proj.transpose(2, 0, 1, 3, 4).reshape(nz, ny, 2, n_t, -1, d)
    lane = jnp.arange(128)
    smalls = jnp.where(lane < experts, grad_router, 0.0)
    smalls = smalls + jnp.pad(grad_norms[:4].T, ((0, 0), (experts, 124 - experts)))
    grad_qkv, grad_proj, smalls = scatter_grads(
        grad_qkv.reshape(nz, ny, 2, d // n_dp, -1), grad_proj, smalls.reshape(nz, ny, 2, n_t, -1, 128), n_dp, n_t
    )
    grad_qkv = grad_qkv.reshape(-1, 3, heads_here, width).transpose(0, 2, 1, 3)
    return (
        home(output, out_edge, tokens),
        home(grad_x, grad_edge, cotangent),
        grad_qkv.reshape(w_qkv.shape),
        grad_proj.reshape(w_proj.shape),
        grad_in[None],
        grad_out[None],
        smalls[:, :experts],
        smalls[:, experts],
        smalls[:, experts + 1],
        smalls[:, experts + 2],
        smalls[:, experts + 3],
    )


def local(*args):
    tokens, w_qkv, live_rows = args[0], args[1], args[10]
    n_t = lax.axis_size("tensor")
    images = live_rows.shape[1] // SEQ
    block = w_qkv.shape[1] * (w_qkv.shape[2] // 3)
    if n_t == 2 and images == 2 and tokens.shape[1] >= SEQ and block % 128 == 0 and w_qkv.shape[2] == 192:
        return fast(*args)
    return general(*args)


def solution(mesh):
    both = ("dp", "tensor")
    return jax.shard_map(
        local,
        mesh=mesh,
        in_specs=(
            P(None, both, None),
            P("dp", "tensor", None),
            P("tensor", "dp", None),
            P("dp", None, "tensor"),
            P("dp", "tensor", None),
            P(both, None),
            P(both),
            P(both),
            P(both),
            P(both),
            P(None, "dp"),
            P(None, "dp", None),
            P(None, "dp", None),
            P(None, both, None),
        ),
        out_specs=(
            P(None, both, None),
            P(None, both, None),
            P("dp", "tensor", None),
            P("tensor", "dp", None),
            P("dp", None, "tensor"),
            P("dp", "tensor", None),
            P(both, None),
            P(both),
            P(both),
            P(both),
            P(both),
        ),
        check_vma=False,
    )
```

```python
import functools

import jax
import jax.numpy as jnp
from jax import lax
from jax.experimental import pallas as pl
from jax.experimental.pallas import tpu as pltpu
from jax.sharding import PartitionSpec as P

SEQ = 197
EPS = 1e-06
F32 = jnp.float32
BF16 = jnp.bfloat16
GELU_A = 0.7978845608028654
GELU_B = 0.044715


def dot(a, b, dims):
    return lax.dot_general(a, b, (dims, ((), ())), preferred_element_type=F32)


def layer_norm(values, gain_vec, shift_vec):
    centre = jnp.mean(values, axis=-1, keepdims=True)
    centered = values - centre
    spread = jnp.mean(centered * centered, axis=-1, keepdims=True)
    return centered * lax.rsqrt(spread + EPS) * gain_vec + shift_vec


def expert_kernel(x_ref, dp_ref, win_ref, wout_ref, y_ref, dx_ref, gin_ref, gout_ref, y_acc, dx_acc):
    step = pl.program_id(0)
    last = pl.num_programs(0) - 1
    x = x_ref[...]
    dprod = dp_ref[...]
    win = win_ref[...]
    wout = wout_ref[...]
    pre = dot(x, win, ((1,), (0,)))
    square = pre * pre
    th = jnp.tanh(GELU_A * pre * (1.0 + GELU_B * square))
    active = (0.5 * pre * (1.0 + th)).astype(BF16)
    slope = 0.5 * (1.0 + th) + 0.5 * pre * (1.0 - th * th) * (GELU_A * (1.0 + 3.0 * GELU_B * square))
    dact = dot(dprod, wout, ((1,), (1,)))
    dpre = (dact * slope).astype(BF16)
    gin_ref[...] = dot(x, dpre, ((0,), (0,))).astype(BF16)
    gout_ref[...] = dot(active, dprod, ((0,), (0,))).astype(BF16)
    part_y = dot(active, wout, ((1,), (0,)))
    part_dx = dot(dpre, win, ((1,), (1,)))

    @pl.when(step == 0)
    def _():
        y_acc[...] = part_y
        dx_acc[...] = part_dx

    @pl.when(step > 0)
    def _():
        y_acc[...] += part_y
        dx_acc[...] += part_dx

    @pl.when(step == last)
    def _():
        y_ref[...] = y_acc[...].astype(BF16)
        dx_ref[...] = dx_acc[...].astype(BF16)


def expert(x, dprod, win, wout, tile=256):
    n, d = x.shape
    ff = win.shape[1]
    return pl.pallas_call(
        expert_kernel,
        grid=(ff // tile,),
        in_specs=[
            pl.BlockSpec((n, d), lambda i: (0, 0)),
            pl.BlockSpec((n, d), lambda i: (0, 0)),
            pl.BlockSpec((d, tile), lambda i: (0, i)),
            pl.BlockSpec((tile, d), lambda i: (i, 0)),
        ],
        out_specs=[
            pl.BlockSpec((n, d), lambda i: (0, 0)),
            pl.BlockSpec((n, d), lambda i: (0, 0)),
            pl.BlockSpec((d, tile), lambda i: (0, i)),
            pl.BlockSpec((tile, d), lambda i: (i, 0)),
        ],
        out_shape=[
            jax.ShapeDtypeStruct((n, d), BF16),
            jax.ShapeDtypeStruct((n, d), BF16),
            jax.ShapeDtypeStruct((d, ff), BF16),
            jax.ShapeDtypeStruct((ff, d), BF16),
        ],
        scratch_shapes=[pltpu.VMEM((n, d), F32), pltpu.VMEM((n, d), F32)],
        compiler_params=pltpu.CompilerParams(vmem_limit_bytes=60 * 1024 * 1024),
        cost_estimate=pl.CostEstimate(
            flops=12 * n * d * ff, transcendentals=n * ff, bytes_accessed=8 * n * d + 8 * d * ff
        ),
    )(x, dprod, win, wout)


MESH = pl.DeviceIdType.MESH
ANYWHERE = pl.BlockSpec(memory_space=pltpu.VMEM)


def grid_sizes(n_dp):
    ny = 1
    while 2 * ny * 2 * ny <= n_dp // 2:
        ny *= 2
    return n_dp // (2 * ny), ny


def position(ny):
    dp = lax.axis_index("dp")
    return dp, lax.axis_index("tensor"), dp % 2, (dp // 2) % ny, dp // (2 * ny)


def neighbours(ny, nz, n_t):
    dp, t, c, y, z = position(ny)

    def along_core(k):
        return (dp - c + (c + k) % 2, t)

    def along_tensor(k):
        return (dp, (t + k) % n_t)

    def along_y(k):
        return (dp + ((y + k) % ny - y) * 2, t)

    def along_z(k):
        return (dp + ((z + k) % nz - z) * 2 * ny, t)

    return {"core": (2, along_core), "tensor": (n_t, along_tensor), "y": (ny, along_y), "z": (nz, along_z)}


def greet(stages):
    barrier = pltpu.get_barrier_semaphore()
    count = 0
    for size, device in stages.values():
        for k in range(1, size):
            pl.semaphore_signal(barrier, inc=1, device_id=device(k), device_id_type=MESH)
            count += 1
    pl.semaphore_wait(barrier, count)


def gather_kernel(ny, nz, n_t, extras, *refs):
    (qkv, proj, small), refs = refs[:3], refs[3:]
    side, refs = refs[:extras], refs[extras:]
    (qkv_out, proj_out, small_out), refs = refs[:3], refs[3:]
    side_out, (send, recv, copied) = refs[:extras], refs[extras:]
    dp, t, c, y, z = position(ny)
    stages = neighbours(ny, nz, n_t)
    greet(stages)
    cols, wide = qkv.shape[1], proj.shape[1]
    whole = slice(None)
    slot = 0

    def start(pieces, device):
        nonlocal slot
        copies = []
        for src, dst in pieces:
            copies.append(
                pltpu.make_async_remote_copy(
                    src_ref=src,
                    dst_ref=dst,
                    send_sem=send.at[slot],
                    recv_sem=recv.at[slot],
                    device_id=device,
                    device_id_type=MESH,
                )
            )
            copies[-1].start()
            slot += 1
        return copies

    def along(name, pieces):
        size, device = stages[name]
        return [copy for k in range(1, size) for copy in start(pieces, device(k))]

    def lanes(ts, half):
        return pl.ds(pl.multiple_of(ts * cols + half * (cols // 2), 128), cols // 2)

    def views(zs, ys, ts, half):
        band = slice(half * (wide // 2), (half + 1) * (wide // 2))
        parts = [qkv_out.at[zs, ys, c, :, lanes(i, half)] for i in ts]
        if len(ts) == 1:
            parts.append(proj_out.at[zs, ys, c, ts[0], :, band])
            if half == 0:
                parts.append(small_out.at[zs, ys, c, ts[0]])
        else:
            parts.append(proj_out.at[zs, ys, c, :, :, band])
        return [(part, part) for part in parts]

    aside = start([(side[i], side_out[i]) for i in range(extras)], (dp, 1 - t)) if extras else []
    mine = (
        qkv_out.at[z, y, c, :, pl.ds(pl.multiple_of(t * cols, 128), cols)],
        proj_out.at[z, y, c, t],
        small_out.at[z, y, c, t],
    )
    inputs = list(zip((qkv, proj, small), mine))
    local = [pltpu.make_async_copy(src, dst, copied.at[i]) for i, (src, dst) in enumerate(inputs)]
    for copy in local:
        copy.start()
    for copy in along("z", inputs) + local:
        copy.wait()
    one = along("y", views(whole, y, [t], 0))
    two = along("tensor", views(whole, y, [t], 1))
    for copy in one:
        copy.wait()
    one = along("tensor", views(whole, whole, [t], 0))
    for copy in two:
        copy.wait()
    two = along("y", views(whole, y, list(range(n_t)), 1))
    for copy in one + two:
        copy.wait()
    rest = [ref.at[:, :, c] for ref in (qkv_out, proj_out, small_out)]
    for copy in along("core", [(part, part) for part in rest]) + aside:
        copy.wait()


def gather_weights(qkv, proj, small, n_dp, n_t, side=()):
    nz, ny = grid_sizes(n_dp)
    slots = 3 * (nz - 1) + 5 * (n_t - 1) + (4 + n_t) * (ny - 1) + 3 + len(side)
    side_shapes = [jax.ShapeDtypeStruct(v.shape, v.dtype) for v in side]
    outs = pl.pallas_call(
        functools.partial(gather_kernel, ny, nz, n_t, len(side)),
        out_shape=[
            jax.ShapeDtypeStruct((nz, ny, 2, qkv.shape[0], n_t * qkv.shape[1]), BF16),
            jax.ShapeDtypeStruct((nz, ny, 2, n_t) + proj.shape, BF16),
            jax.ShapeDtypeStruct((nz, ny, 2, n_t) + small.shape, BF16),
        ]
        + side_shapes,
        in_specs=[ANYWHERE] * (3 + len(side)),
        out_specs=[ANYWHERE] * (3 + len(side)),
        scratch_shapes=[
            pltpu.SemaphoreType.DMA((slots,)),
            pltpu.SemaphoreType.DMA((slots,)),
            pltpu.SemaphoreType.DMA((3,)),
        ],
        compiler_params=pltpu.CompilerParams(collective_id=0, has_side_effects=True),
    )(qkv, proj, small, *side)
    qkv_all = outs[0].reshape(n_dp * qkv.shape[0], n_t * qkv.shape[1])
    return (qkv_all, outs[1].reshape((n_dp, n_t) + proj.shape), outs[2].reshape(-1, small.shape[1])) + tuple(outs[3:])


def scatter_kernel(ny, nz, n_t, *refs):
    ins, refs = refs[:3], refs[3:]
    outs, refs = refs[:3], refs[3:]
    got_core, refs = refs[:3], refs[3:]
    held, refs = refs[:3], refs[3:]
    one_got, one_held, one_last, refs = refs[:3], refs[3:6], refs[6:9], refs[9:]
    two_got, two_held, two_last, refs = refs[:2], refs[2:4], refs[4:6], refs[6:]
    end, end_got, (send, recv) = refs[:3], refs[3:6], refs[6:]
    _, t, c, y, z = position(ny)
    stages = neighbours(ny, nz, n_t)
    greet(stages)
    cols, wide = outs[0].shape[1], outs[1].shape[1]
    slot = 0

    def lanes(ts, half):
        return pl.ds(pl.multiple_of(ts * cols + half * (cols // 2), 128), cols // 2)

    def band(half):
        return slice(half * (wide // 2), (half + 1) * (wide // 2))

    def along(name, me, pieces):
        nonlocal slot
        size, device = stages[name]
        copies = []
        for k in range(1, size):
            for src, dst in pieces((me + k) % size, k - 1):
                copies.append(
                    pltpu.make_async_remote_copy(
                        src_ref=src,
                        dst_ref=dst,
                        send_sem=send.at[slot],
                        recv_sem=recv.at[slot],
                        device_id=device(k),
                        device_id_type=MESH,
                    )
                )
                copies[-1].start()
                slot += 1
        return copies

    def finish(copies):
        for copy in copies:
            copy.wait()

    def total(own, got, index):
        value = own.astype(F32)
        for k in range(got.shape[0]):
            value = value + got[(k,) + index].astype(F32)
        return value

    def loop(count, body):
        def step(n, carry):
            body(n)
            return carry

        lax.fori_loop(0, count, step, 0)

    finish(
        along("core", c, lambda j, k: [(ins[i].at[:, :, j], got_core[i].at[k]) for i in range(3)])
    )

    def add_core(n):
        zi, yi = n // ny, n % ny
        for i in range(3):
            held[i][zi, yi] = total(ins[i][zi, yi, c], got_core[i], (zi, yi)).astype(held[i].dtype)

    loop(nz * ny, add_core)
    one = along(
        "tensor",
        t,
        lambda j, k: [
            (held[0].at[:, :, :, lanes(j, 0)], one_got[0].at[k]),
            (held[1].at[:, :, j, :, band(0)], one_got[1].at[k]),
            (held[2].at[:, :, j], one_got[2].at[k]),
        ],
    )
    two = along(
        "y",
        y,
        lambda j, k: [(held[0].at[:, j, :, lanes(i, 1)], two_got[0].at[k, i]) for i in range(n_t)]
        + [(held[1].at[:, j, i, :, band(1)], two_got[1].at[k, i]) for i in range(n_t)],
    )
    finish(one)

    def add_one(n):
        zi, yi = n // ny, n % ny
        owns = (held[0][zi, yi, :, lanes(t, 0)], held[1][zi, yi, t, :, band(0)], held[2][zi, yi, t])
        for i in range(3):
            one_held[i][zi, yi] = total(owns[i], one_got[i], (zi, yi)).astype(one_held[i].dtype)

    loop(nz * ny, add_one)
    one = along("y", y, lambda j, k: [(one_held[i].at[:, j], one_last[i].at[k]) for i in range(3)])
    finish(two)

    def add_two(zi):
        for i in range(n_t):
            owns = (held[0][zi, y, :, lanes(i, 1)], held[1][zi, y, i, :, band(1)])
            for j in range(2):
                two_held[j][i, zi] = total(owns[j], two_got[j], (i, zi)).astype(two_held[j].dtype)

    loop(nz, add_two)
    two = along("tensor", t, lambda j, k: [(two_held[i].at[j], two_last[i].at[k]) for i in range(2)])
    finish(one)
    halves = [
        (slice(0, cols // 2), slice(cols // 2, cols)),
        (band(0), band(1)),
        (slice(None),),
    ]

    def end_one(zi):
        for i in range(3):
            value = total(one_held[i][zi, y], one_last[i], (zi,))
            end[i][zi, :, halves[i][0]] = value.astype(end[i].dtype)

    loop(nz, end_one)
    finish(two)

    def end_two(zi):
        for i in range(2):
            value = total(two_held[i][t, zi], two_last[i], (zi,))
            end[i][zi, :, halves[i][1]] = value.astype(end[i].dtype)

    loop(nz, end_two)
    finish(along("z", z, lambda j, k: [(end[i].at[j], end_got[i].at[k]) for i in range(3)]))
    for i in range(3):
        outs[i][...] = total(end[i][z], end_got[i], ())


def scatter_grads(qkv, proj, small, n_dp, n_t):
    nz, ny = qkv.shape[:2]
    rows, cols = qkv.shape[3], qkv.shape[4] // n_t
    tails = [(rows, cols), proj.shape[4:], small.shape[4:]]
    kinds = [BF16, BF16, F32]
    parts = [(rows, cols // 2), (proj.shape[4], proj.shape[5] // 2), small.shape[4:]]
    wide = [(rows, n_t * cols), (n_t,) + proj.shape[4:], (n_t,) + small.shape[4:]]

    def room(lead, shapes):
        return [pltpu.VMEM(lead + shape, kind) for shape, kind in zip(shapes, kinds)]

    scratch = room((1, nz, ny), wide) + room((nz, ny), wide)
    scratch += room((n_t - 1, nz, ny), parts) + room((nz, ny), parts) + room((ny - 1, nz), parts)
    scratch += room((ny - 1, n_t, nz), parts[:2]) + room((n_t, nz), parts[:2]) + room((n_t - 1, nz), parts[:2])
    scratch += room((nz,), tails) + room((nz - 1,), tails)
    slots = 3 + 5 * (n_t - 1) + (3 + 2 * n_t) * (ny - 1) + 3 * (nz - 1)
    scratch += [pltpu.SemaphoreType.DMA((slots,)), pltpu.SemaphoreType.DMA((slots,))]
    return pl.pallas_call(
        functools.partial(scatter_kernel, ny, nz, n_t),
        out_shape=[jax.ShapeDtypeStruct(tail, F32) for tail in tails],
        in_specs=[ANYWHERE] * 3,
        out_specs=[ANYWHERE] * 3,
        scratch_shapes=scratch,
        compiler_params=pltpu.CompilerParams(collective_id=1, has_side_effects=True),
    )(qkv, proj, small)


def standardise(v):
    centre = jnp.mean(v, axis=-1, keepdims=True)
    centered = v - centre
    inverse = lax.rsqrt(jnp.mean(centered * centered, axis=-1, keepdims=True) + EPS)
    return centered * inverse, inverse


def norm_back(grad, unit, inverse):
    return inverse * (
        grad
        - jnp.mean(grad, axis=-1, keepdims=True)
        - unit * jnp.mean(grad * unit, axis=-1, keepdims=True)
    )


def two_parts(v):
    high = v.astype(BF16)
    return high, (v - high.astype(F32)).astype(BF16)


def gate_softmax(c, router, experts):
    lane = lax.broadcasted_iota(jnp.int32, (c.shape[0], router.shape[1]), 1)
    logits = jnp.where(lane < experts, dot(c, router, ((1,), (0,))), -1e30)
    raised = jnp.exp(logits - jnp.max(logits, axis=-1, keepdims=True))
    return raised / jnp.sum(raised, axis=-1, keepdims=True), lane


def key_softmax(query, keys, count):
    scores = dot(query, keys, ((1,), (1,)))
    col = lax.broadcasted_iota(jnp.int32, scores.shape, 1)
    scores = jnp.where(col < count, scores, -1e30)
    raised = jnp.exp(scores - jnp.max(scores, axis=-1, keepdims=True))
    return raised * (1.0 / jnp.sum(raised, axis=-1, keepdims=True))


def pairs(n_t, block):
    return [
        (3 * block * s + 128 * i, block * s + 128 * i) for s in range(n_t) for i in range(block // 128)
    ]


def layer_kernel(
    experts,
    n_t,
    block,
    count,
    factor,
    cot_own,
    router,
    flat_row,
    flat_col,
    expert_col,
    code_row,
    code_col,
    win,
    wout,
    x_in,
    live,
    norms,
    qkv,
    proj,
    out,
    grad_x,
    gqkv_out,
    gproj_out,
    grouter,
    gnorms,
    gin_mine,
    gout_mine,
    c_own,
    hidden_in,
    mixed,
    context,
    c_all,
    cot_all,
    gates,
    sent,
    got,
    ret,
    pay,
    paid,
    mix,
    dx,
    dgate,
    dmixed,
    gqkv,
    gproj,
    y_acc,
    dx_acc,
    win_got,
    wout_got,
    gin,
    gout,
    gin_half,
    gout_half,
    gin_got,
    gout_got,
    w_sems,
    c_sems,
    cot_sems,
    go_send,
    go_recv,
    back_send,
    back_recv,
    pay_sems,
    grad_sems,
):
    batches, rows, d = cot_own.shape
    n_dp = lax.axis_size("dp")
    dp, t = lax.axis_index("dp"), lax.axis_index("tensor")
    share = sent.shape[1] // n_dp
    hidden = win.shape[1]
    other = 1 - t
    partner = (dp, other)

    barrier = pltpu.get_barrier_semaphore()
    pl.semaphore_signal(barrier, inc=1, device_id=partner, device_id_type=MESH)

    def hello(k, carry):
        pl.semaphore_signal(barrier, inc=1, device_id=((dp + k) % n_dp, t), device_id_type=MESH)
        return carry

    lax.fori_loop(1, n_dp, hello, 0)
    pl.semaphore_wait(barrier, n_dp)

    def image(i):
        return pl.ds(pl.multiple_of(i * rows, 16), rows)

    def part(i):
        return pl.ds(pl.multiple_of(i * share, 16), share)

    def remote(src, dst, sems, i, j, device):
        return pltpu.make_async_remote_copy(
            src_ref=src,
            dst_ref=dst,
            send_sem=sems[0].at[i, j],
            recv_sem=sems[1].at[i, j],
            device_id=device,
            device_id_type=MESH,
        )

    def c_copy(m):
        return pltpu.make_async_remote_copy(
            src_ref=c_own.at[m],
            dst_ref=c_all.at[m, image(t)],
            send_sem=c_sems.at[0, m],
            recv_sem=c_sems.at[1, m],
            device_id=partner,
            device_id_type=MESH,
        )

    def cot_copy(m):
        return pltpu.make_async_remote_copy(
            src_ref=cot_own.at[m],
            dst_ref=cot_all.at[m, image(t)],
            send_sem=cot_sems.at[0, m],
            recv_sem=cot_sems.at[1, m],
            device_id=partner,
            device_id_type=MESH,
        )

    def go_copy(m, k):
        to = (dp + k) % n_dp
        return remote(sent.at[m, part(to)], got.at[m, part(dp)], (go_send, go_recv), m, k - 1, (to, t))

    def back_copy(m, k):
        to = (dp + k) % n_dp
        return remote(got.at[m, part(to)], ret.at[m, part(dp)], (back_send, back_recv), m, k - 1, (to, t))

    def pay_copy(m):
        return pltpu.make_async_remote_copy(
            src_ref=pay.at[m],
            dst_ref=paid.at[m],
            send_sem=pay_sems.at[0, m],
            recv_sem=pay_sems.at[1, m],
            device_id=partner,
            device_id_type=MESH,
        )

    def grad_copy(i):
        src, dst = ((gin_half, gin_got), (gout_half, gout_got))[i // 2]
        size = src.shape[0] // 2
        band = pl.ds(i % 2 * size, size)
        return pltpu.make_async_remote_copy(
            src_ref=src.at[band],
            dst_ref=dst.at[band],
            send_sem=grad_sems.at[0, i],
            recv_sem=grad_sems.at[1, i],
            device_id=partner,
            device_id_type=MESH,
        )

    def w_copy(i):
        return pltpu.make_async_remote_copy(
            src_ref=(win, wout)[i],
            dst_ref=(win_got, wout_got)[i],
            send_sem=w_sems.at[0, i],
            recv_sem=w_sems.at[1, i],
            device_id=partner,
            device_id_type=MESH,
        )

    def every(body):
        def step(k, carry):
            body(k)
            return carry

        lax.fori_loop(1, n_dp, step, 0)

    low = lax.broadcasted_iota(jnp.int32, (rows, 128), 1) < 64

    def attend(m, carry):
        cot_copy(m).start()
        cot_all[m, image(t)] = cot_own[m]
        xf = x_in[m].astype(F32)
        unit, _ = standardise(xf)
        a = (unit * norms[0:1] + norms[1:2]).astype(BF16)
        for s in range(n_t):
            for i in range(3):
                cols = slice((3 * s + i) * block, (3 * s + i + 1) * block)
                projected = dot(a, qkv[:, cols], ((1,), (0,)))
                mixed[m, :, cols] = (projected * factor if i == 0 else projected).astype(BF16)
        for col, dest in pairs(n_t, block):
            query = mixed[m, :, col : col + 128]
            keys = mixed[m, :, col + block : col + block + 128]
            values = mixed[m, :, col + 2 * block : col + 2 * block + 128]
            zero = jnp.zeros_like(query)
            parts = []
            for own in (low, ~low):
                probs = key_softmax(jnp.where(own, query, zero), keys, count)
                parts.append(dot(probs.astype(BF16), values, ((1,), (0,))))
            context[m, :, dest : dest + 128] = jnp.where(low, parts[0], parts[1]).astype(BF16)
        hidden = xf + live[m] * dot(context[m], proj[...], ((1,), (0,)))
        hidden_in[m] = hidden
        unit, _ = standardise(hidden)
        c = (unit * norms[2:3] + norms[3:4]).astype(BF16)
        c_own[m] = c
        c_all[m, image(t)] = c
        c_copy(m).start()
        return carry

    lax.fori_loop(0, batches, attend, 0)
    w_copy(0).start()
    w_copy(1).start()

    lane = lax.broadcasted_iota(jnp.int32, (2 * rows, router.shape[1]), 1)

    def dispatch(m, carry):
        c_copy(m).wait_recv()
        cot_copy(m).wait_recv()
        c = c_all[m]
        logits = jnp.where(lane < experts, dot(c, router[...], ((1,), (0,))), -1e30)
        raised = jnp.exp(logits - jnp.max(logits, axis=-1, keepdims=True))
        probs = raised / jnp.sum(raised, axis=-1, keepdims=True)
        cot = cot_all[m].astype(F32)
        scaled = []
        for k in range(2):
            gate = jnp.sum(jnp.where(lane == expert_col[m, :, k : k + 1], probs, 0.0), axis=-1, keepdims=True)
            gates[m, :, k : k + 1] = gate
            scaled.append((gate * cot).astype(BF16))
        codes = code_col[...]
        picks = [(flat_row[m, k : k + 1, :] == codes).astype(F32).astype(BF16) for k in range(2)]
        sent[m, :, :d] = dot(picks[0] + picks[1], c, ((1,), (0,))).astype(BF16)
        moved = dot(picks[0], scaled[0], ((1,), (0,))) + dot(picks[1], scaled[1], ((1,), (0,)))
        sent[m, :, d:] = moved.astype(BF16)
        every(lambda k: go_copy(m, k).start())
        got[m, part(dp)] = sent[m, part(dp)]
        return carry

    lax.fori_loop(0, batches, dispatch, 0)

    tile = 256

    def clear(i, carry):
        cols = pl.ds(pl.multiple_of(i * tile, tile), tile)
        for into in (gin, gin_mine):
            into[:, cols] = jnp.zeros((d, tile), F32)
        for into in (gout, gout_mine):
            into[cols, :] = jnp.zeros((tile, d), F32)
        return carry

    lax.fori_loop(0, hidden // tile, clear, 0)

    def expert_step(m, carry):
        every(lambda k: go_copy(m, k).wait_recv())
        y_acc[...] = jnp.zeros_like(y_acc)
        dx_acc[...] = jnp.zeros_like(dx_acc)

        def chunk(win, wout, gin, gout, i, inner):
            cols = pl.ds(pl.multiple_of(i * tile, tile), tile)
            x = got[m, :, :d]
            dprod = got[m, :, d:]
            w1 = win[:, cols]
            w2 = wout[cols, :]
            pre = dot(x, w1, ((1,), (0,)))
            square = pre * pre
            th = jnp.tanh(GELU_A * pre * (1.0 + GELU_B * square))
            active = (0.5 * pre * (1.0 + th)).astype(BF16)
            slope = 0.5 * (1.0 + th) + 0.5 * pre * (1.0 - th * th) * (GELU_A * (1.0 + 3.0 * GELU_B * square))
            dpre = (dot(dprod, w2, ((1,), (1,))) * slope).astype(BF16)
            gin[:, cols] += dot(x, dpre, ((0,), (0,)))
            gout[cols, :] += dot(active, dprod, ((0,), (0,)))
            y_acc[...] += dot(active, w2, ((1,), (0,)))
            dx_acc[...] += dot(dpre, w1, ((1,), (1,)))
            return inner

        lax.fori_loop(
            0, hidden // tile, functools.partial(chunk, win, wout, gin_mine, gout_mine), 0
        )

        @pl.when(m == 0)
        def _():
            w_copy(0).wait_recv()
            w_copy(1).wait_recv()

        lax.fori_loop(
            0, hidden // tile, functools.partial(chunk, win_got, wout_got, gin, gout), 0
        )
        got[m, :, :d] = y_acc[...].astype(BF16)
        got[m, :, d:] = dx_acc[...].astype(BF16)
        every(lambda k: back_copy(m, k).start())
        ret[m, part(dp)] = got[m, part(dp)]
        return carry

    lax.fori_loop(0, batches, expert_step, 0)

    gin_half[...] = gin[...].astype(BF16)
    gout_half[...] = gout[...].astype(BF16)

    def combine(m, carry):
        every(lambda k: back_copy(m, k).wait_recv())
        codes = code_row[...]
        for i in (other, t):
            picks = [(flat_col[m, image(i), k : k + 1] == codes).astype(F32).astype(BF16) for k in range(2)]
            one = dot(picks[0], ret[m, :, :d], ((1,), (0,)))
            two = dot(picks[1], ret[m, :, :d], ((1,), (0,)))
            d_rows = dot(picks[0] + picks[1], ret[m, :, d:], ((1,), (0,)))
            cot = cot_all[m, image(i)].astype(F32)
            gate = gates[m, image(i)]
            mixture = gate[:, 0:1] * one + gate[:, 1:2] * two
            col = lax.broadcasted_iota(jnp.int32, (rows, 128), 1)
            dg = jnp.where(col == 0, jnp.sum(one * cot, axis=-1, keepdims=True), 0.0)
            dg = dg + jnp.where(col == 1, jnp.sum(two * cot, axis=-1, keepdims=True), 0.0)
            if i is other:
                pay[m, :, :d] = mixture.astype(BF16)
                pay[m, :, d : 2 * d] = d_rows.astype(BF16)
                pay[m, :, 2 * d :] = dg.astype(BF16)
                pay_copy(m).start()
            else:
                mix[m] = mixture
                dx[m] = d_rows
                dgate[m] = dg
        return carry

    gqkv[...] = jnp.zeros_like(gqkv)
    gproj[...] = jnp.zeros_like(gproj)
    grouter[...] = jnp.zeros_like(grouter)
    gnorms[...] = jnp.zeros_like(gnorms)

    def retreat(m):
        pay_copy(m).wait_recv()
        hidden = hidden_in[m]
        out[m] = (hidden + mix[m] + paid[m, :, :d].astype(F32)).astype(BF16)
        unit, inverse = standardise(hidden)
        c = (unit * norms[2:3] + norms[3:4]).astype(BF16)
        probs, lane = gate_softmax(c, router[...], experts)
        dg = dgate[m] + paid[m, :, 2 * d :].astype(F32)
        dprobs = jnp.zeros_like(probs)
        for k in range(2):
            dprobs = dprobs + jnp.where(lane == expert_col[m, image(t), k : k + 1], dg[:, k : k + 1], 0.0)
        dlogits = probs * (dprobs - jnp.sum(dprobs * probs, axis=-1, keepdims=True))
        dc = dx[m] + paid[m, :, d : 2 * d].astype(F32)
        for piece in two_parts(dlogits):
            grouter[...] += dot(c, piece, ((0,), (0,)))
            dc = dc + dot(piece, router[...], ((1,), (1,)))
        gnorms[2:3] += jnp.sum(dc * unit, axis=0, keepdims=True)
        gnorms[3:4] += jnp.sum(dc, axis=0, keepdims=True)
        dhidden = cot_all[m, image(t)].astype(F32) + norm_back(dc * norms[2:3], unit, inverse)
        grad_x[m] = dhidden
        dattn = (live[m] * dhidden).astype(BF16)
        gproj[...] += dot(context[m], dattn, ((0,), (0,)))
        dcontext = dot(dattn, proj[...], ((1,), (1,))).astype(BF16)
        for col, dest in pairs(n_t, block):
            query = mixed[m, :, col : col + 128]
            keys = mixed[m, :, col + block : col + block + 128]
            values = mixed[m, :, col + 2 * block : col + 2 * block + 128]
            grads = dcontext[:, dest : dest + 128]
            zero = jnp.zeros_like(query)
            parts = []
            for own in (low, ~low):
                probs = key_softmax(jnp.where(own, query, zero), keys, count)
                dvalues = dot(probs.astype(BF16), grads, ((0,), (0,)))
                dweights = dot(jnp.where(own, grads, zero), values, ((1,), (1,)))
                dscores = probs * (dweights - jnp.sum(dweights * probs, axis=-1, keepdims=True))
                dscores = dscores.astype(BF16)
                parts.append(
                    (dot(dscores, keys, ((1,), (0,))), dot(dscores, query, ((0,), (0,))), dvalues)
                )
            for i in range(3):
                both = jnp.where(low, parts[0][i], parts[1][i]).astype(BF16)
                if i == 0:
                    both = both * BF16(factor)
                dmixed[:, col + i * block : col + i * block + 128] = both
        unit, inverse = standardise(x_in[m].astype(F32))
        a = (unit * norms[0:1] + norms[1:2]).astype(BF16)
        gqkv[...] += dot(a, dmixed[...], ((0,), (0,)))
        da = dot(dmixed[...], qkv[...], ((1,), (1,)))
        gnorms[0:1] += jnp.sum(da * unit, axis=0, keepdims=True)
        gnorms[1:2] += jnp.sum(da, axis=0, keepdims=True)
        grad_x[m] += norm_back(da * norms[0:1], unit, inverse)

    pieces = 4

    def finish(m, carry):
        for i in range(pieces):

            @pl.when(m == i)
            def _(i=i):
                grad_copy(i).start()

        @pl.when(m < batches)
        def _():
            combine(m, 0)

        @pl.when(m > 0)
        def _():
            retreat(m - 1)

        return carry

    lax.fori_loop(0, batches + 1, finish, 0)
    for i in range(batches + 1, pieces):
        grad_copy(i).start()
    gqkv_out[...] = gqkv[...].astype(BF16)
    gproj_out[...] = gproj[...].astype(BF16)
    for i in range(pieces):
        grad_copy(i).wait()
    gin_mine[...] += gin_got[...].astype(F32)
    gout_mine[...] += gout_got[...].astype(F32)
    w_copy(0).wait_send()
    w_copy(1).wait_send()

    def drain(m, carry):
        c_copy(m).wait_send()
        cot_copy(m).wait_send()
        pay_copy(m).wait_send()
        every(lambda k: go_copy(m, k).wait_send())
        every(lambda k: back_copy(m, k).wait_send())
        return carry

    lax.fori_loop(0, batches, drain, 0)


def layer(cot_own, router, flat, expert_of, codes, win, wout, saved, experts, n_dp, n_t, block, count, factor):
    batches, rows, d = cot_own.shape
    slots = codes.shape[0]
    half = win.shape[1]
    wide = 3 * n_t * block
    dma = pltpu.SemaphoreType.DMA
    return pl.pallas_call(
        functools.partial(layer_kernel, experts, n_t, block, count, factor),
        out_shape=[
            jax.ShapeDtypeStruct((batches, rows, d), BF16),
            jax.ShapeDtypeStruct((batches, rows, d), F32),
            jax.ShapeDtypeStruct((d, wide), BF16),
            jax.ShapeDtypeStruct((d, d), BF16),
            jax.ShapeDtypeStruct((d, router.shape[1]), F32),
            jax.ShapeDtypeStruct((8, d), F32),
            jax.ShapeDtypeStruct((d, half), F32),
            jax.ShapeDtypeStruct((half, d), F32),
        ],
        in_specs=[ANYWHERE] * 14,
        out_specs=[ANYWHERE] * 8,
        scratch_shapes=[
            pltpu.VMEM((batches, rows, d), BF16),
            pltpu.VMEM((batches, rows, d), F32),
            pltpu.VMEM((batches, rows, wide), BF16),
            pltpu.VMEM((batches, rows, d), BF16),
            pltpu.VMEM((batches, 2 * rows, d), BF16),
            pltpu.VMEM((batches, 2 * rows, d), BF16),
            pltpu.VMEM((batches, 2 * rows, 128), F32),
            pltpu.VMEM((batches, slots, 2 * d), BF16),
            pltpu.VMEM((batches, slots, 2 * d), BF16),
            pltpu.VMEM((batches, slots, 2 * d), BF16),
            pltpu.VMEM((batches, rows, 2 * d + 128), BF16),
            pltpu.VMEM((batches, rows, 2 * d + 128), BF16),
            pltpu.VMEM((batches, rows, d), F32),
            pltpu.VMEM((batches, rows, d), F32),
            pltpu.VMEM((batches, rows, 128), F32),
            pltpu.VMEM((rows, wide), BF16),
            pltpu.VMEM((d, wide), F32),
            pltpu.VMEM((d, d), F32),
            pltpu.VMEM((slots, d), F32),
            pltpu.VMEM((slots, d), F32),
            pltpu.VMEM((d, half), BF16),
            pltpu.VMEM((half, d), BF16),
            pltpu.VMEM((d, half), F32),
            pltpu.VMEM((half, d), F32),
            pltpu.VMEM((d, half), BF16),
            pltpu.VMEM((half, d), BF16),
            pltpu.VMEM((d, half), BF16),
            pltpu.VMEM((half, d), BF16),
            dma((2, 2)),
            dma((2, batches)),
            dma((2, batches)),
            dma((batches, n_dp - 1)),
            dma((batches, n_dp - 1)),
            dma((batches, n_dp - 1)),
            dma((batches, n_dp - 1)),
            dma((2, batches)),
            dma((2, 4)),
        ],
        compiler_params=pltpu.CompilerParams(
            collective_id=2, has_side_effects=True, vmem_limit_bytes=67043328
        ),
    )(
        cot_own,
        router,
        flat,
        flat.transpose(0, 2, 1),
        expert_of.transpose(0, 2, 1),
        codes[None, :],
        codes[:, None],
        win,
        wout,
        *saved,
    )


def general(
    tokens,
    w_qkv,
    w_proj,
    w_in,
    w_out,
    w_router,
    gain_attn,
    shift_attn,
    gain_moe,
    shift_moe,
    live_rows,
    chosen,
    priority,
    cotangent,
):
    batches, own_rows, d = tokens.shape
    rows = live_rows.shape[1]
    n_dp = lax.axis_size("dp")
    n_t = lax.axis_size("tensor")
    t = lax.axis_index("tensor")
    heads_here = w_qkv.shape[1]
    heads = heads_here * n_t
    width = w_qkv.shape[2] // 3
    experts = w_in.shape[0] * n_dp
    cap = 2 * rows // experts
    share = cap // n_t
    images = rows // SEQ
    span = images * SEQ
    per = -(-images // n_t)
    work = per * SEQ
    total = n_t * work
    factor = width ** (-0.5)
    highest = lax.Precision.HIGHEST

    small = jnp.concatenate(
        [w_router] + [v[:, None] for v in (gain_attn, shift_attn, gain_moe, shift_moe)], axis=1
    )
    small = jnp.pad(small, ((0, 0), (0, 128 - small.shape[1])))
    block = heads_here * width
    qkv_block = w_qkv.reshape(-1, heads_here, 3, width).transpose(0, 2, 1, 3).reshape(-1, 3 * block)
    fill = -3 * block % 128
    qkv_block = jnp.pad(qkv_block, ((0, 0), (0, fill)))
    qkv, proj, small = gather_weights(qkv_block, w_proj.reshape(-1, d), small, n_dp, n_t)
    qkv = qkv.reshape(d, n_t, 3 * block + fill)[:, :, : 3 * block].reshape(d, -1)
    router = small[:, :experts]
    gain_one, shift_one, gain_two, shift_two = (small[:, experts + i].astype(F32) for i in range(4))
    proj = proj.reshape(n_dp, n_t, heads_here, w_proj.shape[1], d)
    proj = proj.transpose(1, 2, 0, 3, 4).reshape(heads * width, d)
    win = lax.all_gather(w_in[0], "tensor", axis=1, tiled=True)
    wout = lax.all_gather(w_out[0], "tensor", axis=0, tiled=True)
    cot_all = lax.all_gather(cotangent, "tensor", axis=1, tiled=True)

    def pad_rows(v, n):
        return jnp.pad(v, ((0, 0), (0, n - v.shape[1])) + ((0, 0),) * (v.ndim - 2))

    def own(v):
        return lax.dynamic_slice_in_dim(v, t * work, work, 1)

    edge = own_rows - work
    direct = n_t == 2 and per == 1 and edge >= 0
    if direct:
        moved = lax.ppermute(tokens[:, work:], "tensor", [(0, 1)])
        x = jnp.where(
            t == 0, tokens[:, :work], jnp.concatenate([moved, tokens[:, : work - edge]], axis=1)
        )
    else:
        x = own(pad_rows(lax.all_gather(tokens, "tensor", axis=1, tiled=True)[:, :span], total))
    x = x.astype(F32)
    live = live_rows[:, :span]
    live_all = pad_rows(live, total)
    live_own = own(live_all).astype(F32)[:, :, None]
    cot_all = pad_rows(cot_all[:, :span], total)
    dy = own(cot_all).astype(F32)

    rank = priority[:, 0, :span]
    first, second = chosen[:, :span, 0], chosen[:, :span, 1]
    labels = jnp.arange(experts, dtype=jnp.int32)
    earlier = (rank[:, None, :] < rank[:, :, None]).astype(BF16)
    hit_one = (first[:, :, None] == labels).astype(F32)
    hit_two = (second[:, :, None] == labels).astype(F32)
    live_one = hit_one * live[:, :, None].astype(F32)
    live_two = hit_two * live[:, :, None].astype(F32)
    counts = jnp.einsum(
        "mrs,mse->mre",
        earlier,
        jnp.concatenate([live_one, live_two], axis=-1).astype(BF16),
        preferred_element_type=F32,
    )
    first_total = jnp.sum(live_one, axis=1, keepdims=True)
    slot_one = jnp.sum(counts[:, :, :experts] * hit_one, axis=-1).astype(jnp.int32)
    slot_two = jnp.sum((counts[:, :, experts:] + first_total) * hit_two, axis=-1).astype(jnp.int32)
    keep_one = (live > 0) & (slot_one < cap)
    keep_two = (live > 0) & (slot_two < cap)
    flat_one = jnp.where(keep_one, first * cap + slot_one, -1)
    flat_two = jnp.where(keep_two, second * cap + slot_two, -1)

    def spread(v, fill):
        return jnp.pad(v, ((0, 0), (0, total - span)), constant_values=fill)

    flat_one, flat_two = spread(flat_one, -1), spread(flat_two, -1)
    keep_one, keep_two = spread(keep_one, False), spread(keep_two, False)
    first, second = spread(first, 0), spread(second, 0)
    codes = (jnp.arange(experts)[:, None] * cap + t * share + jnp.arange(share)[None, :]).reshape(-1)
    pick_one = flat_one[:, None, :] == codes[None, :, None]
    pick_two = flat_two[:, None, :] == codes[None, :, None]

    normed_one = layer_norm(x, gain_one, shift_one).astype(BF16)
    mixed = dot(normed_one, qkv, ((2,), (0,)))
    split = heads * width
    shape = (batches * per, SEQ, heads, width)
    mixed = mixed.reshape(batches, work, n_t, 3, block)
    query = (mixed[:, :, :, 0] * factor).astype(BF16).reshape(shape)
    keys = mixed[:, :, :, 1].astype(BF16).reshape(shape)
    values = mixed[:, :, :, 2].astype(BF16).reshape(shape)
    scores = jnp.einsum("iqhc,ikhc->ihqk", query, keys, preferred_element_type=F32)
    probs = jax.nn.softmax(scores, axis=-1)
    weights = probs.astype(BF16)
    context = jnp.einsum("ihqk,ikhc->iqhc", weights, values, preferred_element_type=F32)
    context = context.astype(BF16).reshape(batches, work, split)
    attn = dot(context, proj, ((2,), (0,)))
    hidden = x + live_own * attn
    normed_two = layer_norm(hidden, gain_two, shift_two).astype(BF16)

    c_all = lax.all_gather(normed_two, "tensor", axis=1, tiled=True)
    gate_probs = jax.nn.softmax(dot(c_all, router, ((2,), (0,))), axis=-1)
    hits_one = (first[:, :, None] == labels).astype(F32)
    hits_two = (second[:, :, None] == labels).astype(F32)
    gate_one = jnp.sum(gate_probs * hits_one, axis=-1) * keep_one
    gate_two = jnp.sum(gate_probs * hits_two, axis=-1) * keep_two
    picked = (pick_one | pick_two).astype(BF16)
    sent = jnp.einsum(
        "mqr,mrd->mqd",
        picked,
        jnp.concatenate([c_all, cot_all], axis=-1),
        preferred_element_type=F32,
    )
    gate_slot = jnp.sum(
        jnp.where(pick_one, gate_one[:, None, :], 0.0) + jnp.where(pick_two, gate_two[:, None, :], 0.0),
        axis=-1,
        keepdims=True,
    )
    sent = jnp.concatenate(
        [sent[..., :d].astype(BF16), (sent[..., d:] * gate_slot).astype(BF16)], axis=-1
    )
    sent = sent.reshape(batches, experts, share, 2 * d)
    got = lax.all_to_all(sent, "dp", 1, 1, tiled=True).reshape(-1, 2 * d)
    produced, d_in, grad_in, grad_out = expert(got[:, :d], got[:, d:], win, wout)
    back = jnp.concatenate([produced, d_in], axis=-1).reshape(batches, n_dp, share, 2 * d)
    back = lax.all_to_all(back, "dp", 1, 1, tiled=True).reshape(batches, experts * share, 2 * d)
    grad_in = lax.psum_scatter(grad_in, "tensor", scatter_dimension=1, tiled=True).astype(F32)
    grad_out = lax.psum_scatter(grad_out, "tensor", scatter_dimension=0, tiled=True).astype(F32)

    part_one = jnp.einsum("mqr,mqd->mrd", pick_one.astype(BF16), back[..., :d], preferred_element_type=F32)
    part_two = jnp.einsum("mqr,mqd->mrd", pick_two.astype(BF16), back[..., :d], preferred_element_type=F32)
    d_rows = jnp.einsum("mqr,mqd->mrd", picked, back[..., d:], preferred_element_type=F32)
    mixture = gate_one[:, :, None] * part_one + gate_two[:, :, None] * part_two
    cot_wide = cot_all.astype(F32)
    dgate_one = jnp.sum(part_one * cot_wide, axis=-1, keepdims=True)
    dgate_two = jnp.sum(part_two * cot_wide, axis=-1, keepdims=True)
    dgates = jnp.concatenate([dgate_one, dgate_two], axis=-1)
    payload = jnp.concatenate(
        [mixture, d_rows, jnp.pad(dgates, ((0, 0), (0, 0), (0, 126)))], axis=-1
    ).astype(BF16)
    pieces = payload.reshape(batches, n_t, work, payload.shape[-1])

    def piece(k):
        return lax.dynamic_index_in_dim(pieces, (t + k) % n_t, 1, keepdims=False)

    payload = piece(0).astype(F32)
    for k in range(1, n_t):
        payload = payload + lax.ppermute(
            piece(k), "tensor", [(j, (j + k) % n_t) for j in range(n_t)]
        ).astype(F32)
    output = (hidden + payload[..., :d]).astype(BF16)
    dgates = payload[..., 2 * d : 2 * d + 2]

    own_probs = own(gate_probs)
    dprobs = own(hits_one) * dgates[..., 0:1] * own(keep_one)[:, :, None]
    dprobs = dprobs + own(hits_two) * dgates[..., 1:2] * own(keep_two)[:, :, None]
    dlogits = own_probs * (dprobs - jnp.sum(dprobs * own_probs, axis=-1, keepdims=True))
    grad_router = lax.dot_general(
        normed_two.astype(F32), dlogits, (((0, 1), (0, 1)), ((), ())), precision=highest
    )
    dc = payload[..., d : 2 * d] + lax.dot_general(
        dlogits, router.astype(F32), (((2,), (1,)), ((), ())), precision=highest
    )
    _, back_two = jax.vjp(layer_norm, hidden, gain_two, shift_two)
    dnorm, grad_gain_two, grad_shift_two = back_two(dc)
    dhidden = dy + dnorm
    dattn = (live_own * dhidden).astype(BF16)

    grad_proj = dot(context, dattn, ((0, 1), (0, 1)))
    dcontext = dot(dattn, proj, ((2,), (1,))).astype(BF16).reshape(shape)
    dvalues = jnp.einsum("ihqk,iqhc->ikhc", weights, dcontext, preferred_element_type=F32).astype(BF16)
    dweights = jnp.einsum("iqhc,ikhc->ihqk", dcontext, values, preferred_element_type=F32)
    dscores = (probs * (dweights - jnp.sum(dweights * probs, axis=-1, keepdims=True))).astype(BF16)
    dquery = jnp.einsum("ihqk,ikhc->iqhc", dscores, keys, preferred_element_type=F32).astype(BF16)
    dkeys = jnp.einsum("ihqk,iqhc->ikhc", dscores, query, preferred_element_type=F32).astype(BF16)
    dmixed = jnp.stack(
        [v.reshape(batches, work, n_t, block) for v in (dquery * BF16(factor), dkeys, dvalues)], axis=3
    ).reshape(batches, work, 3 * split)
    grad_qkv = dot(normed_one, dmixed, ((0, 1), (0, 1)))
    da = dot(dmixed, qkv, ((2,), (1,)))
    _, back_one = jax.vjp(layer_norm, x, gain_one, shift_one)
    dnorm, grad_gain_one, grad_shift_one = back_one(da)
    grad_x = dhidden + dnorm

    if direct:
        out_edge = lax.ppermute(output[:, :edge], "tensor", [(1, 0)])
        grad_edge = lax.ppermute(grad_x[:, :edge], "tensor", [(1, 0)])
        result = jnp.where(
            t == 0,
            jnp.concatenate([output, out_edge], axis=1),
            jnp.concatenate([output[:, edge:], tokens[:, work - edge :]], axis=1),
        )
        grad_tokens = jnp.where(
            t == 0,
            jnp.concatenate([grad_x, grad_edge], axis=1),
            jnp.concatenate([grad_x[:, edge:], cotangent[:, work - edge :].astype(F32)], axis=1),
        )
    else:
        here = (t * own_rows + jnp.arange(own_rows) < span)[None, :, None]

        def home(v, rest):
            full = pad_rows(lax.all_gather(v, "tensor", axis=1, tiled=True)[:, :span], rows)
            return jnp.where(here, lax.dynamic_slice_in_dim(full, t * own_rows, own_rows, 1), rest)

        result = home(output, tokens)
        grad_tokens = home(grad_x, cotangent.astype(F32))

    nz, ny = grid_sizes(n_dp)
    grad_qkv = jnp.pad(grad_qkv.astype(BF16).reshape(d, n_t, 3 * block), ((0, 0), (0, 0), (0, fill)))
    grad_qkv = grad_qkv.reshape(nz, ny, 2, d // n_dp, -1)
    grad_proj = grad_proj.astype(BF16).reshape(n_t, heads_here, n_dp, -1, d)
    grad_proj = grad_proj.transpose(2, 0, 1, 3, 4).reshape(nz, ny, 2, n_t, -1, d)
    smalls = jnp.concatenate(
        [grad_router] + [v[:, None] for v in (grad_gain_one, grad_shift_one, grad_gain_two, grad_shift_two)],
        axis=1,
    )
    smalls = jnp.pad(smalls, ((0, 0), (0, 128 - smalls.shape[1]))).reshape(nz, ny, 2, n_t, -1, 128)
    grad_qkv, grad_proj, smalls = scatter_grads(grad_qkv, grad_proj, smalls, n_dp, n_t)
    grad_qkv = grad_qkv[:, : 3 * block].reshape(-1, 3, heads_here, width).transpose(0, 2, 1, 3)
    return (
        result,
        grad_tokens,
        grad_qkv.reshape(w_qkv.shape),
        grad_proj.reshape(w_proj.shape),
        grad_in[None],
        grad_out[None],
        smalls[:, :experts],
        smalls[:, experts],
        smalls[:, experts + 1],
        smalls[:, experts + 2],
        smalls[:, experts + 3],
    )


def fast(
    tokens,
    w_qkv,
    w_proj,
    w_in,
    w_out,
    w_router,
    gain_attn,
    shift_attn,
    gain_moe,
    shift_moe,
    live_rows,
    chosen,
    priority,
    cotangent,
):
    batches, own_rows, d = tokens.shape
    rows = live_rows.shape[1]
    n_dp = lax.axis_size("dp")
    n_t = lax.axis_size("tensor")
    t = lax.axis_index("tensor")
    heads_here = w_qkv.shape[1]
    width = w_qkv.shape[2] // 3
    block = heads_here * width
    experts = n_dp
    cap = 2 * rows // experts
    share = cap // n_t
    span = n_t * SEQ
    padded = -(-SEQ // 16) * 16
    edge = own_rows - SEQ
    factor = width ** (-0.5)

    small = jnp.concatenate(
        [w_router] + [v[:, None] for v in (gain_attn, shift_attn, gain_moe, shift_moe)], axis=1
    )
    small = jnp.pad(small, ((0, 0), (0, 128 - small.shape[1])))
    qkv_block = w_qkv.reshape(-1, heads_here, 3, width).transpose(0, 2, 1, 3).reshape(-1, 3 * block)
    held = jnp.concatenate([tokens, cotangent], axis=0)
    qkv, proj, small, moved = gather_weights(
        qkv_block, w_proj.reshape(-1, d), small, n_dp, n_t, (held[:, SEQ:],)
    )
    router = jnp.where(jnp.arange(128) < experts, small, 0)
    norms = jnp.pad(small[:, experts : experts + 4].astype(F32).T, ((0, 4), (0, 0)))
    proj = proj.reshape(n_dp, n_t, heads_here, w_proj.shape[1], d)
    proj = proj.transpose(1, 2, 0, 3, 4).reshape(n_t * block, d)

    def pad_rows(v, axis, fill=0):
        spec = [(0, 0)] * v.ndim
        spec[axis] = (0, padded - SEQ)
        return jnp.pad(v, spec, constant_values=fill)

    def lay(v, axis, fill=0):
        shape = v.shape
        v = v.reshape(shape[:axis] + (n_t, SEQ) + shape[axis + 1 :])
        v = pad_rows(v, axis + 1, fill)
        return v.reshape(shape[:axis] + (n_t * padded,) + shape[axis + 1 :])

    def own(v, axis):
        return lax.dynamic_slice_in_dim(v, t * padded, padded, axis)

    laid = jnp.where(t == 0, held[:, :SEQ], jnp.concatenate([moved, held[:, : SEQ - edge]], axis=1))
    laid = pad_rows(laid, 1)
    x, cot_own = laid[:batches], laid[batches:]

    live = live_rows[:, :span]
    rank = priority[:, 0, :span]
    picks = chosen[:, :span].transpose(0, 2, 1)
    labels = jnp.arange(experts, dtype=jnp.int32)
    earlier = (rank[:, None, :] < rank[:, :, None]).astype(BF16)
    hits = (picks[..., None] == labels).astype(F32)
    live_hits = hits * live[:, None, :, None].astype(F32)
    ahead = jnp.einsum("mrs,mkse->mkre", earlier, live_hits.astype(BF16), preferred_element_type=F32)
    firsts = jnp.sum(live_hits[:, :1], axis=2, keepdims=True)
    ahead = ahead + jnp.concatenate([jnp.zeros_like(firsts), firsts], axis=1)
    slot = jnp.sum(ahead * hits, axis=-1).astype(jnp.int32)
    keep = (live[:, None, :] > 0) & (slot < cap)
    flat = lay(jnp.where(keep, picks * cap + slot, -1), 2, -1)
    expert_of = lay(jnp.where(keep, picks, -1), 2, -1)
    codes = (jnp.arange(experts)[:, None] * cap + t * share + jnp.arange(share)[None, :]).reshape(-1)
    live_own = own(lay(live.astype(F32)[:, :, None], 1), 1)

    output, grad_x, grad_qkv, grad_proj, grad_router, grad_norms, grad_in, grad_out = layer(
        cot_own,
        router,
        flat,
        expert_of,
        codes,
        w_in[0],
        w_out[0],
        (x, live_own, norms, qkv, proj),
        experts,
        n_dp,
        n_t,
        block,
        SEQ,
        factor,
    )

    out_edge = lax.ppermute(output[:, :edge], "tensor", [(1, 0)])
    grad_edge = lax.ppermute(grad_x[:, :edge], "tensor", [(1, 0)])
    rest = SEQ - edge

    def home(v, moved_rows, other):
        return jnp.where(
            t == 0,
            jnp.concatenate([v[:, :SEQ], moved_rows], axis=1),
            jnp.concatenate([v[:, edge:SEQ], other[:, rest:].astype(v.dtype)], axis=1),
        )

    nz, ny = grid_sizes(n_dp)
    grad_proj = grad_proj.reshape(n_t, heads_here, n_dp, -1, d)
    grad_proj = grad_proj.transpose(2, 0, 1, 3, 4).reshape(nz, ny, 2, n_t, -1, d)
    lane = jnp.arange(128)
    smalls = jnp.where(lane < experts, grad_router, 0.0)
    smalls = smalls + jnp.pad(grad_norms[:4].T, ((0, 0), (experts, 124 - experts)))
    grad_qkv, grad_proj, smalls = scatter_grads(
        grad_qkv.reshape(nz, ny, 2, d // n_dp, -1), grad_proj, smalls.reshape(nz, ny, 2, n_t, -1, 128), n_dp, n_t
    )
    grad_qkv = grad_qkv.reshape(-1, 3, heads_here, width).transpose(0, 2, 1, 3)
    return (
        home(output, out_edge, tokens),
        home(grad_x, grad_edge, cotangent),
        grad_qkv.reshape(w_qkv.shape),
        grad_proj.reshape(w_proj.shape),
        grad_in[None],
        grad_out[None],
        smalls[:, :experts],
        smalls[:, experts],
        smalls[:, experts + 1],
        smalls[:, experts + 2],
        smalls[:, experts + 3],
    )


def local(*args):
    tokens, w_qkv, live_rows = args[0], args[1], args[10]
    n_t = lax.axis_size("tensor")
    images = live_rows.shape[1] // SEQ
    block = w_qkv.shape[1] * (w_qkv.shape[2] // 3)
    if n_t == 2 and images == 2 and tokens.shape[1] >= SEQ and block % 128 == 0 and w_qkv.shape[2] == 192:
        return fast(*args)
    return general(*args)


def solution(mesh):
    both = ("dp", "tensor")
    return jax.shard_map(
        local,
        mesh=mesh,
        in_specs=(
            P(None, both, None),
            P("dp", "tensor", None),
            P("tensor", "dp", None),
            P("dp", None, "tensor"),
            P("dp", "tensor", None),
            P(both, None),
            P(both),
            P(both),
            P(both),
            P(both),
            P(None, "dp"),
            P(None, "dp", None),
            P(None, "dp", None),
            P(None, both, None),
        ),
        out_specs=(
            P(None, both, None),
            P(None, both, None),
            P("dp", "tensor", None),
            P("tensor", "dp", None),
            P("dp", None, "tensor"),
            P("dp", "tensor", None),
            P(both, None),
            P(both),
            P(both),
            P(both),
            P(both),
        ),
        check_vma=False,
    )
```

```python
import functools

import jax
import jax.numpy as jnp
from jax import lax
from jax.experimental import pallas as pl
from jax.experimental.pallas import tpu as pltpu
from jax.sharding import PartitionSpec as P

SEQ = 197
EPS = 1e-06
F32 = jnp.float32
BF16 = jnp.bfloat16
GELU_A = 0.7978845608028654
GELU_B = 0.044715


def dot(a, b, dims):
    return lax.dot_general(a, b, (dims, ((), ())), preferred_element_type=F32)


def layer_norm(values, gain_vec, shift_vec):
    centre = jnp.mean(values, axis=-1, keepdims=True)
    centered = values - centre
    spread = jnp.mean(centered * centered, axis=-1, keepdims=True)
    return centered * lax.rsqrt(spread + EPS) * gain_vec + shift_vec


def expert_kernel(x_ref, dp_ref, win_ref, wout_ref, y_ref, dx_ref, gin_ref, gout_ref, y_acc, dx_acc):
    step = pl.program_id(0)
    last = pl.num_programs(0) - 1
    x = x_ref[...]
    dprod = dp_ref[...]
    win = win_ref[...]
    wout = wout_ref[...]
    pre = dot(x, win, ((1,), (0,)))
    square = pre * pre
    th = jnp.tanh(GELU_A * pre * (1.0 + GELU_B * square))
    active = (0.5 * pre * (1.0 + th)).astype(BF16)
    slope = 0.5 * (1.0 + th) + 0.5 * pre * (1.0 - th * th) * (GELU_A * (1.0 + 3.0 * GELU_B * square))
    dact = dot(dprod, wout, ((1,), (1,)))
    dpre = (dact * slope).astype(BF16)
    gin_ref[...] = dot(x, dpre, ((0,), (0,))).astype(BF16)
    gout_ref[...] = dot(active, dprod, ((0,), (0,))).astype(BF16)
    part_y = dot(active, wout, ((1,), (0,)))
    part_dx = dot(dpre, win, ((1,), (1,)))

    @pl.when(step == 0)
    def _():
        y_acc[...] = part_y
        dx_acc[...] = part_dx

    @pl.when(step > 0)
    def _():
        y_acc[...] += part_y
        dx_acc[...] += part_dx

    @pl.when(step == last)
    def _():
        y_ref[...] = y_acc[...].astype(BF16)
        dx_ref[...] = dx_acc[...].astype(BF16)


def expert(x, dprod, win, wout, tile=256):
    n, d = x.shape
    ff = win.shape[1]
    return pl.pallas_call(
        expert_kernel,
        grid=(ff // tile,),
        in_specs=[
            pl.BlockSpec((n, d), lambda i: (0, 0)),
            pl.BlockSpec((n, d), lambda i: (0, 0)),
            pl.BlockSpec((d, tile), lambda i: (0, i)),
            pl.BlockSpec((tile, d), lambda i: (i, 0)),
        ],
        out_specs=[
            pl.BlockSpec((n, d), lambda i: (0, 0)),
            pl.BlockSpec((n, d), lambda i: (0, 0)),
            pl.BlockSpec((d, tile), lambda i: (0, i)),
            pl.BlockSpec((tile, d), lambda i: (i, 0)),
        ],
        out_shape=[
            jax.ShapeDtypeStruct((n, d), BF16),
            jax.ShapeDtypeStruct((n, d), BF16),
            jax.ShapeDtypeStruct((d, ff), BF16),
            jax.ShapeDtypeStruct((ff, d), BF16),
        ],
        scratch_shapes=[pltpu.VMEM((n, d), F32), pltpu.VMEM((n, d), F32)],
        compiler_params=pltpu.CompilerParams(vmem_limit_bytes=60 * 1024 * 1024),
        cost_estimate=pl.CostEstimate(
            flops=12 * n * d * ff, transcendentals=n * ff, bytes_accessed=8 * n * d + 8 * d * ff
        ),
    )(x, dprod, win, wout)


MESH = pl.DeviceIdType.MESH
ANYWHERE = pl.BlockSpec(memory_space=pltpu.VMEM)


def grid_sizes(n_dp):
    ny = 1
    while 2 * ny * 2 * ny <= n_dp // 2:
        ny *= 2
    return n_dp // (2 * ny), ny


def position(ny):
    dp = lax.axis_index("dp")
    return dp, lax.axis_index("tensor"), dp % 2, (dp // 2) % ny, dp // (2 * ny)


def neighbours(ny, nz, n_t):
    dp, t, c, y, z = position(ny)

    def along_core(k):
        return (dp - c + (c + k) % 2, t)

    def along_tensor(k):
        return (dp, (t + k) % n_t)

    def along_y(k):
        return (dp + ((y + k) % ny - y) * 2, t)

    def along_z(k):
        return (dp + ((z + k) % nz - z) * 2 * ny, t)

    return {"core": (2, along_core), "tensor": (n_t, along_tensor), "y": (ny, along_y), "z": (nz, along_z)}


def greet(stages):
    barrier = pltpu.get_barrier_semaphore()
    count = 0
    for size, device in stages.values():
        for k in range(1, size):
            pl.semaphore_signal(barrier, inc=1, device_id=device(k), device_id_type=MESH)
            count += 1
    pl.semaphore_wait(barrier, count)


def gather_kernel(ny, nz, n_t, extras, *refs):
    (qkv, proj, small), refs = refs[:3], refs[3:]
    side, refs = refs[:extras], refs[extras:]
    (qkv_out, proj_out, small_out), refs = refs[:3], refs[3:]
    side_out, (send, recv, copied) = refs[:extras], refs[extras:]
    dp, t, c, y, z = position(ny)
    stages = neighbours(ny, nz, n_t)
    greet(stages)
    cols, wide = qkv.shape[1], proj.shape[1]
    whole = slice(None)
    slot = 0

    def start(pieces, device):
        nonlocal slot
        copies = []
        for src, dst in pieces:
            copies.append(
                pltpu.make_async_remote_copy(
                    src_ref=src,
                    dst_ref=dst,
                    send_sem=send.at[slot],
                    recv_sem=recv.at[slot],
                    device_id=device,
                    device_id_type=MESH,
                )
            )
            copies[-1].start()
            slot += 1
        return copies

    def along(name, pieces):
        size, device = stages[name]
        return [copy for k in range(1, size) for copy in start(pieces, device(k))]

    def lanes(ts, half):
        return pl.ds(pl.multiple_of(ts * cols + half * (cols // 2), 128), cols // 2)

    def views(zs, ys, ts, half):
        band = slice(half * (wide // 2), (half + 1) * (wide // 2))
        parts = [qkv_out.at[zs, ys, c, :, lanes(i, half)] for i in ts]
        if len(ts) == 1:
            parts.append(proj_out.at[zs, ys, c, ts[0], :, band])
            if half == 0:
                parts.append(small_out.at[zs, ys, c, ts[0]])
        else:
            parts.append(proj_out.at[zs, ys, c, :, :, band])
        return [(part, part) for part in parts]

    aside = []
    for i in range(extras):
        strip = side_out[i].shape[1]
        aside += start([(side[i].at[:, side[i].shape[1] - strip :], side_out[i])], (dp, 1 - t))
    mine = (
        qkv_out.at[z, y, c, :, pl.ds(pl.multiple_of(t * cols, 128), cols)],
        proj_out.at[z, y, c, t],
        small_out.at[z, y, c, t],
    )
    inputs = list(zip((qkv, proj, small), mine))
    local = [pltpu.make_async_copy(src, dst, copied.at[i]) for i, (src, dst) in enumerate(inputs)]
    for copy in local:
        copy.start()
    for copy in along("z", inputs) + local:
        copy.wait()
    one = along("y", views(whole, y, [t], 0))
    two = along("tensor", views(whole, y, [t], 1))
    for copy in one:
        copy.wait()
    one = along("tensor", views(whole, whole, [t], 0))
    for copy in two:
        copy.wait()
    two = along("y", views(whole, y, list(range(n_t)), 1))
    for copy in one + two:
        copy.wait()
    rest = [ref.at[:, :, c] for ref in (qkv_out, proj_out, small_out)]
    for copy in along("core", [(part, part) for part in rest]) + aside:
        copy.wait()


def gather_weights(qkv, proj, small, n_dp, n_t, side=(), strip=0):
    nz, ny = grid_sizes(n_dp)
    slots = 3 * (nz - 1) + 5 * (n_t - 1) + (4 + n_t) * (ny - 1) + 3 + len(side)
    side_shapes = [jax.ShapeDtypeStruct((v.shape[0], strip) + v.shape[2:], v.dtype) for v in side]
    outs = pl.pallas_call(
        functools.partial(gather_kernel, ny, nz, n_t, len(side)),
        out_shape=[
            jax.ShapeDtypeStruct((nz, ny, 2, qkv.shape[0], n_t * qkv.shape[1]), BF16),
            jax.ShapeDtypeStruct((nz, ny, 2, n_t) + proj.shape, BF16),
            jax.ShapeDtypeStruct((nz, ny, 2, n_t) + small.shape, BF16),
        ]
        + side_shapes,
        in_specs=[ANYWHERE] * (3 + len(side)),
        out_specs=[ANYWHERE] * (3 + len(side)),
        scratch_shapes=[
            pltpu.SemaphoreType.DMA((slots,)),
            pltpu.SemaphoreType.DMA((slots,)),
            pltpu.SemaphoreType.DMA((3,)),
        ],
        compiler_params=pltpu.CompilerParams(collective_id=0, has_side_effects=True),
    )(qkv, proj, small, *side)
    qkv_all = outs[0].reshape(n_dp * qkv.shape[0], n_t * qkv.shape[1])
    return (qkv_all, outs[1].reshape((n_dp, n_t) + proj.shape), outs[2].reshape(-1, small.shape[1])) + tuple(outs[3:])


def scatter_kernel(ny, nz, n_t, heads, *refs):
    ins, refs = refs[:3], refs[3:]
    outs, refs = refs[:3], refs[3:]
    got_core, refs = refs[:3], refs[3:]
    held, refs = refs[:3], refs[3:]
    one_got, one_held, one_last, refs = refs[:3], refs[3:6], refs[6:9], refs[9:]
    two_got, two_held, two_last, refs = refs[:2], refs[2:4], refs[4:6], refs[6:]
    end, end_got, (send, recv) = refs[:3], refs[3:6], refs[6:]
    _, t, c, y, z = position(ny)
    stages = neighbours(ny, nz, n_t)
    greet(stages)
    cols, wide = ins[0].shape[4] // n_t, ins[1].shape[5]
    slot = 0

    def lanes(ts, half):
        return pl.ds(pl.multiple_of(ts * cols + half * (cols // 2), 128), cols // 2)

    def band(half):
        return slice(half * (wide // 2), (half + 1) * (wide // 2))

    def along(name, me, pieces):
        nonlocal slot
        size, device = stages[name]
        copies = []
        for k in range(1, size):
            for src, dst in pieces((me + k) % size, k - 1):
                copies.append(
                    pltpu.make_async_remote_copy(
                        src_ref=src,
                        dst_ref=dst,
                        send_sem=send.at[slot],
                        recv_sem=recv.at[slot],
                        device_id=device(k),
                        device_id_type=MESH,
                    )
                )
                copies[-1].start()
                slot += 1
        return copies

    def finish(copies):
        for copy in copies:
            copy.wait()

    def total(own, got, index):
        value = own.astype(F32)
        for k in range(got.shape[0]):
            value = value + got[(k,) + index].astype(F32)
        return value

    def loop(count, body):
        def step(n, carry):
            body(n)
            return carry

        lax.fori_loop(0, count, step, 0)

    finish(
        along("core", c, lambda j, k: [(ins[i].at[:, :, j], got_core[i].at[k]) for i in range(3)])
    )

    def add_core(n):
        zi, yi = n // ny, n % ny
        for i in range(3):
            held[i][zi, yi] = total(ins[i][zi, yi, c], got_core[i], (zi, yi)).astype(held[i].dtype)

    loop(nz * ny, add_core)
    one = along(
        "tensor",
        t,
        lambda j, k: [
            (held[0].at[:, :, :, lanes(j, 0)], one_got[0].at[k]),
            (held[1].at[:, :, j, :, band(0)], one_got[1].at[k]),
            (held[2].at[:, :, j], one_got[2].at[k]),
        ],
    )
    two = along(
        "y",
        y,
        lambda j, k: [(held[0].at[:, j, :, lanes(i, 1)], two_got[0].at[k, i]) for i in range(n_t)]
        + [(held[1].at[:, j, i, :, band(1)], two_got[1].at[k, i]) for i in range(n_t)],
    )
    finish(one)

    def add_one(n):
        zi, yi = n // ny, n % ny
        owns = (held[0][zi, yi, :, lanes(t, 0)], held[1][zi, yi, t, :, band(0)], held[2][zi, yi, t])
        for i in range(3):
            one_held[i][zi, yi] = total(owns[i], one_got[i], (zi, yi)).astype(one_held[i].dtype)

    loop(nz * ny, add_one)
    one = along("y", y, lambda j, k: [(one_held[i].at[:, j], one_last[i].at[k]) for i in range(3)])
    finish(two)

    def add_two(zi):
        for i in range(n_t):
            owns = (held[0][zi, y, :, lanes(i, 1)], held[1][zi, y, i, :, band(1)])
            for j in range(2):
                two_held[j][i, zi] = total(owns[j], two_got[j], (i, zi)).astype(two_held[j].dtype)

    loop(nz, add_two)
    two = along("tensor", t, lambda j, k: [(two_held[i].at[j], two_last[i].at[k]) for i in range(2)])
    finish(one)
    halves = [
        (slice(0, cols // 2), slice(cols // 2, cols)),
        (band(0), band(1)),
        (slice(None),),
    ]

    def end_one(zi):
        for i in range(3):
            value = total(one_held[i][zi, y], one_last[i], (zi,))
            end[i][zi, :, halves[i][0]] = value.astype(end[i].dtype)

    loop(nz, end_one)
    finish(two)

    def end_two(zi):
        for i in range(2):
            value = total(two_held[i][t, zi], two_last[i], (zi,))
            end[i][zi, :, halves[i][1]] = value.astype(end[i].dtype)

    loop(nz, end_two)
    finish(along("z", z, lambda j, k: [(end[i].at[j], end_got[i].at[k]) for i in range(3)]))
    results = [total(end[i][z], end_got[i], ()) for i in range(3)]
    outs[2][...] = results[2]
    if heads == 0:
        outs[0][...] = results[0]
        outs[1][...] = results[1]
        return
    width = cols // (3 * heads)
    jump = outs[1].shape[1]
    for h in range(heads):
        outs[1][h] = results[1][h * jump : (h + 1) * jump]
        for i in range(3):
            at = (i * heads + h) * width
            outs[0][:, h, i * width : (i + 1) * width] = results[0][:, at : at + width]


def scatter_grads(qkv, proj, small, n_dp, n_t, heads=0):
    nz, ny = qkv.shape[:2]
    rows, cols = qkv.shape[3], qkv.shape[4] // n_t
    tails = [(rows, cols), proj.shape[4:], small.shape[4:]]
    kinds = [BF16, BF16, F32]
    parts = [(rows, cols // 2), (proj.shape[4], proj.shape[5] // 2), small.shape[4:]]
    wide = [(rows, n_t * cols), (n_t,) + proj.shape[4:], (n_t,) + small.shape[4:]]

    def room(lead, shapes):
        return [pltpu.VMEM(lead + shape, kind) for shape, kind in zip(shapes, kinds)]

    scratch = room((1, nz, ny), wide) + room((nz, ny), wide)
    scratch += room((n_t - 1, nz, ny), parts) + room((nz, ny), parts) + room((ny - 1, nz), parts)
    scratch += room((ny - 1, n_t, nz), parts[:2]) + room((n_t, nz), parts[:2]) + room((n_t - 1, nz), parts[:2])
    scratch += room((nz,), tails) + room((nz - 1,), tails)
    slots = 3 + 5 * (n_t - 1) + (3 + 2 * n_t) * (ny - 1) + 3 * (nz - 1)
    shapes = list(tails)
    if heads:
        shapes[:2] = [(rows, heads, cols // heads), (heads, proj.shape[4] // heads, proj.shape[5])]
    scratch += [pltpu.SemaphoreType.DMA((slots,)), pltpu.SemaphoreType.DMA((slots,))]
    return pl.pallas_call(
        functools.partial(scatter_kernel, ny, nz, n_t, heads),
        out_shape=[jax.ShapeDtypeStruct(shape, F32) for shape in shapes],
        in_specs=[ANYWHERE] * 3,
        out_specs=[ANYWHERE] * 3,
        scratch_shapes=scratch,
        compiler_params=pltpu.CompilerParams(collective_id=1, has_side_effects=True),
    )(qkv, proj, small)


def standardise(v):
    centre = jnp.mean(v, axis=-1, keepdims=True)
    centered = v - centre
    inverse = lax.rsqrt(jnp.mean(centered * centered, axis=-1, keepdims=True) + EPS)
    return centered * inverse, inverse


def norm_back(grad, unit, inverse):
    return inverse * (
        grad
        - jnp.mean(grad, axis=-1, keepdims=True)
        - unit * jnp.mean(grad * unit, axis=-1, keepdims=True)
    )


def two_parts(v):
    high = v.astype(BF16)
    return high, (v - high.astype(F32)).astype(BF16)


def gate_softmax(c, router, experts):
    lane = lax.broadcasted_iota(jnp.int32, (c.shape[0], router.shape[1]), 1)
    logits = jnp.where(lane < experts, dot(c, router, ((1,), (0,))), -1e30)
    raised = jnp.exp(logits - jnp.max(logits, axis=-1, keepdims=True))
    return raised / jnp.sum(raised, axis=-1, keepdims=True), lane


def key_softmax(query, keys, gap):
    scores = dot(query, keys, ((1,), (1,)))
    col = lax.broadcasted_iota(jnp.int32, scores.shape, 1)
    scores = jnp.where((col < gap[0]) | (col >= gap[1]), scores, -1e30)
    raised = jnp.exp(scores - jnp.max(scores, axis=-1, keepdims=True))
    return raised * (1.0 / jnp.sum(raised, axis=-1, keepdims=True))


def pairs(n_t, block):
    return [
        (3 * block * s + 128 * i, block * s + 128 * i) for s in range(n_t) for i in range(block // 128)
    ]


def layer_kernel(
    experts,
    n_t,
    block,
    count,
    factor,
    tokens,
    cotangent,
    moved_x,
    moved_cot,
    router,
    flat_row,
    flat_col,
    expert_col,
    order,
    win,
    wout,
    live,
    norms,
    qkv,
    proj_in,
    out,
    grad_x,
    gqkv_out,
    gproj_out,
    grouter,
    gnorms,
    gin_mine,
    gout_mine,
    x_in,
    cot_own,
    proj,
    dhidden_in,
    edge_o,
    edge_g,
    edge_sent,
    edge_o_got,
    edge_g_got,
    c_own,
    hidden_in,
    mixed,
    context,
    c_all,
    cot_all,
    gates,
    sent,
    got,
    ret,
    pay,
    paid,
    mix,
    dx,
    dgate,
    dmixed,
    gqkv,
    gproj,
    y_acc,
    dx_acc,
    win_got,
    wout_got,
    gin,
    gout,
    gin_half,
    gout_half,
    gin_got,
    gout_got,
    w_sems,
    c_sems,
    cot_sems,
    edge_sems,
    go_send,
    go_recv,
    back_send,
    back_recv,
    pay_sems,
    grad_sems,
):
    batches, rows, d = cot_own.shape
    n_dp = lax.axis_size("dp")
    dp, t = lax.axis_index("dp"), lax.axis_index("tensor")
    share = sent.shape[1] // n_dp
    hidden = win.shape[1]
    other = 1 - t
    partner = (dp, other)
    own_rows, strip = tokens.shape[1], edge_o.shape[1]
    head, edge = rows - strip, own_rows - count
    gap = (jnp.where(t == 0, count, count - edge), jnp.where(t == 0, rows, rows - edge))

    barrier = pltpu.get_barrier_semaphore()
    pl.semaphore_signal(barrier, inc=1, device_id=partner, device_id_type=MESH)

    def hello(k, carry):
        pl.semaphore_signal(barrier, inc=1, device_id=((dp + k) % n_dp, t), device_id_type=MESH)
        return carry

    lax.fori_loop(1, n_dp, hello, 0)
    pl.semaphore_wait(barrier, n_dp)

    def slot_codes(shape, axis):
        q = lax.broadcasted_iota(jnp.int32, shape, axis)
        return q + (q >> (share.bit_length() - 1)) * share * (n_t - 1) + t * share

    def image(i):
        return pl.ds(pl.multiple_of(i * rows, 16), rows)

    def part(i):
        return pl.ds(pl.multiple_of(i * share, 16), share)

    def remote(src, dst, sems, i, j, device):
        return pltpu.make_async_remote_copy(
            src_ref=src,
            dst_ref=dst,
            send_sem=sems[0].at[i, j],
            recv_sem=sems[1].at[i, j],
            device_id=device,
            device_id_type=MESH,
        )

    def c_copy(m):
        return pltpu.make_async_remote_copy(
            src_ref=c_own.at[m],
            dst_ref=c_all.at[m, image(t)],
            send_sem=c_sems.at[0, m],
            recv_sem=c_sems.at[1, m],
            device_id=partner,
            device_id_type=MESH,
        )

    def cot_copy(m):
        return pltpu.make_async_remote_copy(
            src_ref=cot_own.at[m],
            dst_ref=cot_all.at[m, image(t)],
            send_sem=cot_sems.at[0, m],
            recv_sem=cot_sems.at[1, m],
            device_id=partner,
            device_id_type=MESH,
        )

    def go_copy(m, k):
        to = (dp + k) % n_dp
        return remote(sent.at[m, part(to)], got.at[m, part(dp)], (go_send, go_recv), m, k - 1, (to, t))

    def back_copy(m, k):
        to = (dp + k) % n_dp
        return remote(got.at[m, part(to)], ret.at[m, part(dp)], (back_send, back_recv), m, k - 1, (to, t))

    def pay_copy(m):
        return pltpu.make_async_remote_copy(
            src_ref=pay.at[m],
            dst_ref=paid.at[m],
            send_sem=pay_sems.at[0, m],
            recv_sem=pay_sems.at[1, m],
            device_id=partner,
            device_id_type=MESH,
        )

    def grad_copy(i):
        src, dst = ((gin_half, gin_got), (gout_half, gout_got))[i // 2]
        size = src.shape[0] // 2
        band = pl.ds(i % 2 * size, size)
        return pltpu.make_async_remote_copy(
            src_ref=src.at[band],
            dst_ref=dst.at[band],
            send_sem=grad_sems.at[0, i],
            recv_sem=grad_sems.at[1, i],
            device_id=partner,
            device_id_type=MESH,
        )

    def w_copy(i):
        return pltpu.make_async_remote_copy(
            src_ref=(win, wout)[i],
            dst_ref=(win_got, wout_got)[i],
            send_sem=w_sems.at[0, i],
            recv_sem=w_sems.at[1, i],
            device_id=partner,
            device_id_type=MESH,
        )

    def every(body):
        def step(k, carry):
            body(k)
            return carry

        lax.fori_loop(1, n_dp, step, 0)

    low = lax.broadcasted_iota(jnp.int32, (rows, 128), 1) < 64

    def edge_copy(i, m):
        return pltpu.make_async_remote_copy(
            src_ref=(edge_o, edge_sent)[i].at[m],
            dst_ref=(edge_o_got, edge_g_got)[i].at[m],
            send_sem=edge_sems.at[2 * i, m],
            recv_sem=edge_sems.at[2 * i + 1, m],
            device_id=partner,
            device_id_type=MESH,
        )

    for own_ref, ref, moved in ((cot_own, cotangent, moved_cot), (x_in, tokens, moved_x)):
        own_ref[:, :head] = ref[:, :head]

        @pl.when(t == 0)
        def _(own_ref=own_ref, ref=ref):
            own_ref[:, head:] = ref[:, head:rows]

        @pl.when(t != 0)
        def _(own_ref=own_ref, moved=moved):
            own_ref[:, head:] = moved[...]

    def permutation():
        return (order[...] == lax.broadcasted_iota(jnp.int32, (d, d), 1)).astype(F32).astype(BF16)

    proj[...] = dot(permutation(), proj_in[...], ((0,), (0,))).astype(BF16)

    def attend(m, carry):
        cot_copy(m).start()
        cot_all[m, image(t)] = cot_own[m]
        xf = x_in[m].astype(F32)
        unit, _ = standardise(xf)
        a = (unit * norms[0:1] + norms[1:2]).astype(BF16)
        for s in range(n_t):
            for i in range(3):
                cols = slice((3 * s + i) * block, (3 * s + i + 1) * block)
                projected = dot(a, qkv[:, cols], ((1,), (0,)))
                mixed[m, :, cols] = (projected * factor if i == 0 else projected).astype(BF16)
        for col, dest in pairs(n_t, block):
            query = mixed[m, :, col : col + 128]
            keys = mixed[m, :, col + block : col + block + 128]
            values = mixed[m, :, col + 2 * block : col + 2 * block + 128]
            zero = jnp.zeros_like(query)
            parts = []
            for own in (low, ~low):
                probs = key_softmax(jnp.where(own, query, zero), keys, gap)
                parts.append(dot(probs.astype(BF16), values, ((1,), (0,))))
            context[m, :, dest : dest + 128] = jnp.where(low, parts[0], parts[1]).astype(BF16)
        hidden = xf + live[m] * dot(context[m], proj[...], ((1,), (0,)))
        hidden_in[m] = hidden
        unit, _ = standardise(hidden)
        c = (unit * norms[2:3] + norms[3:4]).astype(BF16)
        c_own[m] = c
        c_all[m, image(t)] = c
        c_copy(m).start()
        return carry

    lax.fori_loop(0, batches, attend, 0)
    w_copy(0).start()
    w_copy(1).start()

    lane = lax.broadcasted_iota(jnp.int32, (2 * rows, router.shape[1]), 1)

    def dispatch(m, carry):
        c_copy(m).wait_recv()
        cot_copy(m).wait_recv()
        c = c_all[m]
        logits = jnp.where(lane < experts, dot(c, router[...], ((1,), (0,))), -1e30)
        raised = jnp.exp(logits - jnp.max(logits, axis=-1, keepdims=True))
        probs = raised / jnp.sum(raised, axis=-1, keepdims=True)
        cot = cot_all[m].astype(F32)
        scaled = []
        for k in range(2):
            gate = jnp.sum(jnp.where(lane == expert_col[m, :, k : k + 1], probs, 0.0), axis=-1, keepdims=True)
            gates[m, :, k : k + 1] = gate
            scaled.append((gate * cot).astype(BF16))
        codes = slot_codes((n_dp * share, 1), 0)
        picks = [(flat_row[m, k : k + 1, :] == codes).astype(F32).astype(BF16) for k in range(2)]
        sent[m, :, :d] = dot(picks[0] + picks[1], c, ((1,), (0,))).astype(BF16)
        moved = dot(picks[0], scaled[0], ((1,), (0,))) + dot(picks[1], scaled[1], ((1,), (0,)))
        sent[m, :, d:] = moved.astype(BF16)
        every(lambda k: go_copy(m, k).start())
        got[m, part(dp)] = sent[m, part(dp)]
        return carry

    lax.fori_loop(0, batches, dispatch, 0)

    tile = 256

    def clear(i, carry):
        cols = pl.ds(pl.multiple_of(i * tile, tile), tile)
        for into in (gin, gin_mine):
            into[:, cols] = jnp.zeros((d, tile), F32)
        for into in (gout, gout_mine):
            into[cols, :] = jnp.zeros((tile, d), F32)
        return carry

    lax.fori_loop(0, hidden // tile, clear, 0)

    def expert_step(m, carry):
        every(lambda k: go_copy(m, k).wait_recv())
        y_acc[...] = jnp.zeros_like(y_acc)
        dx_acc[...] = jnp.zeros_like(dx_acc)

        def chunk(win, wout, gin, gout, i, inner):
            cols = pl.ds(pl.multiple_of(i * tile, tile), tile)
            x = got[m, :, :d]
            dprod = got[m, :, d:]
            w1 = win[:, cols]
            w2 = wout[cols, :]
            pre = dot(x, w1, ((1,), (0,)))
            square = pre * pre
            th = jnp.tanh(GELU_A * pre * (1.0 + GELU_B * square))
            active = (0.5 * pre * (1.0 + th)).astype(BF16)
            slope = 0.5 * (1.0 + th) + 0.5 * pre * (1.0 - th * th) * (GELU_A * (1.0 + 3.0 * GELU_B * square))
            dpre = (dot(dprod, w2, ((1,), (1,))) * slope).astype(BF16)
            gin[:, cols] += dot(x, dpre, ((0,), (0,)))
            gout[cols, :] += dot(active, dprod, ((0,), (0,)))
            y_acc[...] += dot(active, w2, ((1,), (0,)))
            dx_acc[...] += dot(dpre, w1, ((1,), (1,)))
            return inner

        def own_half():
            lax.fori_loop(0, hidden // tile, functools.partial(chunk, win, wout, gin_mine, gout_mine), 0)

        def other_half():
            lax.fori_loop(0, hidden // tile, functools.partial(chunk, win_got, wout_got, gin, gout), 0)

        @pl.when(m < batches - 1)
        def _():
            own_half()

            @pl.when(m == 0)
            def _():
                w_copy(0).wait_recv()
                w_copy(1).wait_recv()

            other_half()

        @pl.when(m == batches - 1)
        def _():
            other_half()
            gin_half[...] = gin[...].astype(BF16)
            gout_half[...] = gout[...].astype(BF16)
            grad_copy(0).start()
            grad_copy(1).start()
            own_half()

        got[m, :, :d] = y_acc[...].astype(BF16)
        got[m, :, d:] = dx_acc[...].astype(BF16)
        every(lambda k: back_copy(m, k).start())
        ret[m, part(dp)] = got[m, part(dp)]
        return carry

    lax.fori_loop(0, batches, expert_step, 0)

    def combine(m, carry):
        every(lambda k: back_copy(m, k).wait_recv())
        codes = slot_codes((1, n_dp * share), 1)
        for i in (other, t):
            picks = [(flat_col[m, image(i), k : k + 1] == codes).astype(F32).astype(BF16) for k in range(2)]
            one = dot(picks[0], ret[m, :, :d], ((1,), (0,)))
            two = dot(picks[1], ret[m, :, :d], ((1,), (0,)))
            d_rows = dot(picks[0] + picks[1], ret[m, :, d:], ((1,), (0,)))
            cot = cot_all[m, image(i)].astype(F32)
            gate = gates[m, image(i)]
            mixture = gate[:, 0:1] * one + gate[:, 1:2] * two
            col = lax.broadcasted_iota(jnp.int32, (rows, 128), 1)
            dg = jnp.where(col == 0, jnp.sum(one * cot, axis=-1, keepdims=True), 0.0)
            dg = dg + jnp.where(col == 1, jnp.sum(two * cot, axis=-1, keepdims=True), 0.0)
            if i is other:
                pay[m, :, :d] = mixture.astype(BF16)
                pay[m, :, d : 2 * d] = d_rows.astype(BF16)
                pay[m, :, 2 * d :] = dg.astype(BF16)
                pay_copy(m).start()
            else:
                mix[m] = mixture
                dx[m] = d_rows
                dgate[m] = dg
        return carry

    gqkv[...] = jnp.zeros_like(gqkv)
    gproj[...] = jnp.zeros_like(gproj)
    grouter[...] = jnp.zeros_like(grouter)
    gnorms[...] = jnp.zeros_like(gnorms)

    def retreat(m):
        pay_copy(m).wait_recv()
        hidden = hidden_in[m]
        result = (hidden + mix[m] + paid[m, :, :d].astype(F32)).astype(BF16)
        out[m, :head] = result[:head]
        edge_o[m] = result[head:]
        edge_copy(0, m).start()
        unit, inverse = standardise(hidden)
        c = (unit * norms[2:3] + norms[3:4]).astype(BF16)
        probs, lane = gate_softmax(c, router[...], experts)
        dg = dgate[m] + paid[m, :, 2 * d :].astype(F32)
        dprobs = jnp.zeros_like(probs)
        for k in range(2):
            dprobs = dprobs + jnp.where(lane == expert_col[m, image(t), k : k + 1], dg[:, k : k + 1], 0.0)
        dlogits = probs * (dprobs - jnp.sum(dprobs * probs, axis=-1, keepdims=True))
        dc = dx[m] + paid[m, :, d : 2 * d].astype(F32)
        for piece in two_parts(dlogits):
            grouter[...] += dot(c, piece, ((0,), (0,)))
            dc = dc + dot(piece, router[...], ((1,), (1,)))
        gnorms[2:3] += jnp.sum(dc * unit, axis=0, keepdims=True)
        gnorms[3:4] += jnp.sum(dc, axis=0, keepdims=True)
        dhidden = cot_all[m, image(t)].astype(F32) + norm_back(dc * norms[2:3], unit, inverse)
        dhidden_in[...] = dhidden
        dattn = (live[m] * dhidden).astype(BF16)
        gproj[...] += dot(context[m], dattn, ((0,), (0,)))
        dcontext = dot(dattn, proj[...], ((1,), (1,))).astype(BF16)
        for col, dest in pairs(n_t, block):
            query = mixed[m, :, col : col + 128]
            keys = mixed[m, :, col + block : col + block + 128]
            values = mixed[m, :, col + 2 * block : col + 2 * block + 128]
            grads = dcontext[:, dest : dest + 128]
            zero = jnp.zeros_like(query)
            parts = []
            for own in (low, ~low):
                probs = key_softmax(jnp.where(own, query, zero), keys, gap)
                dvalues = dot(probs.astype(BF16), grads, ((0,), (0,)))
                dweights = dot(jnp.where(own, grads, zero), values, ((1,), (1,)))
                dscores = probs * (dweights - jnp.sum(dweights * probs, axis=-1, keepdims=True))
                dscores = dscores.astype(BF16)
                parts.append(
                    (dot(dscores, keys, ((1,), (0,))), dot(dscores, query, ((0,), (0,))), dvalues)
                )
            for i in range(3):
                both = jnp.where(low, parts[0][i], parts[1][i]).astype(BF16)
                if i == 0:
                    both = both * BF16(factor)
                dmixed[:, col + i * block : col + i * block + 128] = both
        unit, inverse = standardise(x_in[m].astype(F32))
        a = (unit * norms[0:1] + norms[1:2]).astype(BF16)
        gqkv[...] += dot(a, dmixed[...], ((0,), (0,)))
        da = dot(dmixed[...], qkv[...], ((1,), (1,)))
        gnorms[0:1] += jnp.sum(da * unit, axis=0, keepdims=True)
        gnorms[1:2] += jnp.sum(da, axis=0, keepdims=True)
        result = dhidden_in[...] + norm_back(da * norms[0:1], unit, inverse)
        grad_x[m, :head] = result[:head]
        edge_g[m] = result[head:]
        edge_sent[m] = result[head:].astype(BF16)
        edge_copy(1, m).start()

    pieces = 4

    def finish(m, carry):
        @pl.when(m < batches)
        def _():
            combine(m, 0)

        @pl.when(m == 0)
        def _():
            grad_copy(2).start()

        @pl.when(m == batches - 1)
        def _():
            grad_copy(3).start()

        @pl.when(m > 0)
        def _():
            retreat(m - 1)

        return carry

    lax.fori_loop(0, batches + 1, finish, 0)
    gqkv_out[...] = gqkv[...].astype(BF16)
    gproj_out[...] = dot(permutation(), gproj[...].astype(BF16), ((1,), (0,))).astype(BF16)

    @pl.when(t != 0)
    def _():
        out[:, head:] = tokens[:, head:]
        grad_x[:, head:] = cotangent[:, head:].astype(F32)

    first = own_rows - strip
    near = lax.broadcasted_iota(jnp.int32, (16, d), 0) < strip - edge

    def place(m, carry):
        edge_copy(0, m).wait()
        edge_copy(1, m).wait()

        @pl.when(t == 0)
        def _():
            for ref, mine, theirs in ((out, edge_o, edge_o_got), (grad_x, edge_g, edge_g_got)):
                ref[m, head:first] = mine[m, : first - head]
                blend = jnp.where(
                    near,
                    mine[m, first - head : first - head + 16].astype(F32),
                    theirs[m, :16].astype(F32),
                )
                ref[m, first : first + 16] = blend.astype(ref.dtype)
                ref[m, first + 16 :] = theirs[m, 16:].astype(ref.dtype)

        return carry

    lax.fori_loop(0, batches, place, 0)
    for i in range(pieces):
        grad_copy(i).wait()
    gin_mine[...] += gin_got[...].astype(F32)
    gout_mine[...] += gout_got[...].astype(F32)
    w_copy(0).wait_send()
    w_copy(1).wait_send()

    def drain(m, carry):
        c_copy(m).wait_send()
        cot_copy(m).wait_send()
        pay_copy(m).wait_send()
        every(lambda k: go_copy(m, k).wait_send())
        every(lambda k: back_copy(m, k).wait_send())
        return carry

    lax.fori_loop(0, batches, drain, 0)


def layer(held, moved, router, flat, expert_of, order, win, wout, live, norms, qkv, proj, statics):
    batches, own_rows, d = held[0].shape
    experts, n_dp, n_t, block, count, factor, cap = statics
    rows, strip = live.shape[1], moved[0].shape[1]
    slots = n_dp * cap // n_t
    half = win.shape[1]
    wide = 3 * n_t * block
    dma = pltpu.SemaphoreType.DMA
    return pl.pallas_call(
        functools.partial(layer_kernel, experts, n_t, block, count, factor),
        out_shape=[
            jax.ShapeDtypeStruct((batches, own_rows, d), BF16),
            jax.ShapeDtypeStruct((batches, own_rows, d), F32),
            jax.ShapeDtypeStruct((d, wide), BF16),
            jax.ShapeDtypeStruct((d, d), BF16),
            jax.ShapeDtypeStruct((d, router.shape[1]), F32),
            jax.ShapeDtypeStruct((8, d), F32),
            jax.ShapeDtypeStruct((d, half), F32),
            jax.ShapeDtypeStruct((half, d), F32),
        ],
        in_specs=[ANYWHERE] * 15,
        out_specs=[ANYWHERE] * 8,
        scratch_shapes=[
            pltpu.VMEM((batches, rows, d), BF16),
            pltpu.VMEM((batches, rows, d), BF16),
            pltpu.VMEM((d, d), BF16),
            pltpu.VMEM((rows, d), F32),
            pltpu.VMEM((batches, strip, d), BF16),
            pltpu.VMEM((batches, strip, d), F32),
            pltpu.VMEM((batches, strip, d), BF16),
            pltpu.VMEM((batches, strip, d), BF16),
            pltpu.VMEM((batches, strip, d), BF16),
            pltpu.VMEM((batches, rows, d), BF16),
            pltpu.VMEM((batches, rows, d), F32),
            pltpu.VMEM((batches, rows, wide), BF16),
            pltpu.VMEM((batches, rows, d), BF16),
            pltpu.VMEM((batches, 2 * rows, d), BF16),
            pltpu.VMEM((batches, 2 * rows, d), BF16),
            pltpu.VMEM((batches, 2 * rows, 128), F32),
            pltpu.VMEM((batches, slots, 2 * d), BF16),
            pltpu.VMEM((batches, slots, 2 * d), BF16),
            pltpu.VMEM((batches, slots, 2 * d), BF16),
            pltpu.VMEM((batches, rows, 2 * d + 128), BF16),
            pltpu.VMEM((batches, rows, 2 * d + 128), BF16),
            pltpu.VMEM((batches, rows, d), F32),
            pltpu.VMEM((batches, rows, d), F32),
            pltpu.VMEM((batches, rows, 128), F32),
            pltpu.VMEM((rows, wide), BF16),
            pltpu.VMEM((d, wide), F32),
            pltpu.VMEM((d, d), F32),
            pltpu.VMEM((slots, d), F32),
            pltpu.VMEM((slots, d), F32),
            pltpu.VMEM((d, half), BF16),
            pltpu.VMEM((half, d), BF16),
            pltpu.VMEM((d, half), F32),
            pltpu.VMEM((half, d), F32),
            pltpu.VMEM((d, half), BF16),
            pltpu.VMEM((half, d), BF16),
            pltpu.VMEM((d, half), BF16),
            pltpu.VMEM((half, d), BF16),
            dma((2, 2)),
            dma((2, batches)),
            dma((2, batches)),
            dma((4, batches)),
            dma((batches, n_dp - 1)),
            dma((batches, n_dp - 1)),
            dma((batches, n_dp - 1)),
            dma((batches, n_dp - 1)),
            dma((2, batches)),
            dma((2, 4)),
        ],
        compiler_params=pltpu.CompilerParams(
            collective_id=2, has_side_effects=True, vmem_limit_bytes=67043328
        ),
    )(
        *held,
        *moved,
        router,
        flat,
        flat.transpose(0, 2, 1),
        expert_of.transpose(0, 2, 1),
        order,
        win,
        wout,
        live,
        norms,
        qkv,
        proj,
    )


def general(
    tokens,
    w_qkv,
    w_proj,
    w_in,
    w_out,
    w_router,
    gain_attn,
    shift_attn,
    gain_moe,
    shift_moe,
    live_rows,
    chosen,
    priority,
    cotangent,
):
    batches, own_rows, d = tokens.shape
    rows = live_rows.shape[1]
    n_dp = lax.axis_size("dp")
    n_t = lax.axis_size("tensor")
    t = lax.axis_index("tensor")
    heads_here = w_qkv.shape[1]
    heads = heads_here * n_t
    width = w_qkv.shape[2] // 3
    experts = w_in.shape[0] * n_dp
    cap = 2 * rows // experts
    share = cap // n_t
    images = rows // SEQ
    span = images * SEQ
    per = -(-images // n_t)
    work = per * SEQ
    total = n_t * work
    factor = width ** (-0.5)
    highest = lax.Precision.HIGHEST

    small = jnp.concatenate(
        [w_router] + [v[:, None] for v in (gain_attn, shift_attn, gain_moe, shift_moe)], axis=1
    )
    small = jnp.pad(small, ((0, 0), (0, 128 - small.shape[1])))
    block = heads_here * width
    qkv_block = w_qkv.reshape(-1, heads_here, 3, width).transpose(0, 2, 1, 3).reshape(-1, 3 * block)
    fill = -3 * block % 128
    qkv_block = jnp.pad(qkv_block, ((0, 0), (0, fill)))
    qkv, proj, small = gather_weights(qkv_block, w_proj.reshape(-1, d), small, n_dp, n_t)
    qkv = qkv.reshape(d, n_t, 3 * block + fill)[:, :, : 3 * block].reshape(d, -1)
    router = small[:, :experts]
    gain_one, shift_one, gain_two, shift_two = (small[:, experts + i].astype(F32) for i in range(4))
    proj = proj.reshape(n_dp, n_t, heads_here, w_proj.shape[1], d)
    proj = proj.transpose(1, 2, 0, 3, 4).reshape(heads * width, d)
    win = lax.all_gather(w_in[0], "tensor", axis=1, tiled=True)
    wout = lax.all_gather(w_out[0], "tensor", axis=0, tiled=True)
    cot_all = lax.all_gather(cotangent, "tensor", axis=1, tiled=True)

    def pad_rows(v, n):
        return jnp.pad(v, ((0, 0), (0, n - v.shape[1])) + ((0, 0),) * (v.ndim - 2))

    def own(v):
        return lax.dynamic_slice_in_dim(v, t * work, work, 1)

    edge = own_rows - work
    direct = n_t == 2 and per == 1 and edge >= 0
    if direct:
        moved = lax.ppermute(tokens[:, work:], "tensor", [(0, 1)])
        x = jnp.where(
            t == 0, tokens[:, :work], jnp.concatenate([moved, tokens[:, : work - edge]], axis=1)
        )
    else:
        x = own(pad_rows(lax.all_gather(tokens, "tensor", axis=1, tiled=True)[:, :span], total))
    x = x.astype(F32)
    live = live_rows[:, :span]
    live_all = pad_rows(live, total)
    live_own = own(live_all).astype(F32)[:, :, None]
    cot_all = pad_rows(cot_all[:, :span], total)
    dy = own(cot_all).astype(F32)

    rank = priority[:, 0, :span]
    first, second = chosen[:, :span, 0], chosen[:, :span, 1]
    labels = jnp.arange(experts, dtype=jnp.int32)
    earlier = (rank[:, None, :] < rank[:, :, None]).astype(BF16)
    hit_one = (first[:, :, None] == labels).astype(F32)
    hit_two = (second[:, :, None] == labels).astype(F32)
    live_one = hit_one * live[:, :, None].astype(F32)
    live_two = hit_two * live[:, :, None].astype(F32)
    counts = jnp.einsum(
        "mrs,mse->mre",
        earlier,
        jnp.concatenate([live_one, live_two], axis=-1).astype(BF16),
        preferred_element_type=F32,
    )
    first_total = jnp.sum(live_one, axis=1, keepdims=True)
    slot_one = jnp.sum(counts[:, :, :experts] * hit_one, axis=-1).astype(jnp.int32)
    slot_two = jnp.sum((counts[:, :, experts:] + first_total) * hit_two, axis=-1).astype(jnp.int32)
    keep_one = (live > 0) & (slot_one < cap)
    keep_two = (live > 0) & (slot_two < cap)
    flat_one = jnp.where(keep_one, first * cap + slot_one, -1)
    flat_two = jnp.where(keep_two, second * cap + slot_two, -1)

    def spread(v, fill):
        return jnp.pad(v, ((0, 0), (0, total - span)), constant_values=fill)

    flat_one, flat_two = spread(flat_one, -1), spread(flat_two, -1)
    keep_one, keep_two = spread(keep_one, False), spread(keep_two, False)
    first, second = spread(first, 0), spread(second, 0)
    codes = (jnp.arange(experts)[:, None] * cap + t * share + jnp.arange(share)[None, :]).reshape(-1)
    pick_one = flat_one[:, None, :] == codes[None, :, None]
    pick_two = flat_two[:, None, :] == codes[None, :, None]

    normed_one = layer_norm(x, gain_one, shift_one).astype(BF16)
    mixed = dot(normed_one, qkv, ((2,), (0,)))
    split = heads * width
    shape = (batches * per, SEQ, heads, width)
    mixed = mixed.reshape(batches, work, n_t, 3, block)
    query = (mixed[:, :, :, 0] * factor).astype(BF16).reshape(shape)
    keys = mixed[:, :, :, 1].astype(BF16).reshape(shape)
    values = mixed[:, :, :, 2].astype(BF16).reshape(shape)
    scores = jnp.einsum("iqhc,ikhc->ihqk", query, keys, preferred_element_type=F32)
    probs = jax.nn.softmax(scores, axis=-1)
    weights = probs.astype(BF16)
    context = jnp.einsum("ihqk,ikhc->iqhc", weights, values, preferred_element_type=F32)
    context = context.astype(BF16).reshape(batches, work, split)
    attn = dot(context, proj, ((2,), (0,)))
    hidden = x + live_own * attn
    normed_two = layer_norm(hidden, gain_two, shift_two).astype(BF16)

    c_all = lax.all_gather(normed_two, "tensor", axis=1, tiled=True)
    gate_probs = jax.nn.softmax(dot(c_all, router, ((2,), (0,))), axis=-1)
    hits_one = (first[:, :, None] == labels).astype(F32)
    hits_two = (second[:, :, None] == labels).astype(F32)
    gate_one = jnp.sum(gate_probs * hits_one, axis=-1) * keep_one
    gate_two = jnp.sum(gate_probs * hits_two, axis=-1) * keep_two
    picked = (pick_one | pick_two).astype(BF16)
    sent = jnp.einsum(
        "mqr,mrd->mqd",
        picked,
        jnp.concatenate([c_all, cot_all], axis=-1),
        preferred_element_type=F32,
    )
    gate_slot = jnp.sum(
        jnp.where(pick_one, gate_one[:, None, :], 0.0) + jnp.where(pick_two, gate_two[:, None, :], 0.0),
        axis=-1,
        keepdims=True,
    )
    sent = jnp.concatenate(
        [sent[..., :d].astype(BF16), (sent[..., d:] * gate_slot).astype(BF16)], axis=-1
    )
    sent = sent.reshape(batches, experts, share, 2 * d)
    got = lax.all_to_all(sent, "dp", 1, 1, tiled=True).reshape(-1, 2 * d)
    produced, d_in, grad_in, grad_out = expert(got[:, :d], got[:, d:], win, wout)
    back = jnp.concatenate([produced, d_in], axis=-1).reshape(batches, n_dp, share, 2 * d)
    back = lax.all_to_all(back, "dp", 1, 1, tiled=True).reshape(batches, experts * share, 2 * d)
    grad_in = lax.psum_scatter(grad_in, "tensor", scatter_dimension=1, tiled=True).astype(F32)
    grad_out = lax.psum_scatter(grad_out, "tensor", scatter_dimension=0, tiled=True).astype(F32)

    part_one = jnp.einsum("mqr,mqd->mrd", pick_one.astype(BF16), back[..., :d], preferred_element_type=F32)
    part_two = jnp.einsum("mqr,mqd->mrd", pick_two.astype(BF16), back[..., :d], preferred_element_type=F32)
    d_rows = jnp.einsum("mqr,mqd->mrd", picked, back[..., d:], preferred_element_type=F32)
    mixture = gate_one[:, :, None] * part_one + gate_two[:, :, None] * part_two
    cot_wide = cot_all.astype(F32)
    dgate_one = jnp.sum(part_one * cot_wide, axis=-1, keepdims=True)
    dgate_two = jnp.sum(part_two * cot_wide, axis=-1, keepdims=True)
    dgates = jnp.concatenate([dgate_one, dgate_two], axis=-1)
    payload = jnp.concatenate(
        [mixture, d_rows, jnp.pad(dgates, ((0, 0), (0, 0), (0, 126)))], axis=-1
    ).astype(BF16)
    pieces = payload.reshape(batches, n_t, work, payload.shape[-1])

    def piece(k):
        return lax.dynamic_index_in_dim(pieces, (t + k) % n_t, 1, keepdims=False)

    payload = piece(0).astype(F32)
    for k in range(1, n_t):
        payload = payload + lax.ppermute(
            piece(k), "tensor", [(j, (j + k) % n_t) for j in range(n_t)]
        ).astype(F32)
    output = (hidden + payload[..., :d]).astype(BF16)
    dgates = payload[..., 2 * d : 2 * d + 2]

    own_probs = own(gate_probs)
    dprobs = own(hits_one) * dgates[..., 0:1] * own(keep_one)[:, :, None]
    dprobs = dprobs + own(hits_two) * dgates[..., 1:2] * own(keep_two)[:, :, None]
    dlogits = own_probs * (dprobs - jnp.sum(dprobs * own_probs, axis=-1, keepdims=True))
    grad_router = lax.dot_general(
        normed_two.astype(F32), dlogits, (((0, 1), (0, 1)), ((), ())), precision=highest
    )
    dc = payload[..., d : 2 * d] + lax.dot_general(
        dlogits, router.astype(F32), (((2,), (1,)), ((), ())), precision=highest
    )
    _, back_two = jax.vjp(layer_norm, hidden, gain_two, shift_two)
    dnorm, grad_gain_two, grad_shift_two = back_two(dc)
    dhidden = dy + dnorm
    dattn = (live_own * dhidden).astype(BF16)

    grad_proj = dot(context, dattn, ((0, 1), (0, 1)))
    dcontext = dot(dattn, proj, ((2,), (1,))).astype(BF16).reshape(shape)
    dvalues = jnp.einsum("ihqk,iqhc->ikhc", weights, dcontext, preferred_element_type=F32).astype(BF16)
    dweights = jnp.einsum("iqhc,ikhc->ihqk", dcontext, values, preferred_element_type=F32)
    dscores = (probs * (dweights - jnp.sum(dweights * probs, axis=-1, keepdims=True))).astype(BF16)
    dquery = jnp.einsum("ihqk,ikhc->iqhc", dscores, keys, preferred_element_type=F32).astype(BF16)
    dkeys = jnp.einsum("ihqk,iqhc->ikhc", dscores, query, preferred_element_type=F32).astype(BF16)
    dmixed = jnp.stack(
        [v.reshape(batches, work, n_t, block) for v in (dquery * BF16(factor), dkeys, dvalues)], axis=3
    ).reshape(batches, work, 3 * split)
    grad_qkv = dot(normed_one, dmixed, ((0, 1), (0, 1)))
    da = dot(dmixed, qkv, ((2,), (1,)))
    _, back_one = jax.vjp(layer_norm, x, gain_one, shift_one)
    dnorm, grad_gain_one, grad_shift_one = back_one(da)
    grad_x = dhidden + dnorm

    if direct:
        out_edge = lax.ppermute(output[:, :edge], "tensor", [(1, 0)])
        grad_edge = lax.ppermute(grad_x[:, :edge], "tensor", [(1, 0)])
        result = jnp.where(
            t == 0,
            jnp.concatenate([output, out_edge], axis=1),
            jnp.concatenate([output[:, edge:], tokens[:, work - edge :]], axis=1),
        )
        grad_tokens = jnp.where(
            t == 0,
            jnp.concatenate([grad_x, grad_edge], axis=1),
            jnp.concatenate([grad_x[:, edge:], cotangent[:, work - edge :].astype(F32)], axis=1),
        )
    else:
        here = (t * own_rows + jnp.arange(own_rows) < span)[None, :, None]

        def home(v, rest):
            full = pad_rows(lax.all_gather(v, "tensor", axis=1, tiled=True)[:, :span], rows)
            return jnp.where(here, lax.dynamic_slice_in_dim(full, t * own_rows, own_rows, 1), rest)

        result = home(output, tokens)
        grad_tokens = home(grad_x, cotangent.astype(F32))

    nz, ny = grid_sizes(n_dp)
    grad_qkv = jnp.pad(grad_qkv.astype(BF16).reshape(d, n_t, 3 * block), ((0, 0), (0, 0), (0, fill)))
    grad_qkv = grad_qkv.reshape(nz, ny, 2, d // n_dp, -1)
    grad_proj = grad_proj.astype(BF16).reshape(n_t, heads_here, n_dp, -1, d)
    grad_proj = grad_proj.transpose(2, 0, 1, 3, 4).reshape(nz, ny, 2, n_t, -1, d)
    smalls = jnp.concatenate(
        [grad_router] + [v[:, None] for v in (grad_gain_one, grad_shift_one, grad_gain_two, grad_shift_two)],
        axis=1,
    )
    smalls = jnp.pad(smalls, ((0, 0), (0, 128 - smalls.shape[1]))).reshape(nz, ny, 2, n_t, -1, 128)
    grad_qkv, grad_proj, smalls = scatter_grads(grad_qkv, grad_proj, smalls, n_dp, n_t)
    grad_qkv = grad_qkv[:, : 3 * block].reshape(-1, 3, heads_here, width).transpose(0, 2, 1, 3)
    return (
        result,
        grad_tokens,
        grad_qkv.reshape(w_qkv.shape),
        grad_proj.reshape(w_proj.shape),
        grad_in[None],
        grad_out[None],
        smalls[:, :experts],
        smalls[:, experts],
        smalls[:, experts + 1],
        smalls[:, experts + 2],
        smalls[:, experts + 3],
    )


def fast(
    tokens,
    w_qkv,
    w_proj,
    w_in,
    w_out,
    w_router,
    gain_attn,
    shift_attn,
    gain_moe,
    shift_moe,
    live_rows,
    chosen,
    priority,
    cotangent,
):
    batches, own_rows, d = tokens.shape
    rows = live_rows.shape[1]
    n_dp = lax.axis_size("dp")
    n_t = lax.axis_size("tensor")
    t = lax.axis_index("tensor")
    heads_here = w_qkv.shape[1]
    width = w_qkv.shape[2] // 3
    block = heads_here * width
    experts = n_dp
    cap = 2 * rows // experts
    share = cap // n_t
    span = n_t * SEQ
    padded = -(-SEQ // 16) * 16
    edge = own_rows - SEQ
    factor = width ** (-0.5)

    small = jnp.concatenate(
        [w_router] + [v[:, None] for v in (gain_attn, shift_attn, gain_moe, shift_moe)], axis=1
    )
    small = jnp.pad(small, ((0, 0), (0, 128 - small.shape[1])))
    qkv_block = w_qkv.reshape(-1, heads_here, 3, width).transpose(0, 2, 1, 3).reshape(-1, 3 * block)
    strip = -(-edge // 16) * 16
    qkv, proj, small, *moved = gather_weights(
        qkv_block, w_proj.reshape(-1, d), small, n_dp, n_t, (tokens, cotangent), strip
    )
    router = jnp.where(jnp.arange(128) < experts, small, 0)
    norms = jnp.pad(small[:, experts : experts + 4].astype(F32).T, ((0, 4), (0, 0)))
    order = jnp.arange(d, dtype=jnp.int32).reshape(n_t, heads_here, n_dp, -1)
    order = order.transpose(2, 0, 1, 3).reshape(d, 1)

    def lay(v, axis, fill=0):
        def rows_of(low, high):
            return lax.slice_in_dim(v, low, high, axis=axis)

        shape = v.shape[:axis] + (padded - SEQ,) + v.shape[axis + 1 :]
        hole = jnp.full(shape, fill, v.dtype)
        return jnp.concatenate(
            [rows_of(0, SEQ), hole, rows_of(own_rows, span), hole, rows_of(SEQ, own_rows)], axis=axis
        )

    def own(v, axis):
        return lax.dynamic_slice_in_dim(v, t * padded, padded, axis)

    live = live_rows[:, :span]
    rank = priority[:, 0, :span]
    picks = chosen[:, :span].transpose(0, 2, 1)
    labels = jnp.arange(experts, dtype=jnp.int32)
    earlier = (rank[:, None, :] < rank[:, :, None]).astype(BF16)
    hits = (picks[..., None] == labels).astype(F32)
    live_hits = hits * live[:, None, :, None].astype(F32)
    ahead = jnp.einsum("mrs,mkse->mkre", earlier, live_hits.astype(BF16), preferred_element_type=F32)
    firsts = jnp.sum(live_hits[:, :1], axis=2, keepdims=True)
    ahead = ahead + jnp.concatenate([jnp.zeros_like(firsts), firsts], axis=1)
    slot = jnp.sum(ahead * hits, axis=-1).astype(jnp.int32)
    keep = (live[:, None, :] > 0) & (slot < cap)
    flat = lay(jnp.where(keep, picks * cap + slot, -1), 2, -1)
    expert_of = lay(jnp.where(keep, picks, -1), 2, -1)
    live_own = own(lay(live.astype(F32)[:, :, None], 1), 1)

    output, grad_x, grad_qkv, grad_proj, grad_router, grad_norms, grad_in, grad_out = layer(
        (tokens, cotangent),
        moved,
        router,
        flat,
        expert_of,
        order,
        w_in[0],
        w_out[0],
        live_own,
        norms,
        qkv,
        proj.reshape(d, d),
        (experts, n_dp, n_t, block, SEQ, factor, cap),
    )
    nz, ny = grid_sizes(n_dp)
    lane = jnp.arange(128)
    smalls = jnp.where(lane < experts, grad_router, 0.0)
    smalls = smalls + jnp.pad(grad_norms[:4].T, ((0, 0), (experts, 124 - experts)))
    grad_qkv, grad_proj, smalls = scatter_grads(
        grad_qkv.reshape(nz, ny, 2, d // n_dp, -1),
        grad_proj.reshape(nz, ny, 2, n_t, -1, d),
        smalls.reshape(nz, ny, 2, n_t, -1, 128),
        n_dp,
        n_t,
        heads_here,
    )
    return (
        output,
        grad_x,
        grad_qkv,
        grad_proj,
        grad_in[None],
        grad_out[None],
        smalls[:, :experts],
        smalls[:, experts],
        smalls[:, experts + 1],
        smalls[:, experts + 2],
        smalls[:, experts + 3],
    )


def local(*args):
    tokens, w_qkv, live_rows = args[0], args[1], args[10]
    n_t = lax.axis_size("tensor")
    images = live_rows.shape[1] // SEQ
    block = w_qkv.shape[1] * (w_qkv.shape[2] // 3)
    edge = tokens.shape[1] - SEQ
    fits = tokens.shape[1] % 16 == 0 and 0 < edge <= SEQ // 2 and args[3].shape[0] == 1
    if n_t == 2 and images == 2 and fits and block % 128 == 0 and w_qkv.shape[2] == 192 and args[0].shape[0] > 1:
        return fast(*args)
    return general(*args)


def solution(mesh):
    both = ("dp", "tensor")
    return jax.shard_map(
        local,
        mesh=mesh,
        in_specs=(
            P(None, both, None),
            P("dp", "tensor", None),
            P("tensor", "dp", None),
            P("dp", None, "tensor"),
            P("dp", "tensor", None),
            P(both, None),
            P(both),
            P(both),
            P(both),
            P(both),
            P(None, "dp"),
            P(None, "dp", None),
            P(None, "dp", None),
            P(None, both, None),
        ),
        out_specs=(
            P(None, both, None),
            P(None, both, None),
            P("dp", "tensor", None),
            P("tensor", "dp", None),
            P("dp", None, "tensor"),
            P("dp", "tensor", None),
            P(both, None),
            P(both),
            P(both),
            P(both),
            P(both),
        ),
        check_vma=False,
    )
```

```python
import functools

import jax
import jax.numpy as jnp
import numpy as np
from jax import lax
from jax.experimental import pallas as pl
from jax.experimental.pallas import tpu as pltpu
from jax.sharding import PartitionSpec as P

SEQ = 197
EPS = 1e-06
F32 = jnp.float32
BF16 = jnp.bfloat16
GELU_A = 0.7978845608028654
GELU_B = 0.044715


def dot(a, b, dims):
    return lax.dot_general(a, b, (dims, ((), ())), preferred_element_type=F32)


def layer_norm(values, gain_vec, shift_vec):
    centre = jnp.mean(values, axis=-1, keepdims=True)
    centered = values - centre
    spread = jnp.mean(centered * centered, axis=-1, keepdims=True)
    return centered * lax.rsqrt(spread + EPS) * gain_vec + shift_vec


def expert_kernel(x_ref, dp_ref, win_ref, wout_ref, y_ref, dx_ref, gin_ref, gout_ref, y_acc, dx_acc):
    step = pl.program_id(0)
    last = pl.num_programs(0) - 1
    x = x_ref[...]
    dprod = dp_ref[...]
    win = win_ref[...]
    wout = wout_ref[...]
    pre = dot(x, win, ((1,), (0,)))
    square = pre * pre
    th = jnp.tanh(GELU_A * pre * (1.0 + GELU_B * square))
    active = (0.5 * pre * (1.0 + th)).astype(BF16)
    slope = 0.5 * (1.0 + th) + 0.5 * pre * (1.0 - th * th) * (GELU_A * (1.0 + 3.0 * GELU_B * square))
    dact = dot(dprod, wout, ((1,), (1,)))
    dpre = (dact * slope).astype(BF16)
    gin_ref[...] = dot(x, dpre, ((0,), (0,))).astype(BF16)
    gout_ref[...] = dot(active, dprod, ((0,), (0,))).astype(BF16)
    part_y = dot(active, wout, ((1,), (0,)))
    part_dx = dot(dpre, win, ((1,), (1,)))

    @pl.when(step == 0)
    def _():
        y_acc[...] = part_y
        dx_acc[...] = part_dx

    @pl.when(step > 0)
    def _():
        y_acc[...] += part_y
        dx_acc[...] += part_dx

    @pl.when(step == last)
    def _():
        y_ref[...] = y_acc[...].astype(BF16)
        dx_ref[...] = dx_acc[...].astype(BF16)


def expert(x, dprod, win, wout, tile=256):
    n, d = x.shape
    ff = win.shape[1]
    return pl.pallas_call(
        expert_kernel,
        grid=(ff // tile,),
        in_specs=[
            pl.BlockSpec((n, d), lambda i: (0, 0)),
            pl.BlockSpec((n, d), lambda i: (0, 0)),
            pl.BlockSpec((d, tile), lambda i: (0, i)),
            pl.BlockSpec((tile, d), lambda i: (i, 0)),
        ],
        out_specs=[
            pl.BlockSpec((n, d), lambda i: (0, 0)),
            pl.BlockSpec((n, d), lambda i: (0, 0)),
            pl.BlockSpec((d, tile), lambda i: (0, i)),
            pl.BlockSpec((tile, d), lambda i: (i, 0)),
        ],
        out_shape=[
            jax.ShapeDtypeStruct((n, d), BF16),
            jax.ShapeDtypeStruct((n, d), BF16),
            jax.ShapeDtypeStruct((d, ff), BF16),
            jax.ShapeDtypeStruct((ff, d), BF16),
        ],
        scratch_shapes=[pltpu.VMEM((n, d), F32), pltpu.VMEM((n, d), F32)],
        compiler_params=pltpu.CompilerParams(vmem_limit_bytes=60 * 1024 * 1024),
        cost_estimate=pl.CostEstimate(
            flops=12 * n * d * ff, transcendentals=n * ff, bytes_accessed=8 * n * d + 8 * d * ff
        ),
    )(x, dprod, win, wout)


MESH = pl.DeviceIdType.MESH
ANYWHERE = pl.BlockSpec(memory_space=pltpu.VMEM)


def grid_sizes(n_dp):
    ny = 1
    while 2 * ny * 2 * ny <= n_dp // 2:
        ny *= 2
    return n_dp // (2 * ny), ny


def position(ny):
    dp = lax.axis_index("dp")
    return dp, lax.axis_index("tensor"), dp % 2, (dp // 2) % ny, dp // (2 * ny)


def neighbours(ny, nz, n_t):
    dp, t, c, y, z = position(ny)

    def along_core(k):
        return (dp - c + (c + k) % 2, t)

    def along_tensor(k):
        return (dp, (t + k) % n_t)

    def along_y(k):
        return (dp + ((y + k) % ny - y) * 2, t)

    def along_z(k):
        return (dp + ((z + k) % nz - z) * 2 * ny, t)

    return {"core": (2, along_core), "tensor": (n_t, along_tensor), "y": (ny, along_y), "z": (nz, along_z)}


def greet(stages):
    barrier = pltpu.get_barrier_semaphore()
    count = 0
    for size, device in stages.values():
        for k in range(1, size):
            pl.semaphore_signal(barrier, inc=1, device_id=device(k), device_id_type=MESH)
            count += 1
    pl.semaphore_wait(barrier, count)


def gather_kernel(ny, nz, n_t, extras, *refs):
    (qkv, proj, small), refs = refs[:3], refs[3:]
    side, refs = refs[:extras], refs[extras:]
    (qkv_out, proj_out, small_out), refs = refs[:3], refs[3:]
    side_out, (send, recv, copied) = refs[:extras], refs[extras:]
    dp, t, c, y, z = position(ny)
    stages = neighbours(ny, nz, n_t)
    greet(stages)
    cols, wide = qkv.shape[1], proj.shape[1]
    whole = slice(None)
    slot = 0

    def start(pieces, device):
        nonlocal slot
        copies = []
        for src, dst in pieces:
            copies.append(
                pltpu.make_async_remote_copy(
                    src_ref=src,
                    dst_ref=dst,
                    send_sem=send.at[slot],
                    recv_sem=recv.at[slot],
                    device_id=device,
                    device_id_type=MESH,
                )
            )
            copies[-1].start()
            slot += 1
        return copies

    def along(name, pieces):
        size, device = stages[name]
        return [copy for k in range(1, size) for copy in start(pieces, device(k))]

    def lanes(ts, half):
        return pl.ds(pl.multiple_of(ts * cols + half * (cols // 2), 128), cols // 2)

    def views(zs, ys, ts, half):
        band = slice(half * (wide // 2), (half + 1) * (wide // 2))
        parts = [qkv_out.at[zs, ys, c, :, lanes(i, half)] for i in ts]
        if len(ts) == 1:
            parts.append(proj_out.at[zs, ys, c, ts[0], :, band])
            if half == 0:
                parts.append(small_out.at[zs, ys, c, ts[0]])
        else:
            parts.append(proj_out.at[zs, ys, c, :, :, band])
        return [(part, part) for part in parts]

    aside = []
    for i in range(extras):
        strip = side_out[i].shape[1]
        aside += start([(side[i].at[:, side[i].shape[1] - strip :], side_out[i])], (dp, 1 - t))
    mine = (
        qkv_out.at[z, y, c, :, pl.ds(pl.multiple_of(t * cols, 128), cols)],
        proj_out.at[z, y, c, t],
        small_out.at[z, y, c, t],
    )
    inputs = list(zip((qkv, proj, small), mine))
    local = [pltpu.make_async_copy(src, dst, copied.at[i]) for i, (src, dst) in enumerate(inputs)]
    for copy in local:
        copy.start()
    for copy in along("z", inputs) + local:
        copy.wait()
    one = along("y", views(whole, y, [t], 0))
    two = along("tensor", views(whole, y, [t], 1))
    for copy in one:
        copy.wait()
    one = along("tensor", views(whole, whole, [t], 0))
    for copy in two:
        copy.wait()
    two = along("y", views(whole, y, list(range(n_t)), 1))
    for copy in one + two:
        copy.wait()
    rest = [ref.at[:, :, c] for ref in (qkv_out, proj_out, small_out)]
    for copy in along("core", [(part, part) for part in rest]) + aside:
        copy.wait()


def gather_weights(qkv, proj, small, n_dp, n_t, side=(), strip=0):
    nz, ny = grid_sizes(n_dp)
    slots = 3 * (nz - 1) + 5 * (n_t - 1) + (4 + n_t) * (ny - 1) + 3 + len(side)
    side_shapes = [jax.ShapeDtypeStruct((v.shape[0], strip) + v.shape[2:], v.dtype) for v in side]
    outs = pl.pallas_call(
        functools.partial(gather_kernel, ny, nz, n_t, len(side)),
        out_shape=[
            jax.ShapeDtypeStruct((nz, ny, 2, qkv.shape[0], n_t * qkv.shape[1]), BF16),
            jax.ShapeDtypeStruct((nz, ny, 2, n_t) + proj.shape, BF16),
            jax.ShapeDtypeStruct((nz, ny, 2, n_t) + small.shape, BF16),
        ]
        + side_shapes,
        in_specs=[ANYWHERE] * (3 + len(side)),
        out_specs=[ANYWHERE] * (3 + len(side)),
        scratch_shapes=[
            pltpu.SemaphoreType.DMA((slots,)),
            pltpu.SemaphoreType.DMA((slots,)),
            pltpu.SemaphoreType.DMA((3,)),
        ],
        compiler_params=pltpu.CompilerParams(collective_id=0, has_side_effects=True),
    )(qkv, proj, small, *side)
    qkv_all = outs[0].reshape(n_dp * qkv.shape[0], n_t * qkv.shape[1])
    return (qkv_all, outs[1].reshape((n_dp, n_t) + proj.shape), outs[2].reshape(-1, small.shape[1])) + tuple(outs[3:])


def scatter_kernel(ny, nz, n_t, heads, *refs):
    ins, refs = refs[:3], refs[3:]
    outs, refs = refs[:3], refs[3:]
    got_core, refs = refs[:3], refs[3:]
    held, refs = refs[:3], refs[3:]
    one_got, one_held, one_last, refs = refs[:3], refs[3:6], refs[6:9], refs[9:]
    two_got, two_held, two_last, refs = refs[:2], refs[2:4], refs[4:6], refs[6:]
    end, end_got, (send, recv) = refs[:3], refs[3:6], refs[6:]
    _, t, c, y, z = position(ny)
    stages = neighbours(ny, nz, n_t)
    greet(stages)
    cols, wide = ins[0].shape[4] // n_t, ins[1].shape[5]
    slot = 0

    def lanes(ts, half):
        return pl.ds(pl.multiple_of(ts * cols + half * (cols // 2), 128), cols // 2)

    def band(half):
        return slice(half * (wide // 2), (half + 1) * (wide // 2))

    def along(name, me, pieces):
        nonlocal slot
        size, device = stages[name]
        copies = []
        for k in range(1, size):
            for src, dst in pieces((me + k) % size, k - 1):
                copies.append(
                    pltpu.make_async_remote_copy(
                        src_ref=src,
                        dst_ref=dst,
                        send_sem=send.at[slot],
                        recv_sem=recv.at[slot],
                        device_id=device(k),
                        device_id_type=MESH,
                    )
                )
                copies[-1].start()
                slot += 1
        return copies

    def finish(copies):
        for copy in copies:
            copy.wait()

    def total(own, got, index):
        value = own.astype(F32)
        for k in range(got.shape[0]):
            value = value + got[(k,) + index].astype(F32)
        return value

    def loop(count, body):
        def step(n, carry):
            body(n)
            return carry

        lax.fori_loop(0, count, step, 0)

    finish(
        along("core", c, lambda j, k: [(ins[i].at[:, :, j], got_core[i].at[k]) for i in range(3)])
    )

    def add_core(n):
        zi, yi = n // ny, n % ny
        for i in range(3):
            held[i][zi, yi] = total(ins[i][zi, yi, c], got_core[i], (zi, yi)).astype(held[i].dtype)

    loop(nz * ny, add_core)
    one = along(
        "tensor",
        t,
        lambda j, k: [
            (held[0].at[:, :, :, lanes(j, 0)], one_got[0].at[k]),
            (held[1].at[:, :, j, :, band(0)], one_got[1].at[k]),
            (held[2].at[:, :, j], one_got[2].at[k]),
        ],
    )
    two = along(
        "y",
        y,
        lambda j, k: [(held[0].at[:, j, :, lanes(i, 1)], two_got[0].at[k, i]) for i in range(n_t)]
        + [(held[1].at[:, j, i, :, band(1)], two_got[1].at[k, i]) for i in range(n_t)],
    )
    finish(one)

    def add_one(n):
        zi, yi = n // ny, n % ny
        owns = (held[0][zi, yi, :, lanes(t, 0)], held[1][zi, yi, t, :, band(0)], held[2][zi, yi, t])
        for i in range(3):
            one_held[i][zi, yi] = total(owns[i], one_got[i], (zi, yi)).astype(one_held[i].dtype)

    loop(nz * ny, add_one)
    one = along("y", y, lambda j, k: [(one_held[i].at[:, j], one_last[i].at[k]) for i in range(3)])
    finish(two)

    def add_two(zi):
        for i in range(n_t):
            owns = (held[0][zi, y, :, lanes(i, 1)], held[1][zi, y, i, :, band(1)])
            for j in range(2):
                two_held[j][i, zi] = total(owns[j], two_got[j], (i, zi)).astype(two_held[j].dtype)

    loop(nz, add_two)
    two = along("tensor", t, lambda j, k: [(two_held[i].at[j], two_last[i].at[k]) for i in range(2)])
    finish(one)
    halves = [
        (slice(0, cols // 2), slice(cols // 2, cols)),
        (band(0), band(1)),
        (slice(None),),
    ]

    def end_one(zi):
        for i in range(3):
            value = total(one_held[i][zi, y], one_last[i], (zi,))
            end[i][zi, :, halves[i][0]] = value.astype(end[i].dtype)

    loop(nz, end_one)
    finish(two)

    def end_two(zi):
        for i in range(2):
            value = total(two_held[i][t, zi], two_last[i], (zi,))
            end[i][zi, :, halves[i][1]] = value.astype(end[i].dtype)

    loop(nz, end_two)
    finish(along("z", z, lambda j, k: [(end[i].at[j], end_got[i].at[k]) for i in range(3)]))
    results = [total(end[i][z], end_got[i], ()) for i in range(3)]
    outs[2][...] = results[2]
    if heads == 0:
        outs[0][...] = results[0]
        outs[1][...] = results[1]
        return
    width = cols // (3 * heads)
    jump = outs[1].shape[1]
    for h in range(heads):
        outs[1][h] = results[1][h * jump : (h + 1) * jump]
        for i in range(3):
            at = (i * heads + h) * width
            outs[0][:, h, i * width : (i + 1) * width] = results[0][:, at : at + width]


def scatter_grads(qkv, proj, small, n_dp, n_t, heads=0):
    nz, ny = qkv.shape[:2]
    rows, cols = qkv.shape[3], qkv.shape[4] // n_t
    tails = [(rows, cols), proj.shape[4:], small.shape[4:]]
    kinds = [BF16, BF16, F32]
    parts = [(rows, cols // 2), (proj.shape[4], proj.shape[5] // 2), small.shape[4:]]
    wide = [(rows, n_t * cols), (n_t,) + proj.shape[4:], (n_t,) + small.shape[4:]]

    def room(lead, shapes):
        return [pltpu.VMEM(lead + shape, kind) for shape, kind in zip(shapes, kinds)]

    scratch = room((1, nz, ny), wide) + room((nz, ny), wide)
    scratch += room((n_t - 1, nz, ny), parts) + room((nz, ny), parts) + room((ny - 1, nz), parts)
    scratch += room((ny - 1, n_t, nz), parts[:2]) + room((n_t, nz), parts[:2]) + room((n_t - 1, nz), parts[:2])
    scratch += room((nz,), tails) + room((nz - 1,), tails)
    slots = 3 + 5 * (n_t - 1) + (3 + 2 * n_t) * (ny - 1) + 3 * (nz - 1)
    shapes = list(tails)
    if heads:
        shapes[:2] = [(rows, heads, cols // heads), (heads, proj.shape[4] // heads, proj.shape[5])]
    scratch += [pltpu.SemaphoreType.DMA((slots,)), pltpu.SemaphoreType.DMA((slots,))]
    return pl.pallas_call(
        functools.partial(scatter_kernel, ny, nz, n_t, heads),
        out_shape=[jax.ShapeDtypeStruct(shape, F32) for shape in shapes],
        in_specs=[ANYWHERE] * 3,
        out_specs=[ANYWHERE] * 3,
        scratch_shapes=scratch,
        compiler_params=pltpu.CompilerParams(collective_id=1, has_side_effects=True),
    )(qkv, proj, small)


def standardise(v):
    centre = jnp.mean(v, axis=-1, keepdims=True)
    centered = v - centre
    inverse = lax.rsqrt(jnp.mean(centered * centered, axis=-1, keepdims=True) + EPS)
    return centered * inverse, inverse


def norm_back(grad, unit, inverse):
    return inverse * (
        grad
        - jnp.mean(grad, axis=-1, keepdims=True)
        - unit * jnp.mean(grad * unit, axis=-1, keepdims=True)
    )


def two_parts(v):
    high = v.astype(BF16)
    return high, (v - high.astype(F32)).astype(BF16)


def gate_softmax(c, router, experts):
    lane = lax.broadcasted_iota(jnp.int32, (c.shape[0], router.shape[1]), 1)
    logits = jnp.where(lane < experts, dot(c, router, ((1,), (0,))), -1e30)
    raised = jnp.exp(logits - jnp.max(logits, axis=-1, keepdims=True))
    return raised / jnp.sum(raised, axis=-1, keepdims=True), lane


def key_softmax(query, keys, gap):
    scores = dot(query, keys, ((1,), (1,)))
    col = lax.broadcasted_iota(jnp.int32, scores.shape, 1)
    scores = jnp.where((col < gap[0]) | (col >= gap[1]), scores, -1e30)
    raised = jnp.exp(scores - jnp.max(scores, axis=-1, keepdims=True))
    return raised * (1.0 / jnp.sum(raised, axis=-1, keepdims=True))


def pairs(n_t, block):
    return [
        (3 * block * s + 128 * i, block * s + 128 * i) for s in range(n_t) for i in range(block // 128)
    ]


def layer_kernel(
    experts,
    n_t,
    block,
    count,
    factor,
    tokens,
    cotangent,
    moved_x,
    moved_cot,
    router,
    flat_row,
    flat_col,
    order,
    win_own,
    wout_own,
    live,
    norms,
    qkv,
    proj_in,
    out,
    grad_x,
    gqkv_out,
    gproj_out,
    grouter,
    gnorms,
    gin_mine,
    gout_mine,
    x_in,
    cot_own,
    proj,
    dhidden_in,
    edge_o,
    edge_g,
    edge_sent,
    edge_o_got,
    edge_g_got,
    c_own,
    hidden_in,
    mixed,
    context,
    c_all,
    cot_all,
    gates,
    sent,
    got,
    ret,
    pay,
    paid,
    mix,
    dx,
    dgate,
    dmixed,
    gqkv,
    gproj,
    y_acc,
    dx_acc,
    win_got,
    wout_got,
    gin_far,
    gout_far,
    gin_half,
    gout_half,
    gin_got,
    gout_got,
    w_sems,
    c_sems,
    cot_sems,
    edge_sems,
    go_send,
    go_recv,
    back_send,
    back_recv,
    pay_sems,
    grad_sems,
):
    batches, rows, d = cot_own.shape
    n_dp = lax.axis_size("dp")
    dp, t = lax.axis_index("dp"), lax.axis_index("tensor")
    share = sent.shape[1] // n_dp
    hidden = win_own.shape[1]
    shift = (share * n_t).bit_length() - 1
    other = 1 - t
    partner = (dp, other)
    own_rows, strip = tokens.shape[1], edge_o.shape[1]
    head, edge = rows - strip, own_rows - count
    gap = (jnp.where(t == 0, count, count - edge), jnp.where(t == 0, rows, rows - edge))

    barrier = pltpu.get_barrier_semaphore()
    pl.semaphore_signal(barrier, inc=1, device_id=partner, device_id_type=MESH)

    def hello(k, carry):
        pl.semaphore_signal(barrier, inc=1, device_id=((dp + k) % n_dp, t), device_id_type=MESH)
        return carry

    lax.fori_loop(1, n_dp, hello, 0)
    pl.semaphore_wait(barrier, n_dp)

    def slot_codes(shape, axis):
        q = lax.broadcasted_iota(jnp.int32, shape, axis)
        return q + (q >> (share.bit_length() - 1)) * share * (n_t - 1) + t * share

    def band(m):
        return pl.ds(pl.multiple_of(m * rows, 16), rows)

    def image(i):
        return pl.ds(pl.multiple_of(i * rows, 16), rows)

    def part(i):
        return pl.ds(pl.multiple_of(i * share, 16), share)

    def remote(src, dst, sems, i, j, device):
        return pltpu.make_async_remote_copy(
            src_ref=src,
            dst_ref=dst,
            send_sem=sems[0].at[i, j],
            recv_sem=sems[1].at[i, j],
            device_id=device,
            device_id_type=MESH,
        )

    def c_copy(m):
        return pltpu.make_async_remote_copy(
            src_ref=c_own.at[m],
            dst_ref=c_all.at[m, image(t)],
            send_sem=c_sems.at[0, m],
            recv_sem=c_sems.at[1, m],
            device_id=partner,
            device_id_type=MESH,
        )

    def cot_copy(m):
        return pltpu.make_async_remote_copy(
            src_ref=cot_own.at[m],
            dst_ref=cot_all.at[m, image(t)],
            send_sem=cot_sems.at[0, m],
            recv_sem=cot_sems.at[1, m],
            device_id=partner,
            device_id_type=MESH,
        )

    def go_copy(m, k):
        to = (dp + k) % n_dp
        return remote(sent.at[m, part(to)], got.at[m, part(dp)], (go_send, go_recv), m, k - 1, (to, t))

    def back_copy(m, k):
        to = (dp + k) % n_dp
        return remote(got.at[m, part(to)], ret.at[m, part(dp)], (back_send, back_recv), m, k - 1, (to, t))

    def pay_copy(m):
        return pltpu.make_async_remote_copy(
            src_ref=pay.at[m],
            dst_ref=paid.at[m],
            send_sem=pay_sems.at[0, m],
            recv_sem=pay_sems.at[1, m],
            device_id=partner,
            device_id_type=MESH,
        )

    def grad_copy(i):
        src, dst = ((gin_half, gin_got), (gout_half, gout_got))[i // 2]
        size = src.shape[0] // 2
        band = pl.ds(i % 2 * size, size)
        return pltpu.make_async_remote_copy(
            src_ref=src.at[band],
            dst_ref=dst.at[band],
            send_sem=grad_sems.at[0, i],
            recv_sem=grad_sems.at[1, i],
            device_id=partner,
            device_id_type=MESH,
        )

    def w_copy(i):
        return pltpu.make_async_remote_copy(
            src_ref=(win_own, wout_own)[i],
            dst_ref=(win_got, wout_got)[i],
            send_sem=w_sems.at[0, i],
            recv_sem=w_sems.at[1, i],
            device_id=partner,
            device_id_type=MESH,
        )

    def every(body):
        def step(k, carry):
            body(k)
            return carry

        lax.fori_loop(1, n_dp, step, 0)

    low = lax.broadcasted_iota(jnp.int32, (rows, 128), 1) < 64

    def edge_copy(i, m):
        return pltpu.make_async_remote_copy(
            src_ref=(edge_o, edge_sent)[i].at[m],
            dst_ref=(edge_o_got, edge_g_got)[i].at[m],
            send_sem=edge_sems.at[2 * i, m],
            recv_sem=edge_sems.at[2 * i + 1, m],
            device_id=partner,
            device_id_type=MESH,
        )

    for own_ref, ref, moved in ((cot_own, cotangent, moved_cot), (x_in, tokens, moved_x)):
        own_ref[:, :head] = ref[:, :head]

        @pl.when(t == 0)
        def _(own_ref=own_ref, ref=ref):
            own_ref[:, head:] = ref[:, head:rows]

        @pl.when(t != 0)
        def _(own_ref=own_ref, moved=moved):
            own_ref[:, head:] = moved[...]

    def permutation():
        return (order[...] == lax.broadcasted_iota(jnp.int32, (d, d), 1)).astype(F32).astype(BF16)

    proj[...] = dot(permutation(), proj_in[...], ((0,), (0,))).astype(BF16)

    def attend(m, carry):
        cot_copy(m).start()
        cot_all[m, image(t)] = cot_own[m]
        xf = x_in[m].astype(F32)
        unit, _ = standardise(xf)
        a = (unit * norms[0:1] + norms[1:2]).astype(BF16)
        for s in range(n_t):
            for i in range(3):
                cols = slice((3 * s + i) * block, (3 * s + i + 1) * block)
                projected = dot(a, qkv[:, cols], ((1,), (0,)))
                mixed[m, :, cols] = (projected * factor if i == 0 else projected).astype(BF16)
        for col, dest in pairs(n_t, block):
            query = mixed[m, :, col : col + 128]
            keys = mixed[m, :, col + block : col + block + 128]
            values = mixed[m, :, col + 2 * block : col + 2 * block + 128]
            zero = jnp.zeros_like(query)
            parts = []
            for own in (low, ~low):
                probs = key_softmax(jnp.where(own, query, zero), keys, gap)
                parts.append(dot(probs.astype(BF16), values, ((1,), (0,))))
            context[m, :, dest : dest + 128] = jnp.where(low, parts[0], parts[1]).astype(BF16)
        hidden = xf + live[m] * dot(context[m], proj[...], ((1,), (0,)))
        hidden_in[m] = hidden
        unit, _ = standardise(hidden)
        c = (unit * norms[2:3] + norms[3:4]).astype(BF16)
        c_own[m] = c
        c_all[m, image(t)] = c
        c_copy(m).start()
        return carry

    lax.fori_loop(0, batches, attend, 0)
    w_copy(0).start()
    w_copy(1).start()

    lane = lax.broadcasted_iota(jnp.int32, (2 * rows, router.shape[1]), 1)

    def dispatch(m, carry):
        c_copy(m).wait_recv()
        cot_copy(m).wait_recv()
        c = c_all[m]
        logits = jnp.where(lane < experts, dot(c, router[...], ((1,), (0,))), -1e30)
        raised = jnp.exp(logits - jnp.max(logits, axis=-1, keepdims=True))
        probs = raised / jnp.sum(raised, axis=-1, keepdims=True)
        cot = cot_all[m].astype(F32)
        scaled = []
        for k in range(2):
            gate = jnp.sum(jnp.where(lane == flat_col[m, :, k : k + 1] >> shift, probs, 0.0), axis=-1, keepdims=True)
            gates[m, :, k : k + 1] = gate
            scaled.append((gate * cot).astype(BF16))
        codes = slot_codes((n_dp * share, 1), 0)
        picks = [(flat_row[m, k : k + 1, :] == codes).astype(F32).astype(BF16) for k in range(2)]
        sent[m, :, :d] = dot(picks[0] + picks[1], c, ((1,), (0,))).astype(BF16)
        moved = dot(picks[0], scaled[0], ((1,), (0,))) + dot(picks[1], scaled[1], ((1,), (0,)))
        sent[m, :, d:] = moved.astype(BF16)
        every(lambda k: go_copy(m, k).start())
        got[m, part(dp)] = sent[m, part(dp)]
        return carry

    lax.fori_loop(0, batches, dispatch, 0)

    tile = 256

    def clear(i, carry):
        cols = pl.ds(pl.multiple_of(i * tile, tile), tile)
        for into in (gin_far, gin_mine):
            into[:, cols] = jnp.zeros((d, tile), F32)
        for into in (gout_far, gout_mine):
            into[cols, :] = jnp.zeros((tile, d), F32)
        return carry

    lax.fori_loop(0, hidden // tile, clear, 0)

    slots = n_dp * share
    sums = ((y_acc, dx_acc), (mix.at[pl.ds(0, slots)], dx.at[pl.ds(0, slots)]))

    def expert_half(m, own):
        y_sum, dx_sum = sums[m % 2]
        win, wout, gin, gout = (win_own, wout_own, gin_mine, gout_mine) if own else (win_got, wout_got, gin_far, gout_far)

        def chunk(i, inner):
            cols = pl.ds(pl.multiple_of(i * tile, tile), tile)
            x = got[m, :, :d]
            dprod = got[m, :, d:]
            w1 = win[:, cols]
            w2 = wout[cols, :]
            pre = dot(x, w1, ((1,), (0,)))
            square = pre * pre
            th = jnp.tanh(GELU_A * pre * (1.0 + GELU_B * square))
            active = (0.5 * pre * (1.0 + th)).astype(BF16)
            slope = 0.5 * (1.0 + th) + 0.5 * pre * (1.0 - th * th) * (GELU_A * (1.0 + 3.0 * GELU_B * square))
            dpre = (dot(dprod, w2, ((1,), (1,))) * slope).astype(BF16)
            gin[:, cols] += dot(x, dpre, ((0,), (0,)))
            gout[cols, :] += dot(active, dprod, ((0,), (0,)))
            y_sum[...] += dot(active, w2, ((1,), (0,)))
            dx_sum[...] += dot(dpre, w1, ((1,), (1,)))
            return inner

        lax.fori_loop(0, hidden // tile, chunk, 0)

    def expert_begin(m):
        every(lambda k: go_copy(m, k).wait_recv())
        for ref in sums[m % 2]:
            ref[...] = jnp.zeros((slots, d), F32)

    def expert_end(m):
        got[m, :, :d] = sums[m % 2][0][...].astype(BF16)
        got[m, :, d:] = sums[m % 2][1][...].astype(BF16)
        every(lambda k: back_copy(m, k).start())
        ret[m, part(dp)] = got[m, part(dp)]

    last = batches - 1
    for m in range(last):
        expert_begin(m)
        expert_half(m, True)
    w_copy(0).wait_recv()
    w_copy(1).wait_recv()
    for m in range(last):
        expert_half(m, False)
        expert_end(m)
    expert_begin(last)
    expert_half(last, False)
    gin_half[...] = gin_far[...].astype(BF16)
    gout_half[...] = gout_far[...].astype(BF16)
    grad_copy(0).start()
    grad_copy(1).start()
    expert_half(last, True)
    expert_end(last)

    def combine(m, carry):
        every(lambda k: back_copy(m, k).wait_recv())
        codes = slot_codes((1, n_dp * share), 1)
        for i in (other, t):
            picks = [(flat_col[m, image(i), k : k + 1] == codes).astype(F32).astype(BF16) for k in range(2)]
            one = dot(picks[0], ret[m, :, :d], ((1,), (0,)))
            two = dot(picks[1], ret[m, :, :d], ((1,), (0,)))
            d_rows = dot(picks[0] + picks[1], ret[m, :, d:], ((1,), (0,)))
            cot = cot_all[m, image(i)].astype(F32)
            gate = gates[m, image(i)]
            mixture = gate[:, 0:1] * one + gate[:, 1:2] * two
            col = lax.broadcasted_iota(jnp.int32, (rows, 128), 1)
            dg = jnp.where(col == 0, jnp.sum(one * cot, axis=-1, keepdims=True), 0.0)
            dg = dg + jnp.where(col == 1, jnp.sum(two * cot, axis=-1, keepdims=True), 0.0)
            if i is other:
                pay[m, :, :d] = mixture.astype(BF16)
                pay[m, :, d : 2 * d] = d_rows.astype(BF16)
                pay[m, :, 2 * d :] = dg.astype(BF16)
                pay_copy(m).start()
            else:
                mix[band(m)] = mixture
                dx[band(m)] = d_rows
                dgate[m] = dg
        return carry

    gqkv[...] = jnp.zeros_like(gqkv)
    gproj[...] = jnp.zeros_like(gproj)
    grouter[...] = jnp.zeros_like(grouter)
    gnorms[...] = jnp.zeros_like(gnorms)

    def retreat(m):
        pay_copy(m).wait_recv()
        hidden = hidden_in[m]
        result = (hidden + mix[band(m)] + paid[m, :, :d].astype(F32)).astype(BF16)
        out[m, :head] = result[:head]
        edge_o[m] = result[head:]
        edge_copy(0, m).start()
        unit, inverse = standardise(hidden)
        c = (unit * norms[2:3] + norms[3:4]).astype(BF16)
        probs, lane = gate_softmax(c, router[...], experts)
        dg = dgate[m] + paid[m, :, 2 * d :].astype(F32)
        dprobs = jnp.zeros_like(probs)
        for k in range(2):
            dprobs = dprobs + jnp.where(lane == flat_col[m, image(t), k : k + 1] >> shift, dg[:, k : k + 1], 0.0)
        dlogits = probs * (dprobs - jnp.sum(dprobs * probs, axis=-1, keepdims=True))
        dc = dx[band(m)] + paid[m, :, d : 2 * d].astype(F32)
        for piece in two_parts(dlogits):
            grouter[...] += dot(c, piece, ((0,), (0,)))
            dc = dc + dot(piece, router[...], ((1,), (1,)))
        gnorms[2:3] += jnp.sum(dc * unit, axis=0, keepdims=True)
        gnorms[3:4] += jnp.sum(dc, axis=0, keepdims=True)
        dhidden = cot_all[m, image(t)].astype(F32) + norm_back(dc * norms[2:3], unit, inverse)
        dhidden_in[...] = dhidden
        dattn = (live[m] * dhidden).astype(BF16)
        gproj[...] += dot(context[m], dattn, ((0,), (0,)))
        dcontext = dot(dattn, proj[...], ((1,), (1,))).astype(BF16)
        for col, dest in pairs(n_t, block):
            query = mixed[m, :, col : col + 128]
            keys = mixed[m, :, col + block : col + block + 128]
            values = mixed[m, :, col + 2 * block : col + 2 * block + 128]
            grads = dcontext[:, dest : dest + 128]
            zero = jnp.zeros_like(query)
            parts = []
            for own in (low, ~low):
                probs = key_softmax(jnp.where(own, query, zero), keys, gap)
                dvalues = dot(probs.astype(BF16), grads, ((0,), (0,)))
                dweights = dot(jnp.where(own, grads, zero), values, ((1,), (1,)))
                dscores = probs * (dweights - jnp.sum(dweights * probs, axis=-1, keepdims=True))
                dscores = dscores.astype(BF16)
                parts.append(
                    (dot(dscores, keys, ((1,), (0,))), dot(dscores, query, ((0,), (0,))), dvalues)
                )
            for i in range(3):
                both = jnp.where(low, parts[0][i], parts[1][i]).astype(BF16)
                if i == 0:
                    both = both * BF16(factor)
                dmixed[:, col + i * block : col + i * block + 128] = both
        unit, inverse = standardise(x_in[m].astype(F32))
        a = (unit * norms[0:1] + norms[1:2]).astype(BF16)
        gqkv[...] += dot(a, dmixed[...], ((0,), (0,)))
        da = dot(dmixed[...], qkv[...], ((1,), (1,)))
        gnorms[0:1] += jnp.sum(da * unit, axis=0, keepdims=True)
        gnorms[1:2] += jnp.sum(da, axis=0, keepdims=True)
        result = dhidden_in[...] + norm_back(da * norms[0:1], unit, inverse)
        grad_x[m, :head] = result[:head]
        edge_g[m] = result[head:]
        edge_sent[m] = result[head:].astype(BF16)
        edge_copy(1, m).start()

    pieces = 4

    def finish(m, carry):
        @pl.when(m < batches)
        def _():
            combine(m, 0)

        @pl.when(m == 0)
        def _():
            grad_copy(2).start()

        @pl.when(m == batches - 1)
        def _():
            grad_copy(3).start()

        @pl.when(m > 0)
        def _():
            retreat(m - 1)

        return carry

    lax.fori_loop(0, batches + 1, finish, 0)
    gqkv_out[...] = gqkv[...].astype(BF16)
    gproj_out[...] = dot(permutation(), gproj[...].astype(BF16), ((1,), (0,))).astype(BF16)

    @pl.when(t != 0)
    def _():
        out[:, head:] = tokens[:, head:]
        grad_x[:, head:] = cotangent[:, head:].astype(F32)

    first = own_rows - strip
    near = lax.broadcasted_iota(jnp.int32, (16, d), 0) < strip - edge

    def place(m, carry):
        edge_copy(0, m).wait()
        edge_copy(1, m).wait()

        @pl.when(t == 0)
        def _():
            for ref, mine, theirs in ((out, edge_o, edge_o_got), (grad_x, edge_g, edge_g_got)):
                ref[m, head:first] = mine[m, : first - head]
                blend = jnp.where(
                    near,
                    mine[m, first - head : first - head + 16].astype(F32),
                    theirs[m, :16].astype(F32),
                )
                ref[m, first : first + 16] = blend.astype(ref.dtype)
                ref[m, first + 16 :] = theirs[m, 16:].astype(ref.dtype)

        return carry

    lax.fori_loop(0, batches, place, 0)
    for i in range(pieces):
        grad_copy(i).wait()
    gin_mine[...] += gin_got[...].astype(F32)
    gout_mine[...] += gout_got[...].astype(F32)
    w_copy(0).wait_send()
    w_copy(1).wait_send()

    def drain(m, carry):
        c_copy(m).wait_send()
        cot_copy(m).wait_send()
        pay_copy(m).wait_send()
        every(lambda k: go_copy(m, k).wait_send())
        every(lambda k: back_copy(m, k).wait_send())
        return carry

    lax.fori_loop(0, batches, drain, 0)


def layer(held, moved, router, flat, order, win, wout, live, norms, qkv, proj, statics):
    batches, own_rows, d = held[0].shape
    experts, n_dp, n_t, block, count, factor, cap = statics
    rows, strip = live.shape[1], moved[0].shape[1]
    slots = n_dp * cap // n_t
    half = win.shape[1]
    wide = 3 * n_t * block
    dma = pltpu.SemaphoreType.DMA
    return pl.pallas_call(
        functools.partial(layer_kernel, experts, n_t, block, count, factor),
        out_shape=[
            jax.ShapeDtypeStruct((batches, own_rows, d), BF16),
            jax.ShapeDtypeStruct((batches, own_rows, d), F32),
            jax.ShapeDtypeStruct((d, wide), BF16),
            jax.ShapeDtypeStruct((d, d), BF16),
            jax.ShapeDtypeStruct((d, router.shape[1]), F32),
            jax.ShapeDtypeStruct((8, d), F32),
            jax.ShapeDtypeStruct((d, half), F32),
            jax.ShapeDtypeStruct((half, d), F32),
        ],
        in_specs=[ANYWHERE] * 14,
        out_specs=[ANYWHERE] * 8,
        scratch_shapes=[
            pltpu.VMEM((batches, rows, d), BF16),
            pltpu.VMEM((batches, rows, d), BF16),
            pltpu.VMEM((d, d), BF16),
            pltpu.VMEM((rows, d), F32),
            pltpu.VMEM((batches, strip, d), BF16),
            pltpu.VMEM((batches, strip, d), F32),
            pltpu.VMEM((batches, strip, d), BF16),
            pltpu.VMEM((batches, strip, d), BF16),
            pltpu.VMEM((batches, strip, d), BF16),
            pltpu.VMEM((batches, rows, d), BF16),
            pltpu.VMEM((batches, rows, d), F32),
            pltpu.VMEM((batches, rows, wide), BF16),
            pltpu.VMEM((batches, rows, d), BF16),
            pltpu.VMEM((batches, 2 * rows, d), BF16),
            pltpu.VMEM((batches, 2 * rows, d), BF16),
            pltpu.VMEM((batches, 2 * rows, 128), F32),
            pltpu.VMEM((batches, slots, 2 * d), BF16),
            pltpu.VMEM((batches, slots, 2 * d), BF16),
            pltpu.VMEM((batches, slots, 2 * d), BF16),
            pltpu.VMEM((batches, rows, 2 * d + 128), BF16),
            pltpu.VMEM((batches, rows, 2 * d + 128), BF16),
            pltpu.VMEM((max(batches * rows, slots), d), F32),
            pltpu.VMEM((max(batches * rows, slots), d), F32),
            pltpu.VMEM((batches, rows, 128), F32),
            pltpu.VMEM((rows, wide), BF16),
            pltpu.VMEM((d, wide), F32),
            pltpu.VMEM((d, d), F32),
            pltpu.VMEM((slots, d), F32),
            pltpu.VMEM((slots, d), F32),
            pltpu.VMEM((d, half), BF16),
            pltpu.VMEM((half, d), BF16),
            pltpu.VMEM((d, half), F32),
            pltpu.VMEM((half, d), F32),
            pltpu.VMEM((d, half), BF16),
            pltpu.VMEM((half, d), BF16),
            pltpu.VMEM((d, half), BF16),
            pltpu.VMEM((half, d), BF16),
            dma((2, 2)),
            dma((2, batches)),
            dma((2, batches)),
            dma((4, batches)),
            dma((batches, n_dp - 1)),
            dma((batches, n_dp - 1)),
            dma((batches, n_dp - 1)),
            dma((batches, n_dp - 1)),
            dma((2, batches)),
            dma((2, 4)),
        ],
        compiler_params=pltpu.CompilerParams(
            collective_id=2, has_side_effects=True, vmem_limit_bytes=67043328
        ),
    )(
        *held,
        *moved,
        router,
        flat,
        flat.transpose(0, 2, 1),
        order,
        win,
        wout,
        live,
        norms,
        qkv,
        proj,
    )


def general(
    tokens,
    w_qkv,
    w_proj,
    w_in,
    w_out,
    w_router,
    gain_attn,
    shift_attn,
    gain_moe,
    shift_moe,
    live_rows,
    chosen,
    priority,
    cotangent,
):
    batches, own_rows, d = tokens.shape
    rows = live_rows.shape[1]
    n_dp = lax.axis_size("dp")
    n_t = lax.axis_size("tensor")
    t = lax.axis_index("tensor")
    heads_here = w_qkv.shape[1]
    heads = heads_here * n_t
    width = w_qkv.shape[2] // 3
    experts = w_in.shape[0] * n_dp
    cap = 2 * rows // experts
    share = cap // n_t
    images = rows // SEQ
    span = images * SEQ
    per = -(-images // n_t)
    work = per * SEQ
    total = n_t * work
    factor = width ** (-0.5)
    highest = lax.Precision.HIGHEST

    small = jnp.concatenate(
        [w_router] + [v[:, None] for v in (gain_attn, shift_attn, gain_moe, shift_moe)], axis=1
    )
    small = jnp.pad(small, ((0, 0), (0, 128 - small.shape[1])))
    block = heads_here * width
    qkv_block = w_qkv.reshape(-1, heads_here, 3, width).transpose(0, 2, 1, 3).reshape(-1, 3 * block)
    fill = -3 * block % 128
    qkv_block = jnp.pad(qkv_block, ((0, 0), (0, fill)))
    qkv, proj, small = gather_weights(qkv_block, w_proj.reshape(-1, d), small, n_dp, n_t)
    qkv = qkv.reshape(d, n_t, 3 * block + fill)[:, :, : 3 * block].reshape(d, -1)
    router = small[:, :experts]
    gain_one, shift_one, gain_two, shift_two = (small[:, experts + i].astype(F32) for i in range(4))
    proj = proj.reshape(n_dp, n_t, heads_here, w_proj.shape[1], d)
    proj = proj.transpose(1, 2, 0, 3, 4).reshape(heads * width, d)
    win = lax.all_gather(w_in[0], "tensor", axis=1, tiled=True)
    wout = lax.all_gather(w_out[0], "tensor", axis=0, tiled=True)
    cot_all = lax.all_gather(cotangent, "tensor", axis=1, tiled=True)

    def pad_rows(v, n):
        return jnp.pad(v, ((0, 0), (0, n - v.shape[1])) + ((0, 0),) * (v.ndim - 2))

    def own(v):
        return lax.dynamic_slice_in_dim(v, t * work, work, 1)

    edge = own_rows - work
    direct = n_t == 2 and per == 1 and edge >= 0
    if direct:
        moved = lax.ppermute(tokens[:, work:], "tensor", [(0, 1)])
        x = jnp.where(
            t == 0, tokens[:, :work], jnp.concatenate([moved, tokens[:, : work - edge]], axis=1)
        )
    else:
        x = own(pad_rows(lax.all_gather(tokens, "tensor", axis=1, tiled=True)[:, :span], total))
    x = x.astype(F32)
    live = live_rows[:, :span]
    live_all = pad_rows(live, total)
    live_own = own(live_all).astype(F32)[:, :, None]
    cot_all = pad_rows(cot_all[:, :span], total)
    dy = own(cot_all).astype(F32)

    rank = priority[:, 0, :span]
    first, second = chosen[:, :span, 0], chosen[:, :span, 1]
    labels = jnp.arange(experts, dtype=jnp.int32)
    earlier = (rank[:, None, :] < rank[:, :, None]).astype(BF16)
    hit_one = (first[:, :, None] == labels).astype(F32)
    hit_two = (second[:, :, None] == labels).astype(F32)
    live_one = hit_one * live[:, :, None].astype(F32)
    live_two = hit_two * live[:, :, None].astype(F32)
    counts = jnp.einsum(
        "mrs,mse->mre",
        earlier,
        jnp.concatenate([live_one, live_two], axis=-1).astype(BF16),
        preferred_element_type=F32,
    )
    first_total = jnp.sum(live_one, axis=1, keepdims=True)
    slot_one = jnp.sum(counts[:, :, :experts] * hit_one, axis=-1).astype(jnp.int32)
    slot_two = jnp.sum((counts[:, :, experts:] + first_total) * hit_two, axis=-1).astype(jnp.int32)
    keep_one = (live > 0) & (slot_one < cap)
    keep_two = (live > 0) & (slot_two < cap)
    flat_one = jnp.where(keep_one, first * cap + slot_one, -1)
    flat_two = jnp.where(keep_two, second * cap + slot_two, -1)

    def spread(v, fill):
        return jnp.pad(v, ((0, 0), (0, total - span)), constant_values=fill)

    flat_one, flat_two = spread(flat_one, -1), spread(flat_two, -1)
    keep_one, keep_two = spread(keep_one, False), spread(keep_two, False)
    first, second = spread(first, 0), spread(second, 0)
    codes = (jnp.arange(experts)[:, None] * cap + t * share + jnp.arange(share)[None, :]).reshape(-1)
    pick_one = flat_one[:, None, :] == codes[None, :, None]
    pick_two = flat_two[:, None, :] == codes[None, :, None]

    normed_one = layer_norm(x, gain_one, shift_one).astype(BF16)
    mixed = dot(normed_one, qkv, ((2,), (0,)))
    split = heads * width
    shape = (batches * per, SEQ, heads, width)
    mixed = mixed.reshape(batches, work, n_t, 3, block)
    query = (mixed[:, :, :, 0] * factor).astype(BF16).reshape(shape)
    keys = mixed[:, :, :, 1].astype(BF16).reshape(shape)
    values = mixed[:, :, :, 2].astype(BF16).reshape(shape)
    scores = jnp.einsum("iqhc,ikhc->ihqk", query, keys, preferred_element_type=F32)
    probs = jax.nn.softmax(scores, axis=-1)
    weights = probs.astype(BF16)
    context = jnp.einsum("ihqk,ikhc->iqhc", weights, values, preferred_element_type=F32)
    context = context.astype(BF16).reshape(batches, work, split)
    attn = dot(context, proj, ((2,), (0,)))
    hidden = x + live_own * attn
    normed_two = layer_norm(hidden, gain_two, shift_two).astype(BF16)

    c_all = lax.all_gather(normed_two, "tensor", axis=1, tiled=True)
    gate_probs = jax.nn.softmax(dot(c_all, router, ((2,), (0,))), axis=-1)
    hits_one = (first[:, :, None] == labels).astype(F32)
    hits_two = (second[:, :, None] == labels).astype(F32)
    gate_one = jnp.sum(gate_probs * hits_one, axis=-1) * keep_one
    gate_two = jnp.sum(gate_probs * hits_two, axis=-1) * keep_two
    picked = (pick_one | pick_two).astype(BF16)
    sent = jnp.einsum(
        "mqr,mrd->mqd",
        picked,
        jnp.concatenate([c_all, cot_all], axis=-1),
        preferred_element_type=F32,
    )
    gate_slot = jnp.sum(
        jnp.where(pick_one, gate_one[:, None, :], 0.0) + jnp.where(pick_two, gate_two[:, None, :], 0.0),
        axis=-1,
        keepdims=True,
    )
    sent = jnp.concatenate(
        [sent[..., :d].astype(BF16), (sent[..., d:] * gate_slot).astype(BF16)], axis=-1
    )
    sent = sent.reshape(batches, experts, share, 2 * d)
    got = lax.all_to_all(sent, "dp", 1, 1, tiled=True).reshape(-1, 2 * d)
    produced, d_in, grad_in, grad_out = expert(got[:, :d], got[:, d:], win, wout)
    back = jnp.concatenate([produced, d_in], axis=-1).reshape(batches, n_dp, share, 2 * d)
    back = lax.all_to_all(back, "dp", 1, 1, tiled=True).reshape(batches, experts * share, 2 * d)
    grad_in = lax.psum_scatter(grad_in, "tensor", scatter_dimension=1, tiled=True).astype(F32)
    grad_out = lax.psum_scatter(grad_out, "tensor", scatter_dimension=0, tiled=True).astype(F32)

    part_one = jnp.einsum("mqr,mqd->mrd", pick_one.astype(BF16), back[..., :d], preferred_element_type=F32)
    part_two = jnp.einsum("mqr,mqd->mrd", pick_two.astype(BF16), back[..., :d], preferred_element_type=F32)
    d_rows = jnp.einsum("mqr,mqd->mrd", picked, back[..., d:], preferred_element_type=F32)
    mixture = gate_one[:, :, None] * part_one + gate_two[:, :, None] * part_two
    cot_wide = cot_all.astype(F32)
    dgate_one = jnp.sum(part_one * cot_wide, axis=-1, keepdims=True)
    dgate_two = jnp.sum(part_two * cot_wide, axis=-1, keepdims=True)
    dgates = jnp.concatenate([dgate_one, dgate_two], axis=-1)
    payload = jnp.concatenate(
        [mixture, d_rows, jnp.pad(dgates, ((0, 0), (0, 0), (0, 126)))], axis=-1
    ).astype(BF16)
    pieces = payload.reshape(batches, n_t, work, payload.shape[-1])

    def piece(k):
        return lax.dynamic_index_in_dim(pieces, (t + k) % n_t, 1, keepdims=False)

    payload = piece(0).astype(F32)
    for k in range(1, n_t):
        payload = payload + lax.ppermute(
            piece(k), "tensor", [(j, (j + k) % n_t) for j in range(n_t)]
        ).astype(F32)
    output = (hidden + payload[..., :d]).astype(BF16)
    dgates = payload[..., 2 * d : 2 * d + 2]

    own_probs = own(gate_probs)
    dprobs = own(hits_one) * dgates[..., 0:1] * own(keep_one)[:, :, None]
    dprobs = dprobs + own(hits_two) * dgates[..., 1:2] * own(keep_two)[:, :, None]
    dlogits = own_probs * (dprobs - jnp.sum(dprobs * own_probs, axis=-1, keepdims=True))
    grad_router = lax.dot_general(
        normed_two.astype(F32), dlogits, (((0, 1), (0, 1)), ((), ())), precision=highest
    )
    dc = payload[..., d : 2 * d] + lax.dot_general(
        dlogits, router.astype(F32), (((2,), (1,)), ((), ())), precision=highest
    )
    _, back_two = jax.vjp(layer_norm, hidden, gain_two, shift_two)
    dnorm, grad_gain_two, grad_shift_two = back_two(dc)
    dhidden = dy + dnorm
    dattn = (live_own * dhidden).astype(BF16)

    grad_proj = dot(context, dattn, ((0, 1), (0, 1)))
    dcontext = dot(dattn, proj, ((2,), (1,))).astype(BF16).reshape(shape)
    dvalues = jnp.einsum("ihqk,iqhc->ikhc", weights, dcontext, preferred_element_type=F32).astype(BF16)
    dweights = jnp.einsum("iqhc,ikhc->ihqk", dcontext, values, preferred_element_type=F32)
    dscores = (probs * (dweights - jnp.sum(dweights * probs, axis=-1, keepdims=True))).astype(BF16)
    dquery = jnp.einsum("ihqk,ikhc->iqhc", dscores, keys, preferred_element_type=F32).astype(BF16)
    dkeys = jnp.einsum("ihqk,iqhc->ikhc", dscores, query, preferred_element_type=F32).astype(BF16)
    dmixed = jnp.stack(
        [v.reshape(batches, work, n_t, block) for v in (dquery * BF16(factor), dkeys, dvalues)], axis=3
    ).reshape(batches, work, 3 * split)
    grad_qkv = dot(normed_one, dmixed, ((0, 1), (0, 1)))
    da = dot(dmixed, qkv, ((2,), (1,)))
    _, back_one = jax.vjp(layer_norm, x, gain_one, shift_one)
    dnorm, grad_gain_one, grad_shift_one = back_one(da)
    grad_x = dhidden + dnorm

    if direct:
        out_edge = lax.ppermute(output[:, :edge], "tensor", [(1, 0)])
        grad_edge = lax.ppermute(grad_x[:, :edge], "tensor", [(1, 0)])
        result = jnp.where(
            t == 0,
            jnp.concatenate([output, out_edge], axis=1),
            jnp.concatenate([output[:, edge:], tokens[:, work - edge :]], axis=1),
        )
        grad_tokens = jnp.where(
            t == 0,
            jnp.concatenate([grad_x, grad_edge], axis=1),
            jnp.concatenate([grad_x[:, edge:], cotangent[:, work - edge :].astype(F32)], axis=1),
        )
    else:
        here = (t * own_rows + jnp.arange(own_rows) < span)[None, :, None]

        def home(v, rest):
            full = pad_rows(lax.all_gather(v, "tensor", axis=1, tiled=True)[:, :span], rows)
            return jnp.where(here, lax.dynamic_slice_in_dim(full, t * own_rows, own_rows, 1), rest)

        result = home(output, tokens)
        grad_tokens = home(grad_x, cotangent.astype(F32))

    nz, ny = grid_sizes(n_dp)
    grad_qkv = jnp.pad(grad_qkv.astype(BF16).reshape(d, n_t, 3 * block), ((0, 0), (0, 0), (0, fill)))
    grad_qkv = grad_qkv.reshape(nz, ny, 2, d // n_dp, -1)
    grad_proj = grad_proj.astype(BF16).reshape(n_t, heads_here, n_dp, -1, d)
    grad_proj = grad_proj.transpose(2, 0, 1, 3, 4).reshape(nz, ny, 2, n_t, -1, d)
    smalls = jnp.concatenate(
        [grad_router] + [v[:, None] for v in (grad_gain_one, grad_shift_one, grad_gain_two, grad_shift_two)],
        axis=1,
    )
    smalls = jnp.pad(smalls, ((0, 0), (0, 128 - smalls.shape[1]))).reshape(nz, ny, 2, n_t, -1, 128)
    grad_qkv, grad_proj, smalls = scatter_grads(grad_qkv, grad_proj, smalls, n_dp, n_t)
    grad_qkv = grad_qkv[:, : 3 * block].reshape(-1, 3, heads_here, width).transpose(0, 2, 1, 3)
    return (
        result,
        grad_tokens,
        grad_qkv.reshape(w_qkv.shape),
        grad_proj.reshape(w_proj.shape),
        grad_in[None],
        grad_out[None],
        smalls[:, :experts],
        smalls[:, experts],
        smalls[:, experts + 1],
        smalls[:, experts + 2],
        smalls[:, experts + 3],
    )


def fast(
    tokens,
    w_qkv,
    w_proj,
    w_in,
    w_out,
    w_router,
    gain_attn,
    shift_attn,
    gain_moe,
    shift_moe,
    live_rows,
    chosen,
    priority,
    cotangent,
):
    batches, own_rows, d = tokens.shape
    rows = live_rows.shape[1]
    n_dp = lax.axis_size("dp")
    n_t = lax.axis_size("tensor")
    t = lax.axis_index("tensor")
    heads_here = w_qkv.shape[1]
    width = w_qkv.shape[2] // 3
    block = heads_here * width
    experts = n_dp
    cap = 2 * rows // experts
    share = cap // n_t
    span = n_t * SEQ
    padded = -(-SEQ // 16) * 16
    edge = own_rows - SEQ
    factor = width ** (-0.5)

    vectors = jnp.stack([gain_attn, shift_attn, gain_moe, shift_moe])
    small = jnp.concatenate([w_router, vectors.T], axis=1)
    small = jnp.pad(small, ((0, 0), (0, 128 - small.shape[1])))
    qkv_block = w_qkv.reshape(-1, heads_here, 3, width).transpose(0, 2, 1, 3).reshape(-1, 3 * block)
    strip = -(-edge // 16) * 16
    qkv, proj, small, *moved = gather_weights(
        qkv_block, w_proj.reshape(-1, d), small, n_dp, n_t, (tokens, cotangent), strip
    )
    router = jnp.where(jnp.arange(128) < experts, small, 0)
    norms = jnp.pad(small[:, experts : experts + 4].astype(F32).T, ((0, 4), (0, 0)))
    order = np.arange(d, dtype=np.int32).reshape(n_t, heads_here, n_dp, -1)
    order = jnp.asarray(order.transpose(2, 0, 1, 3).reshape(d, 1))

    def lay(v, axis, fill=0):
        def rows_of(low, high):
            return lax.slice_in_dim(v, low, high, axis=axis)

        shape = v.shape[:axis] + (padded - SEQ,) + v.shape[axis + 1 :]
        hole = jnp.full(shape, fill, v.dtype)
        return jnp.concatenate(
            [rows_of(0, SEQ), hole, rows_of(own_rows, span), hole, rows_of(SEQ, own_rows)], axis=axis
        )

    def own(v, axis):
        return lax.dynamic_slice_in_dim(v, t * padded, padded, axis)

    live = live_rows[:, :span]
    rank = priority[:, 0, :span]
    picks = chosen[:, :span].transpose(0, 2, 1)
    labels = jnp.arange(experts, dtype=jnp.int32)
    earlier = (rank[:, None, :] < rank[:, :, None]).astype(BF16)
    hits = (picks[..., None] == labels).astype(F32)
    live_hits = hits * live[:, None, :, None].astype(F32)
    ahead = jnp.einsum("mrs,mkse->mkre", earlier, live_hits.astype(BF16), preferred_element_type=F32)
    firsts = jnp.sum(live_hits[:, :1], axis=2, keepdims=True)
    ahead = ahead + jnp.concatenate([jnp.zeros_like(firsts), firsts], axis=1)
    slot = jnp.sum(ahead * hits, axis=-1).astype(jnp.int32)
    keep = (live[:, None, :] > 0) & (slot < cap)
    flat = lay(jnp.where(keep, picks * cap + slot, -1), 2, -1)
    live_own = own(lay(live.astype(F32)[:, :, None], 1), 1)

    output, grad_x, grad_qkv, grad_proj, grad_router, grad_norms, grad_in, grad_out = layer(
        (tokens, cotangent),
        moved,
        router,
        flat,
        order,
        w_in[0],
        w_out[0],
        live_own,
        norms,
        qkv,
        proj.reshape(d, d),
        (experts, n_dp, n_t, block, SEQ, factor, cap),
    )
    nz, ny = grid_sizes(n_dp)
    lane = jnp.arange(128)
    smalls = jnp.where(lane < experts, grad_router, 0.0)
    smalls = smalls + jnp.pad(grad_norms[:4].T, ((0, 0), (experts, 124 - experts)))
    grad_qkv, grad_proj, smalls = scatter_grads(
        grad_qkv.reshape(nz, ny, 2, d // n_dp, -1),
        grad_proj.reshape(nz, ny, 2, n_t, -1, d),
        smalls.reshape(nz, ny, 2, n_t, -1, 128),
        n_dp,
        n_t,
        heads_here,
    )
    return (
        output,
        grad_x,
        grad_qkv,
        grad_proj,
        grad_in[None],
        grad_out[None],
        smalls[:, :experts],
        smalls[:, experts],
        smalls[:, experts + 1],
        smalls[:, experts + 2],
        smalls[:, experts + 3],
    )


def local(*args):
    tokens, w_qkv, live_rows = args[0], args[1], args[10]
    n_t = lax.axis_size("tensor")
    images = live_rows.shape[1] // SEQ
    block = w_qkv.shape[1] * (w_qkv.shape[2] // 3)
    edge = tokens.shape[1] - SEQ
    fits = tokens.shape[1] % 16 == 0 and 0 < edge <= SEQ // 2 and args[3].shape[0] == 1
    if n_t == 2 and images == 2 and fits and block % 128 == 0 and w_qkv.shape[2] == 192 and args[0].shape[0] == 3:
        return fast(*args)
    return general(*args)


def solution(mesh):
    both = ("dp", "tensor")
    return jax.shard_map(
        local,
        mesh=mesh,
        in_specs=(
            P(None, both, None),
            P("dp", "tensor", None),
            P("tensor", "dp", None),
            P("dp", None, "tensor"),
            P("dp", "tensor", None),
            P(both, None),
            P(both),
            P(both),
            P(both),
            P(both),
            P(None, "dp"),
            P(None, "dp", None),
            P(None, "dp", None),
            P(None, both, None),
        ),
        out_specs=(
            P(None, both, None),
            P(None, both, None),
            P("dp", "tensor", None),
            P("tensor", "dp", None),
            P("dp", None, "tensor"),
            P("dp", "tensor", None),
            P(both, None),
            P(both),
            P(both),
            P(both),
            P(both),
        ),
        check_vma=False,
    )
```

```python
import functools

import jax
import jax.numpy as jnp
import numpy as np
from jax import lax
from jax.experimental import pallas as pl
from jax.experimental.pallas import tpu as pltpu
from jax.sharding import PartitionSpec as P

SEQ = 197
EPS = 1e-06
F32 = jnp.float32
BF16 = jnp.bfloat16
GELU_A = 0.7978845608028654
GELU_B = 0.044715


def dot(a, b, dims):
    return lax.dot_general(a, b, (dims, ((), ())), preferred_element_type=F32)


def layer_norm(values, gain_vec, shift_vec):
    centre = jnp.mean(values, axis=-1, keepdims=True)
    centered = values - centre
    spread = jnp.mean(centered * centered, axis=-1, keepdims=True)
    return centered * lax.rsqrt(spread + EPS) * gain_vec + shift_vec


def expert_kernel(x_ref, dp_ref, win_ref, wout_ref, y_ref, dx_ref, gin_ref, gout_ref, y_acc, dx_acc):
    step = pl.program_id(0)
    last = pl.num_programs(0) - 1
    x = x_ref[...]
    dprod = dp_ref[...]
    win = win_ref[...]
    wout = wout_ref[...]
    pre = dot(x, win, ((1,), (0,)))
    square = pre * pre
    th = jnp.tanh(GELU_A * pre * (1.0 + GELU_B * square))
    active = (0.5 * pre * (1.0 + th)).astype(BF16)
    slope = 0.5 * (1.0 + th) + 0.5 * pre * (1.0 - th * th) * (GELU_A * (1.0 + 3.0 * GELU_B * square))
    dact = dot(dprod, wout, ((1,), (1,)))
    dpre = (dact * slope).astype(BF16)
    gin_ref[...] = dot(x, dpre, ((0,), (0,))).astype(BF16)
    gout_ref[...] = dot(active, dprod, ((0,), (0,))).astype(BF16)
    part_y = dot(active, wout, ((1,), (0,)))
    part_dx = dot(dpre, win, ((1,), (1,)))

    @pl.when(step == 0)
    def _():
        y_acc[...] = part_y
        dx_acc[...] = part_dx

    @pl.when(step > 0)
    def _():
        y_acc[...] += part_y
        dx_acc[...] += part_dx

    @pl.when(step == last)
    def _():
        y_ref[...] = y_acc[...].astype(BF16)
        dx_ref[...] = dx_acc[...].astype(BF16)


def expert(x, dprod, win, wout, tile=256):
    n, d = x.shape
    ff = win.shape[1]
    return pl.pallas_call(
        expert_kernel,
        grid=(ff // tile,),
        in_specs=[
            pl.BlockSpec((n, d), lambda i: (0, 0)),
            pl.BlockSpec((n, d), lambda i: (0, 0)),
            pl.BlockSpec((d, tile), lambda i: (0, i)),
            pl.BlockSpec((tile, d), lambda i: (i, 0)),
        ],
        out_specs=[
            pl.BlockSpec((n, d), lambda i: (0, 0)),
            pl.BlockSpec((n, d), lambda i: (0, 0)),
            pl.BlockSpec((d, tile), lambda i: (0, i)),
            pl.BlockSpec((tile, d), lambda i: (i, 0)),
        ],
        out_shape=[
            jax.ShapeDtypeStruct((n, d), BF16),
            jax.ShapeDtypeStruct((n, d), BF16),
            jax.ShapeDtypeStruct((d, ff), BF16),
            jax.ShapeDtypeStruct((ff, d), BF16),
        ],
        scratch_shapes=[pltpu.VMEM((n, d), F32), pltpu.VMEM((n, d), F32)],
        compiler_params=pltpu.CompilerParams(vmem_limit_bytes=60 * 1024 * 1024),
        cost_estimate=pl.CostEstimate(
            flops=12 * n * d * ff, transcendentals=n * ff, bytes_accessed=8 * n * d + 8 * d * ff
        ),
    )(x, dprod, win, wout)


MESH = pl.DeviceIdType.MESH
ANYWHERE = pl.BlockSpec(memory_space=pltpu.VMEM)


def grid_sizes(n_dp):
    ny = 1
    while 2 * ny * 2 * ny <= n_dp // 2:
        ny *= 2
    return n_dp // (2 * ny), ny


def position(ny):
    dp = lax.axis_index("dp")
    return dp, lax.axis_index("tensor"), dp % 2, (dp // 2) % ny, dp // (2 * ny)


def neighbours(ny, nz, n_t):
    dp, t, c, y, z = position(ny)

    def along_core(k):
        return (dp - c + (c + k) % 2, t)

    def along_tensor(k):
        return (dp, (t + k) % n_t)

    def along_y(k):
        return (dp + ((y + k) % ny - y) * 2, t)

    def along_z(k):
        return (dp + ((z + k) % nz - z) * 2 * ny, t)

    return {"core": (2, along_core), "tensor": (n_t, along_tensor), "y": (ny, along_y), "z": (nz, along_z)}


def greet(stages):
    barrier = pltpu.get_barrier_semaphore()
    count = 0
    for size, device in stages.values():
        for k in range(1, size):
            pl.semaphore_signal(barrier, inc=1, device_id=device(k), device_id_type=MESH)
            count += 1
    pl.semaphore_wait(barrier, count)


def gather_kernel(ny, nz, n_t, extras, *refs):
    (qkv, proj, small), refs = refs[:3], refs[3:]
    side, refs = refs[:extras], refs[extras:]
    (qkv_out, proj_out, small_out), refs = refs[:3], refs[3:]
    side_out, (send, recv, copied) = refs[:extras], refs[extras:]
    dp, t, c, y, z = position(ny)
    stages = neighbours(ny, nz, n_t)
    greet(stages)
    cols, wide = qkv.shape[1], proj.shape[1]
    whole = slice(None)
    slot = 0

    def start(pieces, device):
        nonlocal slot
        copies = []
        for src, dst in pieces:
            copies.append(
                pltpu.make_async_remote_copy(
                    src_ref=src,
                    dst_ref=dst,
                    send_sem=send.at[slot],
                    recv_sem=recv.at[slot],
                    device_id=device,
                    device_id_type=MESH,
                )
            )
            copies[-1].start()
            slot += 1
        return copies

    def along(name, pieces):
        size, device = stages[name]
        return [copy for k in range(1, size) for copy in start(pieces, device(k))]

    def lanes(ts, half):
        return pl.ds(pl.multiple_of(ts * cols + half * (cols // 2), 128), cols // 2)

    def views(zs, ys, ts, half):
        band = slice(half * (wide // 2), (half + 1) * (wide // 2))
        parts = [qkv_out.at[zs, ys, c, :, lanes(i, half)] for i in ts]
        if len(ts) == 1:
            parts.append(proj_out.at[zs, ys, c, ts[0], :, band])
            if half == 0:
                parts.append(small_out.at[zs, ys, c, ts[0]])
        else:
            parts.append(proj_out.at[zs, ys, c, :, :, band])
        return [(part, part) for part in parts]

    aside = []
    for i in range(extras):
        strip = side_out[i].shape[1]
        aside += start([(side[i].at[:, side[i].shape[1] - strip :], side_out[i])], (dp, 1 - t))
    mine = (
        qkv_out.at[z, y, c, :, pl.ds(pl.multiple_of(t * cols, 128), cols)],
        proj_out.at[z, y, c, t],
        small_out.at[z, y, c, t],
    )
    inputs = list(zip((qkv, proj, small), mine))
    local = [pltpu.make_async_copy(src, dst, copied.at[i]) for i, (src, dst) in enumerate(inputs)]
    for copy in local:
        copy.start()
    for copy in along("z", inputs) + local:
        copy.wait()
    one = along("y", views(whole, y, [t], 0))
    two = along("tensor", views(whole, y, [t], 1))
    for copy in one:
        copy.wait()
    one = along("tensor", views(whole, whole, [t], 0))
    for copy in two:
        copy.wait()
    two = along("y", views(whole, y, list(range(n_t)), 1))
    for copy in one + two:
        copy.wait()
    rest = [ref.at[:, :, c] for ref in (qkv_out, proj_out, small_out)]
    for copy in along("core", [(part, part) for part in rest]) + aside:
        copy.wait()


def gather_weights(qkv, proj, small, n_dp, n_t, side=(), strip=0):
    nz, ny = grid_sizes(n_dp)
    slots = 3 * (nz - 1) + 5 * (n_t - 1) + (4 + n_t) * (ny - 1) + 3 + len(side)
    side_shapes = [jax.ShapeDtypeStruct((v.shape[0], strip) + v.shape[2:], v.dtype) for v in side]
    outs = pl.pallas_call(
        functools.partial(gather_kernel, ny, nz, n_t, len(side)),
        out_shape=[
            jax.ShapeDtypeStruct((nz, ny, 2, qkv.shape[0], n_t * qkv.shape[1]), BF16),
            jax.ShapeDtypeStruct((nz, ny, 2, n_t) + proj.shape, BF16),
            jax.ShapeDtypeStruct((nz, ny, 2, n_t) + small.shape, BF16),
        ]
        + side_shapes,
        in_specs=[ANYWHERE] * (3 + len(side)),
        out_specs=[ANYWHERE] * (3 + len(side)),
        scratch_shapes=[
            pltpu.SemaphoreType.DMA((slots,)),
            pltpu.SemaphoreType.DMA((slots,)),
            pltpu.SemaphoreType.DMA((3,)),
        ],
        compiler_params=pltpu.CompilerParams(collective_id=0, has_side_effects=True),
    )(qkv, proj, small, *side)
    qkv_all = outs[0].reshape(n_dp * qkv.shape[0], n_t * qkv.shape[1])
    return (qkv_all, outs[1].reshape((n_dp, n_t) + proj.shape), outs[2].reshape(-1, small.shape[1])) + tuple(outs[3:])


def scatter_kernel(ny, nz, n_t, heads, *refs):
    ins, refs = refs[:3], refs[3:]
    outs, refs = refs[:3], refs[3:]
    got_core, refs = refs[:3], refs[3:]
    held, refs = refs[:3], refs[3:]
    one_got, one_held, one_last, refs = refs[:3], refs[3:6], refs[6:9], refs[9:]
    two_got, two_held, two_last, refs = refs[:2], refs[2:4], refs[4:6], refs[6:]
    end, end_got, (send, recv) = refs[:3], refs[3:6], refs[6:]
    _, t, c, y, z = position(ny)
    stages = neighbours(ny, nz, n_t)
    greet(stages)
    cols, wide = ins[0].shape[4] // n_t, ins[1].shape[5]
    slot = 0

    def lanes(ts, half):
        return pl.ds(pl.multiple_of(ts * cols + half * (cols // 2), 128), cols // 2)

    def band(half):
        return slice(half * (wide // 2), (half + 1) * (wide // 2))

    def along(name, me, pieces):
        nonlocal slot
        size, device = stages[name]
        copies = []
        for k in range(1, size):
            for src, dst in pieces((me + k) % size, k - 1):
                copies.append(
                    pltpu.make_async_remote_copy(
                        src_ref=src,
                        dst_ref=dst,
                        send_sem=send.at[slot],
                        recv_sem=recv.at[slot],
                        device_id=device(k),
                        device_id_type=MESH,
                    )
                )
                copies[-1].start()
                slot += 1
        return copies

    def finish(copies):
        for copy in copies:
            copy.wait()

    def total(own, got, index):
        value = own.astype(F32)
        for k in range(got.shape[0]):
            value = value + got[(k,) + index].astype(F32)
        return value

    def loop(count, body):
        def step(n, carry):
            body(n)
            return carry

        lax.fori_loop(0, count, step, 0)

    finish(
        along("core", c, lambda j, k: [(ins[i].at[:, :, j], got_core[i].at[k]) for i in range(3)])
    )

    def add_core(n):
        zi, yi = n // ny, n % ny
        for i in range(3):
            held[i][zi, yi] = total(ins[i][zi, yi, c], got_core[i], (zi, yi)).astype(held[i].dtype)

    loop(nz * ny, add_core)
    one = along(
        "tensor",
        t,
        lambda j, k: [
            (held[0].at[:, :, :, lanes(j, 0)], one_got[0].at[k]),
            (held[1].at[:, :, j, :, band(0)], one_got[1].at[k]),
            (held[2].at[:, :, j], one_got[2].at[k]),
        ],
    )
    two = along(
        "y",
        y,
        lambda j, k: [(held[0].at[:, j, :, lanes(i, 1)], two_got[0].at[k, i]) for i in range(n_t)]
        + [(held[1].at[:, j, i, :, band(1)], two_got[1].at[k, i]) for i in range(n_t)],
    )
    finish(one)

    def add_one(n):
        zi, yi = n // ny, n % ny
        owns = (held[0][zi, yi, :, lanes(t, 0)], held[1][zi, yi, t, :, band(0)], held[2][zi, yi, t])
        for i in range(3):
            one_held[i][zi, yi] = total(owns[i], one_got[i], (zi, yi)).astype(one_held[i].dtype)

    loop(nz * ny, add_one)
    one = along("y", y, lambda j, k: [(one_held[i].at[:, j], one_last[i].at[k]) for i in range(3)])
    finish(two)

    def add_two(zi):
        for i in range(n_t):
            owns = (held[0][zi, y, :, lanes(i, 1)], held[1][zi, y, i, :, band(1)])
            for j in range(2):
                two_held[j][i, zi] = total(owns[j], two_got[j], (i, zi)).astype(two_held[j].dtype)

    loop(nz, add_two)
    two = along("tensor", t, lambda j, k: [(two_held[i].at[j], two_last[i].at[k]) for i in range(2)])
    finish(one)
    halves = [
        (slice(0, cols // 2), slice(cols // 2, cols)),
        (band(0), band(1)),
        (slice(None),),
    ]

    def end_one(zi):
        for i in range(3):
            value = total(one_held[i][zi, y], one_last[i], (zi,))
            end[i][zi, :, halves[i][0]] = value.astype(end[i].dtype)

    loop(nz, end_one)
    finish(two)

    def end_two(zi):
        for i in range(2):
            value = total(two_held[i][t, zi], two_last[i], (zi,))
            end[i][zi, :, halves[i][1]] = value.astype(end[i].dtype)

    loop(nz, end_two)
    finish(along("z", z, lambda j, k: [(end[i].at[j], end_got[i].at[k]) for i in range(3)]))
    results = [total(end[i][z], end_got[i], ()) for i in range(3)]
    outs[2][...] = results[2]
    if heads == 0:
        outs[0][...] = results[0]
        outs[1][...] = results[1]
        return
    width = cols // (3 * heads)
    jump = outs[1].shape[1]
    for h in range(heads):
        outs[1][h] = results[1][h * jump : (h + 1) * jump]
        for i in range(3):
            at = (i * heads + h) * width
            outs[0][:, h, i * width : (i + 1) * width] = results[0][:, at : at + width]


def scatter_grads(qkv, proj, small, n_dp, n_t, heads=0):
    nz, ny = qkv.shape[:2]
    rows, cols = qkv.shape[3], qkv.shape[4] // n_t
    tails = [(rows, cols), proj.shape[4:], small.shape[4:]]
    kinds = [BF16, BF16, F32]
    parts = [(rows, cols // 2), (proj.shape[4], proj.shape[5] // 2), small.shape[4:]]
    wide = [(rows, n_t * cols), (n_t,) + proj.shape[4:], (n_t,) + small.shape[4:]]

    def room(lead, shapes):
        return [pltpu.VMEM(lead + shape, kind) for shape, kind in zip(shapes, kinds)]

    scratch = room((1, nz, ny), wide) + room((nz, ny), wide)
    scratch += room((n_t - 1, nz, ny), parts) + room((nz, ny), parts) + room((ny - 1, nz), parts)
    scratch += room((ny - 1, n_t, nz), parts[:2]) + room((n_t, nz), parts[:2]) + room((n_t - 1, nz), parts[:2])
    scratch += room((nz,), tails) + room((nz - 1,), tails)
    slots = 3 + 5 * (n_t - 1) + (3 + 2 * n_t) * (ny - 1) + 3 * (nz - 1)
    shapes = list(tails)
    if heads:
        shapes[:2] = [(rows, heads, cols // heads), (heads, proj.shape[4] // heads, proj.shape[5])]
    scratch += [pltpu.SemaphoreType.DMA((slots,)), pltpu.SemaphoreType.DMA((slots,))]
    return pl.pallas_call(
        functools.partial(scatter_kernel, ny, nz, n_t, heads),
        out_shape=[jax.ShapeDtypeStruct(shape, F32) for shape in shapes],
        in_specs=[ANYWHERE] * 3,
        out_specs=[ANYWHERE] * 3,
        scratch_shapes=scratch,
        compiler_params=pltpu.CompilerParams(collective_id=1, has_side_effects=True),
    )(qkv, proj, small)


def standardise(v):
    centre = jnp.mean(v, axis=-1, keepdims=True)
    centered = v - centre
    inverse = lax.rsqrt(jnp.mean(centered * centered, axis=-1, keepdims=True) + EPS)
    return centered * inverse, inverse


def norm_back(grad, unit, inverse):
    return inverse * (
        grad
        - jnp.mean(grad, axis=-1, keepdims=True)
        - unit * jnp.mean(grad * unit, axis=-1, keepdims=True)
    )


def two_parts(v):
    high = v.astype(BF16)
    return high, (v - high.astype(F32)).astype(BF16)


def gate_softmax(c, router, experts):
    lane = lax.broadcasted_iota(jnp.int32, (c.shape[0], router.shape[1]), 1)
    logits = jnp.where(lane < experts, dot(c, router, ((1,), (0,))), -1e30)
    raised = jnp.exp(logits - jnp.max(logits, axis=-1, keepdims=True))
    return raised / jnp.sum(raised, axis=-1, keepdims=True), lane


def key_softmax(query, keys, gap):
    scores = dot(query, keys, ((1,), (1,)))
    col = lax.broadcasted_iota(jnp.int32, scores.shape, 1)
    scores = jnp.where((col < gap[0]) | (col >= gap[1]), scores, -1e30)
    raised = jnp.exp(scores - jnp.max(scores, axis=-1, keepdims=True))
    return raised * (1.0 / jnp.sum(raised, axis=-1, keepdims=True))


def pairs(n_t, block):
    return [
        (3 * block * s + 128 * i, block * s + 128 * i) for s in range(n_t) for i in range(block // 128)
    ]


def layer_kernel(
    experts,
    n_t,
    block,
    count,
    factor,
    tokens,
    cotangent,
    moved_x,
    moved_cot,
    router,
    flat_row,
    flat_col,
    order,
    win_own,
    wout_own,
    live,
    norms,
    qkv,
    proj_in,
    out,
    grad_x,
    gqkv_out,
    gproj_out,
    grouter,
    gnorms,
    gin_mine,
    gout_mine,
    x_in,
    cot_own,
    proj,
    dhidden_in,
    edge_o,
    edge_g,
    edge_sent,
    edge_o_got,
    edge_g_got,
    c_own,
    hidden_in,
    mixed,
    context,
    c_all,
    cot_all,
    gates,
    sent,
    got,
    ret,
    pay,
    paid,
    mix,
    dx,
    dgate,
    dmixed,
    gqkv,
    gproj,
    y_acc,
    dx_acc,
    win_got,
    wout_got,
    gin_far,
    gout_far,
    gin_half,
    gout_half,
    gin_got,
    gout_got,
    w_sems,
    c_sems,
    cot_sems,
    edge_sems,
    go_send,
    go_recv,
    back_send,
    back_recv,
    pay_sems,
    grad_sems,
):
    batches, rows, d = cot_own.shape
    n_dp = lax.axis_size("dp")
    dp, t = lax.axis_index("dp"), lax.axis_index("tensor")
    share = sent.shape[1] // n_dp
    hidden = win_own.shape[1]
    shift = (share * n_t).bit_length() - 1
    other = 1 - t
    partner = (dp, other)
    own_rows, strip = tokens.shape[1], edge_o.shape[1]
    head, edge = rows - strip, own_rows - count
    gap = (jnp.where(t == 0, count, count - edge), jnp.where(t == 0, rows, rows - edge))

    barrier = pltpu.get_barrier_semaphore()
    pl.semaphore_signal(barrier, inc=1, device_id=partner, device_id_type=MESH)

    def hello(k, carry):
        pl.semaphore_signal(barrier, inc=1, device_id=((dp + k) % n_dp, t), device_id_type=MESH)
        return carry

    lax.fori_loop(1, n_dp, hello, 0)
    pl.semaphore_wait(barrier, n_dp)

    def slot_codes(shape, axis):
        q = lax.broadcasted_iota(jnp.int32, shape, axis)
        return q + (q >> (share.bit_length() - 1)) * share * (n_t - 1) + t * share

    def band(m):
        return pl.ds(pl.multiple_of(m * rows, 16), rows)

    def image(i):
        return pl.ds(pl.multiple_of(i * rows, 16), rows)

    def part(i):
        return pl.ds(pl.multiple_of(i * share, 16), share)

    def remote(src, dst, sems, i, j, device):
        return pltpu.make_async_remote_copy(
            src_ref=src,
            dst_ref=dst,
            send_sem=sems[0].at[i, j],
            recv_sem=sems[1].at[i, j],
            device_id=device,
            device_id_type=MESH,
        )

    def c_copy(m):
        return pltpu.make_async_remote_copy(
            src_ref=c_own.at[m],
            dst_ref=c_all.at[m, image(t)],
            send_sem=c_sems.at[0, m],
            recv_sem=c_sems.at[1, m],
            device_id=partner,
            device_id_type=MESH,
        )

    def cot_copy(m):
        return pltpu.make_async_remote_copy(
            src_ref=cot_own.at[m],
            dst_ref=cot_all.at[m, image(t)],
            send_sem=cot_sems.at[0, m],
            recv_sem=cot_sems.at[1, m],
            device_id=partner,
            device_id_type=MESH,
        )

    def go_copy(m, k):
        to = (dp + k) % n_dp
        return remote(sent.at[m, part(to)], got.at[m, part(dp)], (go_send, go_recv), m, k - 1, (to, t))

    def back_copy(m, k):
        to = (dp + k) % n_dp
        return remote(got.at[m, part(to)], ret.at[m, part(dp)], (back_send, back_recv), m, k - 1, (to, t))

    def pay_copy(m):
        return pltpu.make_async_remote_copy(
            src_ref=pay.at[m],
            dst_ref=paid.at[m],
            send_sem=pay_sems.at[0, m],
            recv_sem=pay_sems.at[1, m],
            device_id=partner,
            device_id_type=MESH,
        )

    def grad_copy(i):
        src, dst = ((gin_half, gin_got), (gout_half, gout_got))[i // 2]
        size = src.shape[0] // 2
        band = pl.ds(i % 2 * size, size)
        return pltpu.make_async_remote_copy(
            src_ref=src.at[band],
            dst_ref=dst.at[band],
            send_sem=grad_sems.at[0, i],
            recv_sem=grad_sems.at[1, i],
            device_id=partner,
            device_id_type=MESH,
        )

    def w_copy(i):
        return pltpu.make_async_remote_copy(
            src_ref=(win_own, wout_own)[i],
            dst_ref=(win_got, wout_got)[i],
            send_sem=w_sems.at[0, i],
            recv_sem=w_sems.at[1, i],
            device_id=partner,
            device_id_type=MESH,
        )

    def every(body):
        def step(k, carry):
            body(k)
            return carry

        lax.fori_loop(1, n_dp, step, 0)

    low = lax.broadcasted_iota(jnp.int32, (rows, 128), 1) < 64

    def edge_copy(i, m):
        return pltpu.make_async_remote_copy(
            src_ref=(edge_o, edge_sent)[i].at[m],
            dst_ref=(edge_o_got, edge_g_got)[i].at[m],
            send_sem=edge_sems.at[2 * i, m],
            recv_sem=edge_sems.at[2 * i + 1, m],
            device_id=partner,
            device_id_type=MESH,
        )

    for own_ref, ref, moved in ((cot_own, cotangent, moved_cot), (x_in, tokens, moved_x)):
        own_ref[:, :head] = ref[:, :head]

        @pl.when(t == 0)
        def _(own_ref=own_ref, ref=ref):
            own_ref[:, head:] = ref[:, head:rows]

        @pl.when(t != 0)
        def _(own_ref=own_ref, moved=moved):
            own_ref[:, head:] = moved[...]

    def permutation():
        return (order[...] == lax.broadcasted_iota(jnp.int32, (d, d), 1)).astype(F32).astype(BF16)

    proj[...] = dot(permutation(), proj_in[...], ((0,), (0,))).astype(BF16)

    def attend(m, carry):
        cot_copy(m).start()
        cot_all[m, image(t)] = cot_own[m]
        xf = x_in[m].astype(F32)
        unit, _ = standardise(xf)
        a = (unit * norms[0:1] + norms[1:2]).astype(BF16)
        for s in range(n_t):
            for i in range(3):
                cols = slice((3 * s + i) * block, (3 * s + i + 1) * block)
                projected = dot(a, qkv[:, cols], ((1,), (0,)))
                mixed[m, :, cols] = (projected * factor if i == 0 else projected).astype(BF16)
        for col, dest in pairs(n_t, block):
            query = mixed[m, :, col : col + 128]
            keys = mixed[m, :, col + block : col + block + 128]
            values = mixed[m, :, col + 2 * block : col + 2 * block + 128]
            zero = jnp.zeros_like(query)
            parts = []
            for own in (low, ~low):
                probs = key_softmax(jnp.where(own, query, zero), keys, gap)
                parts.append(dot(probs.astype(BF16), values, ((1,), (0,))))
            context[m, :, dest : dest + 128] = jnp.where(low, parts[0], parts[1]).astype(BF16)
        hidden = xf + live[m] * dot(context[m], proj[...], ((1,), (0,)))
        hidden_in[m] = hidden
        unit, _ = standardise(hidden)
        c = (unit * norms[2:3] + norms[3:4]).astype(BF16)
        c_own[m] = c
        c_all[m, image(t)] = c
        c_copy(m).start()
        return carry

    lax.fori_loop(0, batches, attend, 0)
    w_copy(0).start()
    w_copy(1).start()

    lane = lax.broadcasted_iota(jnp.int32, (2 * rows, router.shape[1]), 1)

    def dispatch(m, carry):
        c_copy(m).wait_recv()
        cot_copy(m).wait_recv()
        c = c_all[m]
        logits = jnp.where(lane < experts, dot(c, router[...], ((1,), (0,))), -1e30)
        raised = jnp.exp(logits - jnp.max(logits, axis=-1, keepdims=True))
        probs = raised / jnp.sum(raised, axis=-1, keepdims=True)
        cot = cot_all[m].astype(F32)
        scaled = []
        for k in range(2):
            gate = jnp.sum(jnp.where(lane == flat_col[m, :, k : k + 1] >> shift, probs, 0.0), axis=-1, keepdims=True)
            gates[m, :, k : k + 1] = gate
            scaled.append((gate * cot).astype(BF16))
        codes = slot_codes((n_dp * share, 1), 0)
        picks = [(flat_row[m, k : k + 1, :] == codes).astype(F32).astype(BF16) for k in range(2)]
        sent[m, :, :d] = dot(picks[0] + picks[1], c, ((1,), (0,))).astype(BF16)
        moved = dot(picks[0], scaled[0], ((1,), (0,))) + dot(picks[1], scaled[1], ((1,), (0,)))
        sent[m, :, d:] = moved.astype(BF16)
        every(lambda k: go_copy(m, k).start())
        got[m, part(dp)] = sent[m, part(dp)]
        return carry

    lax.fori_loop(0, batches, dispatch, 0)

    tile = min(512, hidden)

    def clear(i, carry):
        cols = pl.ds(pl.multiple_of(i * tile, tile), tile)
        for into in (gin_far, gin_mine):
            into[:, cols] = jnp.zeros((d, tile), F32)
        for into in (gout_far, gout_mine):
            into[cols, :] = jnp.zeros((tile, d), F32)
        return carry

    lax.fori_loop(0, hidden // tile, clear, 0)

    slots = n_dp * share
    sums = ((y_acc, dx_acc), (mix.at[pl.ds(0, slots)], dx.at[pl.ds(0, slots)]))

    def expert_half(m, own):
        y_sum, dx_sum = sums[m % 2]
        win, wout, gin, gout = (win_own, wout_own, gin_mine, gout_mine) if own else (win_got, wout_got, gin_far, gout_far)

        def chunk(i, inner):
            cols = pl.ds(pl.multiple_of(i * tile, tile), tile)
            x = got[m, :, :d]
            dprod = got[m, :, d:]
            w1 = win[:, cols]
            w2 = wout[cols, :]
            pre = dot(x, w1, ((1,), (0,)))
            square = pre * pre
            th = jnp.tanh(GELU_A * pre * (1.0 + GELU_B * square))
            active = (0.5 * pre * (1.0 + th)).astype(BF16)
            slope = 0.5 * (1.0 + th) + 0.5 * pre * (1.0 - th * th) * (GELU_A * (1.0 + 3.0 * GELU_B * square))
            dpre = (dot(dprod, w2, ((1,), (1,))) * slope).astype(BF16)
            gin[:, cols] += dot(x, dpre, ((0,), (0,)))
            gout[cols, :] += dot(active, dprod, ((0,), (0,)))
            y_sum[...] += dot(active, w2, ((1,), (0,)))
            dx_sum[...] += dot(dpre, w1, ((1,), (1,)))
            return inner

        lax.fori_loop(0, hidden // tile, chunk, 0)

    def expert_begin(m):
        every(lambda k: go_copy(m, k).wait_recv())
        for ref in sums[m % 2]:
            ref[...] = jnp.zeros((slots, d), F32)

    def expert_end(m):
        got[m, :, :d] = sums[m % 2][0][...].astype(BF16)
        got[m, :, d:] = sums[m % 2][1][...].astype(BF16)
        every(lambda k: back_copy(m, k).start())
        ret[m, part(dp)] = got[m, part(dp)]

    last = batches - 1
    for m in range(last):
        expert_begin(m)
        expert_half(m, True)
    w_copy(0).wait_recv()
    w_copy(1).wait_recv()
    for m in range(last):
        expert_half(m, False)
        expert_end(m)
    expert_begin(last)
    expert_half(last, False)
    gin_half[...] = gin_far[...].astype(BF16)
    gout_half[...] = gout_far[...].astype(BF16)
    grad_copy(0).start()
    grad_copy(1).start()
    expert_half(last, True)
    expert_end(last)

    def combine(m, carry):
        every(lambda k: back_copy(m, k).wait_recv())
        codes = slot_codes((1, n_dp * share), 1)
        for i in (other, t):
            picks = [(flat_col[m, image(i), k : k + 1] == codes).astype(F32).astype(BF16) for k in range(2)]
            one = dot(picks[0], ret[m, :, :d], ((1,), (0,)))
            two = dot(picks[1], ret[m, :, :d], ((1,), (0,)))
            d_rows = dot(picks[0] + picks[1], ret[m, :, d:], ((1,), (0,)))
            cot = cot_all[m, image(i)].astype(F32)
            gate = gates[m, image(i)]
            mixture = gate[:, 0:1] * one + gate[:, 1:2] * two
            col = lax.broadcasted_iota(jnp.int32, (rows, 128), 1)
            dg = jnp.where(col == 0, jnp.sum(one * cot, axis=-1, keepdims=True), 0.0)
            dg = dg + jnp.where(col == 1, jnp.sum(two * cot, axis=-1, keepdims=True), 0.0)
            if i is other:
                pay[m, :, :d] = mixture.astype(BF16)
                pay[m, :, d : 2 * d] = d_rows.astype(BF16)
                pay[m, :, 2 * d :] = dg.astype(BF16)
                pay_copy(m).start()
            else:
                mix[band(m)] = mixture
                dx[band(m)] = d_rows
                dgate[m] = dg
        return carry

    gqkv[...] = jnp.zeros_like(gqkv)
    gproj[...] = jnp.zeros_like(gproj)
    grouter[...] = jnp.zeros_like(grouter)
    gnorms[...] = jnp.zeros_like(gnorms)

    def retreat(m):
        pay_copy(m).wait_recv()
        hidden = hidden_in[m]
        result = (hidden + mix[band(m)] + paid[m, :, :d].astype(F32)).astype(BF16)
        out[m, :head] = result[:head]
        edge_o[m] = result[head:]
        edge_copy(0, m).start()
        unit, inverse = standardise(hidden)
        c = (unit * norms[2:3] + norms[3:4]).astype(BF16)
        probs, lane = gate_softmax(c, router[...], experts)
        dg = dgate[m] + paid[m, :, 2 * d :].astype(F32)
        dprobs = jnp.zeros_like(probs)
        for k in range(2):
            dprobs = dprobs + jnp.where(lane == flat_col[m, image(t), k : k + 1] >> shift, dg[:, k : k + 1], 0.0)
        dlogits = probs * (dprobs - jnp.sum(dprobs * probs, axis=-1, keepdims=True))
        dc = dx[band(m)] + paid[m, :, d : 2 * d].astype(F32)
        for piece in two_parts(dlogits):
            grouter[...] += dot(c, piece, ((0,), (0,)))
            dc = dc + dot(piece, router[...], ((1,), (1,)))
        gnorms[2:3] += jnp.sum(dc * unit, axis=0, keepdims=True)
        gnorms[3:4] += jnp.sum(dc, axis=0, keepdims=True)
        dhidden = cot_all[m, image(t)].astype(F32) + norm_back(dc * norms[2:3], unit, inverse)
        dhidden_in[...] = dhidden
        dattn = (live[m] * dhidden).astype(BF16)
        gproj[...] += dot(context[m], dattn, ((0,), (0,)))
        dcontext = dot(dattn, proj[...], ((1,), (1,))).astype(BF16)
        for col, dest in pairs(n_t, block):
            query = mixed[m, :, col : col + 128]
            keys = mixed[m, :, col + block : col + block + 128]
            values = mixed[m, :, col + 2 * block : col + 2 * block + 128]
            grads = dcontext[:, dest : dest + 128]
            zero = jnp.zeros_like(query)
            parts = []
            for own in (low, ~low):
                probs = key_softmax(jnp.where(own, query, zero), keys, gap)
                dvalues = dot(probs.astype(BF16), grads, ((0,), (0,)))
                dweights = dot(jnp.where(own, grads, zero), values, ((1,), (1,)))
                dscores = probs * (dweights - jnp.sum(dweights * probs, axis=-1, keepdims=True))
                dscores = dscores.astype(BF16)
                parts.append(
                    (dot(dscores, keys, ((1,), (0,))), dot(dscores, query, ((0,), (0,))), dvalues)
                )
            for i in range(3):
                both = jnp.where(low, parts[0][i], parts[1][i]).astype(BF16)
                if i == 0:
                    both = both * BF16(factor)
                dmixed[:, col + i * block : col + i * block + 128] = both
        unit, inverse = standardise(x_in[m].astype(F32))
        a = (unit * norms[0:1] + norms[1:2]).astype(BF16)
        gqkv[...] += dot(a, dmixed[...], ((0,), (0,)))
        da = dot(dmixed[...], qkv[...], ((1,), (1,)))
        gnorms[0:1] += jnp.sum(da * unit, axis=0, keepdims=True)
        gnorms[1:2] += jnp.sum(da, axis=0, keepdims=True)
        result = dhidden_in[...] + norm_back(da * norms[0:1], unit, inverse)
        grad_x[m, :head] = result[:head]
        edge_g[m] = result[head:]
        edge_sent[m] = result[head:].astype(BF16)
        edge_copy(1, m).start()

    pieces = 4

    def finish(m, carry):
        @pl.when(m < batches)
        def _():
            combine(m, 0)

        @pl.when(m == 0)
        def _():
            grad_copy(2).start()

        @pl.when(m == batches - 1)
        def _():
            grad_copy(3).start()

        @pl.when(m > 0)
        def _():
            retreat(m - 1)

        return carry

    lax.fori_loop(0, batches + 1, finish, 0)
    gqkv_out[...] = gqkv[...].astype(BF16)
    gproj_out[...] = dot(permutation(), gproj[...].astype(BF16), ((1,), (0,))).astype(BF16)

    @pl.when(t != 0)
    def _():
        out[:, head:] = tokens[:, head:]
        grad_x[:, head:] = cotangent[:, head:].astype(F32)

    first = own_rows - strip
    near = lax.broadcasted_iota(jnp.int32, (16, d), 0) < strip - edge

    def place(m, carry):
        edge_copy(0, m).wait()
        edge_copy(1, m).wait()

        @pl.when(t == 0)
        def _():
            for ref, mine, theirs in ((out, edge_o, edge_o_got), (grad_x, edge_g, edge_g_got)):
                ref[m, head:first] = mine[m, : first - head]
                blend = jnp.where(
                    near,
                    mine[m, first - head : first - head + 16].astype(F32),
                    theirs[m, :16].astype(F32),
                )
                ref[m, first : first + 16] = blend.astype(ref.dtype)
                ref[m, first + 16 :] = theirs[m, 16:].astype(ref.dtype)

        return carry

    lax.fori_loop(0, batches, place, 0)
    for i in range(pieces):
        grad_copy(i).wait()
    gin_mine[...] += gin_got[...].astype(F32)
    gout_mine[...] += gout_got[...].astype(F32)
    w_copy(0).wait_send()
    w_copy(1).wait_send()

    def drain(m, carry):
        c_copy(m).wait_send()
        cot_copy(m).wait_send()
        pay_copy(m).wait_send()
        every(lambda k: go_copy(m, k).wait_send())
        every(lambda k: back_copy(m, k).wait_send())
        return carry

    lax.fori_loop(0, batches, drain, 0)


def layer(held, moved, router, flat, order, win, wout, live, norms, qkv, proj, statics):
    batches, own_rows, d = held[0].shape
    experts, n_dp, n_t, block, count, factor, cap = statics
    rows, strip = live.shape[1], moved[0].shape[1]
    slots = n_dp * cap // n_t
    half = win.shape[1]
    wide = 3 * n_t * block
    dma = pltpu.SemaphoreType.DMA
    return pl.pallas_call(
        functools.partial(layer_kernel, experts, n_t, block, count, factor),
        out_shape=[
            jax.ShapeDtypeStruct((batches, own_rows, d), BF16),
            jax.ShapeDtypeStruct((batches, own_rows, d), F32),
            jax.ShapeDtypeStruct((d, wide), BF16),
            jax.ShapeDtypeStruct((d, d), BF16),
            jax.ShapeDtypeStruct((d, router.shape[1]), F32),
            jax.ShapeDtypeStruct((8, d), F32),
            jax.ShapeDtypeStruct((d, half), F32),
            jax.ShapeDtypeStruct((half, d), F32),
        ],
        in_specs=[ANYWHERE] * 14,
        out_specs=[ANYWHERE] * 8,
        scratch_shapes=[
            pltpu.VMEM((batches, rows, d), BF16),
            pltpu.VMEM((batches, rows, d), BF16),
            pltpu.VMEM((d, d), BF16),
            pltpu.VMEM((rows, d), F32),
            pltpu.VMEM((batches, strip, d), BF16),
            pltpu.VMEM((batches, strip, d), F32),
            pltpu.VMEM((batches, strip, d), BF16),
            pltpu.VMEM((batches, strip, d), BF16),
            pltpu.VMEM((batches, strip, d), BF16),
            pltpu.VMEM((batches, rows, d), BF16),
            pltpu.VMEM((batches, rows, d), F32),
            pltpu.VMEM((batches, rows, wide), BF16),
            pltpu.VMEM((batches, rows, d), BF16),
            pltpu.VMEM((batches, 2 * rows, d), BF16),
            pltpu.VMEM((batches, 2 * rows, d), BF16),
            pltpu.VMEM((batches, 2 * rows, 128), F32),
            pltpu.VMEM((batches, slots, 2 * d), BF16),
            pltpu.VMEM((batches, slots, 2 * d), BF16),
            pltpu.VMEM((batches, slots, 2 * d), BF16),
            pltpu.VMEM((batches, rows, 2 * d + 128), BF16),
            pltpu.VMEM((batches, rows, 2 * d + 128), BF16),
            pltpu.VMEM((max(batches * rows, slots), d), F32),
            pltpu.VMEM((max(batches * rows, slots), d), F32),
            pltpu.VMEM((batches, rows, 128), F32),
            pltpu.VMEM((rows, wide), BF16),
            pltpu.VMEM((d, wide), F32),
            pltpu.VMEM((d, d), F32),
            pltpu.VMEM((slots, d), F32),
            pltpu.VMEM((slots, d), F32),
            pltpu.VMEM((d, half), BF16),
            pltpu.VMEM((half, d), BF16),
            pltpu.VMEM((d, half), F32),
            pltpu.VMEM((half, d), F32),
            pltpu.VMEM((d, half), BF16),
            pltpu.VMEM((half, d), BF16),
            pltpu.VMEM((d, half), BF16),
            pltpu.VMEM((half, d), BF16),
            dma((2, 2)),
            dma((2, batches)),
            dma((2, batches)),
            dma((4, batches)),
            dma((batches, n_dp - 1)),
            dma((batches, n_dp - 1)),
            dma((batches, n_dp - 1)),
            dma((batches, n_dp - 1)),
            dma((2, batches)),
            dma((2, 4)),
        ],
        compiler_params=pltpu.CompilerParams(
            collective_id=2, has_side_effects=True, vmem_limit_bytes=67043328
        ),
    )(
        *held,
        *moved,
        router,
        flat,
        flat.transpose(0, 2, 1),
        order,
        win,
        wout,
        live,
        norms,
        qkv,
        proj,
    )


def general(
    tokens,
    w_qkv,
    w_proj,
    w_in,
    w_out,
    w_router,
    gain_attn,
    shift_attn,
    gain_moe,
    shift_moe,
    live_rows,
    chosen,
    priority,
    cotangent,
):
    batches, own_rows, d = tokens.shape
    rows = live_rows.shape[1]
    n_dp = lax.axis_size("dp")
    n_t = lax.axis_size("tensor")
    t = lax.axis_index("tensor")
    heads_here = w_qkv.shape[1]
    heads = heads_here * n_t
    width = w_qkv.shape[2] // 3
    experts = w_in.shape[0] * n_dp
    cap = 2 * rows // experts
    share = cap // n_t
    images = rows // SEQ
    span = images * SEQ
    per = -(-images // n_t)
    work = per * SEQ
    total = n_t * work
    factor = width ** (-0.5)
    highest = lax.Precision.HIGHEST

    small = jnp.concatenate(
        [w_router] + [v[:, None] for v in (gain_attn, shift_attn, gain_moe, shift_moe)], axis=1
    )
    small = jnp.pad(small, ((0, 0), (0, 128 - small.shape[1])))
    block = heads_here * width
    qkv_block = w_qkv.reshape(-1, heads_here, 3, width).transpose(0, 2, 1, 3).reshape(-1, 3 * block)
    fill = -3 * block % 128
    qkv_block = jnp.pad(qkv_block, ((0, 0), (0, fill)))
    qkv, proj, small = gather_weights(qkv_block, w_proj.reshape(-1, d), small, n_dp, n_t)
    qkv = qkv.reshape(d, n_t, 3 * block + fill)[:, :, : 3 * block].reshape(d, -1)
    router = small[:, :experts]
    gain_one, shift_one, gain_two, shift_two = (small[:, experts + i].astype(F32) for i in range(4))
    proj = proj.reshape(n_dp, n_t, heads_here, w_proj.shape[1], d)
    proj = proj.transpose(1, 2, 0, 3, 4).reshape(heads * width, d)
    win = lax.all_gather(w_in[0], "tensor", axis=1, tiled=True)
    wout = lax.all_gather(w_out[0], "tensor", axis=0, tiled=True)
    cot_all = lax.all_gather(cotangent, "tensor", axis=1, tiled=True)

    def pad_rows(v, n):
        return jnp.pad(v, ((0, 0), (0, n - v.shape[1])) + ((0, 0),) * (v.ndim - 2))

    def own(v):
        return lax.dynamic_slice_in_dim(v, t * work, work, 1)

    edge = own_rows - work
    direct = n_t == 2 and per == 1 and edge >= 0
    if direct:
        moved = lax.ppermute(tokens[:, work:], "tensor", [(0, 1)])
        x = jnp.where(
            t == 0, tokens[:, :work], jnp.concatenate([moved, tokens[:, : work - edge]], axis=1)
        )
    else:
        x = own(pad_rows(lax.all_gather(tokens, "tensor", axis=1, tiled=True)[:, :span], total))
    x = x.astype(F32)
    live = live_rows[:, :span]
    live_all = pad_rows(live, total)
    live_own = own(live_all).astype(F32)[:, :, None]
    cot_all = pad_rows(cot_all[:, :span], total)
    dy = own(cot_all).astype(F32)

    rank = priority[:, 0, :span]
    first, second = chosen[:, :span, 0], chosen[:, :span, 1]
    labels = jnp.arange(experts, dtype=jnp.int32)
    earlier = (rank[:, None, :] < rank[:, :, None]).astype(BF16)
    hit_one = (first[:, :, None] == labels).astype(F32)
    hit_two = (second[:, :, None] == labels).astype(F32)
    live_one = hit_one * live[:, :, None].astype(F32)
    live_two = hit_two * live[:, :, None].astype(F32)
    counts = jnp.einsum(
        "mrs,mse->mre",
        earlier,
        jnp.concatenate([live_one, live_two], axis=-1).astype(BF16),
        preferred_element_type=F32,
    )
    first_total = jnp.sum(live_one, axis=1, keepdims=True)
    slot_one = jnp.sum(counts[:, :, :experts] * hit_one, axis=-1).astype(jnp.int32)
    slot_two = jnp.sum((counts[:, :, experts:] + first_total) * hit_two, axis=-1).astype(jnp.int32)
    keep_one = (live > 0) & (slot_one < cap)
    keep_two = (live > 0) & (slot_two < cap)
    flat_one = jnp.where(keep_one, first * cap + slot_one, -1)
    flat_two = jnp.where(keep_two, second * cap + slot_two, -1)

    def spread(v, fill):
        return jnp.pad(v, ((0, 0), (0, total - span)), constant_values=fill)

    flat_one, flat_two = spread(flat_one, -1), spread(flat_two, -1)
    keep_one, keep_two = spread(keep_one, False), spread(keep_two, False)
    first, second = spread(first, 0), spread(second, 0)
    codes = (jnp.arange(experts)[:, None] * cap + t * share + jnp.arange(share)[None, :]).reshape(-1)
    pick_one = flat_one[:, None, :] == codes[None, :, None]
    pick_two = flat_two[:, None, :] == codes[None, :, None]

    normed_one = layer_norm(x, gain_one, shift_one).astype(BF16)
    mixed = dot(normed_one, qkv, ((2,), (0,)))
    split = heads * width
    shape = (batches * per, SEQ, heads, width)
    mixed = mixed.reshape(batches, work, n_t, 3, block)
    query = (mixed[:, :, :, 0] * factor).astype(BF16).reshape(shape)
    keys = mixed[:, :, :, 1].astype(BF16).reshape(shape)
    values = mixed[:, :, :, 2].astype(BF16).reshape(shape)
    scores = jnp.einsum("iqhc,ikhc->ihqk", query, keys, preferred_element_type=F32)
    probs = jax.nn.softmax(scores, axis=-1)
    weights = probs.astype(BF16)
    context = jnp.einsum("ihqk,ikhc->iqhc", weights, values, preferred_element_type=F32)
    context = context.astype(BF16).reshape(batches, work, split)
    attn = dot(context, proj, ((2,), (0,)))
    hidden = x + live_own * attn
    normed_two = layer_norm(hidden, gain_two, shift_two).astype(BF16)

    c_all = lax.all_gather(normed_two, "tensor", axis=1, tiled=True)
    gate_probs = jax.nn.softmax(dot(c_all, router, ((2,), (0,))), axis=-1)
    hits_one = (first[:, :, None] == labels).astype(F32)
    hits_two = (second[:, :, None] == labels).astype(F32)
    gate_one = jnp.sum(gate_probs * hits_one, axis=-1) * keep_one
    gate_two = jnp.sum(gate_probs * hits_two, axis=-1) * keep_two
    picked = (pick_one | pick_two).astype(BF16)
    sent = jnp.einsum(
        "mqr,mrd->mqd",
        picked,
        jnp.concatenate([c_all, cot_all], axis=-1),
        preferred_element_type=F32,
    )
    gate_slot = jnp.sum(
        jnp.where(pick_one, gate_one[:, None, :], 0.0) + jnp.where(pick_two, gate_two[:, None, :], 0.0),
        axis=-1,
        keepdims=True,
    )
    sent = jnp.concatenate(
        [sent[..., :d].astype(BF16), (sent[..., d:] * gate_slot).astype(BF16)], axis=-1
    )
    sent = sent.reshape(batches, experts, share, 2 * d)
    got = lax.all_to_all(sent, "dp", 1, 1, tiled=True).reshape(-1, 2 * d)
    produced, d_in, grad_in, grad_out = expert(got[:, :d], got[:, d:], win, wout)
    back = jnp.concatenate([produced, d_in], axis=-1).reshape(batches, n_dp, share, 2 * d)
    back = lax.all_to_all(back, "dp", 1, 1, tiled=True).reshape(batches, experts * share, 2 * d)
    grad_in = lax.psum_scatter(grad_in, "tensor", scatter_dimension=1, tiled=True).astype(F32)
    grad_out = lax.psum_scatter(grad_out, "tensor", scatter_dimension=0, tiled=True).astype(F32)

    part_one = jnp.einsum("mqr,mqd->mrd", pick_one.astype(BF16), back[..., :d], preferred_element_type=F32)
    part_two = jnp.einsum("mqr,mqd->mrd", pick_two.astype(BF16), back[..., :d], preferred_element_type=F32)
    d_rows = jnp.einsum("mqr,mqd->mrd", picked, back[..., d:], preferred_element_type=F32)
    mixture = gate_one[:, :, None] * part_one + gate_two[:, :, None] * part_two
    cot_wide = cot_all.astype(F32)
    dgate_one = jnp.sum(part_one * cot_wide, axis=-1, keepdims=True)
    dgate_two = jnp.sum(part_two * cot_wide, axis=-1, keepdims=True)
    dgates = jnp.concatenate([dgate_one, dgate_two], axis=-1)
    payload = jnp.concatenate(
        [mixture, d_rows, jnp.pad(dgates, ((0, 0), (0, 0), (0, 126)))], axis=-1
    ).astype(BF16)
    pieces = payload.reshape(batches, n_t, work, payload.shape[-1])

    def piece(k):
        return lax.dynamic_index_in_dim(pieces, (t + k) % n_t, 1, keepdims=False)

    payload = piece(0).astype(F32)
    for k in range(1, n_t):
        payload = payload + lax.ppermute(
            piece(k), "tensor", [(j, (j + k) % n_t) for j in range(n_t)]
        ).astype(F32)
    output = (hidden + payload[..., :d]).astype(BF16)
    dgates = payload[..., 2 * d : 2 * d + 2]

    own_probs = own(gate_probs)
    dprobs = own(hits_one) * dgates[..., 0:1] * own(keep_one)[:, :, None]
    dprobs = dprobs + own(hits_two) * dgates[..., 1:2] * own(keep_two)[:, :, None]
    dlogits = own_probs * (dprobs - jnp.sum(dprobs * own_probs, axis=-1, keepdims=True))
    grad_router = lax.dot_general(
        normed_two.astype(F32), dlogits, (((0, 1), (0, 1)), ((), ())), precision=highest
    )
    dc = payload[..., d : 2 * d] + lax.dot_general(
        dlogits, router.astype(F32), (((2,), (1,)), ((), ())), precision=highest
    )
    _, back_two = jax.vjp(layer_norm, hidden, gain_two, shift_two)
    dnorm, grad_gain_two, grad_shift_two = back_two(dc)
    dhidden = dy + dnorm
    dattn = (live_own * dhidden).astype(BF16)

    grad_proj = dot(context, dattn, ((0, 1), (0, 1)))
    dcontext = dot(dattn, proj, ((2,), (1,))).astype(BF16).reshape(shape)
    dvalues = jnp.einsum("ihqk,iqhc->ikhc", weights, dcontext, preferred_element_type=F32).astype(BF16)
    dweights = jnp.einsum("iqhc,ikhc->ihqk", dcontext, values, preferred_element_type=F32)
    dscores = (probs * (dweights - jnp.sum(dweights * probs, axis=-1, keepdims=True))).astype(BF16)
    dquery = jnp.einsum("ihqk,ikhc->iqhc", dscores, keys, preferred_element_type=F32).astype(BF16)
    dkeys = jnp.einsum("ihqk,iqhc->ikhc", dscores, query, preferred_element_type=F32).astype(BF16)
    dmixed = jnp.stack(
        [v.reshape(batches, work, n_t, block) for v in (dquery * BF16(factor), dkeys, dvalues)], axis=3
    ).reshape(batches, work, 3 * split)
    grad_qkv = dot(normed_one, dmixed, ((0, 1), (0, 1)))
    da = dot(dmixed, qkv, ((2,), (1,)))
    _, back_one = jax.vjp(layer_norm, x, gain_one, shift_one)
    dnorm, grad_gain_one, grad_shift_one = back_one(da)
    grad_x = dhidden + dnorm

    if direct:
        out_edge = lax.ppermute(output[:, :edge], "tensor", [(1, 0)])
        grad_edge = lax.ppermute(grad_x[:, :edge], "tensor", [(1, 0)])
        result = jnp.where(
            t == 0,
            jnp.concatenate([output, out_edge], axis=1),
            jnp.concatenate([output[:, edge:], tokens[:, work - edge :]], axis=1),
        )
        grad_tokens = jnp.where(
            t == 0,
            jnp.concatenate([grad_x, grad_edge], axis=1),
            jnp.concatenate([grad_x[:, edge:], cotangent[:, work - edge :].astype(F32)], axis=1),
        )
    else:
        here = (t * own_rows + jnp.arange(own_rows) < span)[None, :, None]

        def home(v, rest):
            full = pad_rows(lax.all_gather(v, "tensor", axis=1, tiled=True)[:, :span], rows)
            return jnp.where(here, lax.dynamic_slice_in_dim(full, t * own_rows, own_rows, 1), rest)

        result = home(output, tokens)
        grad_tokens = home(grad_x, cotangent.astype(F32))

    nz, ny = grid_sizes(n_dp)
    grad_qkv = jnp.pad(grad_qkv.astype(BF16).reshape(d, n_t, 3 * block), ((0, 0), (0, 0), (0, fill)))
    grad_qkv = grad_qkv.reshape(nz, ny, 2, d // n_dp, -1)
    grad_proj = grad_proj.astype(BF16).reshape(n_t, heads_here, n_dp, -1, d)
    grad_proj = grad_proj.transpose(2, 0, 1, 3, 4).reshape(nz, ny, 2, n_t, -1, d)
    smalls = jnp.concatenate(
        [grad_router] + [v[:, None] for v in (grad_gain_one, grad_shift_one, grad_gain_two, grad_shift_two)],
        axis=1,
    )
    smalls = jnp.pad(smalls, ((0, 0), (0, 128 - smalls.shape[1]))).reshape(nz, ny, 2, n_t, -1, 128)
    grad_qkv, grad_proj, smalls = scatter_grads(grad_qkv, grad_proj, smalls, n_dp, n_t)
    grad_qkv = grad_qkv[:, : 3 * block].reshape(-1, 3, heads_here, width).transpose(0, 2, 1, 3)
    return (
        result,
        grad_tokens,
        grad_qkv.reshape(w_qkv.shape),
        grad_proj.reshape(w_proj.shape),
        grad_in[None],
        grad_out[None],
        smalls[:, :experts],
        smalls[:, experts],
        smalls[:, experts + 1],
        smalls[:, experts + 2],
        smalls[:, experts + 3],
    )


def fast(
    tokens,
    w_qkv,
    w_proj,
    w_in,
    w_out,
    w_router,
    gain_attn,
    shift_attn,
    gain_moe,
    shift_moe,
    live_rows,
    chosen,
    priority,
    cotangent,
):
    batches, own_rows, d = tokens.shape
    rows = live_rows.shape[1]
    n_dp = lax.axis_size("dp")
    n_t = lax.axis_size("tensor")
    t = lax.axis_index("tensor")
    heads_here = w_qkv.shape[1]
    width = w_qkv.shape[2] // 3
    block = heads_here * width
    experts = n_dp
    cap = 2 * rows // experts
    share = cap // n_t
    span = n_t * SEQ
    padded = -(-SEQ // 16) * 16
    edge = own_rows - SEQ
    factor = width ** (-0.5)

    vectors = jnp.stack([gain_attn, shift_attn, gain_moe, shift_moe])
    small = jnp.concatenate([w_router, vectors.T], axis=1)
    small = jnp.pad(small, ((0, 0), (0, 128 - small.shape[1])))
    qkv_block = w_qkv.reshape(-1, heads_here, 3, width).transpose(0, 2, 1, 3).reshape(-1, 3 * block)
    strip = -(-edge // 16) * 16
    qkv, proj, small, *moved = gather_weights(
        qkv_block, w_proj.reshape(-1, d), small, n_dp, n_t, (tokens, cotangent), strip
    )
    router = jnp.where(jnp.arange(128) < experts, small, 0)
    norms = jnp.pad(small[:, experts : experts + 4].astype(F32).T, ((0, 4), (0, 0)))
    order = np.arange(d, dtype=np.int32).reshape(n_t, heads_here, n_dp, -1)
    order = jnp.asarray(order.transpose(2, 0, 1, 3).reshape(d, 1))

    def lay(v, axis, fill=0):
        def rows_of(low, high):
            return lax.slice_in_dim(v, low, high, axis=axis)

        shape = v.shape[:axis] + (padded - SEQ,) + v.shape[axis + 1 :]
        hole = jnp.full(shape, fill, v.dtype)
        return jnp.concatenate(
            [rows_of(0, SEQ), hole, rows_of(own_rows, span), hole, rows_of(SEQ, own_rows)], axis=axis
        )

    def own(v, axis):
        return lax.dynamic_slice_in_dim(v, t * padded, padded, axis)

    live = live_rows[:, :span]
    rank = priority[:, 0, :span]
    picks = chosen[:, :span].transpose(0, 2, 1)
    labels = jnp.arange(experts, dtype=jnp.int32)
    earlier = (rank[:, None, :] < rank[:, :, None]).astype(BF16)
    hits = (picks[..., None] == labels).astype(F32)
    live_hits = hits * live[:, None, :, None].astype(F32)
    ahead = jnp.einsum("mrs,mkse->mkre", earlier, live_hits.astype(BF16), preferred_element_type=F32)
    firsts = jnp.sum(live_hits[:, :1], axis=2, keepdims=True)
    ahead = ahead + jnp.concatenate([jnp.zeros_like(firsts), firsts], axis=1)
    slot = jnp.sum(ahead * hits, axis=-1).astype(jnp.int32)
    keep = (live[:, None, :] > 0) & (slot < cap)
    flat = lay(jnp.where(keep, picks * cap + slot, -1), 2, -1)
    live_own = own(lay(live.astype(F32)[:, :, None], 1), 1)

    output, grad_x, grad_qkv, grad_proj, grad_router, grad_norms, grad_in, grad_out = layer(
        (tokens, cotangent),
        moved,
        router,
        flat,
        order,
        w_in[0],
        w_out[0],
        live_own,
        norms,
        qkv,
        proj.reshape(d, d),
        (experts, n_dp, n_t, block, SEQ, factor, cap),
    )
    nz, ny = grid_sizes(n_dp)
    lane = jnp.arange(128)
    smalls = jnp.where(lane < experts, grad_router, 0.0)
    smalls = smalls + jnp.pad(grad_norms[:4].T, ((0, 0), (experts, 124 - experts)))
    grad_qkv, grad_proj, smalls = scatter_grads(
        grad_qkv.reshape(nz, ny, 2, d // n_dp, -1),
        grad_proj.reshape(nz, ny, 2, n_t, -1, d),
        smalls.reshape(nz, ny, 2, n_t, -1, 128),
        n_dp,
        n_t,
        heads_here,
    )
    return (
        output,
        grad_x,
        grad_qkv,
        grad_proj,
        grad_in[None],
        grad_out[None],
        smalls[:, :experts],
        smalls[:, experts],
        smalls[:, experts + 1],
        smalls[:, experts + 2],
        smalls[:, experts + 3],
    )


def local(*args):
    tokens, w_qkv, live_rows = args[0], args[1], args[10]
    n_t = lax.axis_size("tensor")
    images = live_rows.shape[1] // SEQ
    block = w_qkv.shape[1] * (w_qkv.shape[2] // 3)
    edge = tokens.shape[1] - SEQ
    fits = tokens.shape[1] % 16 == 0 and 0 < edge <= SEQ // 2 and args[3].shape[0] == 1
    if n_t == 2 and images == 2 and fits and block % 128 == 0 and w_qkv.shape[2] == 192 and args[0].shape[0] == 3:
        return fast(*args)
    return general(*args)


def solution(mesh):
    both = ("dp", "tensor")
    return jax.shard_map(
        local,
        mesh=mesh,
        in_specs=(
            P(None, both, None),
            P("dp", "tensor", None),
            P("tensor", "dp", None),
            P("dp", None, "tensor"),
            P("dp", "tensor", None),
            P(both, None),
            P(both),
            P(both),
            P(both),
            P(both),
            P(None, "dp"),
            P(None, "dp", None),
            P(None, "dp", None),
            P(None, both, None),
        ),
        out_specs=(
            P(None, both, None),
            P(None, both, None),
            P("dp", "tensor", None),
            P("tensor", "dp", None),
            P("dp", None, "tensor"),
            P("dp", "tensor", None),
            P(both, None),
            P(both),
            P(both),
            P(both),
            P(both),
        ),
        check_vma=False,
    )
```

```python
import functools

import jax
import jax.numpy as jnp
import numpy as np
from jax import lax
from jax.experimental import pallas as pl
from jax.experimental.pallas import tpu as pltpu
from jax.sharding import PartitionSpec as P

SEQ = 197
EPS = 1e-06
F32 = jnp.float32
BF16 = jnp.bfloat16
GELU_A = 0.7978845608028654
GELU_B = 0.044715


def dot(a, b, dims):
    return lax.dot_general(a, b, (dims, ((), ())), preferred_element_type=F32)


def layer_norm(values, gain_vec, shift_vec):
    centre = jnp.mean(values, axis=-1, keepdims=True)
    centered = values - centre
    spread = jnp.mean(centered * centered, axis=-1, keepdims=True)
    return centered * lax.rsqrt(spread + EPS) * gain_vec + shift_vec


def expert_kernel(x_ref, dp_ref, win_ref, wout_ref, y_ref, dx_ref, gin_ref, gout_ref, y_acc, dx_acc):
    step = pl.program_id(0)
    last = pl.num_programs(0) - 1
    x = x_ref[...]
    dprod = dp_ref[...]
    win = win_ref[...]
    wout = wout_ref[...]
    pre = dot(x, win, ((1,), (0,)))
    square = pre * pre
    th = jnp.tanh(GELU_A * pre * (1.0 + GELU_B * square))
    active = (0.5 * pre * (1.0 + th)).astype(BF16)
    slope = 0.5 * (1.0 + th) + 0.5 * pre * (1.0 - th * th) * (GELU_A * (1.0 + 3.0 * GELU_B * square))
    dact = dot(dprod, wout, ((1,), (1,)))
    dpre = (dact * slope).astype(BF16)
    gin_ref[...] = dot(x, dpre, ((0,), (0,))).astype(BF16)
    gout_ref[...] = dot(active, dprod, ((0,), (0,))).astype(BF16)
    part_y = dot(active, wout, ((1,), (0,)))
    part_dx = dot(dpre, win, ((1,), (1,)))

    @pl.when(step == 0)
    def _():
        y_acc[...] = part_y
        dx_acc[...] = part_dx

    @pl.when(step > 0)
    def _():
        y_acc[...] += part_y
        dx_acc[...] += part_dx

    @pl.when(step == last)
    def _():
        y_ref[...] = y_acc[...].astype(BF16)
        dx_ref[...] = dx_acc[...].astype(BF16)


def expert(x, dprod, win, wout, tile=256):
    n, d = x.shape
    ff = win.shape[1]
    return pl.pallas_call(
        expert_kernel,
        grid=(ff // tile,),
        in_specs=[
            pl.BlockSpec((n, d), lambda i: (0, 0)),
            pl.BlockSpec((n, d), lambda i: (0, 0)),
            pl.BlockSpec((d, tile), lambda i: (0, i)),
            pl.BlockSpec((tile, d), lambda i: (i, 0)),
        ],
        out_specs=[
            pl.BlockSpec((n, d), lambda i: (0, 0)),
            pl.BlockSpec((n, d), lambda i: (0, 0)),
            pl.BlockSpec((d, tile), lambda i: (0, i)),
            pl.BlockSpec((tile, d), lambda i: (i, 0)),
        ],
        out_shape=[
            jax.ShapeDtypeStruct((n, d), BF16),
            jax.ShapeDtypeStruct((n, d), BF16),
            jax.ShapeDtypeStruct((d, ff), BF16),
            jax.ShapeDtypeStruct((ff, d), BF16),
        ],
        scratch_shapes=[pltpu.VMEM((n, d), F32), pltpu.VMEM((n, d), F32)],
        compiler_params=pltpu.CompilerParams(vmem_limit_bytes=60 * 1024 * 1024),
        cost_estimate=pl.CostEstimate(
            flops=12 * n * d * ff, transcendentals=n * ff, bytes_accessed=8 * n * d + 8 * d * ff
        ),
    )(x, dprod, win, wout)


MESH = pl.DeviceIdType.MESH
ANYWHERE = pl.BlockSpec(memory_space=pltpu.VMEM)


def grid_sizes(n_dp):
    ny = 1
    while 2 * ny * 2 * ny <= n_dp // 2:
        ny *= 2
    return n_dp // (2 * ny), ny


def position(ny):
    dp = lax.axis_index("dp")
    return dp, lax.axis_index("tensor"), dp % 2, (dp // 2) % ny, dp // (2 * ny)


def neighbours(ny, nz, n_t):
    dp, t, c, y, z = position(ny)

    def along_core(k):
        return (dp - c + (c + k) % 2, t)

    def along_tensor(k):
        return (dp, (t + k) % n_t)

    def along_y(k):
        return (dp + ((y + k) % ny - y) * 2, t)

    def along_z(k):
        return (dp + ((z + k) % nz - z) * 2 * ny, t)

    return {"core": (2, along_core), "tensor": (n_t, along_tensor), "y": (ny, along_y), "z": (nz, along_z)}


def greet(stages):
    barrier = pltpu.get_barrier_semaphore()
    count = 0
    for size, device in stages.values():
        for k in range(1, size):
            pl.semaphore_signal(barrier, inc=1, device_id=device(k), device_id_type=MESH)
            count += 1
    pl.semaphore_wait(barrier, count)


def gather_kernel(ny, nz, n_t, extras, *refs):
    (qkv, proj, small), refs = refs[:3], refs[3:]
    side, refs = refs[:extras], refs[extras:]
    (qkv_out, proj_out, small_out), refs = refs[:3], refs[3:]
    side_out, (send, recv, copied) = refs[:extras], refs[extras:]
    dp, t, c, y, z = position(ny)
    stages = neighbours(ny, nz, n_t)
    greet(stages)
    cols, wide = qkv.shape[1], proj.shape[1]
    whole = slice(None)
    slot = 0

    def start(pieces, device):
        nonlocal slot
        copies = []
        for src, dst in pieces:
            copies.append(
                pltpu.make_async_remote_copy(
                    src_ref=src,
                    dst_ref=dst,
                    send_sem=send.at[slot],
                    recv_sem=recv.at[slot],
                    device_id=device,
                    device_id_type=MESH,
                )
            )
            copies[-1].start()
            slot += 1
        return copies

    def along(name, pieces):
        size, device = stages[name]
        return [copy for k in range(1, size) for copy in start(pieces, device(k))]

    def lanes(ts, half):
        return pl.ds(pl.multiple_of(ts * cols + half * (cols // 2), 128), cols // 2)

    def views(zs, ys, ts, half):
        band = slice(half * (wide // 2), (half + 1) * (wide // 2))
        parts = [qkv_out.at[zs, ys, c, :, lanes(i, half)] for i in ts]
        if len(ts) == 1:
            parts.append(proj_out.at[zs, ys, c, ts[0], :, band])
            if half == 0:
                parts.append(small_out.at[zs, ys, c, ts[0]])
        else:
            parts.append(proj_out.at[zs, ys, c, :, :, band])
        return [(part, part) for part in parts]

    aside = []
    for i in range(extras):
        strip = side_out[i].shape[1]
        aside += start([(side[i].at[:, side[i].shape[1] - strip :], side_out[i])], (dp, 1 - t))
    mine = (
        qkv_out.at[z, y, c, :, pl.ds(pl.multiple_of(t * cols, 128), cols)],
        proj_out.at[z, y, c, t],
        small_out.at[z, y, c, t],
    )
    inputs = list(zip((qkv, proj, small), mine))
    local = [pltpu.make_async_copy(src, dst, copied.at[i]) for i, (src, dst) in enumerate(inputs)]
    for copy in local:
        copy.start()
    for copy in along("z", inputs) + local:
        copy.wait()
    one = along("y", views(whole, y, [t], 0))
    two = along("tensor", views(whole, y, [t], 1))
    for copy in one:
        copy.wait()
    one = along("tensor", views(whole, whole, [t], 0))
    for copy in two:
        copy.wait()
    two = along("y", views(whole, y, list(range(n_t)), 1))
    for copy in one + two:
        copy.wait()
    rest = [ref.at[:, :, c] for ref in (qkv_out, proj_out, small_out)]
    for copy in along("core", [(part, part) for part in rest]) + aside:
        copy.wait()


def gather_weights(qkv, proj, small, n_dp, n_t, side=(), strip=0):
    nz, ny = grid_sizes(n_dp)
    slots = 3 * (nz - 1) + 5 * (n_t - 1) + (4 + n_t) * (ny - 1) + 3 + len(side)
    side_shapes = [jax.ShapeDtypeStruct((v.shape[0], strip) + v.shape[2:], v.dtype) for v in side]
    outs = pl.pallas_call(
        functools.partial(gather_kernel, ny, nz, n_t, len(side)),
        out_shape=[
            jax.ShapeDtypeStruct((nz, ny, 2, qkv.shape[0], n_t * qkv.shape[1]), BF16),
            jax.ShapeDtypeStruct((nz, ny, 2, n_t) + proj.shape, BF16),
            jax.ShapeDtypeStruct((nz, ny, 2, n_t) + small.shape, BF16),
        ]
        + side_shapes,
        in_specs=[ANYWHERE] * (3 + len(side)),
        out_specs=[ANYWHERE] * (3 + len(side)),
        scratch_shapes=[
            pltpu.SemaphoreType.DMA((slots,)),
            pltpu.SemaphoreType.DMA((slots,)),
            pltpu.SemaphoreType.DMA((3,)),
        ],
        compiler_params=pltpu.CompilerParams(collective_id=0, has_side_effects=True),
    )(qkv, proj, small, *side)
    qkv_all = outs[0].reshape(n_dp * qkv.shape[0], n_t * qkv.shape[1])
    return (qkv_all, outs[1].reshape((n_dp, n_t) + proj.shape), outs[2].reshape(-1, small.shape[1])) + tuple(outs[3:])


def scatter_kernel(ny, nz, n_t, heads, *refs):
    ins, refs = refs[:3], refs[3:]
    outs, refs = refs[:3], refs[3:]
    got_core, refs = refs[:3], refs[3:]
    held, refs = refs[:3], refs[3:]
    one_got, one_held, one_last, refs = refs[:3], refs[3:6], refs[6:9], refs[9:]
    two_got, two_held, two_last, refs = refs[:2], refs[2:4], refs[4:6], refs[6:]
    end, end_got, (send, recv) = refs[:3], refs[3:6], refs[6:]
    _, t, c, y, z = position(ny)
    stages = neighbours(ny, nz, n_t)
    greet(stages)
    cols, wide = ins[0].shape[4] // n_t, ins[1].shape[5]
    slot = 0

    def lanes(ts, half):
        return pl.ds(pl.multiple_of(ts * cols + half * (cols // 2), 128), cols // 2)

    def band(half):
        return slice(half * (wide // 2), (half + 1) * (wide // 2))

    def along(name, me, pieces):
        nonlocal slot
        size, device = stages[name]
        copies = []
        for k in range(1, size):
            for src, dst in pieces((me + k) % size, k - 1):
                copies.append(
                    pltpu.make_async_remote_copy(
                        src_ref=src,
                        dst_ref=dst,
                        send_sem=send.at[slot],
                        recv_sem=recv.at[slot],
                        device_id=device(k),
                        device_id_type=MESH,
                    )
                )
                copies[-1].start()
                slot += 1
        return copies

    def finish(copies):
        for copy in copies:
            copy.wait()

    def total(own, got, index):
        value = own.astype(F32)
        for k in range(got.shape[0]):
            value = value + got[(k,) + index].astype(F32)
        return value

    def loop(count, body):
        def step(n, carry):
            body(n)
            return carry

        lax.fori_loop(0, count, step, 0)

    finish(
        along("core", c, lambda j, k: [(ins[i].at[:, :, j], got_core[i].at[k]) for i in range(3)])
    )

    def add_core(n):
        zi, yi = n // ny, n % ny
        for i in range(3):
            held[i][zi, yi] = total(ins[i][zi, yi, c], got_core[i], (zi, yi)).astype(held[i].dtype)

    loop(nz * ny, add_core)
    one = along(
        "tensor",
        t,
        lambda j, k: [
            (held[0].at[:, :, :, lanes(j, 0)], one_got[0].at[k]),
            (held[1].at[:, :, j, :, band(0)], one_got[1].at[k]),
            (held[2].at[:, :, j], one_got[2].at[k]),
        ],
    )
    two = along(
        "y",
        y,
        lambda j, k: [(held[0].at[:, j, :, lanes(i, 1)], two_got[0].at[k, i]) for i in range(n_t)]
        + [(held[1].at[:, j, i, :, band(1)], two_got[1].at[k, i]) for i in range(n_t)],
    )
    finish(one)

    def add_one(n):
        zi, yi = n // ny, n % ny
        owns = (held[0][zi, yi, :, lanes(t, 0)], held[1][zi, yi, t, :, band(0)], held[2][zi, yi, t])
        for i in range(3):
            one_held[i][zi, yi] = total(owns[i], one_got[i], (zi, yi)).astype(one_held[i].dtype)

    loop(nz * ny, add_one)
    one = along("y", y, lambda j, k: [(one_held[i].at[:, j], one_last[i].at[k]) for i in range(3)])
    finish(two)

    def add_two(zi):
        for i in range(n_t):
            owns = (held[0][zi, y, :, lanes(i, 1)], held[1][zi, y, i, :, band(1)])
            for j in range(2):
                two_held[j][i, zi] = total(owns[j], two_got[j], (i, zi)).astype(two_held[j].dtype)

    loop(nz, add_two)
    two = along("tensor", t, lambda j, k: [(two_held[i].at[j], two_last[i].at[k]) for i in range(2)])
    finish(one)
    halves = [
        (slice(0, cols // 2), slice(cols // 2, cols)),
        (band(0), band(1)),
        (slice(None),),
    ]

    def end_one(zi):
        for i in range(3):
            value = total(one_held[i][zi, y], one_last[i], (zi,))
            end[i][zi, :, halves[i][0]] = value.astype(end[i].dtype)

    loop(nz, end_one)
    finish(two)

    def end_two(zi):
        for i in range(2):
            value = total(two_held[i][t, zi], two_last[i], (zi,))
            end[i][zi, :, halves[i][1]] = value.astype(end[i].dtype)

    loop(nz, end_two)
    finish(along("z", z, lambda j, k: [(end[i].at[j], end_got[i].at[k]) for i in range(3)]))
    results = [total(end[i][z], end_got[i], ()) for i in range(3)]
    outs[2][...] = results[2]
    if heads == 0:
        outs[0][...] = results[0]
        outs[1][...] = results[1]
        return
    width = cols // (3 * heads)
    jump = outs[1].shape[1]
    for h in range(heads):
        outs[1][h] = results[1][h * jump : (h + 1) * jump]
        for i in range(3):
            at = (i * heads + h) * width
            outs[0][:, h, i * width : (i + 1) * width] = results[0][:, at : at + width]


def scatter_grads(qkv, proj, small, n_dp, n_t, heads=0):
    nz, ny = qkv.shape[:2]
    rows, cols = qkv.shape[3], qkv.shape[4] // n_t
    tails = [(rows, cols), proj.shape[4:], small.shape[4:]]
    kinds = [BF16, BF16, F32]
    parts = [(rows, cols // 2), (proj.shape[4], proj.shape[5] // 2), small.shape[4:]]
    wide = [(rows, n_t * cols), (n_t,) + proj.shape[4:], (n_t,) + small.shape[4:]]

    def room(lead, shapes):
        return [pltpu.VMEM(lead + shape, kind) for shape, kind in zip(shapes, kinds)]

    scratch = room((1, nz, ny), wide) + room((nz, ny), wide)
    scratch += room((n_t - 1, nz, ny), parts) + room((nz, ny), parts) + room((ny - 1, nz), parts)
    scratch += room((ny - 1, n_t, nz), parts[:2]) + room((n_t, nz), parts[:2]) + room((n_t - 1, nz), parts[:2])
    scratch += room((nz,), tails) + room((nz - 1,), tails)
    slots = 3 + 5 * (n_t - 1) + (3 + 2 * n_t) * (ny - 1) + 3 * (nz - 1)
    shapes = list(tails)
    if heads:
        shapes[:2] = [(rows, heads, cols // heads), (heads, proj.shape[4] // heads, proj.shape[5])]
    scratch += [pltpu.SemaphoreType.DMA((slots,)), pltpu.SemaphoreType.DMA((slots,))]
    return pl.pallas_call(
        functools.partial(scatter_kernel, ny, nz, n_t, heads),
        out_shape=[jax.ShapeDtypeStruct(shape, F32) for shape in shapes],
        in_specs=[ANYWHERE] * 3,
        out_specs=[ANYWHERE] * 3,
        scratch_shapes=scratch,
        compiler_params=pltpu.CompilerParams(collective_id=1, has_side_effects=True),
    )(qkv, proj, small)


def standardise(v):
    centre = jnp.mean(v, axis=-1, keepdims=True)
    centered = v - centre
    inverse = lax.rsqrt(jnp.mean(centered * centered, axis=-1, keepdims=True) + EPS)
    return centered * inverse, inverse


def norm_back(grad, unit, inverse):
    return inverse * (
        grad
        - jnp.mean(grad, axis=-1, keepdims=True)
        - unit * jnp.mean(grad * unit, axis=-1, keepdims=True)
    )


def two_parts(v):
    high = v.astype(BF16)
    return high, (v - high.astype(F32)).astype(BF16)


def gate_softmax(c, router, experts):
    lane = lax.broadcasted_iota(jnp.int32, (c.shape[0], router.shape[1]), 1)
    logits = jnp.where(lane < experts, dot(c, router, ((1,), (0,))), -1e30)
    raised = jnp.exp(logits - jnp.max(logits, axis=-1, keepdims=True))
    return raised / jnp.sum(raised, axis=-1, keepdims=True), lane


def key_softmax(query, keys, gap):
    scores = dot(query, keys, ((1,), (1,)))
    col = lax.broadcasted_iota(jnp.int32, scores.shape, 1)
    scores = jnp.where((col < gap[0]) | (col >= gap[1]), scores, -1e30)
    raised = jnp.exp(scores - jnp.max(scores, axis=-1, keepdims=True))
    return raised * (1.0 / jnp.sum(raised, axis=-1, keepdims=True))


def pairs(n_t, block):
    return [
        (3 * block * s + 128 * i, block * s + 128 * i) for s in range(n_t) for i in range(block // 128)
    ]


def layer_kernel(
    experts,
    n_t,
    block,
    count,
    factor,
    tokens,
    cotangent,
    moved_x,
    moved_cot,
    router,
    flat_row,
    flat_col,
    order,
    win_own,
    wout_own,
    live,
    norms,
    qkv,
    proj_in,
    out,
    grad_x,
    gqkv_out,
    gproj_out,
    grouter,
    gnorms,
    gin_mine,
    gout_mine,
    x_in,
    cot_own,
    proj,
    dhidden_in,
    edge_o,
    edge_g,
    edge_sent,
    edge_o_got,
    edge_g_got,
    c_own,
    hidden_in,
    mixed,
    context,
    c_all,
    cot_all,
    gates,
    sent,
    got,
    ret,
    pay,
    paid,
    mix,
    dx,
    dgate,
    dmixed,
    gqkv,
    gproj,
    y_acc,
    dx_acc,
    win_got,
    wout_got,
    gin_far,
    gout_far,
    gin_half,
    gout_half,
    gin_got,
    gout_got,
    w_sems,
    c_sems,
    cot_sems,
    edge_sems,
    go_send,
    go_recv,
    back_send,
    back_recv,
    pay_sems,
    grad_sems,
):
    batches, rows, d = cot_own.shape
    n_dp = lax.axis_size("dp")
    dp, t = lax.axis_index("dp"), lax.axis_index("tensor")
    share = sent.shape[1] // n_dp
    hidden = win_own.shape[1]
    shift = (share * n_t).bit_length() - 1
    other = 1 - t
    partner = (dp, other)
    own_rows, strip = tokens.shape[1], edge_o.shape[1]
    head, edge = rows - strip, own_rows - count
    gap = (jnp.where(t == 0, count, count - edge), jnp.where(t == 0, rows, rows - edge))

    barrier = pltpu.get_barrier_semaphore()
    pl.semaphore_signal(barrier, inc=1, device_id=partner, device_id_type=MESH)

    def hello(k, carry):
        pl.semaphore_signal(barrier, inc=1, device_id=((dp + k) % n_dp, t), device_id_type=MESH)
        return carry

    lax.fori_loop(1, n_dp, hello, 0)
    pl.semaphore_wait(barrier, n_dp)

    def slot_codes(shape, axis):
        q = lax.broadcasted_iota(jnp.int32, shape, axis)
        return q + (q >> (share.bit_length() - 1)) * share * (n_t - 1) + t * share

    def band(m):
        return pl.ds(pl.multiple_of(m * rows, 16), rows)

    def image(i):
        return pl.ds(pl.multiple_of(i * rows, 16), rows)

    def part(i):
        return pl.ds(pl.multiple_of(i * share, 16), share)

    def remote(src, dst, sems, i, j, device):
        return pltpu.make_async_remote_copy(
            src_ref=src,
            dst_ref=dst,
            send_sem=sems[0].at[i, j],
            recv_sem=sems[1].at[i, j],
            device_id=device,
            device_id_type=MESH,
        )

    def c_copy(m):
        return pltpu.make_async_remote_copy(
            src_ref=c_own.at[m],
            dst_ref=c_all.at[m, image(t)],
            send_sem=c_sems.at[0, m],
            recv_sem=c_sems.at[1, m],
            device_id=partner,
            device_id_type=MESH,
        )

    def cot_copy(m):
        return pltpu.make_async_remote_copy(
            src_ref=cot_own.at[m],
            dst_ref=cot_all.at[m, image(t)],
            send_sem=cot_sems.at[0, m],
            recv_sem=cot_sems.at[1, m],
            device_id=partner,
            device_id_type=MESH,
        )

    def go_copy(m, k):
        to = (dp + k) % n_dp
        return remote(sent.at[m, part(to)], got.at[m, part(dp)], (go_send, go_recv), m, k - 1, (to, t))

    def back_copy(m, k):
        to = (dp + k) % n_dp
        return remote(got.at[m, part(to)], ret.at[m, part(dp)], (back_send, back_recv), m, k - 1, (to, t))

    def pay_copy(m):
        return pltpu.make_async_remote_copy(
            src_ref=pay.at[m],
            dst_ref=paid.at[m],
            send_sem=pay_sems.at[0, m],
            recv_sem=pay_sems.at[1, m],
            device_id=partner,
            device_id_type=MESH,
        )

    def grad_copy(i):
        src, dst = ((gin_half, gin_got), (gout_half, gout_got))[i // 2]
        size = src.shape[0] // 2
        band = pl.ds(i % 2 * size, size)
        return pltpu.make_async_remote_copy(
            src_ref=src.at[band],
            dst_ref=dst.at[band],
            send_sem=grad_sems.at[0, i],
            recv_sem=grad_sems.at[1, i],
            device_id=partner,
            device_id_type=MESH,
        )

    def w_copy(i):
        return pltpu.make_async_remote_copy(
            src_ref=(win_own, wout_own)[i],
            dst_ref=(win_got, wout_got)[i],
            send_sem=w_sems.at[0, i],
            recv_sem=w_sems.at[1, i],
            device_id=partner,
            device_id_type=MESH,
        )

    def every(body):
        def step(k, carry):
            body(k)
            return carry

        lax.fori_loop(1, n_dp, step, 0)

    low = lax.broadcasted_iota(jnp.int32, (rows, 128), 1) < 64

    def edge_copy(i, m):
        return pltpu.make_async_remote_copy(
            src_ref=(edge_o, edge_sent)[i].at[m],
            dst_ref=(edge_o_got, edge_g_got)[i].at[m],
            send_sem=edge_sems.at[2 * i, m],
            recv_sem=edge_sems.at[2 * i + 1, m],
            device_id=partner,
            device_id_type=MESH,
        )

    for own_ref, ref, moved in ((cot_own, cotangent, moved_cot), (x_in, tokens, moved_x)):
        own_ref[:, :head] = ref[:, :head]

        @pl.when(t == 0)
        def _(own_ref=own_ref, ref=ref):
            own_ref[:, head:] = ref[:, head:rows]

        @pl.when(t != 0)
        def _(own_ref=own_ref, moved=moved):
            own_ref[:, head:] = moved[...]

    def permutation():
        return (order[...] == lax.broadcasted_iota(jnp.int32, (d, d), 1)).astype(F32).astype(BF16)

    proj[...] = dot(permutation(), proj_in[...], ((0,), (0,))).astype(BF16)

    def attend(m, carry):
        cot_copy(m).start()
        cot_all[m, image(t)] = cot_own[m]
        xf = x_in[m].astype(F32)
        unit, _ = standardise(xf)
        a = (unit * norms[0:1] + norms[1:2]).astype(BF16)
        for s in range(n_t):
            for i in range(3):
                cols = slice((3 * s + i) * block, (3 * s + i + 1) * block)
                projected = dot(a, qkv[:, cols], ((1,), (0,)))
                mixed[m, :, cols] = (projected * factor if i == 0 else projected).astype(BF16)
        for col, dest in pairs(n_t, block):
            query = mixed[m, :, col : col + 128]
            keys = mixed[m, :, col + block : col + block + 128]
            values = mixed[m, :, col + 2 * block : col + 2 * block + 128]
            zero = jnp.zeros_like(query)
            parts = []
            for own in (low, ~low):
                probs = key_softmax(jnp.where(own, query, zero), keys, gap)
                parts.append(dot(probs.astype(BF16), values, ((1,), (0,))))
            context[m, :, dest : dest + 128] = jnp.where(low, parts[0], parts[1]).astype(BF16)
        hidden = xf + live[m] * dot(context[m], proj[...], ((1,), (0,)))
        hidden_in[m] = hidden
        unit, _ = standardise(hidden)
        c = (unit * norms[2:3] + norms[3:4]).astype(BF16)
        c_own[m] = c
        c_all[m, image(t)] = c
        c_copy(m).start()
        return carry

    lax.fori_loop(0, batches, attend, 0)
    w_copy(0).start()
    w_copy(1).start()

    lane = lax.broadcasted_iota(jnp.int32, (2 * rows, router.shape[1]), 1)

    def dispatch(m, carry):
        c_copy(m).wait_recv()
        cot_copy(m).wait_recv()
        c = c_all[m]
        logits = jnp.where(lane < experts, dot(c, router[...], ((1,), (0,))), -1e30)
        raised = jnp.exp(logits - jnp.max(logits, axis=-1, keepdims=True))
        probs = raised / jnp.sum(raised, axis=-1, keepdims=True)
        cot = cot_all[m].astype(F32)
        scaled = []
        for k in range(2):
            gate = jnp.sum(jnp.where(lane == flat_col[m, :, k : k + 1] >> shift, probs, 0.0), axis=-1, keepdims=True)
            gates[m, :, k : k + 1] = gate
            scaled.append((gate * cot).astype(BF16))
        codes = slot_codes((n_dp * share, 1), 0)
        picks = [(flat_row[m, k : k + 1, :] == codes).astype(F32).astype(BF16) for k in range(2)]
        sent[m, :, :d] = dot(picks[0] + picks[1], c, ((1,), (0,))).astype(BF16)
        moved = dot(picks[0], scaled[0], ((1,), (0,))) + dot(picks[1], scaled[1], ((1,), (0,)))
        sent[m, :, d:] = moved.astype(BF16)
        every(lambda k: go_copy(m, k).start())
        got[m, part(dp)] = sent[m, part(dp)]
        return carry

    lax.fori_loop(0, batches, dispatch, 0)

    tile = min(512, hidden)

    def clear(i, carry):
        cols = pl.ds(pl.multiple_of(i * tile, tile), tile)
        for into in (gin_far, gin_mine):
            into[:, cols] = jnp.zeros((d, tile), F32)
        for into in (gout_far, gout_mine):
            into[cols, :] = jnp.zeros((tile, d), F32)
        return carry

    lax.fori_loop(0, hidden // tile, clear, 0)

    slots = n_dp * share
    sums = ((y_acc, dx_acc), (mix.at[pl.ds(0, slots)], dx.at[pl.ds(0, slots)]))

    def expert_half(m, own):
        y_sum, dx_sum = sums[m % 2]
        win, wout, gin, gout = (win_own, wout_own, gin_mine, gout_mine) if own else (win_got, wout_got, gin_far, gout_far)

        def chunk(i, inner):
            cols = pl.ds(pl.multiple_of(i * tile, tile), tile)
            x = got[m, :, :d]
            dprod = got[m, :, d:]
            w1 = win[:, cols]
            w2 = wout[cols, :]
            pre = dot(x, w1, ((1,), (0,)))
            square = pre * pre
            th = jnp.tanh(GELU_A * pre * (1.0 + GELU_B * square))
            active = (0.5 * pre * (1.0 + th)).astype(BF16)
            slope = 0.5 * (1.0 + th) + 0.5 * pre * (1.0 - th * th) * (GELU_A * (1.0 + 3.0 * GELU_B * square))
            dpre = (dot(dprod, w2, ((1,), (1,))) * slope).astype(BF16)
            gin[:, cols] += dot(x, dpre, ((0,), (0,)))
            gout[cols, :] += dot(active, dprod, ((0,), (0,)))
            y_sum[...] += dot(active, w2, ((1,), (0,)))
            dx_sum[...] += dot(dpre, w1, ((1,), (1,)))
            return inner

        lax.fori_loop(0, hidden // tile, chunk, 0)

    def expert_begin(m):
        every(lambda k: go_copy(m, k).wait_recv())
        for ref in sums[m % 2]:
            ref[...] = jnp.zeros((slots, d), F32)

    def expert_end(m):
        got[m, :, :d] = sums[m % 2][0][...].astype(BF16)
        got[m, :, d:] = sums[m % 2][1][...].astype(BF16)
        every(lambda k: back_copy(m, k).start())
        ret[m, part(dp)] = got[m, part(dp)]

    last = batches - 1
    for m in range(last):
        expert_begin(m)
        expert_half(m, True)
    w_copy(0).wait_recv()
    w_copy(1).wait_recv()
    for m in range(last):
        expert_half(m, False)
        expert_end(m)
    expert_begin(last)
    expert_half(last, False)
    gin_half[...] = gin_far[...].astype(BF16)
    gout_half[...] = gout_far[...].astype(BF16)
    grad_copy(0).start()
    grad_copy(1).start()
    expert_half(last, True)
    expert_end(last)

    def combine(m, carry):
        every(lambda k: back_copy(m, k).wait_recv())
        codes = slot_codes((1, n_dp * share), 1)
        for i in (other, t):
            picks = [(flat_col[m, image(i), k : k + 1] == codes).astype(F32).astype(BF16) for k in range(2)]
            one = dot(picks[0], ret[m, :, :d], ((1,), (0,)))
            two = dot(picks[1], ret[m, :, :d], ((1,), (0,)))
            d_rows = dot(picks[0] + picks[1], ret[m, :, d:], ((1,), (0,)))
            cot = cot_all[m, image(i)].astype(F32)
            gate = gates[m, image(i)]
            mixture = gate[:, 0:1] * one + gate[:, 1:2] * two
            col = lax.broadcasted_iota(jnp.int32, (rows, 128), 1)
            dg = jnp.where(col == 0, jnp.sum(one * cot, axis=-1, keepdims=True), 0.0)
            dg = dg + jnp.where(col == 1, jnp.sum(two * cot, axis=-1, keepdims=True), 0.0)
            if i is other:
                pay[m, :, :d] = mixture.astype(BF16)
                pay[m, :, d : 2 * d] = d_rows.astype(BF16)
                pay[m, :, 2 * d :] = dg.astype(BF16)
                pay_copy(m).start()
            else:
                mix[band(m)] = mixture
                dx[band(m)] = d_rows
                dgate[m] = dg
        return carry

    gqkv[...] = jnp.zeros_like(gqkv)
    gproj[...] = jnp.zeros_like(gproj)
    grouter[...] = jnp.zeros_like(grouter)
    gnorms[...] = jnp.zeros_like(gnorms)

    def retreat(m):
        pay_copy(m).wait_recv()
        hidden = hidden_in[m]
        result = (hidden + mix[band(m)] + paid[m, :, :d].astype(F32)).astype(BF16)
        out[m, :head] = result[:head]
        edge_o[m] = result[head:]
        edge_copy(0, m).start()
        unit, inverse = standardise(hidden)
        c = (unit * norms[2:3] + norms[3:4]).astype(BF16)
        probs, lane = gate_softmax(c, router[...], experts)
        dg = dgate[m] + paid[m, :, 2 * d :].astype(F32)
        dprobs = jnp.zeros_like(probs)
        for k in range(2):
            dprobs = dprobs + jnp.where(lane == flat_col[m, image(t), k : k + 1] >> shift, dg[:, k : k + 1], 0.0)
        dlogits = probs * (dprobs - jnp.sum(dprobs * probs, axis=-1, keepdims=True))
        dc = dx[band(m)] + paid[m, :, d : 2 * d].astype(F32)
        for piece in two_parts(dlogits):
            grouter[...] += dot(c, piece, ((0,), (0,)))
            dc = dc + dot(piece, router[...], ((1,), (1,)))
        gnorms[2:3] += jnp.sum(dc * unit, axis=0, keepdims=True)
        gnorms[3:4] += jnp.sum(dc, axis=0, keepdims=True)
        dhidden = cot_all[m, image(t)].astype(F32) + norm_back(dc * norms[2:3], unit, inverse)
        dhidden_in[...] = dhidden
        dattn = (live[m] * dhidden).astype(BF16)
        gproj[...] += dot(context[m], dattn, ((0,), (0,)))
        dcontext = dot(dattn, proj[...], ((1,), (1,))).astype(BF16)
        for col, dest in pairs(n_t, block):
            query = mixed[m, :, col : col + 128]
            keys = mixed[m, :, col + block : col + block + 128]
            values = mixed[m, :, col + 2 * block : col + 2 * block + 128]
            grads = dcontext[:, dest : dest + 128]
            zero = jnp.zeros_like(query)
            parts = []
            for own in (low, ~low):
                probs = key_softmax(jnp.where(own, query, zero), keys, gap)
                dvalues = dot(probs.astype(BF16), grads, ((0,), (0,)))
                dweights = dot(jnp.where(own, grads, zero), values, ((1,), (1,)))
                dscores = probs * (dweights - jnp.sum(dweights * probs, axis=-1, keepdims=True))
                dscores = dscores.astype(BF16)
                parts.append(
                    (dot(dscores, keys, ((1,), (0,))), dot(dscores, query, ((0,), (0,))), dvalues)
                )
            for i in range(3):
                both = jnp.where(low, parts[0][i], parts[1][i]).astype(BF16)
                if i == 0:
                    both = both * BF16(factor)
                dmixed[:, col + i * block : col + i * block + 128] = both
        unit, inverse = standardise(x_in[m].astype(F32))
        a = (unit * norms[0:1] + norms[1:2]).astype(BF16)
        gqkv[...] += dot(a, dmixed[...], ((0,), (0,)))
        da = dot(dmixed[...], qkv[...], ((1,), (1,)))
        gnorms[0:1] += jnp.sum(da * unit, axis=0, keepdims=True)
        gnorms[1:2] += jnp.sum(da, axis=0, keepdims=True)
        result = dhidden_in[...] + norm_back(da * norms[0:1], unit, inverse)
        grad_x[m, :head] = result[:head]
        edge_g[m] = result[head:]
        edge_sent[m] = result[head:].astype(BF16)
        edge_copy(1, m).start()

    pieces = 4

    def finish(m, carry):
        @pl.when(m < batches)
        def _():
            combine(m, 0)

        @pl.when(m == 0)
        def _():
            grad_copy(2).start()

        @pl.when(m == batches - 1)
        def _():
            grad_copy(3).start()

        @pl.when(m > 0)
        def _():
            retreat(m - 1)

        return carry

    lax.fori_loop(0, batches + 1, finish, 0)
    gqkv_out[...] = gqkv[...].astype(BF16)
    gproj_out[...] = dot(permutation(), gproj[...].astype(BF16), ((1,), (0,))).astype(BF16)

    @pl.when(t != 0)
    def _():
        out[:, head:] = tokens[:, head:]
        grad_x[:, head:] = cotangent[:, head:].astype(F32)

    first = own_rows - strip
    near = lax.broadcasted_iota(jnp.int32, (16, d), 0) < strip - edge

    def place(m, carry):
        edge_copy(0, m).wait()
        edge_copy(1, m).wait()

        @pl.when(t == 0)
        def _():
            for ref, mine, theirs in ((out, edge_o, edge_o_got), (grad_x, edge_g, edge_g_got)):
                ref[m, head:first] = mine[m, : first - head]
                blend = jnp.where(
                    near,
                    mine[m, first - head : first - head + 16].astype(F32),
                    theirs[m, :16].astype(F32),
                )
                ref[m, first : first + 16] = blend.astype(ref.dtype)
                ref[m, first + 16 :] = theirs[m, 16:].astype(ref.dtype)

        return carry

    lax.fori_loop(0, batches, place, 0)
    for i in range(pieces):
        grad_copy(i).wait()
    gin_mine[...] += gin_got[...].astype(F32)
    gout_mine[...] += gout_got[...].astype(F32)
    w_copy(0).wait_send()
    w_copy(1).wait_send()

    def drain(m, carry):
        c_copy(m).wait_send()
        cot_copy(m).wait_send()
        pay_copy(m).wait_send()
        every(lambda k: go_copy(m, k).wait_send())
        every(lambda k: back_copy(m, k).wait_send())
        return carry

    lax.fori_loop(0, batches, drain, 0)


def layer(held, moved, router, flat, order, win, wout, live, norms, qkv, proj, statics):
    batches, own_rows, d = held[0].shape
    experts, n_dp, n_t, block, count, factor, cap = statics
    rows, strip = live.shape[1], moved[0].shape[1]
    slots = n_dp * cap // n_t
    half = win.shape[1]
    wide = 3 * n_t * block
    dma = pltpu.SemaphoreType.DMA
    return pl.pallas_call(
        functools.partial(layer_kernel, experts, n_t, block, count, factor),
        out_shape=[
            jax.ShapeDtypeStruct((batches, own_rows, d), BF16),
            jax.ShapeDtypeStruct((batches, own_rows, d), F32),
            jax.ShapeDtypeStruct((d, wide), BF16),
            jax.ShapeDtypeStruct((d, d), BF16),
            jax.ShapeDtypeStruct((d, router.shape[1]), F32),
            jax.ShapeDtypeStruct((8, d), F32),
            jax.ShapeDtypeStruct((d, half), F32),
            jax.ShapeDtypeStruct((half, d), F32),
        ],
        in_specs=[ANYWHERE] * 14,
        out_specs=[ANYWHERE] * 8,
        scratch_shapes=[
            pltpu.VMEM((batches, rows, d), BF16),
            pltpu.VMEM((batches, rows, d), BF16),
            pltpu.VMEM((d, d), BF16),
            pltpu.VMEM((rows, d), F32),
            pltpu.VMEM((batches, strip, d), BF16),
            pltpu.VMEM((batches, strip, d), F32),
            pltpu.VMEM((batches, strip, d), BF16),
            pltpu.VMEM((batches, strip, d), BF16),
            pltpu.VMEM((batches, strip, d), BF16),
            pltpu.VMEM((batches, rows, d), BF16),
            pltpu.VMEM((batches, rows, d), F32),
            pltpu.VMEM((batches, rows, wide), BF16),
            pltpu.VMEM((batches, rows, d), BF16),
            pltpu.VMEM((batches, 2 * rows, d), BF16),
            pltpu.VMEM((batches, 2 * rows, d), BF16),
            pltpu.VMEM((batches, 2 * rows, 128), F32),
            pltpu.VMEM((batches, slots, 2 * d), BF16),
            pltpu.VMEM((batches, slots, 2 * d), BF16),
            pltpu.VMEM((batches, slots, 2 * d), BF16),
            pltpu.VMEM((batches, rows, 2 * d + 128), BF16),
            pltpu.VMEM((batches, rows, 2 * d + 128), BF16),
            pltpu.VMEM((max(batches * rows, slots), d), F32),
            pltpu.VMEM((max(batches * rows, slots), d), F32),
            pltpu.VMEM((batches, rows, 128), F32),
            pltpu.VMEM((rows, wide), BF16),
            pltpu.VMEM((d, wide), F32),
            pltpu.VMEM((d, d), F32),
            pltpu.VMEM((slots, d), F32),
            pltpu.VMEM((slots, d), F32),
            pltpu.VMEM((d, half), BF16),
            pltpu.VMEM((half, d), BF16),
            pltpu.VMEM((d, half), F32),
            pltpu.VMEM((half, d), F32),
            pltpu.VMEM((d, half), BF16),
            pltpu.VMEM((half, d), BF16),
            pltpu.VMEM((d, half), BF16),
            pltpu.VMEM((half, d), BF16),
            dma((2, 2)),
            dma((2, batches)),
            dma((2, batches)),
            dma((4, batches)),
            dma((batches, n_dp - 1)),
            dma((batches, n_dp - 1)),
            dma((batches, n_dp - 1)),
            dma((batches, n_dp - 1)),
            dma((2, batches)),
            dma((2, 4)),
        ],
        compiler_params=pltpu.CompilerParams(
            collective_id=2, has_side_effects=True, vmem_limit_bytes=67043328
        ),
    )(
        *held,
        *moved,
        router,
        flat,
        flat.transpose(0, 2, 1),
        order,
        win,
        wout,
        live,
        norms,
        qkv,
        proj,
    )


def general(
    tokens,
    w_qkv,
    w_proj,
    w_in,
    w_out,
    w_router,
    gain_attn,
    shift_attn,
    gain_moe,
    shift_moe,
    live_rows,
    chosen,
    priority,
    cotangent,
):
    batches, own_rows, d = tokens.shape
    rows = live_rows.shape[1]
    n_dp = lax.axis_size("dp")
    n_t = lax.axis_size("tensor")
    t = lax.axis_index("tensor")
    heads_here = w_qkv.shape[1]
    heads = heads_here * n_t
    width = w_qkv.shape[2] // 3
    experts = w_in.shape[0] * n_dp
    cap = 2 * rows // experts
    share = cap // n_t
    images = rows // SEQ
    span = images * SEQ
    per = -(-images // n_t)
    work = per * SEQ
    total = n_t * work
    factor = width ** (-0.5)
    highest = lax.Precision.HIGHEST

    small = jnp.concatenate(
        [w_router] + [v[:, None] for v in (gain_attn, shift_attn, gain_moe, shift_moe)], axis=1
    )
    small = jnp.pad(small, ((0, 0), (0, 128 - small.shape[1])))
    block = heads_here * width
    qkv_block = w_qkv.reshape(-1, heads_here, 3, width).transpose(0, 2, 1, 3).reshape(-1, 3 * block)
    fill = -3 * block % 128
    qkv_block = jnp.pad(qkv_block, ((0, 0), (0, fill)))
    qkv, proj, small = gather_weights(qkv_block, w_proj.reshape(-1, d), small, n_dp, n_t)
    qkv = qkv.reshape(d, n_t, 3 * block + fill)[:, :, : 3 * block].reshape(d, -1)
    router = small[:, :experts]
    gain_one, shift_one, gain_two, shift_two = (small[:, experts + i].astype(F32) for i in range(4))
    proj = proj.reshape(n_dp, n_t, heads_here, w_proj.shape[1], d)
    proj = proj.transpose(1, 2, 0, 3, 4).reshape(heads * width, d)
    win = lax.all_gather(w_in[0], "tensor", axis=1, tiled=True)
    wout = lax.all_gather(w_out[0], "tensor", axis=0, tiled=True)
    cot_all = lax.all_gather(cotangent, "tensor", axis=1, tiled=True)

    def pad_rows(v, n):
        return jnp.pad(v, ((0, 0), (0, n - v.shape[1])) + ((0, 0),) * (v.ndim - 2))

    def own(v):
        return lax.dynamic_slice_in_dim(v, t * work, work, 1)

    edge = own_rows - work
    direct = n_t == 2 and per == 1 and edge >= 0
    if direct:
        moved = lax.ppermute(tokens[:, work:], "tensor", [(0, 1)])
        x = jnp.where(
            t == 0, tokens[:, :work], jnp.concatenate([moved, tokens[:, : work - edge]], axis=1)
        )
    else:
        x = own(pad_rows(lax.all_gather(tokens, "tensor", axis=1, tiled=True)[:, :span], total))
    x = x.astype(F32)
    live = live_rows[:, :span]
    live_all = pad_rows(live, total)
    live_own = own(live_all).astype(F32)[:, :, None]
    cot_all = pad_rows(cot_all[:, :span], total)
    dy = own(cot_all).astype(F32)

    rank = priority[:, 0, :span]
    first, second = chosen[:, :span, 0], chosen[:, :span, 1]
    labels = jnp.arange(experts, dtype=jnp.int32)
    earlier = (rank[:, None, :] < rank[:, :, None]).astype(BF16)
    hit_one = (first[:, :, None] == labels).astype(F32)
    hit_two = (second[:, :, None] == labels).astype(F32)
    live_one = hit_one * live[:, :, None].astype(F32)
    live_two = hit_two * live[:, :, None].astype(F32)
    counts = jnp.einsum(
        "mrs,mse->mre",
        earlier,
        jnp.concatenate([live_one, live_two], axis=-1).astype(BF16),
        preferred_element_type=F32,
    )
    first_total = jnp.sum(live_one, axis=1, keepdims=True)
    slot_one = jnp.sum(counts[:, :, :experts] * hit_one, axis=-1).astype(jnp.int32)
    slot_two = jnp.sum((counts[:, :, experts:] + first_total) * hit_two, axis=-1).astype(jnp.int32)
    keep_one = (live > 0) & (slot_one < cap)
    keep_two = (live > 0) & (slot_two < cap)
    flat_one = jnp.where(keep_one, first * cap + slot_one, -1)
    flat_two = jnp.where(keep_two, second * cap + slot_two, -1)

    def spread(v, fill):
        return jnp.pad(v, ((0, 0), (0, total - span)), constant_values=fill)

    flat_one, flat_two = spread(flat_one, -1), spread(flat_two, -1)
    keep_one, keep_two = spread(keep_one, False), spread(keep_two, False)
    first, second = spread(first, 0), spread(second, 0)
    codes = (jnp.arange(experts)[:, None] * cap + t * share + jnp.arange(share)[None, :]).reshape(-1)
    pick_one = flat_one[:, None, :] == codes[None, :, None]
    pick_two = flat_two[:, None, :] == codes[None, :, None]

    normed_one = layer_norm(x, gain_one, shift_one).astype(BF16)
    mixed = dot(normed_one, qkv, ((2,), (0,)))
    split = heads * width
    shape = (batches * per, SEQ, heads, width)
    mixed = mixed.reshape(batches, work, n_t, 3, block)
    query = (mixed[:, :, :, 0] * factor).astype(BF16).reshape(shape)
    keys = mixed[:, :, :, 1].astype(BF16).reshape(shape)
    values = mixed[:, :, :, 2].astype(BF16).reshape(shape)
    scores = jnp.einsum("iqhc,ikhc->ihqk", query, keys, preferred_element_type=F32)
    probs = jax.nn.softmax(scores, axis=-1)
    weights = probs.astype(BF16)
    context = jnp.einsum("ihqk,ikhc->iqhc", weights, values, preferred_element_type=F32)
    context = context.astype(BF16).reshape(batches, work, split)
    attn = dot(context, proj, ((2,), (0,)))
    hidden = x + live_own * attn
    normed_two = layer_norm(hidden, gain_two, shift_two).astype(BF16)

    c_all = lax.all_gather(normed_two, "tensor", axis=1, tiled=True)
    gate_probs = jax.nn.softmax(dot(c_all, router, ((2,), (0,))), axis=-1)
    hits_one = (first[:, :, None] == labels).astype(F32)
    hits_two = (second[:, :, None] == labels).astype(F32)
    gate_one = jnp.sum(gate_probs * hits_one, axis=-1) * keep_one
    gate_two = jnp.sum(gate_probs * hits_two, axis=-1) * keep_two
    picked = (pick_one | pick_two).astype(BF16)
    sent = jnp.einsum(
        "mqr,mrd->mqd",
        picked,
        jnp.concatenate([c_all, cot_all], axis=-1),
        preferred_element_type=F32,
    )
    gate_slot = jnp.sum(
        jnp.where(pick_one, gate_one[:, None, :], 0.0) + jnp.where(pick_two, gate_two[:, None, :], 0.0),
        axis=-1,
        keepdims=True,
    )
    sent = jnp.concatenate(
        [sent[..., :d].astype(BF16), (sent[..., d:] * gate_slot).astype(BF16)], axis=-1
    )
    sent = sent.reshape(batches, experts, share, 2 * d)
    got = lax.all_to_all(sent, "dp", 1, 1, tiled=True).reshape(-1, 2 * d)
    produced, d_in, grad_in, grad_out = expert(got[:, :d], got[:, d:], win, wout)
    back = jnp.concatenate([produced, d_in], axis=-1).reshape(batches, n_dp, share, 2 * d)
    back = lax.all_to_all(back, "dp", 1, 1, tiled=True).reshape(batches, experts * share, 2 * d)
    grad_in = lax.psum_scatter(grad_in, "tensor", scatter_dimension=1, tiled=True).astype(F32)
    grad_out = lax.psum_scatter(grad_out, "tensor", scatter_dimension=0, tiled=True).astype(F32)

    part_one = jnp.einsum("mqr,mqd->mrd", pick_one.astype(BF16), back[..., :d], preferred_element_type=F32)
    part_two = jnp.einsum("mqr,mqd->mrd", pick_two.astype(BF16), back[..., :d], preferred_element_type=F32)
    d_rows = jnp.einsum("mqr,mqd->mrd", picked, back[..., d:], preferred_element_type=F32)
    mixture = gate_one[:, :, None] * part_one + gate_two[:, :, None] * part_two
    cot_wide = cot_all.astype(F32)
    dgate_one = jnp.sum(part_one * cot_wide, axis=-1, keepdims=True)
    dgate_two = jnp.sum(part_two * cot_wide, axis=-1, keepdims=True)
    dgates = jnp.concatenate([dgate_one, dgate_two], axis=-1)
    payload = jnp.concatenate(
        [mixture, d_rows, jnp.pad(dgates, ((0, 0), (0, 0), (0, 126)))], axis=-1
    ).astype(BF16)
    pieces = payload.reshape(batches, n_t, work, payload.shape[-1])

    def piece(k):
        return lax.dynamic_index_in_dim(pieces, (t + k) % n_t, 1, keepdims=False)

    payload = piece(0).astype(F32)
    for k in range(1, n_t):
        payload = payload + lax.ppermute(
            piece(k), "tensor", [(j, (j + k) % n_t) for j in range(n_t)]
        ).astype(F32)
    output = (hidden + payload[..., :d]).astype(BF16)
    dgates = payload[..., 2 * d : 2 * d + 2]

    own_probs = own(gate_probs)
    dprobs = own(hits_one) * dgates[..., 0:1] * own(keep_one)[:, :, None]
    dprobs = dprobs + own(hits_two) * dgates[..., 1:2] * own(keep_two)[:, :, None]
    dlogits = own_probs * (dprobs - jnp.sum(dprobs * own_probs, axis=-1, keepdims=True))
    grad_router = lax.dot_general(
        normed_two.astype(F32), dlogits, (((0, 1), (0, 1)), ((), ())), precision=highest
    )
    dc = payload[..., d : 2 * d] + lax.dot_general(
        dlogits, router.astype(F32), (((2,), (1,)), ((), ())), precision=highest
    )
    _, back_two = jax.vjp(layer_norm, hidden, gain_two, shift_two)
    dnorm, grad_gain_two, grad_shift_two = back_two(dc)
    dhidden = dy + dnorm
    dattn = (live_own * dhidden).astype(BF16)

    grad_proj = dot(context, dattn, ((0, 1), (0, 1)))
    dcontext = dot(dattn, proj, ((2,), (1,))).astype(BF16).reshape(shape)
    dvalues = jnp.einsum("ihqk,iqhc->ikhc", weights, dcontext, preferred_element_type=F32).astype(BF16)
    dweights = jnp.einsum("iqhc,ikhc->ihqk", dcontext, values, preferred_element_type=F32)
    dscores = (probs * (dweights - jnp.sum(dweights * probs, axis=-1, keepdims=True))).astype(BF16)
    dquery = jnp.einsum("ihqk,ikhc->iqhc", dscores, keys, preferred_element_type=F32).astype(BF16)
    dkeys = jnp.einsum("ihqk,iqhc->ikhc", dscores, query, preferred_element_type=F32).astype(BF16)
    dmixed = jnp.stack(
        [v.reshape(batches, work, n_t, block) for v in (dquery * BF16(factor), dkeys, dvalues)], axis=3
    ).reshape(batches, work, 3 * split)
    grad_qkv = dot(normed_one, dmixed, ((0, 1), (0, 1)))
    da = dot(dmixed, qkv, ((2,), (1,)))
    _, back_one = jax.vjp(layer_norm, x, gain_one, shift_one)
    dnorm, grad_gain_one, grad_shift_one = back_one(da)
    grad_x = dhidden + dnorm

    if direct:
        out_edge = lax.ppermute(output[:, :edge], "tensor", [(1, 0)])
        grad_edge = lax.ppermute(grad_x[:, :edge], "tensor", [(1, 0)])
        result = jnp.where(
            t == 0,
            jnp.concatenate([output, out_edge], axis=1),
            jnp.concatenate([output[:, edge:], tokens[:, work - edge :]], axis=1),
        )
        grad_tokens = jnp.where(
            t == 0,
            jnp.concatenate([grad_x, grad_edge], axis=1),
            jnp.concatenate([grad_x[:, edge:], cotangent[:, work - edge :].astype(F32)], axis=1),
        )
    else:
        here = (t * own_rows + jnp.arange(own_rows) < span)[None, :, None]

        def home(v, rest):
            full = pad_rows(lax.all_gather(v, "tensor", axis=1, tiled=True)[:, :span], rows)
            return jnp.where(here, lax.dynamic_slice_in_dim(full, t * own_rows, own_rows, 1), rest)

        result = home(output, tokens)
        grad_tokens = home(grad_x, cotangent.astype(F32))

    nz, ny = grid_sizes(n_dp)
    grad_qkv = jnp.pad(grad_qkv.astype(BF16).reshape(d, n_t, 3 * block), ((0, 0), (0, 0), (0, fill)))
    grad_qkv = grad_qkv.reshape(nz, ny, 2, d // n_dp, -1)
    grad_proj = grad_proj.astype(BF16).reshape(n_t, heads_here, n_dp, -1, d)
    grad_proj = grad_proj.transpose(2, 0, 1, 3, 4).reshape(nz, ny, 2, n_t, -1, d)
    smalls = jnp.concatenate(
        [grad_router] + [v[:, None] for v in (grad_gain_one, grad_shift_one, grad_gain_two, grad_shift_two)],
        axis=1,
    )
    smalls = jnp.pad(smalls, ((0, 0), (0, 128 - smalls.shape[1]))).reshape(nz, ny, 2, n_t, -1, 128)
    grad_qkv, grad_proj, smalls = scatter_grads(grad_qkv, grad_proj, smalls, n_dp, n_t)
    grad_qkv = grad_qkv[:, : 3 * block].reshape(-1, 3, heads_here, width).transpose(0, 2, 1, 3)
    return (
        result,
        grad_tokens,
        grad_qkv.reshape(w_qkv.shape),
        grad_proj.reshape(w_proj.shape),
        grad_in[None],
        grad_out[None],
        smalls[:, :experts],
        smalls[:, experts],
        smalls[:, experts + 1],
        smalls[:, experts + 2],
        smalls[:, experts + 3],
    )


def fast(
    tokens,
    w_qkv,
    w_proj,
    w_in,
    w_out,
    w_router,
    gain_attn,
    shift_attn,
    gain_moe,
    shift_moe,
    live_rows,
    chosen,
    priority,
    cotangent,
):
    batches, own_rows, d = tokens.shape
    rows = live_rows.shape[1]
    n_dp = lax.axis_size("dp")
    n_t = lax.axis_size("tensor")
    t = lax.axis_index("tensor")
    heads_here = w_qkv.shape[1]
    width = w_qkv.shape[2] // 3
    block = heads_here * width
    experts = n_dp
    cap = 2 * rows // experts
    share = cap // n_t
    span = n_t * SEQ
    padded = -(-SEQ // 16) * 16
    edge = own_rows - SEQ
    factor = width ** (-0.5)

    vectors = jnp.stack([gain_attn, shift_attn, gain_moe, shift_moe])
    small = jnp.concatenate([w_router, vectors.T], axis=1)
    small = jnp.pad(small, ((0, 0), (0, 128 - small.shape[1])))
    qkv_block = w_qkv.reshape(-1, heads_here, 3, width).transpose(0, 2, 1, 3).reshape(-1, 3 * block)
    strip = -(-edge // 16) * 16
    qkv, proj, small, *moved = gather_weights(
        qkv_block, w_proj.reshape(-1, d), small, n_dp, n_t, (tokens, cotangent), strip
    )
    router = small
    norms = jnp.pad(small[:, experts : experts + 4].astype(F32).T, ((0, 4), (0, 0)))
    order = np.arange(d, dtype=np.int32).reshape(n_t, heads_here, n_dp, -1)
    order = jnp.asarray(order.transpose(2, 0, 1, 3).reshape(d, 1))

    def lay(v, axis, fill=0):
        def rows_of(low, high):
            return lax.slice_in_dim(v, low, high, axis=axis)

        shape = v.shape[:axis] + (padded - SEQ,) + v.shape[axis + 1 :]
        hole = jnp.full(shape, fill, v.dtype)
        return jnp.concatenate(
            [rows_of(0, SEQ), hole, rows_of(own_rows, span), hole, rows_of(SEQ, own_rows)], axis=axis
        )

    def own(v, axis):
        return lax.dynamic_slice_in_dim(v, t * padded, padded, axis)

    live = live_rows[:, :span]
    rank = priority[:, 0, :span]
    picks = chosen[:, :span].transpose(0, 2, 1)
    labels = jnp.arange(experts, dtype=jnp.int32)
    earlier = (rank[:, None, :] < rank[:, :, None]).astype(BF16)
    hits = (picks[..., None] == labels).astype(F32)
    live_hits = hits * live[:, None, :, None].astype(F32)
    ahead = jnp.einsum("mrs,mkse->mkre", earlier, live_hits.astype(BF16), preferred_element_type=F32)
    firsts = jnp.sum(live_hits[:, :1], axis=2, keepdims=True)
    ahead = ahead + jnp.concatenate([jnp.zeros_like(firsts), firsts], axis=1)
    slot = jnp.sum(ahead * hits, axis=-1).astype(jnp.int32)
    keep = (live[:, None, :] > 0) & (slot < cap)
    flat = lay(jnp.where(keep, picks * cap + slot, -1), 2, -1)
    live_own = own(lay(live.astype(F32)[:, :, None], 1), 1)

    output, grad_x, grad_qkv, grad_proj, grad_router, grad_norms, grad_in, grad_out = layer(
        (tokens, cotangent),
        moved,
        router,
        flat,
        order,
        w_in[0],
        w_out[0],
        live_own,
        norms,
        qkv,
        proj.reshape(d, d),
        (experts, n_dp, n_t, block, SEQ, factor, cap),
    )
    nz, ny = grid_sizes(n_dp)
    lane = jnp.arange(128)
    smalls = jnp.where(lane < experts, grad_router, 0.0)
    smalls = smalls + jnp.pad(grad_norms[:4].T, ((0, 0), (experts, 124 - experts)))
    grad_qkv, grad_proj, smalls = scatter_grads(
        grad_qkv.reshape(nz, ny, 2, d // n_dp, -1),
        grad_proj.reshape(nz, ny, 2, n_t, -1, d),
        smalls.reshape(nz, ny, 2, n_t, -1, 128),
        n_dp,
        n_t,
        heads_here,
    )
    return (
        output,
        grad_x,
        grad_qkv,
        grad_proj,
        grad_in[None],
        grad_out[None],
        smalls[:, :experts],
        smalls[:, experts],
        smalls[:, experts + 1],
        smalls[:, experts + 2],
        smalls[:, experts + 3],
    )


def local(*args):
    tokens, w_qkv, live_rows = args[0], args[1], args[10]
    n_t = lax.axis_size("tensor")
    images = live_rows.shape[1] // SEQ
    block = w_qkv.shape[1] * (w_qkv.shape[2] // 3)
    edge = tokens.shape[1] - SEQ
    fits = tokens.shape[1] % 16 == 0 and 0 < edge <= SEQ // 2 and args[3].shape[0] == 1
    if n_t == 2 and images == 2 and fits and block % 128 == 0 and w_qkv.shape[2] == 192 and args[0].shape[0] == 3:
        return fast(*args)
    return general(*args)


def solution(mesh):
    both = ("dp", "tensor")
    return jax.shard_map(
        local,
        mesh=mesh,
        in_specs=(
            P(None, both, None),
            P("dp", "tensor", None),
            P("tensor", "dp", None),
            P("dp", None, "tensor"),
            P("dp", "tensor", None),
            P(both, None),
            P(both),
            P(both),
            P(both),
            P(both),
            P(None, "dp"),
            P(None, "dp", None),
            P(None, "dp", None),
            P(None, both, None),
        ),
        out_specs=(
            P(None, both, None),
            P(None, both, None),
            P("dp", "tensor", None),
            P("tensor", "dp", None),
            P("dp", None, "tensor"),
            P("dp", "tensor", None),
            P(both, None),
            P(both),
            P(both),
            P(both),
            P(both),
        ),
        check_vma=False,
    )
```
